32 devices in a mesh: seq: 4 (over z), shard: 8 (over y, x, core).
Axes of the slice: x: 2, y: 2, z: 4, core: 2. Of those that a mesh axis runs over, the one named last changes fastest.
Arguments:
- inputs: bfloat16 [4096, 1024], P(('seq', 'shard')), may hold values from -16 to 16
- positions: int32 [4096], P(('seq', 'shard')), may hold values from 0 to 8191
- segments: int32 [4096], replicated, may hold values from 0 to 7, never falling along the last dimension, each value on 1 to 1024 neighbouring positions
- pos_table: bfloat16 [8192, 1024], P('shard'), may hold values from -3 to 3
- w_qkv: bfloat16 [1024, 3072], P('shard'), may hold values from -0.1875 to 0.1875
- b_query: bfloat16 [1024], P('shard'), may hold values from -3 to 3
- b_value: bfloat16 [1024], P('shard'), may hold values from -3 to 3
- w_out: bfloat16 [1024, 1024], P('shard'), may hold values from -3 to 3
- b_out: bfloat16 [1024], P('shard'), may hold values from -3 to 3
- ln1_gain: bfloat16 [1024], P('shard'), may hold values from 0.5 to 1.5
- ln1_bias: bfloat16 [1024], P('shard'), may hold values from -2 to 2
- w_up: bfloat16 [1024, 4096], P('shard'), may hold values from -0.1875 to 0.1875
- b_up: bfloat16 [4096], P('shard'), may hold values from -3 to 3
- w_down: bfloat16 [4096, 1024], P('shard'), may hold values from -0.09375 to 0.09375
- b_down: bfloat16 [1024], P('shard'), may hold values from -3 to 3
- ln2_gain: bfloat16 [1024], P('shard'), may hold values from 0.5 to 1.5
- ln2_bias: bfloat16 [1024], P('shard'), may hold values from -2 to 2
- cotangent: bfloat16 [4096, 1024], P(('seq', 'shard')), may hold values from -6 to 6
Outputs:
- result: bfloat16 [4096, 1024], P(('seq', 'shard'))
- grad_inputs: bfloat16 [4096, 1024], P(('seq', 'shard'))
- grad_pos_table: float32 [8192, 1024], P('shard')
- grad_w_qkv: float32 [1024, 3072], P('shard')
- grad_b_query: float32 [1024], P('shard')
- grad_b_value: float32 [1024], P('shard')
- grad_w_out: float32 [1024, 1024], P('shard')
- grad_b_out: float32 [1024], P('shard')
- grad_ln1_gain: float32 [1024], P('shard')
- grad_ln1_bias: float32 [1024], P('shard')
- grad_w_up: float32 [1024, 4096], P('shard')
- grad_b_up: float32 [4096], P('shard')
- grad_w_down: float32 [4096, 1024], P('shard')
- grad_b_down: float32 [1024], P('shard')
- grad_ln2_gain: float32 [1024], P('shard')
- grad_ln2_bias: float32 [1024], P('shard')
The draws below stay inside these ranges and needn't reach their ends.
Inputs may be any that keep to these rules, and one draw needn't show every extreme that they name: `segments`: never falls along the tokens; every id from 0 to 7 holds 1 to 1024 consecutive tokens, one id exactly 1024.
All inputs are finite; a program needn't handle non-finite values.
Results may differ from the reference program's by a relative error of at most 0.017.
Values may be sent and summed in bfloat16 or wider, within the bound.
A program may use at most 384 MiB of HBM per device.

```python
import math
import jax
import jax.numpy as jnp
import numpy as np
from jax import lax

D = 1024
HEADS = 16
HEAD_DIM = 64
FF = 4096
TABLE_ROWS = 8192
TOKENS = 4096
SEQ_LEN = 1024
SEGS = 8


def draw_inputs(key, part):
    key_values = jax.random.fold_in(key, 0)
    values = jnp.clip(jax.random.normal(key_values, (TOKENS, D), jnp.float32), -4.0, 4.0)
    return values.astype(jnp.bfloat16)


def draw_cotangent(key, part):
    key_noise = jax.random.fold_in(key, 0)
    position_ramp = jnp.arange(TOKENS, dtype=jnp.float32)[:, None] / TOKENS
    noise_part = jnp.clip(jax.random.normal(key_noise, (TOKENS, D), jnp.float32), -3.0, 3.0)
    scaled = noise_part * (0.6 + 1.2 * position_ramp)
    return scaled.astype(jnp.bfloat16)


def plant(entries, own_key, least, top_value):
    extent = entries.shape
    spot = [jax.random.randint(jax.random.fold_in(own_key, axis), (), 0, extent[axis]) for axis in range(len(extent))]
    entries = entries.at[tuple(spot)].set(least)
    longest = extent.index(max(extent))
    spot[longest] = (spot[longest] + 1) % extent[longest]
    return entries.at[tuple(spot)].set(top_value)


def block_levels(stream_key, shape, cuts, low, top_value):
    factor_of, own = 1.0, jax.random.fold_in(stream_key, 6)
    for position, shards_of in cuts:
        heights = jnp.exp(jax.random.uniform(jax.random.fold_in(own, position), (shards_of,), jnp.float32, low / len(cuts), top_value / len(cuts)))
        factor_of = factor_of * jnp.repeat(heights, shape[position] // shards_of).reshape([-1 if axis == position else 1 for axis in range(len(shape))])
    return factor_of


def profile(number_of, total, bound, skew):
    portions = [(1 << 20) // math.isqrt(grade ** skew) + 1 for grade in range(2, number_of + 1)]
    surplus, holding = total - bound - (number_of - 1), [1] * (number_of - 1)
    while surplus > 0:
        candidates = [i for i in range(number_of - 1) if holding[i] < bound]
        mass, left = sum([portions[i] for i in candidates]), surplus
        for i in candidates:
            more = min(bound - holding[i], max(1, left * portions[i] // mass), surplus)
            holding[i] = holding[i] + more
            surplus = surplus - more
    return np.array([bound] + holding)


def ragged_sizes(key, number_of, total, reach, slope):
    if number_of == 2:
        one = jax.random.randint(key, (), max(1, total - reach), min(reach, total - 1) + 1)
        return jnp.stack([one, total - one])
    lengths = jnp.asarray(profile(number_of, total, reach, slope), jnp.int32)
    pairs = (number_of - 1) // 2
    donor, sink = lengths[1:1 + 2 * pairs:2], lengths[2:2 + 2 * pairs:2]
    margin = jnp.minimum(donor - 1, reach - sink)
    shifted = jax.random.randint(jax.random.fold_in(key, 1), (pairs,), 0, 1 << 20) % (margin + 1)
    lengths = lengths.at[1:1 + 2 * pairs:2].set(donor - shifted).at[2:2 + 2 * pairs:2].set(sink + shifted)
    return lengths[jax.random.permutation(jax.random.fold_in(key, 2), number_of)]


def noise(rng, shape, scale, bound, pieces=(), held_as=jnp.bfloat16):
    values = scale * jax.random.normal(rng, shape, jnp.float32)
    if pieces:
        values = values * block_levels(rng, shape, pieces, -0.22, 0.18)
    return jnp.clip(values, -bound, bound).astype(held_as)


def setup_inputs(seed: int = 0) -> dict:
    key_of = jax.random.split(jax.random.key(seed), 19)
    inputs = draw_inputs(jax.random.fold_in(key_of[18], 71), 0)
    positions = plant(jax.random.randint(key_of[1], (TOKENS,), 0, TABLE_ROWS), jax.random.fold_in(key_of[1], 1), 0, TABLE_ROWS - 1).astype(jnp.int32)
    segments = jnp.searchsorted(jnp.cumsum(ragged_sizes(key_of[2], SEGS, TOKENS, SEQ_LEN, 0)), jnp.arange(TOKENS), side="right").astype(jnp.int32)
    pos_table = noise(key_of[3], (TABLE_ROWS, D), 0.5, 3.0, ((0, 8),))
    w_qkv = noise(key_of[4], (D, 3 * D), D ** -0.5, 0.1875, ((0, 8),))
    b_query = noise(key_of[5], (D,), 0.5, 3.0, ((0, 8),))
    b_value = noise(key_of[6], (D,), 0.5, 3.0, ((0, 8),))
    w_out = noise(key_of[7], (D, D), 4 ** -0.5, 3.0, ((0, 8),))
    b_out = noise(key_of[8], (D,), 0.5, 3.0, ((0, 8),))
    ln1_gain = jnp.clip(1.0 + 0.1 * jax.random.normal(key_of[9], (D,), jnp.float32), 0.5, 1.5).astype(jnp.bfloat16)
    ln1_bias = noise(key_of[10], (D,), 0.3, 2.0, ((0, 8),))
    w_up = noise(key_of[11], (D, FF), D ** -0.5, 0.1875, ((0, 8),))
    b_up = noise(key_of[12], (FF,), 0.5, 3.0, ((0, 8),))
    w_down = noise(key_of[13], (FF, D), FF ** -0.5, 0.09375, ((0, 8),))
    b_down = noise(key_of[14], (D,), 0.5, 3.0, ((0, 8),))
    ln2_gain = jnp.clip(1.0 + 0.1 * jax.random.normal(key_of[15], (D,), jnp.float32), 0.5, 1.5).astype(jnp.bfloat16)
    ln2_bias = noise(key_of[16], (D,), 0.3, 2.0, ((0, 8),))
    cotangent = draw_cotangent(jax.random.fold_in(key_of[18], 71), 0)
    return {"inputs": inputs, "positions": positions, "segments": segments, "pos_table": pos_table, "w_qkv": w_qkv, "b_query": b_query, "b_value": b_value, "w_out": w_out, "b_out": b_out, "ln1_gain": ln1_gain, "ln1_bias": ln1_bias, "w_up": w_up, "b_up": b_up, "w_down": w_down, "b_down": b_down, "ln2_gain": ln2_gain, "ln2_bias": ln2_bias, "cotangent": cotangent}


score_scale = 0.125
neg_large = -1e+30
epsilon = 1e-06
root_half = 0.7071067811865476
inv_root_two_pi = 0.3989422804014327

def layer_normalize(summed):
    center = summed - lax.optimization_barrier(jnp.mean(summed, axis=-1, keepdims=True))
    inverse = lax.rsqrt(lax.optimization_barrier(jnp.mean(center * center, axis=-1, keepdims=True)) + epsilon)
    return (center * inverse, inverse)

def normalize_back(grad_normed, normed, inverse):
    first_mean = lax.optimization_barrier(jnp.mean(grad_normed, axis=-1, keepdims=True))
    second_mean = lax.optimization_barrier(jnp.mean(grad_normed * normed, axis=-1, keepdims=True))
    return inverse * (grad_normed - first_mean - normed * second_mean)

def gelu_value(pre_act):
    return 0.5 * pre_act * (1.0 + jax.scipy.special.erf(pre_act * root_half))

def gelu_slope(pre_act):
    return 0.5 * (1.0 + jax.scipy.special.erf(pre_act * root_half)) + pre_act * jnp.exp(-0.5 * pre_act * pre_act) * inv_root_two_pi

def contract_rows(left_side, right_side):
    return lax.dot_general(left_side, right_side, (((0,), (0,)), ((), ())), preferred_element_type=jnp.float32)

def head_forward(query_head, key_head, value_head, segments, block_size):
    block_count = query_head.shape[0] // block_size

    def one_block(block_item):
        query_block, seg_block = block_item
        scores = jnp.dot(query_block, key_head.T, preferred_element_type=jnp.float32) * score_scale
        same_seq = seg_block[:, None] == segments[None, :]
        scores = jnp.where(same_seq, scores, neg_large)
        row_max = lax.optimization_barrier(jnp.max(scores, axis=1, keepdims=True))
        exp_scores = jnp.where(same_seq, jnp.exp(scores - row_max), 0.0)
        row_total = lax.optimization_barrier(jnp.sum(exp_scores, axis=1, keepdims=True))
        mixed_rows = jnp.dot(exp_scores.astype(jnp.bfloat16), value_head, preferred_element_type=jnp.float32) / row_total
        return (mixed_rows, (row_max + jnp.log(row_total))[:, 0])
    mixed_rows, log_total = lax.map(one_block, (query_head.reshape(block_count, block_size, HEAD_DIM), segments.reshape(block_count, block_size)))
    return (mixed_rows.reshape(-1, HEAD_DIM), log_total.reshape(-1))

def head_backward(query_head, key_head, value_head, attended_head, grad_head, log_total, segments, block_size):
    block_count = query_head.shape[0] // block_size
    delta = lax.optimization_barrier(jnp.sum(grad_head.astype(jnp.float32) * attended_head.astype(jnp.float32), axis=1))

    def one_block(grad_carry, block_item):
        grad_key, grad_value = grad_carry
        query_block, grad_block, log_block, delta_block, seg_block = block_item
        scores = jnp.dot(query_block, key_head.T, preferred_element_type=jnp.float32) * score_scale
        same_seq = seg_block[:, None] == segments[None, :]
        probs = jnp.where(same_seq, jnp.exp(scores - log_block[:, None]), 0.0)
        grad_probs = jnp.dot(grad_block, value_head.T, preferred_element_type=jnp.float32)
        grad_scores = (probs * (grad_probs - delta_block[:, None]) * score_scale).astype(jnp.bfloat16)
        grad_query = jnp.dot(grad_scores, key_head, preferred_element_type=jnp.float32)
        grad_key = grad_key + contract_rows(grad_scores, query_block)
        grad_value = grad_value + contract_rows(probs.astype(jnp.bfloat16), grad_block)
        return ((grad_key, grad_value), grad_query)
    zero_grads = jnp.zeros(key_head.shape, jnp.float32)
    block_items = (query_head.reshape(block_count, block_size, HEAD_DIM), grad_head.reshape(block_count, block_size, HEAD_DIM), log_total.reshape(block_count, block_size), delta.reshape(block_count, block_size), segments.reshape(block_count, block_size))
    (grad_key, grad_value), grad_query = lax.scan(one_block, (zero_grads, zero_grads), block_items)
    return (grad_query.reshape(-1, HEAD_DIM), grad_key, grad_value)

def split_heads(matrix):
    return matrix.reshape(TOKENS, HEADS, HEAD_DIM).transpose(1, 0, 2)

def join_heads(stacked):
    return stacked.transpose(1, 0, 2).reshape(TOKENS, D)

def reference(inputs, positions, segments, pos_table, w_qkv, b_query, b_value, w_out, b_out, ln1_gain, ln1_bias, w_up, b_up, w_down, b_down, ln2_gain, ln2_bias, cotangent):
    block_size = 4096 if TOKENS % 4096 == 0 else TOKENS
    hidden = inputs.astype(jnp.float32) + jnp.take(pos_table, positions, axis=0).astype(jnp.float32)
    hidden_bf = hidden.astype(jnp.bfloat16)
    projected = jnp.dot(hidden_bf, w_qkv, preferred_element_type=jnp.float32)
    query_rows = (projected[:, :D] + b_query.astype(jnp.float32)).astype(jnp.bfloat16)
    key_rows = projected[:, D:2 * D].astype(jnp.bfloat16)
    value_rows = (projected[:, 2 * D:] + b_value.astype(jnp.float32)).astype(jnp.bfloat16)
    heads_query = split_heads(query_rows)
    heads_key = split_heads(key_rows)
    heads_value = split_heads(value_rows)

    def head_front(group):
        return head_forward(group[0], group[1], group[2], segments, block_size)
    attended_heads, log_total = lax.map(head_front, (heads_query, heads_key, heads_value))
    attended = join_heads(attended_heads).astype(jnp.bfloat16)
    first_sum = hidden + jnp.dot(attended, w_out, preferred_element_type=jnp.float32) + b_out.astype(jnp.float32)
    normed_one, inverse_one = layer_normalize(first_sum)
    first_norm = normed_one * ln1_gain.astype(jnp.float32) + ln1_bias.astype(jnp.float32)
    first_bf = first_norm.astype(jnp.bfloat16)
    up_pre = jnp.dot(first_bf, w_up, preferred_element_type=jnp.float32) + b_up.astype(jnp.float32)
    activated = gelu_value(up_pre).astype(jnp.bfloat16)
    second_sum = first_norm + jnp.dot(activated, w_down, preferred_element_type=jnp.float32) + b_down.astype(jnp.float32)
    normed_two, inverse_two = layer_normalize(second_sum)
    result = (normed_two * ln2_gain.astype(jnp.float32) + ln2_bias.astype(jnp.float32)).astype(jnp.bfloat16)
    grad_rows = cotangent.astype(jnp.float32)
    grad_ln2_gain = lax.optimization_barrier(jnp.sum(grad_rows * normed_two, axis=0))
    grad_ln2_bias = lax.optimization_barrier(jnp.sum(grad_rows, axis=0))
    d_second = normalize_back(grad_rows * ln2_gain.astype(jnp.float32), normed_two, inverse_two)
    grad_b_down = lax.optimization_barrier(jnp.sum(d_second, axis=0))
    d_second_bf = d_second.astype(jnp.bfloat16)
    grad_w_down = contract_rows(activated, d_second_bf)
    d_up = jnp.dot(d_second_bf, w_down.T, preferred_element_type=jnp.float32) * gelu_slope(up_pre)
    grad_b_up = lax.optimization_barrier(jnp.sum(d_up, axis=0))
    d_up_bf = d_up.astype(jnp.bfloat16)
    grad_w_up = contract_rows(first_bf, d_up_bf)
    d_first_norm = d_second + jnp.dot(d_up_bf, w_up.T, preferred_element_type=jnp.float32)
    grad_ln1_gain = lax.optimization_barrier(jnp.sum(d_first_norm * normed_one, axis=0))
    grad_ln1_bias = lax.optimization_barrier(jnp.sum(d_first_norm, axis=0))
    d_first = normalize_back(d_first_norm * ln1_gain.astype(jnp.float32), normed_one, inverse_one)
    grad_b_out = lax.optimization_barrier(jnp.sum(d_first, axis=0))
    d_first_bf = d_first.astype(jnp.bfloat16)
    grad_w_out = contract_rows(attended, d_first_bf)
    d_attended = jnp.dot(d_first_bf, w_out.T, preferred_element_type=jnp.float32).astype(jnp.bfloat16)

    def head_back(group):
        return head_backward(group[0], group[1], group[2], group[3], group[4], group[5], segments, block_size)
    grads_query, grads_key, grads_value = lax.map(head_back, (heads_query, heads_key, heads_value, split_heads(attended), split_heads(d_attended), log_total))
    d_query = join_heads(grads_query).astype(jnp.bfloat16)
    d_key = join_heads(grads_key).astype(jnp.bfloat16)
    d_value = join_heads(grads_value).astype(jnp.bfloat16)
    grad_b_query = lax.optimization_barrier(jnp.sum(d_query.astype(jnp.float32), axis=0))
    grad_b_value = lax.optimization_barrier(jnp.sum(d_value.astype(jnp.float32), axis=0))
    d_project = jnp.concatenate([d_query, d_key, d_value], axis=1)
    grad_w_qkv = contract_rows(hidden_bf, d_project)
    d_hidden = d_first + jnp.dot(d_project, w_qkv.T, preferred_element_type=jnp.float32)
    grad_inputs = d_hidden.astype(jnp.bfloat16)
    grad_pos_table = jax.ops.segment_sum(d_hidden, positions, num_segments=TABLE_ROWS)
    return (result, grad_inputs, grad_pos_table, grad_w_qkv, grad_b_query, grad_b_value, grad_w_out, grad_b_out, grad_ln1_gain, grad_ln1_bias, grad_w_up, grad_b_up, grad_w_down, grad_b_down, grad_ln2_gain, grad_ln2_bias)
```

```python
import functools
import math

import jax
import jax.numpy as jnp
from jax import lax
from jax.experimental import pallas as pl
from jax.experimental.pallas import tpu as pltpu
from jax.sharding import PartitionSpec as P

HEADS = 16
HEAD_DIM = 64
score_scale = 0.125
neg_large = -1e30
epsilon = 1e-06
root_half = 0.7071067811865476
inv_root_two_pi = 0.3989422804014327
MESH = pl.DeviceIdType.MESH
F32 = jnp.float32
BF16 = jnp.bfloat16
VMEM_LIMIT = 60 * 1024 * 1024


def flip(value, mask, width):
    total, bit = 0, 1
    while bit < width:
        a = lax.rem(value // bit, 2)
        b = (mask // bit) % 2 if isinstance(mask, int) else lax.rem(mask // bit, 2)
        total = total + lax.rem(a + b, 2) * bit
        bit *= 2
    return total


def remote(src, dst, send_sem, recv_sem, device):
    return pltpu.make_async_remote_copy(
        src_ref=src,
        dst_ref=dst,
        send_sem=send_sem,
        recv_sem=recv_sem,
        device_id=device,
        device_id_type=MESH,
    )


def await_recv(dst, sem, device):
    remote(dst, dst, sem, sem, device).wait_recv()


def await_send(src, sem, device):
    remote(src, src, sem, sem, device).wait_send()


def rows_dot(a, b):
    return lax.dot_general(a, b, (((1,), (0,)), ((), ())), preferred_element_type=F32)


def rows_dot_t(a, b):
    return lax.dot_general(a, b, (((1,), (1,)), ((), ())), preferred_element_type=F32)


def cols_dot(a, b):
    return lax.dot_general(a, b, (((0,), (0,)), ((), ())), preferred_element_type=F32)


def entry_kernel(
    dims,
    pos_ref,
    inp_ref,
    table_ref,
    wqkv_ref,
    wup_ref,
    wdn_ref,
    wout_ref,
    par_ref,
    bup_ref,
    q_ref,
    kv_ref,
    hid_half_ref,
    hidden_ref,
    wq_ref,
    wup2_ref,
    wdn_o_ref,
    wout_o_ref,
    par_all_ref,
    bup_o_ref,
    pos_glob_ref,
    table_v,
    pstage,
    precv,
    cstage,
    crecv,
    qst,
    kvst,
    wup_own,
    wq_tmp,
    pos_ss,
    pos_rs,
    par_ss,
    par_rs,
    posz_ss,
    posz_rs,
    wq_ss,
    wq_rs,
    wqf_ss,
    wqf_rs,
    wup_ss,
    wup_rs,
    wupf_ss,
    wupf_rs,
    misc_ss,
    misc_rs,
    rsp_ss,
    rsp_rs,
    rsc_ss,
    rsc_rs,
    ag_ss,
    ag_rs,
    qx_ss,
    qx_rs,
    zx_ss,
    zx_rs,
    loc,
):
    S, n, C, L, D, hc, R, F2 = dims
    z = lax.axis_index("seq")
    s = lax.axis_index("shard")
    core = lax.rem(s, 2)
    chip = s // 2
    other = 1 - core
    partner = 2 * chip + other
    h2 = 2 * hc
    Dn = D // n

    table_copy = pltpu.make_async_copy(table_ref, table_v, loc.at[0])
    table_copy.start()
    own_wq = []
    for part in range(3):
        own_wq.append(
            pltpu.make_async_copy(
                wqkv_ref.at[:, pl.ds(pl.multiple_of(part * D + chip * h2, 128), h2)],
                wq_ref.at[s, :, part * h2 : (part + 1) * h2],
                loc.at[1 + part],
            )
        )
        own_wq[-1].start()
    own_wup_in = pltpu.make_async_copy(
        wup_ref.at[:, pl.ds(pl.multiple_of(chip * F2, 128), F2)], wup_own, loc.at[4]
    )
    own_wup_in.start()

    barrier = pltpu.get_barrier_semaphore()
    for d in range(1, n):
        pl.semaphore_signal(barrier, inc=1, device_id=(z, flip(s, d, n)), device_id_type=MESH)
    for d in range(1, S):
        pl.semaphore_signal(barrier, inc=1, device_id=(lax.rem(z + d, S), s), device_id_type=MESH)

    for d in (1, S - 1):
        pl.semaphore_signal(
            barrier, inc=1, device_id=(lax.rem(z + d, S), partner), device_id_type=MESH
        )
    pl.semaphore_wait(barrier, n - 1 + S - 1 + 2)

    pos_glob_ref[z, s] = pos_ref[...]
    par_all_ref[s] = par_ref[...]
    for d in range(1, n):
        peer = (z, flip(s, d, n))
        remote(pos_ref, pos_glob_ref.at[z, s], pos_ss.at[d], pos_rs.at[d], peer).start()
        remote(par_ref, par_all_ref.at[s], par_ss.at[d], par_rs.at[d], peer).start()

    for own in own_wq:
        own.wait()

    def wq_src(peer_chip, part):
        return wqkv_ref.at[:, pl.ds(pl.multiple_of(part * D + peer_chip * h2, 128), h2)]

    for j in range(C - 1, 0, -1):
        pc = flip(chip, j, C)
        for part in range(3):
            remote(
                wq_src(pc, part),
                wq_ref.at[s, :, part * h2 : (part + 1) * h2],
                wq_ss.at[j, part],
                wq_rs.at[j, part],
                (z, 2 * pc + core),
            ).start()
    remote(wq_ref.at[s], wq_ref.at[s], wqf_ss.at[0], wqf_rs.at[0], (z, partner)).start()

    for d in range(1, n):
        src = flip(s, d, n)
        await_recv(pos_glob_ref.at[z, src], pos_rs.at[d], (z, src))
    for d in range(1, S):
        remote(
            pos_glob_ref.at[z],
            pos_glob_ref.at[z],
            posz_ss.at[d],
            posz_rs.at[d],
            (lax.rem(z + d, S), s),
        ).start()

    table_copy.wait()
    lane_ids = lax.broadcasted_iota(jnp.int32, (L, R), 1) + s * R

    def picked(block):
        ids = jnp.broadcast_to(pos_glob_ref[z, block], (L, L)).T
        ids = jnp.concatenate([ids] * (R // L), axis=1)
        hot = jnp.where(ids == lane_ids, 1.0, 0.0).astype(BF16)
        return rows_dot(hot, table_v[...])

    def send_partner(j):
        pstage[j] = picked(2 * flip(chip, j, C) + other).astype(BF16)
        remote(pstage.at[j], precv.at[j], rsp_ss.at[j], rsp_rs.at[j], (z, partner)).start()

    def combined(j):
        mine = picked(2 * flip(chip, j, C) + core)
        await_recv(precv.at[j], rsp_rs.at[j], (z, partner))
        return mine + precv[j].astype(F32)

    send_partner(C - 1)

    def scatter_step(k, carry):
        j = C - 1 - k
        send_partner(j - 1)
        cstage[j] = combined(j).astype(BF16)
        remote(
            cstage.at[j], crecv.at[j], rsc_ss.at[j], rsc_rs.at[j], (z, 2 * flip(chip, j, C) + core)
        ).start()
        return carry

    lax.fori_loop(0, C - 1, scatter_step, 0)
    hidden = combined(0) + inp_ref[...].astype(F32)

    for j in range(1, C):
        src = 2 * flip(chip, j, C) + core
        for part in range(3):
            await_recv(
                wq_ref.at[src, :, part * h2 : (part + 1) * h2], wq_rs.at[j, part], (z, src)
            )
        remote(wq_ref.at[src], wq_ref.at[src], wqf_ss.at[j], wqf_rs.at[j], (z, partner)).start()

    for j in range(1, C):
        await_recv(crecv.at[j], rsc_rs.at[j], (z, 2 * flip(chip, j, C) + core))
        hidden = hidden + crecv[j].astype(F32)
    hidden_ref[...] = hidden
    hid_half_ref[chip] = hidden.astype(BF16)
    for j in range(C - 1, 0, -1):
        remote(
            hid_half_ref.at[chip],
            hid_half_ref.at[chip],
            ag_ss.at[j],
            ag_rs.at[j],
            (z, 2 * flip(chip, j, C) + core),
        ).start()

    own_wup_in.wait()
    own_wup_out = pltpu.make_async_copy(wup_own, wup2_ref.at[s], loc.at[5])
    own_wup_out.start()
    for j in range(C - 1, 0, -1):
        pc = flip(chip, j, C)
        remote(
            wup_ref.at[:, pl.ds(pl.multiple_of(pc * F2, 128), F2)],
            wup2_ref.at[s],
            wup_ss.at[j],
            wup_rs.at[j],
            (z, 2 * pc + core),
        ).start()
    remote(wup_own, wup2_ref.at[s], wupf_ss.at[0], wupf_rs.at[0], (z, partner)).start()
    remote(wdn_ref, wdn_o_ref, misc_ss.at[0], misc_rs.at[0], (z, partner)).start()
    remote(wout_ref, wout_o_ref, misc_ss.at[1], misc_rs.at[1], (z, partner)).start()
    remote(bup_ref, bup_o_ref, misc_ss.at[2], misc_rs.at[2], (z, partner)).start()

    for j in range(C):
        src = 2 * flip(chip, j, C) + other
        await_recv(wq_ref.at[src], wqf_rs.at[j], (z, partner))
    for d in range(1, n):
        src = flip(s, d, n)
        await_recv(par_all_ref.at[src], par_rs.at[d], (z, src))
    bias = jnp.concatenate([par_all_ref[2 * chip], par_all_ref[2 * chip + 1]], axis=1)
    bias_q, bias_v = bias[6:7], bias[7:8]
    first_core = core == 0

    def project(j, carry):
        c = flip(chip, j, C)

        @pl.when(j > 0)
        def _():
            await_recv(hid_half_ref.at[c], ag_rs.at[j], (z, 2 * c + core))

        res = rows_dot(hid_half_ref[c], wq_ref[...].reshape(D, 3 * h2))
        query = (res[:, :h2] + bias_q).astype(BF16) * score_scale
        key = res[:, h2 : 2 * h2].astype(BF16)
        value = (res[:, 2 * h2 :] + bias_v).astype(BF16)
        q_ref[c, core] = jnp.where(first_core, query[:, :hc], query[:, hc:])
        kv_ref[1, c, core, :, :hc] = jnp.where(first_core, key[:, :hc], key[:, hc:])
        kv_ref[1, c, core, :, hc:] = jnp.where(first_core, value[:, :hc], value[:, hc:])
        qst[j] = jnp.where(first_core, query[:, hc:], query[:, :hc])
        kvst[j, :, :hc] = jnp.where(first_core, key[:, hc:], key[:, :hc])
        kvst[j, :, hc:] = jnp.where(first_core, value[:, hc:], value[:, :hc])
        own_kv = kv_ref.at[1, c, core]

        @pl.when(z < S - 1)
        def _():
            remote(
                own_kv, kv_ref.at[0, c, core], zx_ss.at[j, 0], zx_rs.at[j, 0], (z + 1, s)
            ).start()
            remote(
                kvst.at[j], kv_ref.at[0, c, core], zx_ss.at[j, 1], zx_rs.at[j, 1], (z + 1, partner)
            ).start()

        @pl.when(z > 0)
        def _():
            remote(
                own_kv, kv_ref.at[2, c, core], zx_ss.at[j, 2], zx_rs.at[j, 2], (z - 1, s)
            ).start()
            remote(
                kvst.at[j], kv_ref.at[2, c, core], zx_ss.at[j, 3], zx_rs.at[j, 3], (z - 1, partner)
            ).start()

        remote(qst.at[j], q_ref.at[c, core], qx_ss.at[j, 0], qx_rs.at[j, 0], (z, partner)).start()
        remote(
            kvst.at[j], kv_ref.at[1, c, core], qx_ss.at[j, 1], qx_rs.at[j, 1], (z, partner)
        ).start()
        return carry

    lax.fori_loop(0, C, project, 0)

    for j in range(1, C):
        src = 2 * flip(chip, j, C) + core
        await_recv(wup2_ref.at[src], wup_rs.at[j], (z, src))
        remote(
            wup2_ref.at[src], wup2_ref.at[src], wupf_ss.at[j], wupf_rs.at[j], (z, partner)
        ).start()

    def settle(j, carry):
        c = flip(chip, j, C)
        await_recv(q_ref.at[c, other], qx_rs.at[j, 0], (z, partner))
        await_recv(kv_ref.at[1, c, other], qx_rs.at[j, 1], (z, partner))
        await_send(qst.at[j], qx_ss.at[j, 0], (z, partner))
        await_send(kvst.at[j], qx_ss.at[j, 1], (z, partner))

        @pl.when(z > 0)
        def _():
            await_recv(kv_ref.at[0, c, core], zx_rs.at[j, 0], (z - 1, s))
            await_recv(kv_ref.at[0, c, other], zx_rs.at[j, 1], (z - 1, partner))
            await_send(kvst.at[j], zx_ss.at[j, 2], (z - 1, s))
            await_send(kvst.at[j], zx_ss.at[j, 3], (z - 1, partner))

        @pl.when(z < S - 1)
        def _():
            await_recv(kv_ref.at[2, c, core], zx_rs.at[j, 2], (z + 1, s))
            await_recv(kv_ref.at[2, c, other], zx_rs.at[j, 3], (z + 1, partner))
            await_send(kvst.at[j], zx_ss.at[j, 0], (z + 1, s))
            await_send(kvst.at[j], zx_ss.at[j, 1], (z + 1, partner))

        await_send(pstage.at[j], rsp_ss.at[j], (z, partner))
        await_send(wq_ref.at[s], wqf_ss.at[j], (z, partner))
        await_recv(wup2_ref.at[2 * c + other], wupf_rs.at[j], (z, partner))
        await_send(wup2_ref.at[s], wupf_ss.at[j], (z, partner))
        return carry

    lax.fori_loop(0, C, settle, 0)
    for j in range(1, C):
        peer = (z, 2 * flip(chip, j, C) + core)
        await_send(cstage.at[j], rsc_ss.at[j], peer)
        await_send(hid_half_ref.at[chip], ag_ss.at[j], peer)
        await_send(wup_own, wup_ss.at[j], peer)
        for part in range(3):
            await_send(
                wq_ref.at[s, :, part * h2 : (part + 1) * h2], wq_ss.at[j, part], peer
            )
    for d in range(1, n):
        peer = (z, flip(s, d, n))
        await_send(pos_ref, pos_ss.at[d], peer)
        await_send(par_ref, par_ss.at[d], peer)
    for d in range(1, S):
        src = lax.rem(z + S - d, S)
        await_recv(pos_glob_ref.at[src], posz_rs.at[d], (src, s))
        await_send(pos_glob_ref.at[z], posz_ss.at[d], (lax.rem(z + d, S), s))
    for i, (mine, got) in enumerate(
        ((wdn_ref, wdn_o_ref), (wout_ref, wout_o_ref), (bup_ref, bup_o_ref))
    ):
        await_recv(got, misc_rs.at[i], (z, partner))
        await_send(mine, misc_ss.at[i], (z, partner))
    own_wup_out.wait()


def entry_call(S, n, pos, inp, table, wqkv, wup, wdn, wout, par, bup):
    C = n // 2
    L, D = inp.shape
    hc = D // n
    R = table.shape[0]
    F = wup.shape[1]
    F1, F2 = F // n, 2 * F // n
    dims = (S, n, C, L, D, hc, R, F2)
    dma = pltpu.SemaphoreType.DMA
    vm = pl.BlockSpec(memory_space=pltpu.VMEM)
    anyw = pl.BlockSpec(memory_space=pl.ANY)
    sds = jax.ShapeDtypeStruct
    return pl.pallas_call(
        functools.partial(entry_kernel, dims),
        out_shape=(
            sds((C, 2, L, hc), BF16),
            sds((3, C, 2, L, 2 * hc), BF16),
            sds((C, L, D), BF16),
            sds((L, D), F32),
            sds((n, D // n, 6 * hc), BF16),
            sds((n, D // n, F2), BF16),
            sds((F1, D), BF16),
            sds((D // n, D), BF16),
            sds((n, 8, hc), F32),
            sds((1, F1), F32),
            sds((S, n, 1, L), jnp.int32),
        ),
        in_specs=[vm, vm, anyw, anyw, anyw, anyw, anyw, vm, vm],
        out_specs=(vm, vm, vm, vm, vm, anyw, anyw, anyw, vm, vm, vm),
        scratch_shapes=[
            pltpu.VMEM((R, D), BF16),
            pltpu.VMEM((C, L, D), BF16),
            pltpu.VMEM((C, L, D), BF16),
            pltpu.VMEM((C, L, D), BF16),
            pltpu.VMEM((C, L, D), BF16),
            pltpu.VMEM((C, L, hc), BF16),
            pltpu.VMEM((C, L, 2 * hc), BF16),
            pltpu.VMEM((D // n, F2), BF16),
            pltpu.VMEM((8, 128), BF16),
            dma((n,)),
            dma((n,)),
            dma((n,)),
            dma((n,)),
            dma((S,)),
            dma((S,)),
            dma((C, 3)),
            dma((C, 3)),
            dma((C,)),
            dma((C,)),
            dma((C,)),
            dma((C,)),
            dma((C,)),
            dma((C,)),
            dma((3,)),
            dma((3,)),
            dma((C,)),
            dma((C,)),
            dma((C,)),
            dma((C,)),
            dma((C,)),
            dma((C,)),
            dma((C, 2)),
            dma((C, 2)),
            dma((C, 4)),
            dma((C, 4)),
            dma((6,)),
        ],
        compiler_params=pltpu.CompilerParams(
            collective_id=0, has_side_effects=True, vmem_limit_bytes=VMEM_LIMIT
        ),
        name="entry_stage",
    )(pos, inp, table, wqkv, wup, wdn, wout, par, bup)


def attend_kernel(dims, bounds_ref, q_ref, kv_ref, lohi_ref, att_ref, lse_ref, vt_ref):
    P_, hc, hh, bq, bk = dims
    lanes = lax.broadcasted_iota(jnp.int32, (bq, hc), 1) // HEAD_DIM
    nq = P_ // bq

    def flip_value(kb, carry):
        at = pl.multiple_of(kb * bk, bk)
        vt_ref[kb] = kv_ref[pl.ds(at, bk), hc:].T
        return carry

    lax.fori_loop(bounds_ref[0, 0], bounds_ref[1, nq - 1], flip_value, 0)

    def one_query_block(qi, carry):
        rows = pl.ds(pl.multiple_of(qi * bq, bq), bq)
        query = q_ref[rows, :]
        heads_q = [jnp.where(lanes == h, query, jnp.zeros_like(query)) for h in range(hh)]
        low, high = lohi_ref[0:1, rows], lohi_ref[1:2, rows]

        def one_key_block(kb, state):
            at = pl.multiple_of(kb * bk, bk)
            keys = kv_ref[pl.ds(at, bk), :hc]
            ids = lax.broadcasted_iota(jnp.int32, (bk, bq), 0) + kb * bk
            keep = (ids >= low) & (ids < high)
            fresh = []
            for h in range(hh):
                top, total, acc = state[h]
                scores = jnp.where(keep, rows_dot_t(keys, heads_q[h]), neg_large)
                new_top = jnp.maximum(top, jnp.max(scores, axis=0, keepdims=True))
                weights = jnp.exp(scores - new_top)
                shrink = jnp.exp(top - new_top)
                total = total * shrink + jnp.sum(weights, axis=0, keepdims=True)
                values = vt_ref[kb, h * HEAD_DIM : (h + 1) * HEAD_DIM, :]
                acc = acc * shrink + rows_dot(values, weights.astype(BF16))
                fresh.append((new_top, total, acc))
            return tuple(fresh)

        start = tuple(
            (
                jnp.full((1, bq), neg_large, F32),
                jnp.zeros((1, bq), F32),
                jnp.zeros((HEAD_DIM, bq), F32),
            )
            for _ in range(hh)
        )
        state = lax.fori_loop(bounds_ref[0, qi], bounds_ref[1, qi], one_key_block, start)
        mixed = jnp.concatenate([acc / total for _, total, acc in state], axis=0)
        att_ref[rows, :] = mixed.T.astype(BF16)
        for h in range(hh):
            lse_ref[h : h + 1, rows] = state[h][0] + jnp.log(state[h][1])
        return carry

    lax.fori_loop(0, nq, one_query_block, 0)


def attend_call(q, kv, bounds, lohi, bq, bk):
    P_, hc = q.shape
    hh = hc // HEAD_DIM
    vm = pl.BlockSpec(memory_space=pltpu.VMEM)
    sm = pl.BlockSpec(memory_space=pltpu.SMEM)
    return pl.pallas_call(
        functools.partial(attend_kernel, (P_, hc, hh, bq, bk)),
        out_shape=(
            jax.ShapeDtypeStruct((P_, hc), BF16),
            jax.ShapeDtypeStruct((hh, P_), F32),
        ),
        in_specs=[sm, vm, vm, vm],
        out_specs=(vm, vm),
        scratch_shapes=[pltpu.VMEM((3 * P_ // bk, hc, bk), BF16)],
        compiler_params=pltpu.CompilerParams(vmem_limit_bytes=VMEM_LIMIT),
        name="attend_stage",
    )(bounds, q, kv, lohi)


def attend_back_kernel(
    dims, bounds_ref, q_ref, kv_ref, lohi_ref, att_ref, datt_ref, lse_ref, dq_ref, dkv_ref, kt_ref, acc_ref
):
    P_, hc, hh, bq, bk = dims
    lanes = lax.broadcasted_iota(jnp.int32, (bq, hc), 1) // HEAD_DIM
    nq = P_ // bq
    acc_ref[...] = jnp.zeros_like(acc_ref)

    def flip_key(kb, carry):
        at = pl.multiple_of(kb * bk, bk)
        kt_ref[kb] = kv_ref[pl.ds(at, bk), :hc].T
        return carry

    lax.fori_loop(bounds_ref[0, 0], bounds_ref[1, nq - 1], flip_key, 0)

    def one_query_block(qi, carry):
        rows = pl.ds(pl.multiple_of(qi * bq, bq), bq)
        query, grad = q_ref[rows, :], datt_ref[rows, :]
        zero = jnp.zeros_like(query)
        heads_q = [jnp.where(lanes == h, query, zero) for h in range(hh)]
        heads_g = [jnp.where(lanes == h, grad, zero) for h in range(hh)]
        stack_q = jnp.concatenate(heads_q, axis=0)
        stack_g = jnp.concatenate(heads_g, axis=0)
        product = (grad.astype(F32) * att_ref[rows, :].astype(F32)).T
        delta = [
            jnp.sum(product[h * HEAD_DIM : (h + 1) * HEAD_DIM], axis=0, keepdims=True)
            for h in range(hh)
        ]
        logs = [lse_ref[h : h + 1, rows] for h in range(hh)]
        low, high = lohi_ref[0:1, rows], lohi_ref[1:2, rows]

        def one_key_block(kb, state):
            at = pl.multiple_of(kb * bk, bk)
            keys = kv_ref[pl.ds(at, bk), :hc]
            values = kv_ref[pl.ds(at, bk), hc:]
            ids = lax.broadcasted_iota(jnp.int32, (bk, bq), 0) + kb * bk
            keep = (ids >= low) & (ids < high)
            fresh, all_p, all_s = [], [], []
            for h in range(hh):
                scores = rows_dot_t(keys, heads_q[h])
                probs = jnp.where(keep, jnp.exp(scores - logs[h]), 0.0)
                grad_probs = rows_dot_t(values, heads_g[h])
                grad_scores = (probs * (grad_probs - delta[h])).astype(BF16)
                all_p.append(probs.astype(BF16))
                all_s.append(grad_scores)
                key_cols = kt_ref[kb, h * HEAD_DIM : (h + 1) * HEAD_DIM, :]
                fresh.append(state[h] + rows_dot(key_cols, grad_scores))
            acc_ref[pl.ds(at, bk), :hc] += rows_dot(jnp.concatenate(all_s, axis=1), stack_q)
            acc_ref[pl.ds(at, bk), hc:] += rows_dot(jnp.concatenate(all_p, axis=1), stack_g)
            return tuple(fresh)

        start = tuple(jnp.zeros((HEAD_DIM, bq), F32) for _ in range(hh))
        state = lax.fori_loop(bounds_ref[0, qi], bounds_ref[1, qi], one_key_block, start)
        dq_ref[rows, :] = (jnp.concatenate(state, axis=0).T * score_scale).astype(BF16)
        return carry

    lax.fori_loop(0, nq, one_query_block, 0)
    dkv_ref[...] = acc_ref[...].astype(BF16)


def attend_back_call(q, kv, bounds, lohi, att, datt, lse, bq, bk):
    P_, hc = q.shape
    hh = hc // HEAD_DIM
    vm = pl.BlockSpec(memory_space=pltpu.VMEM)
    sm = pl.BlockSpec(memory_space=pltpu.SMEM)
    return pl.pallas_call(
        functools.partial(attend_back_kernel, (P_, hc, hh, bq, bk)),
        out_shape=(
            jax.ShapeDtypeStruct((P_, hc), BF16),
            jax.ShapeDtypeStruct((3 * P_, 2 * hc), BF16),
        ),
        in_specs=[sm, vm, vm, vm, vm, vm, vm],
        out_specs=(vm, vm),
        scratch_shapes=[
            pltpu.VMEM((3 * P_ // bk, hc, bk), BF16),
            pltpu.VMEM((3 * P_, 2 * hc), F32),
        ],
        compiler_params=pltpu.CompilerParams(vmem_limit_bytes=VMEM_LIMIT),
        name="attend_back_stage",
    )(bounds, q, kv, lohi, att, datt, lse)


def ranges(segments, P_, bq, bk):
    z = lax.axis_index("seq")
    own = lax.dynamic_slice_in_dim(segments, z * P_, P_)
    low = jnp.sum((segments[:, None] < own[None, :]).astype(jnp.int32), axis=0) - (z - 1) * P_
    high = jnp.sum((segments[:, None] <= own[None, :]).astype(jnp.int32), axis=0) - (z - 1) * P_
    lohi = jnp.stack([low, high])
    bounds = jnp.stack([low[::bq] // bk, (high[bq - 1 :: bq] + bk - 1) // bk])
    return bounds, lohi


def layer_stats(summed):
    center = summed - jnp.mean(summed, axis=1, keepdims=True)
    inverse = lax.rsqrt(jnp.mean(center * center, axis=1, keepdims=True) + epsilon)
    return center * inverse, inverse


def layer_back(grad, normed, inverse):
    first = jnp.mean(grad, axis=1, keepdims=True)
    second = jnp.mean(grad * normed, axis=1, keepdims=True)
    return inverse * (grad - first - normed * second)


def col_sum(x):
    return jnp.sum(x, axis=0, keepdims=True)


def middle_kernel(
    dims,
    att_ref,
    hidden_ref,
    cot_ref,
    par_ref,
    wout_ref,
    wout_o_ref,
    wup_ref,
    wdn_ref,
    wdn_o_ref,
    bup_ref,
    bup_o_ref,
    result_ref,
    dfirst_ref,
    datt_ref,
    gdn_ref,
    gup_ref,
    gout_ref,
    stats_ref,
    gbup_ref,
    wout_v,
    wup_v,
    wdn_v,
    attp,
    fa,
    da,
    dfa,
    act,
    slope,
    dup,
    stage,
    recv,
    normed_v,
    first_v,
    dnorm_v,
    gdn_v,
    gdn_r,
    gup_v,
    gup_r,
    gout_v,
    gout_r,
    gb_v,
    gb_r,
    dattst,
    ap_ss,
    ap_rs,
    sc_ss,
    sc_rs,
    ag_ss,
    ag_rs,
    gx_ss,
    gx_rs,
    dx_ss,
    dx_rs,
    loc,
):
    S, n, C, L, D, hc, F1 = dims
    Dn, F2, Ph = D // n, 2 * F1, C * L
    z = lax.axis_index("seq")
    s = lax.axis_index("shard")
    core = lax.rem(s, 2)
    chip = s // 2
    other = 1 - core
    partner = (z, 2 * chip + other)

    loads = [
        pltpu.make_async_copy(wout_ref, wout_v.at[core], loc.at[0]),
        pltpu.make_async_copy(wout_o_ref, wout_v.at[other], loc.at[1]),
        pltpu.make_async_copy(wup_ref, wup_v, loc.at[2]),
        pltpu.make_async_copy(wdn_ref, wdn_v.at[core], loc.at[3]),
        pltpu.make_async_copy(wdn_o_ref, wdn_v.at[other], loc.at[4]),
    ]
    for load in loads:
        load.start()

    def peer(j):
        return (z, 2 * flip(chip, j, C) + core)

    barrier = pltpu.get_barrier_semaphore()
    pl.semaphore_signal(barrier, inc=1, device_id=partner, device_id_type=MESH)
    for j in range(1, C):
        pl.semaphore_signal(barrier, inc=1, device_id=peer(j), device_id_type=MESH)
    pl.semaphore_wait(barrier, C)

    def put_stat(row, value):
        for i in range(n):
            stats_ref[i, row : row + 1] = value[:, i * hc : (i + 1) * hc]

    def give(i, src, dst):
        remote(src, dst, gx_ss.at[i], gx_rs.at[i], partner).start()

    def taken(i, src, dst):
        await_recv(dst, gx_rs.at[i], partner)

    def spread(r, buf):
        for j in range(C - 1, 0, -1):
            remote(buf.at[chip], buf.at[chip], ag_ss.at[r, j], ag_rs.at[r, j], peer(j)).start()

    def arrived(r, buf, j):
        @pl.when(j > 0)
        def _():
            c = flip(chip, j, C)
            await_recv(buf.at[c], ag_rs.at[r, j], (z, 2 * c + core))

    def hand(r, j, part):
        stage[r, j] = part.astype(BF16)
        remote(stage.at[r, j], recv.at[r, j], sc_ss.at[r, j], sc_rs.at[r, j], peer(j)).start()

    def collected(r, total):
        for j in range(1, C):
            await_recv(recv.at[r, j], sc_rs.at[r, j], peer(j))
            total = total + recv[r, j].astype(F32)
        return total

    par = jnp.concatenate([par_ref[i] for i in range(n)], axis=1)
    b_out, gain1, shift1 = par[0:1], par[1:2], par[2:3]
    b_down, gain2, shift2 = par[3:4], par[4:5], par[5:6]

    remote(att_ref.at[:, other], attp, ap_ss.at[0], ap_rs.at[0], partner).start()
    loads[0].wait()
    loads[1].wait()
    await_recv(attp, ap_rs.at[0], partner)

    def out_part(j):
        c = flip(chip, j, C)
        return rows_dot(att_ref[c, core], wout_v[core]) + rows_dot(attp[c], wout_v[other])

    def out_step(k, carry):
        hand(0, C - 1 - k, out_part(C - 1 - k))
        return carry

    lax.fori_loop(0, C - 1, out_step, 0)
    first_sum = collected(0, out_part(0) + hidden_ref[...] + b_out)
    normed_one, inverse_one = layer_stats(first_sum)
    normed_v[...] = normed_one
    first_norm = normed_one * gain1 + shift1
    first_v[...] = first_norm
    fa[chip] = first_norm.astype(BF16)
    spread(0, fa)

    loads[2].wait()
    loads[3].wait()
    loads[4].wait()
    first_core = core == 0
    bup_mine, bup_theirs = bup_ref[...], bup_o_ref[...]
    bias_up = jnp.concatenate(
        [jnp.where(first_core, bup_mine, bup_theirs), jnp.where(first_core, bup_theirs, bup_mine)],
        axis=1,
    )

    def up_part(j):
        c = flip(chip, j, C)
        pre = rows_dot(fa[c], wup_v[...].reshape(D, F2)) + bias_up
        half = 0.5 * (1.0 + lax.erf(pre * root_half))
        act[c] = (pre * half).astype(BF16)
        slope[c] = half + pre * jnp.exp(-0.5 * pre * pre) * inv_root_two_pi
        return rows_dot(act[c], wdn_v[...].reshape(F2, D))

    own = up_part(0)

    def up_step(j, carry):
        arrived(0, fa, j)
        hand(1, j, up_part(j))
        return carry

    lax.fori_loop(1, C, up_step, 0)
    second_sum = collected(1, own + first_v[...] + b_down)
    normed_two, inverse_two = layer_stats(second_sum)
    result_ref[...] = (normed_two * gain2 + shift2).astype(BF16)
    grad_rows = cot_ref[...].astype(F32)
    put_stat(0, col_sum(grad_rows * normed_two))
    put_stat(1, col_sum(grad_rows))
    d_second = layer_back(grad_rows * gain2, normed_two, inverse_two)
    put_stat(2, col_sum(d_second))
    dnorm_v[...] = d_second
    da[chip] = d_second.astype(BF16)
    spread(1, da)

    def down_back(j):
        c = flip(chip, j, C)
        d_up = rows_dot_t(da[c], wdn_v[...].reshape(F2, D)) * slope[c]
        gb_v[...] += col_sum(d_up)
        dup[c] = d_up.astype(BF16)
        return rows_dot_t(dup[c], wup_v[...].reshape(D, F2))

    gb_v[...] = jnp.zeros_like(gb_v)
    own = down_back(0)

    def back_step(j, carry):
        arrived(1, da, j)
        hand(2, j, down_back(j))
        return carry

    lax.fori_loop(1, C, back_step, 0)
    dnorm_v[...] = dnorm_v[...] + own

    tile = 256
    da_all = da[...].reshape(Ph, D)

    def down_grad(t, carry):
        cols = pl.ds(pl.multiple_of(t * tile, tile), tile)
        gdn_v[pl.ds(pl.multiple_of(t * tile, tile), tile), :] = cols_dot(
            act[:, :, cols].reshape(Ph, tile), da_all
        ).astype(BF16)
        return carry

    lax.fori_loop(0, F2 // tile, down_grad, 0)
    half_rows = pl.ds(pl.multiple_of(other * F1, F1), F1)
    give(0, gdn_v.at[half_rows], gdn_r)

    d_first_norm = collected(2, dnorm_v[...])
    normed_one = normed_v[...]
    put_stat(3, col_sum(d_first_norm * normed_one))
    put_stat(4, col_sum(d_first_norm))
    d_first = layer_back(d_first_norm * gain1, normed_one, inverse_one)
    put_stat(5, col_sum(d_first))
    stats_ref[:, 6:8] = jnp.zeros((n, 2, hc), F32)
    dfirst_ref[...] = d_first
    dfa[chip] = d_first.astype(BF16)
    spread(2, dfa)

    def up_grad(c, carry):
        cols = pl.ds(pl.multiple_of(c * 2 * Dn, 128), 2 * Dn)
        res = cols_dot(fa[:, :, cols].reshape(Ph, 2 * Dn), dup[...].reshape(Ph, F2)).astype(BF16)
        gup_v[c, 0] = res[:Dn]
        gup_v[c, 1] = res[Dn:]
        return carry

    lax.fori_loop(0, C, up_grad, 0)
    give(1, gup_v.at[:, other], gup_r)
    gb_r[0] = jnp.where(first_core, gb_v[:, F1:], gb_v[:, :F1])
    give(2, gb_r.at[0], gb_r.at[1])

    def att_back(j, carry):
        arrived(2, dfa, j)
        c = flip(chip, j, C)
        datt_ref[c, core] = rows_dot_t(dfa[c], wout_v[core]).astype(BF16)
        dattst[j] = rows_dot_t(dfa[c], wout_v[other]).astype(BF16)
        remote(dattst.at[j], datt_ref.at[c, core], dx_ss.at[j], dx_rs.at[j], partner).start()
        return carry

    lax.fori_loop(0, C, att_back, 0)
    dfa_all = dfa[...].reshape(Ph, D)
    gout_v[0] = cols_dot(attp[...].reshape(Ph, hc), dfa_all).astype(BF16)
    give(3, gout_v.at[0], gout_r)
    gout_v[1] = cols_dot(att_ref[:, core].reshape(Ph, hc), dfa_all).astype(BF16)

    taken(0, None, gdn_r)
    own_rows = pl.ds(pl.multiple_of(core * F1, F1), F1)
    gdn_ref[...] = (gdn_v[own_rows, :].astype(F32) + gdn_r[...].astype(F32)).astype(BF16)
    taken(1, None, gup_r)
    gup_ref[...] = (gup_v[:, core].astype(F32) + gup_r[...].astype(F32)).astype(BF16)
    taken(2, None, gb_r.at[1])
    gbup_ref[...] = jnp.where(first_core, gb_v[:, :F1], gb_v[:, F1:]) + gb_r[1]
    taken(3, None, gout_r)
    gout_ref[...] = (gout_v[1].astype(F32) + gout_r[...].astype(F32)).astype(BF16)

    await_send(attp, ap_ss.at[0], partner)
    await_send(gdn_r, gx_ss.at[0], partner)
    await_send(gup_r, gx_ss.at[1], partner)
    await_send(gb_r.at[0], gx_ss.at[2], partner)
    await_send(gout_r, gx_ss.at[3], partner)

    def settle(j, carry):
        c = flip(chip, j, C)
        await_recv(datt_ref.at[c, other], dx_rs.at[j], partner)
        await_send(dattst.at[j], dx_ss.at[j], partner)

        @pl.when(j > 0)
        def _():
            for r in range(3):
                await_send(stage.at[r, j], sc_ss.at[r, j], peer(j))
            await_send(fa.at[chip], ag_ss.at[0, j], peer(j))
            await_send(da.at[chip], ag_ss.at[1, j], peer(j))
            await_send(dfa.at[chip], ag_ss.at[2, j], peer(j))

        return carry

    lax.fori_loop(0, C, settle, 0)


def middle_call(S, n, att, hidden, cot, par, wout, wout_o, wup2, wdn, wdn_o, bup, bup_o):
    C = n // 2
    L, D = hidden.shape
    hc = D // n
    F1 = wdn.shape[0]
    F2 = 2 * F1
    dims = (S, n, C, L, D, hc, F1)
    dma = pltpu.SemaphoreType.DMA
    vm = pl.BlockSpec(memory_space=pltpu.VMEM)
    anyw = pl.BlockSpec(memory_space=pl.ANY)
    sds = jax.ShapeDtypeStruct
    Dn = D // n
    return pl.pallas_call(
        functools.partial(middle_kernel, dims),
        out_shape=(
            sds((L, D), BF16),
            sds((L, D), F32),
            sds((C, 2, L, hc), BF16),
            sds((F1, D), BF16),
            sds((C, Dn, F2), BF16),
            sds((hc, D), BF16),
            sds((n, 8, hc), F32),
            sds((1, F1), F32),
        ),
        in_specs=[vm, vm, vm, vm, anyw, anyw, anyw, anyw, anyw, vm, vm],
        out_specs=(vm,) * 8,
        scratch_shapes=[
            pltpu.VMEM((2, hc, D), BF16),
            pltpu.VMEM((n, Dn, F2), BF16),
            pltpu.VMEM((2, F1, D), BF16),
            pltpu.VMEM((C, L, hc), BF16),
            pltpu.VMEM((C, L, D), BF16),
            pltpu.VMEM((C, L, D), BF16),
            pltpu.VMEM((C, L, D), BF16),
            pltpu.VMEM((C, L, F2), BF16),
            pltpu.VMEM((C, L, F2), F32),
            pltpu.VMEM((C, L, F2), BF16),
            pltpu.VMEM((3, C, L, D), BF16),
            pltpu.VMEM((3, C, L, D), BF16),
            pltpu.VMEM((L, D), F32),
            pltpu.VMEM((L, D), F32),
            pltpu.VMEM((L, D), F32),
            pltpu.VMEM((F2, D), BF16),
            pltpu.VMEM((F1, D), BF16),
            pltpu.VMEM((C, 2, Dn, F2), BF16),
            pltpu.VMEM((C, Dn, F2), BF16),
            pltpu.VMEM((2, hc, D), BF16),
            pltpu.VMEM((hc, D), BF16),
            pltpu.VMEM((1, F2), F32),
            pltpu.VMEM((2, 1, F1), F32),
            pltpu.VMEM((C, L, hc), BF16),
            dma((1,)),
            dma((1,)),
            dma((3, C)),
            dma((3, C)),
            dma((3, C)),
            dma((3, C)),
            dma((4,)),
            dma((4,)),
            dma((C,)),
            dma((C,)),
            dma((5,)),
        ],
        compiler_params=pltpu.CompilerParams(
            collective_id=1, has_side_effects=True, vmem_limit_bytes=VMEM_LIMIT
        ),
        name="middle_stage",
    )(att, hidden, cot, par, wout, wout_o, wup2, wdn, wdn_o, bup, bup_o)


def exit_kernel(
    dims,
    dq_ref,
    dkv_ref,
    hid_ref,
    wq_ref,
    dfirst_ref,
    stats_ref,
    gbup_ref,
    ginp_ref,
    dh_ref,
    gqkv_ref,
    small_ref,
    gbo_ref,
    zr,
    own3,
    got3,
    x6,
    stage,
    recv,
    dhb,
    gq_v,
    gq_r,
    st_r,
    st_v,
    zst,
    zgb,
    zk_ss,
    zk_rs,
    x_ss,
    x_rs,
    sc_ss,
    sc_rs,
    st_ss,
    st_rs,
    zs_ss,
    zs_rs,
    gq_ss,
    gq_rs,
    zl_ss,
    zl_rs,
    ag_ss,
    ag_rs,
    pf_ss,
    pf_rs,
    loc,
):
    S, n, C, L, D, hc, F1 = dims
    Dn, Ph = D // n, C * L
    z = lax.axis_index("seq")
    s = lax.axis_index("shard")
    core = lax.rem(s, 2)
    chip = s // 2
    other = 1 - core
    twin = 2 * chip + other
    partner = (z, twin)
    first_core = core == 0

    def peer(j):
        return (z, 2 * flip(chip, j, C) + core)

    barrier = pltpu.get_barrier_semaphore()
    for d in range(1, n):
        pl.semaphore_signal(barrier, inc=1, device_id=(z, flip(s, d, n)), device_id_type=MESH)
    for d in range(1, S):
        pl.semaphore_signal(barrier, inc=1, device_id=(lax.rem(z + d, S), s), device_id_type=MESH)
    pl.semaphore_wait(barrier, n - 1 + S - 1)

    for j in range(C - 1, -1, -1):
        c = flip(chip, j, C)

        @pl.when(z > 0)
        def _():
            remote(
                dkv_ref.at[0, c], zr.at[1, c], zk_ss.at[j, 0], zk_rs.at[j, 1], (z - 1, s)
            ).start()

        @pl.when(z < S - 1)
        def _():
            remote(
                dkv_ref.at[2, c], zr.at[0, c], zk_ss.at[j, 1], zk_rs.at[j, 0], (z + 1, s)
            ).start()

    st_r[s] = stats_ref[s]
    for d in range(1, n):
        to = flip(s, d, n)
        remote(stats_ref.at[to], st_r.at[s], st_ss.at[d], st_rs.at[d], (z, to)).start()

    def fold(k, carry):
        j = C - 1 - k
        c = flip(chip, j, C)
        whole = dkv_ref[1, c].astype(F32)

        @pl.when(z > 0)
        def _():
            await_recv(zr.at[0, c], zk_rs.at[j, 0], (z - 1, s))

        @pl.when(z < S - 1)
        def _():
            await_recv(zr.at[1, c], zk_rs.at[j, 1], (z + 1, s))

        whole = whole + jnp.where(z > 0, zr[0, c].astype(F32), 0.0)
        whole = whole + jnp.where(z < S - 1, zr[1, c].astype(F32), 0.0)
        whole = whole.astype(BF16)
        own3[c, :, :, :hc] = dq_ref[c]
        own3[c, :, :, hc:] = whole
        remote(own3.at[c, other], got3.at[c], x_ss.at[j], x_rs.at[j], partner).start()
        sums = jnp.sum(own3[c].astype(F32), axis=(0, 1), keepdims=False)
        st_v[0:1] += sums[None, :hc]
        st_v[1:2] += sums[None, 2 * hc :]
        return carry

    st_v[...] = jnp.zeros_like(st_v)
    lax.fori_loop(0, C, fold, 0)

    def partial(j):
        c = flip(chip, j, C)
        await_recv(got3.at[c], x_rs.at[j], partner)
        mine, theirs = own3[c, core], got3[c]
        low = jnp.where(first_core, mine, theirs)
        high = jnp.where(first_core, theirs, mine)
        pieces = []
        for part in range(3):
            pieces += [low[:, part * hc : (part + 1) * hc], high[:, part * hc : (part + 1) * hc]]
        x6[c] = jnp.concatenate(pieces, axis=1)
        return rows_dot_t(x6[c], wq_ref[...].reshape(D, 6 * hc))

    def scatter(k, carry):
        j = C - 1 - k
        stage[j] = partial(j).astype(BF16)
        remote(stage.at[j], recv.at[j], sc_ss.at[j], sc_rs.at[j], peer(j)).start()
        return carry

    lax.fori_loop(0, C - 1, scatter, 0)
    total = partial(0) + dfirst_ref[...]

    def qkv_grad(c, carry):
        cols = pl.ds(pl.multiple_of(c * 2 * Dn, 128), 2 * Dn)
        res = cols_dot(hid_ref[:, :, cols].reshape(Ph, 2 * Dn), x6[...].reshape(Ph, 6 * hc))
        gq_v[c, 0] = res[:Dn].astype(BF16)
        gq_v[c, 1] = res[Dn:].astype(BF16)
        return carry

    lax.fori_loop(0, C, qkv_grad, 0)
    remote(gq_v.at[:, other], gq_r, gq_ss.at[0], gq_rs.at[0], partner).start()

    sums = st_r[s]
    for d in range(1, n):
        src = flip(s, d, n)
        await_recv(st_r.at[src], st_rs.at[d], (z, src))
    sums = st_r[0]
    for i in range(1, n):
        sums = sums + st_r[i]
    zst[z] = sums
    zst[z, 6:8] = st_v[...]
    zgb[z] = gbup_ref[...]
    for d in range(1, S):
        to = (lax.rem(z + d, S), s)
        remote(zst.at[z], zst.at[z], zs_ss.at[d, 0], zs_rs.at[d, 0], to).start()
        remote(zgb.at[z], zgb.at[z], zs_ss.at[d, 1], zs_rs.at[d, 1], to).start()

    for j in range(1, C):
        await_recv(recv.at[j], sc_rs.at[j], peer(j))
        total = total + recv[j].astype(F32)
    ginp = total.astype(BF16)
    ginp_ref[...] = ginp
    dhb[...] = ginp
    keep = pltpu.make_async_copy(dhb, dh_ref.at[z, s], loc.at[0])
    keep.start()

    def broadcast(src, at):
        for j in range(C - 1, 0, -1):
            remote(src, dh_ref.at[at, s], ag_ss.at[at, j], ag_rs.at[at, j], peer(j)).start()
        remote(src, dh_ref.at[at, s], pf_ss.at[at, 0], pf_rs.at[at, 0], partner).start()

    @pl.when(z < S - 1)
    def _():
        remote(dhb, dh_ref.at[z, s], zl_ss.at[z, 0], zl_rs.at[z, 0], (z + 1, s)).start()

    @pl.when(z > 0)
    def _():
        remote(dhb, dh_ref.at[z, s], zl_ss.at[z, 1], zl_rs.at[z, 1], (z - 1, s)).start()

    broadcast(dhb, z)
    for d in range(1, S):

        @pl.when(z - d >= 0)
        def _():
            at = z - d
            await_recv(dh_ref.at[at, s], zl_rs.at[at, 0], (z - 1, s))

            @pl.when(z < S - 1)
            def _():
                remote(
                    dh_ref.at[at, s], dh_ref.at[at, s], zl_ss.at[at, 0], zl_rs.at[at, 0], (z + 1, s)
                ).start()

            broadcast(dh_ref.at[at, s], at)

        @pl.when(z + d <= S - 1)
        def _():
            at = z + d
            await_recv(dh_ref.at[at, s], zl_rs.at[at, 1], (z + 1, s))

            @pl.when(z > 0)
            def _():
                remote(
                    dh_ref.at[at, s], dh_ref.at[at, s], zl_ss.at[at, 1], zl_rs.at[at, 1], (z - 1, s)
                ).start()

            broadcast(dh_ref.at[at, s], at)

    def relay(at):
        for j in range(1, C):
            src = 2 * flip(chip, j, C) + core
            await_recv(dh_ref.at[at, src], ag_rs.at[at, j], (z, src))
            remote(
                dh_ref.at[at, src], dh_ref.at[at, src], pf_ss.at[at, j], pf_rs.at[at, j], partner
            ).start()

    relay(z)
    for d in range(1, S):

        @pl.when(z - d >= 0)
        def _():
            relay(z - d)

        @pl.when(z + d <= S - 1)
        def _():
            relay(z + d)

    await_recv(gq_r, gq_rs.at[0], partner)
    gqkv_ref[...] = (gq_v[:, core].astype(F32) + gq_r[...].astype(F32)).astype(BF16)
    for d in range(1, S):
        src = lax.rem(z + S - d, S)
        await_recv(zst.at[src], zs_rs.at[d, 0], (src, s))
        await_recv(zgb.at[src], zs_rs.at[d, 1], (src, s))
    small, big = zst[0], zgb[0]
    for i in range(1, S):
        small = small + zst[i]
        big = big + zgb[i]
    small_ref[...] = small
    gbo_ref[...] = big

    keep.wait()

    def settle_plane(at, carry):
        for j in range(C):
            src = 2 * flip(chip, j, C) + other
            await_recv(dh_ref.at[at, src], pf_rs.at[at, j], partner)
            await_send(dhb, pf_ss.at[at, j], partner)
            if j > 0:
                await_send(dhb, ag_ss.at[at, j], peer(j))
        return carry

    lax.fori_loop(0, S, settle_plane, 0)
    for at in range(S):

        @pl.when((z >= at) & (z < S - 1))
        def _():
            await_send(dhb, zl_ss.at[at, 0], (z + 1, s))

        @pl.when((z <= at) & (z > 0))
        def _():
            await_send(dhb, zl_ss.at[at, 1], (z - 1, s))

    for j in range(C):

        @pl.when(z > 0)
        def _():
            await_send(zr.at[0, 0], zk_ss.at[j, 0], (z - 1, s))

        @pl.when(z < S - 1)
        def _():
            await_send(zr.at[0, 0], zk_ss.at[j, 1], (z + 1, s))

        await_send(got3.at[0], x_ss.at[j], partner)
        if j > 0:
            await_send(stage.at[j], sc_ss.at[j], peer(j))
    for d in range(1, n):
        await_send(st_r.at[s], st_ss.at[d], (z, flip(s, d, n)))
    for d in range(1, S):
        to = (lax.rem(z + d, S), s)
        await_send(zst.at[z], zs_ss.at[d, 0], to)
        await_send(zgb.at[z], zs_ss.at[d, 1], to)
    await_send(gq_r, gq_ss.at[0], partner)


def exit_call(S, n, dq, dkv, hid_half, wq, dfirst, stats, gbup):
    C = n // 2
    L, D = dfirst.shape
    hc = D // n
    F1 = gbup.shape[1]
    Dn = D // n
    dims = (S, n, C, L, D, hc, F1)
    dma = pltpu.SemaphoreType.DMA
    vm = pl.BlockSpec(memory_space=pltpu.VMEM)
    anyw = pl.BlockSpec(memory_space=pl.ANY)
    sds = jax.ShapeDtypeStruct
    return pl.pallas_call(
        functools.partial(exit_kernel, dims),
        out_shape=(
            sds((L, D), BF16),
            sds((S, n, L, D), BF16),
            sds((C, Dn, 6 * hc), BF16),
            sds((8, hc), F32),
            sds((1, F1), F32),
        ),
        in_specs=[vm] * 7,
        out_specs=(vm, anyw, vm, vm, vm),
        scratch_shapes=[
            pltpu.VMEM((2, C, 2, L, 2 * hc), BF16),
            pltpu.VMEM((C, 2, L, 3 * hc), BF16),
            pltpu.VMEM((C, L, 3 * hc), BF16),
            pltpu.VMEM((C, L, 6 * hc), BF16),
            pltpu.VMEM((C, L, D), BF16),
            pltpu.VMEM((C, L, D), BF16),
            pltpu.VMEM((L, D), BF16),
            pltpu.VMEM((C, 2, Dn, 6 * hc), BF16),
            pltpu.VMEM((C, Dn, 6 * hc), BF16),
            pltpu.VMEM((n, 8, hc), F32),
            pltpu.VMEM((2, hc), F32),
            pltpu.VMEM((S, 8, hc), F32),
            pltpu.VMEM((S, 1, F1), F32),
            dma((C, 2)),
            dma((C, 2)),
            dma((C,)),
            dma((C,)),
            dma((C,)),
            dma((C,)),
            dma((n,)),
            dma((n,)),
            dma((S, 2)),
            dma((S, 2)),
            dma((1,)),
            dma((1,)),
            dma((S, 2)),
            dma((S, 2)),
            dma((S, C)),
            dma((S, C)),
            dma((S, C)),
            dma((S, C)),
            dma((1,)),
        ],
        compiler_params=pltpu.CompilerParams(
            collective_id=2, has_side_effects=True, vmem_limit_bytes=VMEM_LIMIT
        ),
        name="exit_stage",
    )(dq, dkv, hid_half, wq, dfirst, stats, gbup)


def table_kernel(dims, base_ref, pos_ref, dh_ref, out_ref, buf, sems):
    S, P_, R, D, rt = dims
    base = base_ref[0, 0]

    def load(at, slot):
        return pltpu.make_async_copy(dh_ref.at[at], buf.at[slot], sems.at[slot])

    load(0, 0).start()
    for at in range(S):
        slot = at % 2
        if at + 1 < S:
            load(at + 1, 1 - slot).start()
        load(at, slot).wait()

        def rows_tile(t, carry):
            start = pl.multiple_of(t * rt, rt)
            ids = lax.broadcasted_iota(jnp.int32, (rt, P_), 0) + (start + base)
            hot = jnp.where(ids == pos_ref[at], 1.0, 0.0).astype(BF16)
            part = rows_dot(hot, buf[slot])
            if at == 0:
                out_ref[pl.ds(start, rt), :] = part
            else:
                out_ref[pl.ds(start, rt), :] += part
            return carry

        lax.fori_loop(0, R // rt, rows_tile, 0)


def table_call(S, n, R, base, pos, dh):
    L, D = dh.shape[2:]
    P_ = n * L
    vm = pl.BlockSpec(memory_space=pltpu.VMEM)
    sm = pl.BlockSpec(memory_space=pltpu.SMEM)
    anyw = pl.BlockSpec(memory_space=pl.ANY)
    return pl.pallas_call(
        functools.partial(table_kernel, (S, P_, R, D, 256)),
        out_shape=jax.ShapeDtypeStruct((R, D), F32),
        in_specs=[sm, vm, anyw],
        out_specs=vm,
        scratch_shapes=[pltpu.VMEM((2, P_, D), BF16), pltpu.SemaphoreType.DMA((2,))],
        compiler_params=pltpu.CompilerParams(vmem_limit_bytes=VMEM_LIMIT),
        name="table_stage",
    )(base, pos.reshape(S, 1, P_), dh.reshape(S, P_, D))


def owner_kernel(
    dims, gup_ref, gqkv_ref, up_ref, qkv_ref, up_r, qkv_r, up_ss, up_rs, qk_ss, qk_rs
):
    n, C, D, hc, F2 = dims
    z = lax.axis_index("seq")
    s = lax.axis_index("shard")
    core = lax.rem(s, 2)
    chip = s // 2

    def peer(j):
        return (z, 2 * flip(chip, j, C) + core)

    barrier = pltpu.get_barrier_semaphore()
    for j in range(1, C):
        pl.semaphore_signal(barrier, inc=1, device_id=peer(j), device_id_type=MESH)
    pl.semaphore_wait(barrier, C - 1)
    for j in range(C - 1, 0, -1):
        c = flip(chip, j, C)
        remote(gup_ref.at[c], up_r.at[chip], up_ss.at[j], up_rs.at[j], peer(j)).start()
        remote(gqkv_ref.at[c], qkv_r.at[chip], qk_ss.at[j], qk_rs.at[j], peer(j)).start()
    up_r[chip] = gup_ref[chip]
    qkv_r[chip] = gqkv_ref[chip]
    for j in range(1, C):
        c = flip(chip, j, C)
        await_recv(up_r.at[c], up_rs.at[j], peer(j))
        await_recv(qkv_r.at[c], qk_rs.at[j], peer(j))
    h2 = 2 * hc
    for c in range(C):
        up_ref[:, c * F2 : (c + 1) * F2] = up_r[c].astype(F32)
        for part in range(3):
            qkv_ref[:, part * D + c * h2 : part * D + (c + 1) * h2] = qkv_r[
                c, :, part * h2 : (part + 1) * h2
            ].astype(F32)
    for j in range(1, C):
        await_send(up_r.at[chip], up_ss.at[j], peer(j))
        await_send(qkv_r.at[chip], qk_ss.at[j], peer(j))


def owner_call(n, gup, gqkv):
    C, Dn, F2 = gup.shape
    D = Dn * n
    hc = D // n
    vm = pl.BlockSpec(memory_space=pltpu.VMEM)
    dma = pltpu.SemaphoreType.DMA
    return pl.pallas_call(
        functools.partial(owner_kernel, (n, C, D, hc, F2)),
        out_shape=(
            jax.ShapeDtypeStruct((Dn, C * F2), F32),
            jax.ShapeDtypeStruct((Dn, 3 * D), F32),
        ),
        in_specs=[vm, vm],
        out_specs=(vm, vm),
        scratch_shapes=[
            pltpu.VMEM(gup.shape, BF16),
            pltpu.VMEM(gqkv.shape, BF16),
            dma((C,)),
            dma((C,)),
            dma((C,)),
            dma((C,)),
        ],
        compiler_params=pltpu.CompilerParams(
            collective_id=3, has_side_effects=True, vmem_limit_bytes=VMEM_LIMIT
        ),
        name="owner_stage",
    )(gup, gqkv)


QUERY_BLOCK = 256
KEY_BLOCK = 256


def local(
    inputs,
    positions,
    segments,
    pos_table,
    w_qkv,
    b_query,
    b_value,
    w_out,
    b_out,
    ln1_gain,
    ln1_bias,
    w_up,
    b_up,
    w_down,
    b_down,
    ln2_gain,
    ln2_bias,
    cotangent,
):
    S, n = lax.axis_size("seq"), lax.axis_size("shard")
    L, D = inputs.shape
    P_, hc, C = L * n, D // n, n // 2
    R = pos_table.shape[0]
    par = jnp.stack(
        [b_out, ln1_gain, ln1_bias, b_down, ln2_gain, ln2_bias, b_query, b_value]
    ).astype(F32)
    bup = b_up.astype(F32)[None, :]
    q, kv, hid_half, hidden, wq, wup2, wdn_o, wout_o, par_all, bup_o, pos_glob = entry_call(
        S, n, positions[None, :], inputs, pos_table, w_qkv, w_up, w_down, w_out, par, bup
    )
    bounds, lohi = ranges(segments, P_, QUERY_BLOCK, KEY_BLOCK)
    q = q.reshape(P_, hc)
    kv = kv.reshape(3 * P_, 2 * hc)
    att, lse = attend_call(q, kv, bounds, lohi, QUERY_BLOCK, KEY_BLOCK)
    result, dfirst, datt, gdn, gup, gout, stats, gbup = middle_call(
        S,
        n,
        att.reshape(C, 2, L, hc),
        hidden,
        cotangent,
        par_all,
        w_out,
        wout_o,
        wup2,
        w_down,
        wdn_o,
        bup,
        bup_o,
    )
    gdn, gup, gout = lax.psum((gdn, gup, gout), "seq")
    dq, dkv = attend_back_call(
        q, kv, bounds, lohi, att, datt.reshape(P_, hc), lse, QUERY_BLOCK, KEY_BLOCK
    )
    ginp, dh, gqkv, small, gbo = exit_call(
        S,
        n,
        dq.reshape(C, 2, L, hc),
        dkv.reshape(3, C, 2, L, 2 * hc),
        hid_half,
        wq,
        dfirst,
        stats,
        gbup,
    )
    gqkv = lax.psum(gqkv, "seq")
    base = (lax.axis_index("shard") * R).astype(jnp.int32).reshape(1, 1)
    gtable = table_call(S, n, R, base, pos_glob, dh)
    up, qkv = owner_call(n, gup, gqkv)
    return (
        result,
        ginp,
        gtable,
        qkv,
        small[6],
        small[7],
        gout.astype(F32),
        small[5],
        small[3],
        small[4],
        up,
        gbo[0],
        gdn.astype(F32),
        small[2],
        small[0],
        small[1],
    )


def solution(mesh):
    in_specs = (
        P(("seq", "shard"), None),
        P(("seq", "shard")),
        P(),
        P("shard", None),
        P("shard", None),
        P("shard"),
        P("shard"),
        P("shard", None),
        P("shard"),
        P("shard"),
        P("shard"),
        P("shard", None),
        P("shard"),
        P("shard", None),
        P("shard"),
        P("shard"),
        P("shard"),
        P(("seq", "shard"), None),
    )
    out_specs = (
        P(("seq", "shard"), None),
        P(("seq", "shard"), None),
        P("shard", None),
        P("shard", None),
        P("shard"),
        P("shard"),
        P("shard", None),
        P("shard"),
        P("shard"),
        P("shard"),
        P("shard", None),
        P("shard"),
        P("shard", None),
        P("shard"),
        P("shard"),
        P("shard"),
    )
    return jax.shard_map(local, mesh=mesh, in_specs=in_specs, out_specs=out_specs, check_vma=False)
```

```python
import functools
import math

import jax
import jax.numpy as jnp
from jax import lax
from jax.experimental import pallas as pl
from jax.experimental.pallas import tpu as pltpu
from jax.sharding import PartitionSpec as P

HEADS = 16
HEAD_DIM = 64
score_scale = 0.125
neg_large = -1e30
epsilon = 1e-06
root_half = 0.7071067811865476
inv_root_two_pi = 0.3989422804014327
MESH = pl.DeviceIdType.MESH
F32 = jnp.float32
BF16 = jnp.bfloat16
VMEM_LIMIT = 60 * 1024 * 1024


def flip(value, mask, width):
    total, bit = 0, 1
    while bit < width:
        a = lax.rem(value // bit, 2)
        b = (mask // bit) % 2 if isinstance(mask, int) else lax.rem(mask // bit, 2)
        total = total + lax.rem(a + b, 2) * bit
        bit *= 2
    return total


def remote(src, dst, send_sem, recv_sem, device):
    return pltpu.make_async_remote_copy(
        src_ref=src,
        dst_ref=dst,
        send_sem=send_sem,
        recv_sem=recv_sem,
        device_id=device,
        device_id_type=MESH,
    )


def await_recv(dst, sem, device):
    remote(dst, dst, sem, sem, device).wait_recv()


def await_send(src, sem, device):
    remote(src, src, sem, sem, device).wait_send()


class Chain:
    def __init__(self, S, z, s, own, land, cross, fin, sems, lag=3):
        self.S, self.s, self.lag, self.sems = S, s, lag, sems
        self.own, self.land, self.cross, self.fin = own, land, cross, fin
        low = 1 - (2 * z) // S
        self.depth = low * z + (1 - low) * (S - 1 - z)
        self.inward = (z + 2 * low - 1, s)
        self.outward = (z + 1 - 2 * low, s)
        self.mid = S // 2 - 1
        self.pieces = own.shape[0]
        self.slots = self.pieces + lag * self.mid + lag * max(self.mid - 1, 0)

    def give_out(self, start, stop):
        @pl.when(self.depth == 0)
        def _():
            def step(p, carry):
                remote(
                    self.own.at[p], self.land.at[p], self.sems.at[0, p], self.sems.at[1, p], self.inward
                ).start()
                return carry

            lax.fori_loop(start, stop, step, 0)

    def slot(self, k):
        p = k - self.lag * (self.depth - 1)

        @pl.when((self.depth > 0) & (p >= 0) & (p < self.pieces))
        def _():
            await_recv(self.land.at[p], self.sems.at[1, p], self.outward)
            both = self.own[p].astype(F32) + self.land[p].astype(F32)
            self.own[p] = both.astype(BF16)

            @pl.when(self.depth < self.mid)
            def _():
                remote(
                    self.own.at[p], self.land.at[p], self.sems.at[0, p], self.sems.at[1, p], self.inward
                ).start()

            @pl.when(self.depth == self.mid)
            def _():
                remote(
                    self.own.at[p], self.cross.at[p], self.sems.at[2, p], self.sems.at[3, p], self.inward
                ).start()

        x = k - self.lag * self.mid

        @pl.when((self.depth == self.mid) & (x >= 0) & (x < self.pieces))
        def _():
            await_recv(self.cross.at[x], self.sems.at[3, x], self.inward)
            both = self.own[x].astype(F32) + self.cross[x].astype(F32)
            self.fin[x] = both.astype(BF16)
            remote(
                self.fin.at[x], self.fin.at[x], self.sems.at[4, x], self.sems.at[5, x], self.outward
            ).start()

        b = k - self.lag * self.mid - self.lag * (self.mid - self.depth)

        @pl.when((self.depth < self.mid) & (self.depth > 0) & (b >= 0) & (b < self.pieces))
        def _():
            await_recv(self.fin.at[b], self.sems.at[5, b], self.inward)
            remote(
                self.fin.at[b], self.fin.at[b], self.sems.at[4, b], self.sems.at[5, b], self.outward
            ).start()

    def run(self, start, stop):
        def step(k, carry):
            self.slot(k)
            return carry

        lax.fori_loop(start, stop, step, 0)

    def settle(self):
        def step(p, carry):
            @pl.when(self.depth == 0)
            def _():
                await_recv(self.fin.at[p], self.sems.at[5, p], self.inward)

            @pl.when(self.depth < self.mid)
            def _():
                await_send(self.own.at[p], self.sems.at[0, p], self.inward)

            @pl.when(self.depth == self.mid)
            def _():
                await_send(self.own.at[p], self.sems.at[2, p], self.inward)

            @pl.when(self.depth > 0)
            def _():
                await_send(self.fin.at[p], self.sems.at[4, p], self.outward)

            return carry

        lax.fori_loop(0, self.pieces, step, 0)


def rows_dot(a, b):
    return lax.dot_general(a, b, (((1,), (0,)), ((), ())), preferred_element_type=F32)


def rows_dot_t(a, b):
    return lax.dot_general(a, b, (((1,), (1,)), ((), ())), preferred_element_type=F32)


def cols_dot(a, b):
    return lax.dot_general(a, b, (((0,), (0,)), ((), ())), preferred_element_type=F32)


def entry_kernel(
    dims,
    pos_ref,
    inp_ref,
    table_ref,
    wqkv_ref,
    wup_ref,
    wdn_ref,
    wout_ref,
    seg_ref,
    bup_in_ref,
    row0_ref,
    row1_ref,
    row2_ref,
    row3_ref,
    row4_ref,
    row5_ref,
    row6_ref,
    row7_ref,
    q_ref,
    kv_ref,
    hid_half_ref,
    hidden_ref,
    wq_ref,
    wup2_ref,
    wdn_o_ref,
    wout_o_ref,
    par_all_ref,
    bup2_ref,
    pos_glob_ref,
    lohi_ref,
    table_v,
    pstage,
    precv,
    cstage,
    crecv,
    qst,
    kvst,
    wup_own,
    par_ref,
    bup_ref,
    pos_ss,
    pos_rs,
    par_ss,
    par_rs,
    posz_ss,
    posz_rs,
    wq_ss,
    wq_rs,
    wqf_ss,
    wqf_rs,
    wup_ss,
    wup_rs,
    wupf_ss,
    wupf_rs,
    misc_ss,
    misc_rs,
    rsp_ss,
    rsp_rs,
    rsc_ss,
    rsc_rs,
    ag_ss,
    ag_rs,
    qx_ss,
    qx_rs,
    zx_ss,
    zx_rs,
    loc,
):
    S, n, C, L, D, hc, R, F2 = dims
    z = lax.axis_index("seq")
    s = lax.axis_index("shard")
    core = lax.rem(s, 2)
    chip = s // 2
    other = 1 - core
    partner = 2 * chip + other
    h2 = 2 * hc
    Dn = D // n

    table_copy = pltpu.make_async_copy(table_ref, table_v, loc.at[0])
    table_copy.start()
    own_wq = []
    for part in range(3):
        own_wq.append(
            pltpu.make_async_copy(
                wqkv_ref.at[:, pl.ds(pl.multiple_of(part * D + chip * h2, 128), h2)],
                wq_ref.at[s, :, part * h2 : (part + 1) * h2],
                loc.at[1 + part],
            )
        )
        own_wq[-1].start()
    own_wup_in = pltpu.make_async_copy(
        wup_ref.at[:, pl.ds(pl.multiple_of(chip * F2, 128), F2)], wup_own, loc.at[4]
    )
    own_wup_in.start()

    rows = (row0_ref, row1_ref, row2_ref, row3_ref, row4_ref, row5_ref, row6_ref, row7_ref)
    for i, row in enumerate(rows):
        par_ref[i : i + 1] = row[...].astype(F32)
    bup_ref[...] = bup_in_ref[...].astype(F32)
    F1 = F2 // 2
    bup_mine = pl.ds(pl.multiple_of(core * F1, 128), F1)
    bup_theirs = pl.ds(pl.multiple_of(other * F1, 128), F1)
    bup2_ref[:, bup_mine] = bup_ref[...]

    barrier = pltpu.get_barrier_semaphore()
    for d in range(1, n):
        pl.semaphore_signal(barrier, inc=1, device_id=(z, flip(s, d, n)), device_id_type=MESH)
    for d in range(1, S):
        pl.semaphore_signal(barrier, inc=1, device_id=(lax.rem(z + d, S), s), device_id_type=MESH)

    for d in (1, S - 1):
        pl.semaphore_signal(
            barrier, inc=1, device_id=(lax.rem(z + d, S), partner), device_id_type=MESH
        )
    pl.semaphore_wait(barrier, n - 1 + S - 1 + 2)

    pos_glob_ref[z, s] = pos_ref[...]
    par_all_ref[s] = par_ref[...]
    for d in range(1, n):
        peer = (z, flip(s, d, n))
        remote(pos_ref, pos_glob_ref.at[z, s], pos_ss.at[d], pos_rs.at[d], peer).start()
        remote(par_ref, par_all_ref.at[s], par_ss.at[d], par_rs.at[d], peer).start()

    for own in own_wq:
        own.wait()

    def wq_src(peer_chip, part):
        return wqkv_ref.at[:, pl.ds(pl.multiple_of(part * D + peer_chip * h2, 128), h2)]

    for j in range(C - 1, 0, -1):
        pc = flip(chip, j, C)
        for part in range(3):
            remote(
                wq_src(pc, part),
                wq_ref.at[s, :, part * h2 : (part + 1) * h2],
                wq_ss.at[j, part],
                wq_rs.at[j, part],
                (z, 2 * pc + core),
            ).start()
    remote(wq_ref.at[s], wq_ref.at[s], wqf_ss.at[0], wqf_rs.at[0], (z, partner)).start()

    own_segs = jnp.concatenate([seg_ref[z * n + i] for i in range(n)], axis=1)

    def count(g, carry):
        low, high = carry
        keys = jnp.broadcast_to(seg_ref[g], (L, L)).T
        lows, highs = [], []
        for i in range(n):
            mine = own_segs[:, i * L : (i + 1) * L]
            lows.append(jnp.sum(jnp.where(keys < mine, 1.0, 0.0), axis=0, keepdims=True))
            highs.append(jnp.sum(jnp.where(keys <= mine, 1.0, 0.0), axis=0, keepdims=True))
        return low + jnp.concatenate(lows, axis=1), high + jnp.concatenate(highs, axis=1)

    none = jnp.zeros((1, n * L), F32)
    low, high = lax.fori_loop(0, S * n, count, (none, none))
    origin = ((z - 1) * n * L).astype(F32)
    lohi_ref[0:1] = low - origin
    lohi_ref[1:2] = high - origin

    for d in range(1, n):
        src = flip(s, d, n)
        await_recv(pos_glob_ref.at[z, src], pos_rs.at[d], (z, src))
    for d in range(1, S):
        remote(
            pos_glob_ref.at[z],
            pos_glob_ref.at[z],
            posz_ss.at[d],
            posz_rs.at[d],
            (lax.rem(z + d, S), s),
        ).start()

    table_copy.wait()
    lane_ids = lax.broadcasted_iota(jnp.int32, (L, R), 1) + s * R

    def picked(block):
        ids = jnp.broadcast_to(pos_glob_ref[z, block], (L, L)).T
        ids = jnp.concatenate([ids] * (R // L), axis=1)
        hot = jnp.where(ids == lane_ids, 1.0, 0.0).astype(BF16)
        return rows_dot(hot, table_v[...])

    def send_partner(j):
        pstage[j] = picked(2 * flip(chip, j, C) + other).astype(BF16)
        remote(pstage.at[j], precv.at[j], rsp_ss.at[j], rsp_rs.at[j], (z, partner)).start()

    def combined(j):
        mine = picked(2 * flip(chip, j, C) + core)
        await_recv(precv.at[j], rsp_rs.at[j], (z, partner))
        return mine + precv[j].astype(F32)

    send_partner(C - 1)

    def scatter_step(k, carry):
        j = C - 1 - k
        send_partner(j - 1)
        cstage[j] = combined(j).astype(BF16)
        remote(
            cstage.at[j], crecv.at[j], rsc_ss.at[j], rsc_rs.at[j], (z, 2 * flip(chip, j, C) + core)
        ).start()
        return carry

    lax.fori_loop(0, C - 1, scatter_step, 0)
    hidden = combined(0) + inp_ref[...].astype(F32)

    for j in range(1, C):
        src = 2 * flip(chip, j, C) + core
        for part in range(3):
            await_recv(
                wq_ref.at[src, :, part * h2 : (part + 1) * h2], wq_rs.at[j, part], (z, src)
            )
        remote(wq_ref.at[src], wq_ref.at[src], wqf_ss.at[j], wqf_rs.at[j], (z, partner)).start()

    for j in range(1, C):
        await_recv(crecv.at[j], rsc_rs.at[j], (z, 2 * flip(chip, j, C) + core))
        hidden = hidden + crecv[j].astype(F32)
    hidden_ref[...] = hidden
    hid_half_ref[chip] = hidden.astype(BF16)
    for j in range(C - 1, 0, -1):
        remote(
            hid_half_ref.at[chip],
            hid_half_ref.at[chip],
            ag_ss.at[j],
            ag_rs.at[j],
            (z, 2 * flip(chip, j, C) + core),
        ).start()

    own_wup_in.wait()
    own_wup_out = pltpu.make_async_copy(wup_own, wup2_ref.at[s], loc.at[5])
    own_wup_out.start()
    for j in range(C - 1, 0, -1):
        pc = flip(chip, j, C)
        remote(
            wup_ref.at[:, pl.ds(pl.multiple_of(pc * F2, 128), F2)],
            wup2_ref.at[s],
            wup_ss.at[j],
            wup_rs.at[j],
            (z, 2 * pc + core),
        ).start()
    remote(wup_own, wup2_ref.at[s], wupf_ss.at[0], wupf_rs.at[0], (z, partner)).start()
    remote(wdn_ref, wdn_o_ref, misc_ss.at[0], misc_rs.at[0], (z, partner)).start()
    remote(wout_ref, wout_o_ref, misc_ss.at[1], misc_rs.at[1], (z, partner)).start()
    remote(bup_ref, bup2_ref.at[:, bup_mine], misc_ss.at[2], misc_rs.at[2], (z, partner)).start()

    for j in range(C):
        src = 2 * flip(chip, j, C) + other
        await_recv(wq_ref.at[src], wqf_rs.at[j], (z, partner))
    for d in range(1, n):
        src = flip(s, d, n)
        await_recv(par_all_ref.at[src], par_rs.at[d], (z, src))
    bias = jnp.concatenate([par_all_ref[2 * chip], par_all_ref[2 * chip + 1]], axis=1)
    bias_q, bias_v = bias[6:7], bias[7:8]
    first_core = core == 0

    def project(j, carry):
        c = flip(chip, j, C)

        @pl.when(j > 0)
        def _():
            await_recv(hid_half_ref.at[c], ag_rs.at[j], (z, 2 * c + core))

        res = rows_dot(hid_half_ref[c], wq_ref[...].reshape(D, 3 * h2))
        query = (res[:, :h2] + bias_q).astype(BF16) * score_scale
        key = res[:, h2 : 2 * h2].astype(BF16)
        value = (res[:, 2 * h2 :] + bias_v).astype(BF16)
        q_ref[c, core] = jnp.where(first_core, query[:, :hc], query[:, hc:])
        kv_ref[1, c, core, :, :hc] = jnp.where(first_core, key[:, :hc], key[:, hc:])
        kv_ref[1, c, core, :, hc:] = jnp.where(first_core, value[:, :hc], value[:, hc:])
        qst[j] = jnp.where(first_core, query[:, hc:], query[:, :hc])
        kvst[j, :, :hc] = jnp.where(first_core, key[:, hc:], key[:, :hc])
        kvst[j, :, hc:] = jnp.where(first_core, value[:, hc:], value[:, :hc])
        own_kv = kv_ref.at[1, c, core]

        @pl.when(z < S - 1)
        def _():
            remote(
                own_kv, kv_ref.at[0, c, core], zx_ss.at[j, 0], zx_rs.at[j, 0], (z + 1, s)
            ).start()
            remote(
                kvst.at[j], kv_ref.at[0, c, core], zx_ss.at[j, 1], zx_rs.at[j, 1], (z + 1, partner)
            ).start()

        @pl.when(z > 0)
        def _():
            remote(
                own_kv, kv_ref.at[2, c, core], zx_ss.at[j, 2], zx_rs.at[j, 2], (z - 1, s)
            ).start()
            remote(
                kvst.at[j], kv_ref.at[2, c, core], zx_ss.at[j, 3], zx_rs.at[j, 3], (z - 1, partner)
            ).start()

        remote(qst.at[j], q_ref.at[c, core], qx_ss.at[j, 0], qx_rs.at[j, 0], (z, partner)).start()
        remote(
            kvst.at[j], kv_ref.at[1, c, core], qx_ss.at[j, 1], qx_rs.at[j, 1], (z, partner)
        ).start()
        return carry

    lax.fori_loop(0, C, project, 0)

    for j in range(1, C):
        src = 2 * flip(chip, j, C) + core
        await_recv(wup2_ref.at[src], wup_rs.at[j], (z, src))
        remote(
            wup2_ref.at[src], wup2_ref.at[src], wupf_ss.at[j], wupf_rs.at[j], (z, partner)
        ).start()

    def settle(j, carry):
        c = flip(chip, j, C)
        await_recv(q_ref.at[c, other], qx_rs.at[j, 0], (z, partner))
        await_recv(kv_ref.at[1, c, other], qx_rs.at[j, 1], (z, partner))
        await_send(qst.at[j], qx_ss.at[j, 0], (z, partner))
        await_send(kvst.at[j], qx_ss.at[j, 1], (z, partner))

        @pl.when(z > 0)
        def _():
            await_recv(kv_ref.at[0, c, core], zx_rs.at[j, 0], (z - 1, s))
            await_recv(kv_ref.at[0, c, other], zx_rs.at[j, 1], (z - 1, partner))
            await_send(kvst.at[j], zx_ss.at[j, 2], (z - 1, s))
            await_send(kvst.at[j], zx_ss.at[j, 3], (z - 1, partner))

        @pl.when(z < S - 1)
        def _():
            await_recv(kv_ref.at[2, c, core], zx_rs.at[j, 2], (z + 1, s))
            await_recv(kv_ref.at[2, c, other], zx_rs.at[j, 3], (z + 1, partner))
            await_send(kvst.at[j], zx_ss.at[j, 0], (z + 1, s))
            await_send(kvst.at[j], zx_ss.at[j, 1], (z + 1, partner))

        await_send(pstage.at[j], rsp_ss.at[j], (z, partner))
        await_send(wq_ref.at[s], wqf_ss.at[j], (z, partner))
        await_recv(wup2_ref.at[2 * c + other], wupf_rs.at[j], (z, partner))
        await_send(wup2_ref.at[s], wupf_ss.at[j], (z, partner))
        return carry

    lax.fori_loop(0, C, settle, 0)
    for j in range(1, C):
        peer = (z, 2 * flip(chip, j, C) + core)
        await_send(cstage.at[j], rsc_ss.at[j], peer)
        await_send(hid_half_ref.at[chip], ag_ss.at[j], peer)
        await_send(wup_own, wup_ss.at[j], peer)
        for part in range(3):
            await_send(
                wq_ref.at[s, :, part * h2 : (part + 1) * h2], wq_ss.at[j, part], peer
            )
    for d in range(1, n):
        peer = (z, flip(s, d, n))
        await_send(pos_ref, pos_ss.at[d], peer)
        await_send(par_ref, par_ss.at[d], peer)
    for d in range(1, S):
        src = lax.rem(z + S - d, S)
        await_recv(pos_glob_ref.at[src], posz_rs.at[d], (src, s))
        await_send(pos_glob_ref.at[z], posz_ss.at[d], (lax.rem(z + d, S), s))
    for i, (mine, got) in enumerate(
        ((wdn_ref, wdn_o_ref), (wout_ref, wout_o_ref), (bup_ref, bup2_ref.at[:, bup_theirs]))
    ):
        await_recv(got, misc_rs.at[i], (z, partner))
        await_send(mine, misc_ss.at[i], (z, partner))
    own_wup_out.wait()


def entry_call(S, n, pos, inp, table, wqkv, wup, wdn, wout, seg, bup, rows):
    C = n // 2
    L, D = inp.shape
    hc = D // n
    R = table.shape[0]
    F = wup.shape[1]
    F1, F2 = F // n, 2 * F // n
    dims = (S, n, C, L, D, hc, R, F2)
    dma = pltpu.SemaphoreType.DMA
    vm = pl.BlockSpec(memory_space=pltpu.VMEM)
    anyw = pl.BlockSpec(memory_space=pl.ANY)
    sds = jax.ShapeDtypeStruct
    return pl.pallas_call(
        functools.partial(entry_kernel, dims),
        out_shape=(
            sds((C, 2, L, hc), BF16),
            sds((3, C, 2, L, 2 * hc), BF16),
            sds((C, L, D), BF16),
            sds((L, D), F32),
            sds((n, D // n, 6 * hc), BF16),
            sds((n, D // n, F2), BF16),
            sds((F1, D), BF16),
            sds((D // n, D), BF16),
            sds((n, 8, hc), F32),
            sds((1, F2), F32),
            sds((S, n, 1, L), jnp.int32),
            sds((2, n * L), F32),
        ),
        in_specs=[vm, vm, anyw, anyw, anyw, anyw, anyw] + [vm] * 10,
        out_specs=(vm, vm, vm, vm, vm, anyw, anyw, anyw, vm, vm, vm, vm),
        scratch_shapes=[
            pltpu.VMEM((R, D), BF16),
            pltpu.VMEM((C, L, D), BF16),
            pltpu.VMEM((C, L, D), BF16),
            pltpu.VMEM((C, L, D), BF16),
            pltpu.VMEM((C, L, D), BF16),
            pltpu.VMEM((C, L, hc), BF16),
            pltpu.VMEM((C, L, 2 * hc), BF16),
            pltpu.VMEM((D // n, F2), BF16),
            pltpu.VMEM((8, hc), F32),
            pltpu.VMEM((1, F1), F32),
            dma((n,)),
            dma((n,)),
            dma((n,)),
            dma((n,)),
            dma((S,)),
            dma((S,)),
            dma((C, 3)),
            dma((C, 3)),
            dma((C,)),
            dma((C,)),
            dma((C,)),
            dma((C,)),
            dma((C,)),
            dma((C,)),
            dma((3,)),
            dma((3,)),
            dma((C,)),
            dma((C,)),
            dma((C,)),
            dma((C,)),
            dma((C,)),
            dma((C,)),
            dma((C, 2)),
            dma((C, 2)),
            dma((C, 4)),
            dma((C, 4)),
            dma((6,)),
        ],
        compiler_params=pltpu.CompilerParams(
            collective_id=0, has_side_effects=True, vmem_limit_bytes=VMEM_LIMIT
        ),
        name="entry_stage",
    )(pos, inp, table, wqkv, wup, wdn, wout, seg, bup, *rows)


def key_blocks(lohi_ref, rows, bk):
    first = jnp.min(lohi_ref[0:1, rows]).astype(jnp.int32)
    last = jnp.max(lohi_ref[1:2, rows]).astype(jnp.int32)
    return first // bk, (last + bk - 1) // bk


def attend_kernel(dims, q_ref, kv_ref, lohi_ref, att_ref, lse_ref, vt_ref):
    P_, hc, hh, bq, bk = dims
    lanes = lax.broadcasted_iota(jnp.int32, (bq, hc), 1) // HEAD_DIM
    nq = P_ // bq

    def flip_value(kb, carry):
        at = pl.multiple_of(kb * bk, bk)
        vt_ref[kb] = kv_ref[pl.ds(at, bk), hc:].T
        return carry

    first, last = key_blocks(lohi_ref, pl.ds(0, P_), bk)
    lax.fori_loop(first, last, flip_value, 0)

    def one_query_block(qi, carry):
        rows = pl.ds(pl.multiple_of(qi * bq, bq), bq)
        query = q_ref[rows, :]
        heads_q = [jnp.where(lanes == h, query, jnp.zeros_like(query)) for h in range(hh)]
        low = lohi_ref[0:1, rows].astype(jnp.int32)
        high = lohi_ref[1:2, rows].astype(jnp.int32)
        first, last = key_blocks(lohi_ref, rows, bk)

        def one_key_block(kb, state):
            at = pl.multiple_of(kb * bk, bk)
            keys = kv_ref[pl.ds(at, bk), :hc]
            ids = lax.broadcasted_iota(jnp.int32, (bk, bq), 0) + kb * bk
            keep = (ids >= low) & (ids < high)
            fresh = []
            for h in range(hh):
                top, total, acc = state[h]
                scores = jnp.where(keep, rows_dot_t(keys, heads_q[h]), neg_large)
                new_top = jnp.maximum(top, jnp.max(scores, axis=0, keepdims=True))
                weights = jnp.exp(scores - new_top)
                shrink = jnp.exp(top - new_top)
                total = total * shrink + jnp.sum(weights, axis=0, keepdims=True)
                values = vt_ref[kb, h * HEAD_DIM : (h + 1) * HEAD_DIM, :]
                acc = acc * shrink + rows_dot(values, weights.astype(BF16))
                fresh.append((new_top, total, acc))
            return tuple(fresh)

        start = tuple(
            (
                jnp.full((1, bq), neg_large, F32),
                jnp.zeros((1, bq), F32),
                jnp.zeros((HEAD_DIM, bq), F32),
            )
            for _ in range(hh)
        )
        state = lax.fori_loop(first, last, one_key_block, start)
        mixed = jnp.concatenate([acc / total for _, total, acc in state], axis=0)
        att_ref[rows, :] = mixed.T.astype(BF16)
        for h in range(hh):
            lse_ref[h : h + 1, rows] = state[h][0] + jnp.log(state[h][1])
        return carry

    lax.fori_loop(0, nq, one_query_block, 0)


def attend_call(q, kv, lohi, bq, bk):
    P_, hc = q.shape
    hh = hc // HEAD_DIM
    vm = pl.BlockSpec(memory_space=pltpu.VMEM)
    return pl.pallas_call(
        functools.partial(attend_kernel, (P_, hc, hh, bq, bk)),
        out_shape=(
            jax.ShapeDtypeStruct((P_, hc), BF16),
            jax.ShapeDtypeStruct((hh, P_), F32),
        ),
        in_specs=[vm, vm, vm],
        out_specs=(vm, vm),
        scratch_shapes=[pltpu.VMEM((3 * P_ // bk, hc, bk), BF16)],
        compiler_params=pltpu.CompilerParams(vmem_limit_bytes=VMEM_LIMIT),
        name="attend_stage",
    )(q, kv, lohi)


def attend_back_kernel(
    dims, q_ref, kv_ref, lohi_ref, att_ref, datt_ref, lse_ref, dq_ref, dkv_ref, kt_ref, acc_ref
):
    P_, hc, hh, bq, bk = dims
    lanes = lax.broadcasted_iota(jnp.int32, (bq, hc), 1) // HEAD_DIM
    nq = P_ // bq
    acc_ref[...] = jnp.zeros_like(acc_ref)

    def flip_key(kb, carry):
        at = pl.multiple_of(kb * bk, bk)
        kt_ref[kb] = kv_ref[pl.ds(at, bk), :hc].T
        return carry

    first, last = key_blocks(lohi_ref, pl.ds(0, P_), bk)
    lax.fori_loop(first, last, flip_key, 0)

    def one_query_block(qi, carry):
        rows = pl.ds(pl.multiple_of(qi * bq, bq), bq)
        query, grad = q_ref[rows, :], datt_ref[rows, :]
        zero = jnp.zeros_like(query)
        heads_q = [jnp.where(lanes == h, query, zero) for h in range(hh)]
        heads_g = [jnp.where(lanes == h, grad, zero) for h in range(hh)]
        stack_q = jnp.concatenate(heads_q, axis=0)
        stack_g = jnp.concatenate(heads_g, axis=0)
        product = (grad.astype(F32) * att_ref[rows, :].astype(F32)).T
        delta = [
            jnp.sum(product[h * HEAD_DIM : (h + 1) * HEAD_DIM], axis=0, keepdims=True)
            for h in range(hh)
        ]
        logs = [lse_ref[h : h + 1, rows] for h in range(hh)]
        low = lohi_ref[0:1, rows].astype(jnp.int32)
        high = lohi_ref[1:2, rows].astype(jnp.int32)
        first, last = key_blocks(lohi_ref, rows, bk)

        def one_key_block(kb, state):
            at = pl.multiple_of(kb * bk, bk)
            keys = kv_ref[pl.ds(at, bk), :hc]
            values = kv_ref[pl.ds(at, bk), hc:]
            ids = lax.broadcasted_iota(jnp.int32, (bk, bq), 0) + kb * bk
            keep = (ids >= low) & (ids < high)
            fresh, all_p, all_s = [], [], []
            for h in range(hh):
                scores = rows_dot_t(keys, heads_q[h])
                probs = jnp.where(keep, jnp.exp(scores - logs[h]), 0.0)
                grad_probs = rows_dot_t(values, heads_g[h])
                grad_scores = (probs * (grad_probs - delta[h])).astype(BF16)
                all_p.append(probs.astype(BF16))
                all_s.append(grad_scores)
                key_cols = kt_ref[kb, h * HEAD_DIM : (h + 1) * HEAD_DIM, :]
                fresh.append(state[h] + rows_dot(key_cols, grad_scores))
            acc_ref[pl.ds(at, bk), :hc] += rows_dot(jnp.concatenate(all_s, axis=1), stack_q)
            acc_ref[pl.ds(at, bk), hc:] += rows_dot(jnp.concatenate(all_p, axis=1), stack_g)
            return tuple(fresh)

        start = tuple(jnp.zeros((HEAD_DIM, bq), F32) for _ in range(hh))
        state = lax.fori_loop(first, last, one_key_block, start)
        dq_ref[rows, :] = (jnp.concatenate(state, axis=0).T * score_scale).astype(BF16)
        return carry

    lax.fori_loop(0, nq, one_query_block, 0)
    dkv_ref[...] = acc_ref[...].astype(BF16)


def attend_back_call(q, kv, lohi, att, datt, lse, bq, bk):
    P_, hc = q.shape
    hh = hc // HEAD_DIM
    vm = pl.BlockSpec(memory_space=pltpu.VMEM)
    return pl.pallas_call(
        functools.partial(attend_back_kernel, (P_, hc, hh, bq, bk)),
        out_shape=(
            jax.ShapeDtypeStruct((P_, hc), BF16),
            jax.ShapeDtypeStruct((3 * P_, 2 * hc), BF16),
        ),
        in_specs=[vm, vm, vm, vm, vm, vm],
        out_specs=(vm, vm),
        scratch_shapes=[
            pltpu.VMEM((3 * P_ // bk, hc, bk), BF16),
            pltpu.VMEM((3 * P_, 2 * hc), F32),
        ],
        compiler_params=pltpu.CompilerParams(vmem_limit_bytes=VMEM_LIMIT),
        name="attend_back_stage",
    )(q, kv, lohi, att, datt, lse)


def layer_stats(summed):
    center = summed - jnp.mean(summed, axis=1, keepdims=True)
    inverse = lax.rsqrt(jnp.mean(center * center, axis=1, keepdims=True) + epsilon)
    return center * inverse, inverse


def layer_back(grad, normed, inverse):
    first = jnp.mean(grad, axis=1, keepdims=True)
    second = jnp.mean(grad * normed, axis=1, keepdims=True)
    return inverse * (grad - first - normed * second)


def col_sum(x):
    return jnp.sum(x, axis=0, keepdims=True)


def middle_kernel(
    dims,
    att_ref,
    hidden_ref,
    cot_ref,
    par_ref,
    wout_ref,
    wout_o_ref,
    wup_ref,
    wdn_ref,
    wdn_o_ref,
    bup_ref,
    result_ref,
    dfirst_ref,
    datt_ref,
    gdn_ref,
    gup_ref,
    gout_ref,
    stats_ref,
    gbup_ref,
    gdn_done_ref,
    wout_v,
    wup_v,
    wdn_v,
    attp,
    fa,
    da,
    dfa,
    act,
    slope,
    dup,
    stage,
    recv,
    normed_v,
    first_v,
    dnorm_v,
    gdn_v,
    gdn_r,
    gdn_h,
    gdn_l,
    gdn_x,
    gdn_f,
    gup_v,
    gup_r,
    gout_v,
    gout_r,
    gb_v,
    gb_r,
    dattst,
    ap_ss,
    ap_rs,
    sc_ss,
    sc_rs,
    ag_ss,
    ag_rs,
    gx_ss,
    gx_rs,
    dx_ss,
    dx_rs,
    zsem,
    loc,
):
    S, n, C, L, D, hc, F1 = dims
    Dn, F2, Ph = D // n, 2 * F1, C * L
    z = lax.axis_index("seq")
    s = lax.axis_index("shard")
    core = lax.rem(s, 2)
    chip = s // 2
    other = 1 - core
    partner = (z, 2 * chip + other)

    loads = [
        pltpu.make_async_copy(wout_ref, wout_v.at[core], loc.at[0]),
        pltpu.make_async_copy(wout_o_ref, wout_v.at[other], loc.at[1]),
        pltpu.make_async_copy(wup_ref, wup_v, loc.at[2]),
        pltpu.make_async_copy(wdn_ref, wdn_v.at[core], loc.at[3]),
        pltpu.make_async_copy(wdn_o_ref, wdn_v.at[other], loc.at[4]),
    ]
    for load in loads:
        load.start()

    def peer(j):
        return (z, 2 * flip(chip, j, C) + core)

    barrier = pltpu.get_barrier_semaphore()
    pl.semaphore_signal(barrier, inc=1, device_id=partner, device_id_type=MESH)
    for j in range(1, C):
        pl.semaphore_signal(barrier, inc=1, device_id=peer(j), device_id_type=MESH)
    for d in (1, S - 1):
        pl.semaphore_signal(barrier, inc=1, device_id=(lax.rem(z + d, S), s), device_id_type=MESH)
    pl.semaphore_wait(barrier, C + 2)

    def put_stat(row, value):
        for i in range(n):
            stats_ref[i, row : row + 1] = value[:, i * hc : (i + 1) * hc]

    def give(i, src, dst):
        remote(src, dst, gx_ss.at[i], gx_rs.at[i], partner).start()

    def taken(i, src, dst):
        await_recv(dst, gx_rs.at[i], partner)

    def spread(r, buf):
        for j in range(C - 1, 0, -1):
            remote(buf.at[chip], buf.at[chip], ag_ss.at[r, j], ag_rs.at[r, j], peer(j)).start()

    def arrived(r, buf, j):
        @pl.when(j > 0)
        def _():
            c = flip(chip, j, C)
            await_recv(buf.at[c], ag_rs.at[r, j], (z, 2 * c + core))

    def hand(r, j, part):
        stage[r, j] = part.astype(BF16)
        remote(stage.at[r, j], recv.at[r, j], sc_ss.at[r, j], sc_rs.at[r, j], peer(j)).start()

    def collected(r, total):
        for j in range(1, C):
            await_recv(recv.at[r, j], sc_rs.at[r, j], peer(j))
            total = total + recv[r, j].astype(F32)
        return total

    par = jnp.concatenate([par_ref[i] for i in range(n)], axis=1)
    b_out, gain1, shift1 = par[0:1], par[1:2], par[2:3]
    b_down, gain2, shift2 = par[3:4], par[4:5], par[5:6]

    remote(att_ref.at[:, other], attp, ap_ss.at[0], ap_rs.at[0], partner).start()
    loads[0].wait()
    loads[1].wait()
    await_recv(attp, ap_rs.at[0], partner)

    def out_part(j):
        c = flip(chip, j, C)
        return rows_dot(att_ref[c, core], wout_v[core]) + rows_dot(attp[c], wout_v[other])

    def out_step(k, carry):
        hand(0, C - 1 - k, out_part(C - 1 - k))
        return carry

    lax.fori_loop(0, C - 1, out_step, 0)
    first_sum = collected(0, out_part(0) + hidden_ref[...] + b_out)
    normed_one, inverse_one = layer_stats(first_sum)
    normed_v[...] = normed_one
    first_norm = normed_one * gain1 + shift1
    first_v[...] = first_norm
    fa[chip] = first_norm.astype(BF16)
    spread(0, fa)

    loads[2].wait()
    loads[3].wait()
    loads[4].wait()
    first_core = core == 0
    bias_up = bup_ref[...]

    def up_part(j):
        c = flip(chip, j, C)
        pre = rows_dot(fa[c], wup_v[...].reshape(D, F2)) + bias_up
        half = 0.5 * (1.0 + lax.erf(pre * root_half))
        act[c] = (pre * half).astype(BF16)
        slope[c] = half + pre * jnp.exp(-0.5 * pre * pre) * inv_root_two_pi
        return rows_dot(act[c], wdn_v[...].reshape(F2, D))

    own = up_part(0)

    def up_step(j, carry):
        arrived(0, fa, j)
        hand(1, j, up_part(j))
        return carry

    lax.fori_loop(1, C, up_step, 0)
    second_sum = collected(1, own + first_v[...] + b_down)
    normed_two, inverse_two = layer_stats(second_sum)
    result_ref[...] = (normed_two * gain2 + shift2).astype(BF16)
    grad_rows = cot_ref[...].astype(F32)
    put_stat(0, col_sum(grad_rows * normed_two))
    put_stat(1, col_sum(grad_rows))
    d_second = layer_back(grad_rows * gain2, normed_two, inverse_two)
    put_stat(2, col_sum(d_second))
    dnorm_v[...] = d_second
    da[chip] = d_second.astype(BF16)
    spread(1, da)

    def down_back(j):
        c = flip(chip, j, C)
        d_up = rows_dot_t(da[c], wdn_v[...].reshape(F2, D)) * slope[c]
        gb_v[...] += col_sum(d_up)
        dup[c] = d_up.astype(BF16)
        return rows_dot_t(dup[c], wup_v[...].reshape(D, F2))

    gb_v[...] = jnp.zeros_like(gb_v)
    own = down_back(0)

    def back_step(j, carry):
        arrived(1, da, j)
        hand(2, j, down_back(j))
        return carry

    lax.fori_loop(1, C, back_step, 0)
    dnorm_v[...] = dnorm_v[...] + own

    tile = 256
    da_all = da[...].reshape(Ph, D)

    per_half = F1 // tile
    per_tile = gdn_v.shape[1] // per_half

    def down_grad(i, carry):
        t = lax.rem(i + other * per_half, 2 * per_half)
        cols = pl.ds(pl.multiple_of(t * tile, tile), tile)
        res = cols_dot(act[:, :, cols].reshape(Ph, tile), da_all).astype(BF16)
        gdn_v[t // per_half, pl.ds(lax.rem(t, per_half) * per_tile, per_tile)] = res.reshape(
            per_tile, tile // per_tile, D
        )
        return carry

    lax.fori_loop(0, per_half, down_grad, 0)
    give(0, gdn_v.at[other], gdn_r)
    lax.fori_loop(per_half, 2 * per_half, down_grad, 0)

    def up_grad(c, carry):
        cols = pl.ds(pl.multiple_of(c * 2 * Dn, 128), 2 * Dn)
        res = cols_dot(fa[:, :, cols].reshape(Ph, 2 * Dn), dup[...].reshape(Ph, F2)).astype(BF16)
        gup_v[c, 0] = res[:Dn]
        gup_v[c, 1] = res[Dn:]
        return carry

    early = gdn_h.shape[0]
    taken(0, None, gdn_r)
    gdn_h[...] = (gdn_v[core, :early].astype(F32) + gdn_r[:early].astype(F32)).astype(BF16)
    gdn_ref[...] = (gdn_v[core, early:].astype(F32) + gdn_r[early:].astype(F32)).astype(BF16)
    chain = Chain(S, z, s, gdn_h, gdn_l, gdn_x, gdn_f, zsem)
    chain.give_out(0, early)

    lax.fori_loop(0, C, up_grad, 0)
    give(1, gup_v.at[:, other], gup_r)
    gb_r[0] = jnp.where(first_core, gb_v[:, F1:], gb_v[:, :F1])
    give(2, gb_r.at[0], gb_r.at[1])
    chain.run(0, 2)
    d_first_norm = collected(2, dnorm_v[...])
    normed_one = normed_v[...]
    put_stat(3, col_sum(d_first_norm * normed_one))
    put_stat(4, col_sum(d_first_norm))
    d_first = layer_back(d_first_norm * gain1, normed_one, inverse_one)
    put_stat(5, col_sum(d_first))
    stats_ref[:, 6:8] = jnp.zeros((n, 2, hc), F32)
    dfirst_ref[...] = d_first
    dfa[chip] = d_first.astype(BF16)
    spread(2, dfa)

    def att_back(j, carry):
        chain.run(2 * j + 2, 2 * j + 4)
        arrived(2, dfa, j)
        c = flip(chip, j, C)
        datt_ref[c, core] = rows_dot_t(dfa[c], wout_v[core]).astype(BF16)
        dattst[j] = rows_dot_t(dfa[c], wout_v[other]).astype(BF16)
        remote(dattst.at[j], datt_ref.at[c, core], dx_ss.at[j], dx_rs.at[j], partner).start()
        return carry

    lax.fori_loop(0, C, att_back, 0)
    dfa_all = dfa[...].reshape(Ph, D)
    gout_v[0] = cols_dot(attp[...].reshape(Ph, hc), dfa_all).astype(BF16)
    give(3, gout_v.at[0], gout_r)
    gout_v[1] = cols_dot(att_ref[:, core].reshape(Ph, hc), dfa_all).astype(BF16)

    chain.run(2 * C + 2, chain.slots)
    taken(1, None, gup_r)
    gup_ref[...] = (gup_v[:, core].astype(F32) + gup_r[...].astype(F32)).astype(BF16)
    taken(2, None, gb_r.at[1])
    gbup_ref[...] = jnp.where(first_core, gb_v[:, :F1], gb_v[:, F1:]) + gb_r[1]
    taken(3, None, gout_r)
    gout_ref[...] = (gout_v[1].astype(F32) + gout_r[...].astype(F32)).astype(BF16)

    chain.settle()
    gdn_done_ref[...] = gdn_f[...]
    await_send(attp, ap_ss.at[0], partner)
    await_send(gdn_r, gx_ss.at[0], partner)
    await_send(gup_r, gx_ss.at[1], partner)
    await_send(gb_r.at[0], gx_ss.at[2], partner)
    await_send(gout_r, gx_ss.at[3], partner)

    def settle(j, carry):
        c = flip(chip, j, C)
        await_recv(datt_ref.at[c, other], dx_rs.at[j], partner)
        await_send(dattst.at[j], dx_ss.at[j], partner)

        @pl.when(j > 0)
        def _():
            for r in range(3):
                await_send(stage.at[r, j], sc_ss.at[r, j], peer(j))
            await_send(fa.at[chip], ag_ss.at[0, j], peer(j))
            await_send(da.at[chip], ag_ss.at[1, j], peer(j))
            await_send(dfa.at[chip], ag_ss.at[2, j], peer(j))

        return carry

    lax.fori_loop(0, C, settle, 0)


def middle_call(S, n, att, hidden, cot, par, wout, wout_o, wup2, wdn, wdn_o, bup):
    C = n // 2
    L, D = hidden.shape
    hc = D // n
    F1 = wdn.shape[0]
    F2 = 2 * F1
    dims = (S, n, C, L, D, hc, F1)
    dma = pltpu.SemaphoreType.DMA
    vm = pl.BlockSpec(memory_space=pltpu.VMEM)
    anyw = pl.BlockSpec(memory_space=pl.ANY)
    sds = jax.ShapeDtypeStruct
    Dn = D // n
    pc, early = 16, EARLY_PIECES
    return pl.pallas_call(
        functools.partial(middle_kernel, dims),
        out_shape=(
            sds((L, D), BF16),
            sds((L, D), F32),
            sds((C, 2, L, hc), BF16),
            sds((pc - early, F1 // pc, D), BF16),
            sds((C, Dn, F2), BF16),
            sds((hc, D), BF16),
            sds((n, 8, hc), F32),
            sds((1, F1), F32),
            sds((early, F1 // pc, D), BF16),
        ),
        in_specs=[vm, vm, vm, vm, anyw, anyw, anyw, anyw, anyw, vm],
        out_specs=(vm,) * 9,
        scratch_shapes=[
            pltpu.VMEM((2, hc, D), BF16),
            pltpu.VMEM((n, Dn, F2), BF16),
            pltpu.VMEM((2, F1, D), BF16),
            pltpu.VMEM((C, L, hc), BF16),
            pltpu.VMEM((C, L, D), BF16),
            pltpu.VMEM((C, L, D), BF16),
            pltpu.VMEM((C, L, D), BF16),
            pltpu.VMEM((C, L, F2), BF16),
            pltpu.VMEM((C, L, F2), F32),
            pltpu.VMEM((C, L, F2), BF16),
            pltpu.VMEM((3, C, L, D), BF16),
            pltpu.VMEM((3, C, L, D), BF16),
            pltpu.VMEM((L, D), F32),
            pltpu.VMEM((L, D), F32),
            pltpu.VMEM((L, D), F32),
            pltpu.VMEM((2, pc, F1 // pc, D), BF16),
            pltpu.VMEM((pc, F1 // pc, D), BF16),
            pltpu.VMEM((early, F1 // pc, D), BF16),
            pltpu.VMEM((early, F1 // pc, D), BF16),
            pltpu.VMEM((early, F1 // pc, D), BF16),
            pltpu.VMEM((early, F1 // pc, D), BF16),
            pltpu.VMEM((C, 2, Dn, F2), BF16),
            pltpu.VMEM((C, Dn, F2), BF16),
            pltpu.VMEM((2, hc, D), BF16),
            pltpu.VMEM((hc, D), BF16),
            pltpu.VMEM((1, F2), F32),
            pltpu.VMEM((2, 1, F1), F32),
            pltpu.VMEM((C, L, hc), BF16),
            dma((1,)),
            dma((1,)),
            dma((3, C)),
            dma((3, C)),
            dma((3, C)),
            dma((3, C)),
            dma((4,)),
            dma((4,)),
            dma((C,)),
            dma((C,)),
            dma((6, early)),
            dma((5,)),
        ],
        compiler_params=pltpu.CompilerParams(
            collective_id=1, has_side_effects=True, vmem_limit_bytes=VMEM_LIMIT
        ),
        name="middle_stage",
    )(att, hidden, cot, par, wout, wout_o, wup2, wdn, wdn_o, bup)


def exit_kernel(
    dims,
    dq_ref,
    dkv_ref,
    hid_ref,
    wq_ref,
    dfirst_ref,
    stats_ref,
    gbup_ref,
    pos_ref,
    gupc_ref,
    goutc_ref,
    gdnc_ref,
    ginp_ref,
    dh_ref,
    gq_f,
    up_f,
    out_f,
    dn_f,
    gtable_ref,
    small_ref,
    gbo_ref,
    zr,
    own3,
    got3,
    x6,
    stage,
    recv,
    dhb,
    gq_v,
    gq_r,
    gq_s,
    gq_o,
    gq_l,
    gq_x,
    up_o,
    up_l,
    up_x,
    out_o,
    out_l,
    out_x,
    dn_o,
    dn_l,
    dn_x,
    plane,
    prod,
    st_r,
    st_v,
    zst,
    zgb,
    zk_ss,
    zk_rs,
    x_ss,
    x_rs,
    sc_ss,
    sc_rs,
    st_ss,
    st_rs,
    zs_ss,
    zs_rs,
    gq_ss,
    gq_rs,
    gx_ss,
    gx_rs,
    ua_ss,
    ua_rs,
    qc,
    uc,
    oc,
    dc,
    zl_ss,
    zl_rs,
    ag_ss,
    ag_rs,
    pf_ss,
    pf_rs,
    loc,
):
    S, n, C, L, D, hc, F1, R, rt = dims
    Dn, Ph = D // n, C * L
    z = lax.axis_index("seq")
    s = lax.axis_index("shard")
    core = lax.rem(s, 2)
    chip = s // 2
    other = 1 - core
    twin = 2 * chip + other
    partner = (z, twin)
    first_core = core == 0

    def peer(j):
        return (z, 2 * flip(chip, j, C) + core)

    barrier = pltpu.get_barrier_semaphore()
    for d in range(1, n):
        pl.semaphore_signal(barrier, inc=1, device_id=(z, flip(s, d, n)), device_id_type=MESH)
    for d in range(1, S):
        pl.semaphore_signal(barrier, inc=1, device_id=(lax.rem(z + d, S), s), device_id_type=MESH)
    pl.semaphore_wait(barrier, n - 1 + S - 1)

    for j in range(C - 1, -1, -1):
        c = flip(chip, j, C)

        @pl.when(z > 0)
        def _():
            remote(
                dkv_ref.at[0, c], zr.at[1, c], zk_ss.at[j, 0], zk_rs.at[j, 1], (z - 1, s)
            ).start()

        @pl.when(z < S - 1)
        def _():
            remote(
                dkv_ref.at[2, c], zr.at[0, c], zk_ss.at[j, 1], zk_rs.at[j, 0], (z + 1, s)
            ).start()

    quarter = Dn // 4
    mine = pl.ds(4 * chip, 4)

    def block_of(j):
        return pl.ds(4 * flip(chip, j, C), 4)

    for j in range(C - 1, 0, -1):
        remote(
            gupc_ref.at[flip(chip, j, C)], up_o.at[mine], ua_ss.at[j], ua_rs.at[j], peer(j)
        ).start()
    up_o[mine] = gupc_ref[chip]
    out_o[...] = goutc_ref[...].reshape(4, quarter, D)
    dn_o[...] = gdnc_ref[...]
    wide = Chain(S, z, s, up_o, up_l, up_x, up_f, uc)
    square = Chain(S, z, s, out_o, out_l, out_x, out_f, oc)
    late = Chain(S, z, s, dn_o, dn_l, dn_x, dn_f, dc)
    inner = Chain(S, z, s, gq_o, gq_l, gq_x, gq_f, qc)
    late.give_out(0, late.pieces)
    square.give_out(0, square.pieces)

    st_r[s] = stats_ref[s]
    for d in range(1, n):
        to = flip(s, d, n)
        remote(stats_ref.at[to], st_r.at[s], st_ss.at[d], st_rs.at[d], (z, to)).start()

    def fold(k, carry):
        j = C - 1 - k
        c = flip(chip, j, C)
        whole = dkv_ref[1, c].astype(F32)

        @pl.when(z > 0)
        def _():
            await_recv(zr.at[0, c], zk_rs.at[j, 0], (z - 1, s))

        @pl.when(z < S - 1)
        def _():
            await_recv(zr.at[1, c], zk_rs.at[j, 1], (z + 1, s))

        whole = whole + jnp.where(z > 0, zr[0, c].astype(F32), 0.0)
        whole = whole + jnp.where(z < S - 1, zr[1, c].astype(F32), 0.0)
        whole = whole.astype(BF16)
        own3[c, :, :, :hc] = dq_ref[c]
        own3[c, :, :, hc:] = whole
        remote(own3.at[c, other], got3.at[c], x_ss.at[j], x_rs.at[j], partner).start()
        sums = jnp.sum(own3[c].astype(F32), axis=(0, 1), keepdims=False)
        st_v[0:1] += sums[None, :hc]
        st_v[1:2] += sums[None, 2 * hc :]
        return carry

    st_v[...] = jnp.zeros_like(st_v)
    lax.fori_loop(0, C, fold, 0)

    def partial(j):
        c = flip(chip, j, C)
        await_recv(got3.at[c], x_rs.at[j], partner)
        mine, theirs = own3[c, core], got3[c]
        low = jnp.where(first_core, mine, theirs)
        high = jnp.where(first_core, theirs, mine)
        pieces = []
        for part in range(3):
            pieces += [low[:, part * hc : (part + 1) * hc], high[:, part * hc : (part + 1) * hc]]
        x6[c] = jnp.concatenate(pieces, axis=1)
        return rows_dot_t(x6[c], wq_ref[...].reshape(D, 6 * hc))

    def scatter(k, carry):
        j = C - 1 - k
        stage[j] = partial(j).astype(BF16)
        remote(stage.at[j], recv.at[j], sc_ss.at[j], sc_rs.at[j], peer(j)).start()
        return carry

    lax.fori_loop(0, C - 1, scatter, 0)
    total = partial(0) + dfirst_ref[...]

    def qkv_grad(c, carry):
        cols = pl.ds(pl.multiple_of(c * 2 * Dn, 128), 2 * Dn)
        res = cols_dot(hid_ref[:, :, cols].reshape(Ph, 2 * Dn), x6[...].reshape(Ph, 6 * hc))
        gq_v[c] = res.astype(BF16).reshape(2, 4, quarter, 6 * hc)
        return carry

    lax.fori_loop(0, C, qkv_grad, 0)
    remote(gq_v.at[:, other], gq_r, gq_ss.at[0], gq_rs.at[0], partner).start()

    sums = st_r[s]
    for d in range(1, n):
        src = flip(s, d, n)
        await_recv(st_r.at[src], st_rs.at[d], (z, src))
    sums = st_r[0]
    for i in range(1, n):
        sums = sums + st_r[i]
    zst[z] = sums
    zst[z, 6:8] = st_v[...]
    zgb[z] = gbup_ref[...]
    for d in range(1, S):
        to = (lax.rem(z + d, S), s)
        remote(zst.at[z], zst.at[z], zs_ss.at[d, 0], zs_rs.at[d, 0], to).start()
        remote(zgb.at[z], zgb.at[z], zs_ss.at[d, 1], zs_rs.at[d, 1], to).start()

    for j in range(1, C):
        await_recv(up_o.at[block_of(j)], ua_rs.at[j], peer(j))
    wide.give_out(0, wide.pieces // 2)
    late.run(0, 6)
    await_recv(gq_r, gq_rs.at[0], partner)
    gq_s[...] = (gq_v[:, core].astype(F32) + gq_r[...].astype(F32)).astype(BF16)
    for j in range(C - 1, 0, -1):
        remote(
            gq_s.at[flip(chip, j, C)], gq_o.at[mine], gx_ss.at[j], gx_rs.at[j], peer(j)
        ).start()
    gq_o[mine] = gq_s[chip]

    for j in range(1, C):
        await_recv(recv.at[j], sc_rs.at[j], peer(j))
        total = total + recv[j].astype(F32)
    ginp = total.astype(BF16)
    ginp_ref[...] = ginp
    dhb[...] = ginp
    keep = pltpu.make_async_copy(dhb, dh_ref.at[z, s], loc.at[0])
    keep.start()

    def broadcast(src, at):
        for j in range(C - 1, 0, -1):
            remote(src, dh_ref.at[at, s], ag_ss.at[at, j], ag_rs.at[at, j], peer(j)).start()
        remote(src, dh_ref.at[at, s], pf_ss.at[at, 0], pf_rs.at[at, 0], partner).start()

    @pl.when(z < S - 1)
    def _():
        remote(dhb, dh_ref.at[z, s], zl_ss.at[z, 0], zl_rs.at[z, 0], (z + 1, s)).start()

    @pl.when(z > 0)
    def _():
        remote(dhb, dh_ref.at[z, s], zl_ss.at[z, 1], zl_rs.at[z, 1], (z - 1, s)).start()

    broadcast(dhb, z)
    late.run(6, late.slots)
    square.run(0, square.slots)
    wide.run(0, 2)
    for d in range(1, S):

        @pl.when(z - d >= 0)
        def _():
            at = z - d
            await_recv(dh_ref.at[at, s], zl_rs.at[at, 0], (z - 1, s))

            @pl.when(z < S - 1)
            def _():
                remote(
                    dh_ref.at[at, s], dh_ref.at[at, s], zl_ss.at[at, 0], zl_rs.at[at, 0], (z + 1, s)
                ).start()

            broadcast(dh_ref.at[at, s], at)

        @pl.when(z + d <= S - 1)
        def _():
            at = z + d
            await_recv(dh_ref.at[at, s], zl_rs.at[at, 1], (z + 1, s))

            @pl.when(z > 0)
            def _():
                remote(
                    dh_ref.at[at, s], dh_ref.at[at, s], zl_ss.at[at, 1], zl_rs.at[at, 1], (z - 1, s)
                ).start()

            broadcast(dh_ref.at[at, s], at)

    def relay(at):
        for j in range(1, C):
            src = 2 * flip(chip, j, C) + core
            await_recv(dh_ref.at[at, src], ag_rs.at[at, j], (z, src))
            remote(
                dh_ref.at[at, src], dh_ref.at[at, src], pf_ss.at[at, j], pf_rs.at[at, j], partner
            ).start()

    wide.give_out(wide.pieces // 2, wide.pieces)
    for j in range(1, C):
        await_recv(gq_o.at[block_of(j)], gx_rs.at[j], peer(j))
    inner.give_out(0, inner.pieces)

    def plane_sum(t, carry):
        at = flip(z, t, S)
        relay(at)

        wide.run(2 + 6 * t, 8 + 6 * t)
        inner.run(6 * (t - 1), 6 * t)

        for j in range(C):
            src = 2 * flip(chip, j, C) + other
            await_recv(dh_ref.at[at, src], pf_rs.at[at, j], partner)

        @pl.when(t == 0)
        def _():
            keep.wait()

        load = pltpu.make_async_copy(dh_ref.at[at], plane, loc.at[1])
        load.start()
        load.wait()

        def rows_tile(r, inner):
            start = pl.multiple_of(r * rt, rt)
            ids = lax.broadcasted_iota(jnp.int32, (rt, L), 0) + (start + s * R)
            hot = jnp.concatenate(
                [jnp.where(ids == pos_ref[at, i], 1.0, 0.0).astype(BF16) for i in range(n)], axis=1
            )
            prod[at, pl.ds(start, rt), :] = rows_dot(hot, plane[...].reshape(n * L, D))
            return inner

        lax.fori_loop(0, R // rt, rows_tile, 0)
        return carry

    lax.fori_loop(0, S, plane_sum, 0)

    def add_tile(r, carry):
        at = pl.ds(pl.multiple_of(r * rt, rt), rt)
        rows = prod[0, at]
        for i in range(1, S):
            rows = rows + prod[i, at]
        gtable_ref[at] = rows.astype(BF16)
        return carry

    lax.fori_loop(0, R // rt, add_tile, 0)

    wide.run(2 + 6 * S, wide.slots)
    inner.run(6 * (S - 1), inner.slots)
    for d in range(1, S):
        src = lax.rem(z + S - d, S)
        await_recv(zst.at[src], zs_rs.at[d, 0], (src, s))
        await_recv(zgb.at[src], zs_rs.at[d, 1], (src, s))
    small, big = zst[0], zgb[0]
    for i in range(1, S):
        small = small + zst[i]
        big = big + zgb[i]
    small_ref[...] = small
    gbo_ref[...] = big

    def settle_plane(at, carry):
        for j in range(C):
            await_send(dhb, pf_ss.at[at, j], partner)
            if j > 0:
                await_send(dhb, ag_ss.at[at, j], peer(j))
        return carry

    lax.fori_loop(0, S, settle_plane, 0)
    for at in range(S):

        @pl.when((z >= at) & (z < S - 1))
        def _():
            await_send(dhb, zl_ss.at[at, 0], (z + 1, s))

        @pl.when((z <= at) & (z > 0))
        def _():
            await_send(dhb, zl_ss.at[at, 1], (z - 1, s))

    for j in range(C):

        @pl.when(z > 0)
        def _():
            await_send(zr.at[0, 0], zk_ss.at[j, 0], (z - 1, s))

        @pl.when(z < S - 1)
        def _():
            await_send(zr.at[0, 0], zk_ss.at[j, 1], (z + 1, s))

        await_send(got3.at[0], x_ss.at[j], partner)
        if j > 0:
            await_send(stage.at[j], sc_ss.at[j], peer(j))
    for d in range(1, n):
        await_send(st_r.at[s], st_ss.at[d], (z, flip(s, d, n)))
    for d in range(1, S):
        to = (lax.rem(z + d, S), s)
        await_send(zst.at[z], zs_ss.at[d, 0], to)
        await_send(zgb.at[z], zs_ss.at[d, 1], to)
    for j in range(1, C):
        await_send(gq_s.at[chip], gx_ss.at[j], peer(j))
        await_send(gupc_ref.at[chip], ua_ss.at[j], peer(j))
    wide.settle()
    square.settle()
    late.settle()
    inner.settle()
    await_send(gq_r, gq_ss.at[0], partner)


def exit_call(S, n, R, dq, dkv, hid_half, wq, dfirst, stats, gbup, pos, gupc, goutc, gdnc):
    C = n // 2
    L, D = dfirst.shape
    hc = D // n
    F1 = gbup.shape[1]
    Dn = D // n
    F2 = gupc.shape[3]
    dims = (S, n, C, L, D, hc, F1, R, 256)
    dma = pltpu.SemaphoreType.DMA
    vm = pl.BlockSpec(memory_space=pltpu.VMEM)
    anyw = pl.BlockSpec(memory_space=pl.ANY)
    sds = jax.ShapeDtypeStruct
    return pl.pallas_call(
        functools.partial(exit_kernel, dims),
        out_shape=(
            sds((L, D), BF16),
            sds((S, n, L, D), BF16),
            sds((4 * C, Dn // 4, 6 * hc), BF16),
            sds((4 * C, Dn // 4, F2), BF16),
            sds((4, Dn // 4, D), BF16),
            sds(gdnc.shape, BF16),
            sds((R, D), BF16),
            sds((8, hc), F32),
            sds((1, F1), F32),
        ),
        in_specs=[vm] * 11,
        out_specs=(vm, anyw) + (vm,) * 7,
        scratch_shapes=[
            pltpu.VMEM((2, C, 2, L, 2 * hc), BF16),
            pltpu.VMEM((C, 2, L, 3 * hc), BF16),
            pltpu.VMEM((C, L, 3 * hc), BF16),
            pltpu.VMEM((C, L, 6 * hc), BF16),
            pltpu.VMEM((C, L, D), BF16),
            pltpu.VMEM((C, L, D), BF16),
            pltpu.VMEM((L, D), BF16),
            pltpu.VMEM((C, 2, 4, Dn // 4, 6 * hc), BF16),
            pltpu.VMEM((C, 4, Dn // 4, 6 * hc), BF16),
            pltpu.VMEM((C, 4, Dn // 4, 6 * hc), BF16),
            pltpu.VMEM((4 * C, Dn // 4, 6 * hc), BF16),
            pltpu.VMEM((4 * C, Dn // 4, 6 * hc), BF16),
            pltpu.VMEM((4 * C, Dn // 4, 6 * hc), BF16),
            pltpu.VMEM((4 * C, Dn // 4, F2), BF16),
            pltpu.VMEM((4 * C, Dn // 4, F2), BF16),
            pltpu.VMEM((4 * C, Dn // 4, F2), BF16),
            pltpu.VMEM((4, Dn // 4, D), BF16),
            pltpu.VMEM((4, Dn // 4, D), BF16),
            pltpu.VMEM((4, Dn // 4, D), BF16),
            pltpu.VMEM(gdnc.shape, BF16),
            pltpu.VMEM(gdnc.shape, BF16),
            pltpu.VMEM(gdnc.shape, BF16),
            pltpu.VMEM((n, L, D), BF16),
            pltpu.VMEM((S, R, D), F32),
            pltpu.VMEM((n, 8, hc), F32),
            pltpu.VMEM((2, hc), F32),
            pltpu.VMEM((S, 8, hc), F32),
            pltpu.VMEM((S, 1, F1), F32),
            dma((C, 2)),
            dma((C, 2)),
            dma((C,)),
            dma((C,)),
            dma((C,)),
            dma((C,)),
            dma((n,)),
            dma((n,)),
            dma((S, 2)),
            dma((S, 2)),
            dma((1,)),
            dma((1,)),
            dma((C,)),
            dma((C,)),
            dma((C,)),
            dma((C,)),
            dma((6, 4 * C)),
            dma((6, 4 * C)),
            dma((6, 4)),
            dma((6, gdnc.shape[0])),
            dma((S, 2)),
            dma((S, 2)),
            dma((S, C)),
            dma((S, C)),
            dma((S, C)),
            dma((S, C)),
            dma((2,)),
        ],
        compiler_params=pltpu.CompilerParams(
            collective_id=2, has_side_effects=True, vmem_limit_bytes=VMEM_LIMIT
        ),
        name="exit_stage",
    )(dq, dkv, hid_half, wq, dfirst, stats, gbup, pos, gupc, goutc, gdnc)


def finish_kernel(
    dims,
    table_ref,
    gq_ref,
    up_ref,
    out_ref,
    early_ref,
    late_ref,
    res_ref,
    inp_ref,
    small_ref,
    gb_ref,
    table_o,
    gq_o,
    up_o,
    out_o,
    dn_o,
    res_o,
    inp_o,
    gb_o,
    *small_o,
):
    C, D, hc = dims
    i = pl.program_id(0)
    h2 = 2 * hc
    F2 = up_ref.shape[3]
    table_o[...] = table_ref[...].astype(F32)
    for c in range(C):
        up_o[:, c * F2 : (c + 1) * F2] = up_ref[c, 0].astype(F32)
        for part in range(3):
            gq_o[:, part * D + c * h2 : part * D + (c + 1) * h2] = gq_ref[
                c, 0, :, part * h2 : (part + 1) * h2
            ].astype(F32)
    out_o[...] = out_ref[0].astype(F32)
    piece = early_ref.shape[0] * early_ref.shape[1]
    dn_o[...] = jnp.where(i < 4, early_ref[...], late_ref[...]).reshape(piece, D).astype(F32)
    res_o[...] = res_ref[...]
    inp_o[...] = inp_ref[...]
    gb_o[...] = gb_ref[...]
    for r, o in enumerate(small_o):
        o[...] = small_ref[r : r + 1]


def finish_call(n, table, gq, up, out, early, late, res, inp, small, gb):
    C = n // 2
    R, D = table.shape
    L = res.shape[0]
    Dn = D // n
    hc = Dn
    q, F2 = up.shape[1:]
    h = q // 2
    piece = early.shape[1]
    F1 = gb.shape[1]
    sds = jax.ShapeDtypeStruct
    steps = 8
    two = lambda rows, cols: pl.BlockSpec((rows, cols), lambda i: (i, 0))
    quad = lambda cols: pl.BlockSpec((C, 1, h, cols), lambda i: (0, i // 2, i % 2, 0))
    fixed = lambda rows, cols: pl.BlockSpec((rows, cols), lambda i: (0, 0))
    return pl.pallas_call(
        functools.partial(finish_kernel, (C, D, hc)),
        grid=(steps,),
        out_shape=(
            sds((R, D), F32),
            sds((Dn, 3 * D), F32),
            sds((Dn, C * F2), F32),
            sds((Dn, D), F32),
            sds((F1, D), F32),
            sds((L, D), BF16),
            sds((L, D), BF16),
            sds((1, F1), F32),
        )
        + (sds((1, hc), F32),) * 8,
        in_specs=[
            two(R // steps, D),
            quad(6 * hc),
            quad(F2),
            pl.BlockSpec((1, h, D), lambda i: (i // 2, i % 2, 0)),
            pl.BlockSpec((2, piece, D), lambda i: (jnp.minimum(i, 3), 0, 0)),
            pl.BlockSpec((2, piece, D), lambda i: (jnp.maximum(i - 4, 0), 0, 0)),
            two(L // steps, D),
            two(L // steps, D),
            fixed(8, hc),
            fixed(1, F1),
        ],
        out_specs=(
            two(R // steps, D),
            two(h, 3 * D),
            two(h, C * F2),
            two(h, D),
            two(2 * piece, D),
            two(L // steps, D),
            two(L // steps, D),
            fixed(1, F1),
        )
        + (fixed(1, hc),) * 8,
        compiler_params=pltpu.CompilerParams(vmem_limit_bytes=VMEM_LIMIT),
        name="finish_stage",
    )(
        table,
        gq.reshape(C, 4, q, 6 * hc),
        up.reshape(C, 4, q, F2),
        out,
        early,
        late,
        res,
        inp,
        small,
        gb,
    )


QUERY_BLOCK = 256
KEY_BLOCK = 256
EARLY_PIECES = 8


def local(
    inputs,
    positions,
    segments,
    pos_table,
    w_qkv,
    b_query,
    b_value,
    w_out,
    b_out,
    ln1_gain,
    ln1_bias,
    w_up,
    b_up,
    w_down,
    b_down,
    ln2_gain,
    ln2_bias,
    cotangent,
):
    S, n = lax.axis_size("seq"), lax.axis_size("shard")
    L, D = inputs.shape
    P_, hc, C = L * n, D // n, n // 2
    R = pos_table.shape[0]
    row = lambda v: v.reshape(1, -1)
    rows = [row(v) for v in (b_out, ln1_gain, ln1_bias, b_down, ln2_gain, ln2_bias, b_query, b_value)]
    q, kv, hid_half, hidden, wq, wup2, wdn_o, wout_o, par_all, bup2, pos_glob, lohi = entry_call(
        S,
        n,
        row(positions),
        inputs,
        pos_table,
        w_qkv,
        w_up,
        w_down,
        w_out,
        segments.reshape(S * n, 1, L),
        row(b_up),
        rows,
    )
    q = q.reshape(P_, hc)
    kv = kv.reshape(3 * P_, 2 * hc)
    att, lse = attend_call(q, kv, lohi, QUERY_BLOCK, KEY_BLOCK)
    result, dfirst, datt, gdn_late, gup, gout, stats, gbup, gdn_early = middle_call(
        S,
        n,
        att.reshape(C, 2, L, hc),
        hidden,
        cotangent,
        par_all,
        w_out,
        wout_o,
        wup2,
        w_down,
        wdn_o,
        bup2,
    )
    dq, dkv = attend_back_call(
        q, kv, lohi, att, datt.reshape(P_, hc), lse, QUERY_BLOCK, KEY_BLOCK
    )
    ginp, dh, gqkv, gup, gout, gdn_late, gtable, small, gbo = exit_call(
        S,
        n,
        R,
        dq.reshape(C, 2, L, hc),
        dkv.reshape(3, C, 2, L, 2 * hc),
        hid_half,
        wq,
        dfirst,
        stats,
        gbup,
        pos_glob,
        gup.reshape(C, 4, D // n // 4, gup.shape[2]),
        gout,
        gdn_late,
    )
    gtable, gqkv, gup, gout, gdn, result, ginp, gbo, *small = finish_call(
        n, gtable, gqkv, gup, gout, gdn_early, gdn_late, result, ginp, small, gbo
    )
    small = [v[0] for v in small]
    return (
        result,
        ginp,
        gtable,
        gqkv,
        small[6],
        small[7],
        gout,
        small[5],
        small[3],
        small[4],
        gup,
        gbo[0],
        gdn,
        small[2],
        small[0],
        small[1],
    )


def solution(mesh):
    in_specs = (
        P(("seq", "shard"), None),
        P(("seq", "shard")),
        P(),
        P("shard", None),
        P("shard", None),
        P("shard"),
        P("shard"),
        P("shard", None),
        P("shard"),
        P("shard"),
        P("shard"),
        P("shard", None),
        P("shard"),
        P("shard", None),
        P("shard"),
        P("shard"),
        P("shard"),
        P(("seq", "shard"), None),
    )
    out_specs = (
        P(("seq", "shard"), None),
        P(("seq", "shard"), None),
        P("shard", None),
        P("shard", None),
        P("shard"),
        P("shard"),
        P("shard", None),
        P("shard"),
        P("shard"),
        P("shard"),
        P("shard", None),
        P("shard"),
        P("shard", None),
        P("shard"),
        P("shard"),
        P("shard"),
    )
    return jax.shard_map(local, mesh=mesh, in_specs=in_specs, out_specs=out_specs, check_vma=False)
```

```python
import functools
import math

import jax
import jax.numpy as jnp
from jax import lax
from jax.experimental import pallas as pl
from jax.experimental.pallas import tpu as pltpu
from jax.sharding import PartitionSpec as P

HEADS = 16
HEAD_DIM = 64
score_scale = 0.125
neg_large = -1e30
epsilon = 1e-06
root_half = 0.7071067811865476
inv_root_two_pi = 0.3989422804014327
MESH = pl.DeviceIdType.MESH
F32 = jnp.float32
BF16 = jnp.bfloat16
MIB = 1024 * 1024
ENTRY_VMEM, ATTEND_VMEM, MIDDLE_VMEM, BACK_VMEM, EXIT_VMEM = 24, 16, 44, 20, 48


def flip(value, mask, width):
    total, bit = 0, 1
    while bit < width:
        a = lax.rem(value // bit, 2)
        b = (mask // bit) % 2 if isinstance(mask, int) else lax.rem(mask // bit, 2)
        total = total + lax.rem(a + b, 2) * bit
        bit *= 2
    return total


def remote(src, dst, send_sem, recv_sem, device):
    return pltpu.make_async_remote_copy(
        src_ref=src,
        dst_ref=dst,
        send_sem=send_sem,
        recv_sem=recv_sem,
        device_id=device,
        device_id_type=MESH,
    )


def await_recv(dst, sem, device):
    remote(dst, dst, sem, sem, device).wait_recv()


def await_send(src, sem, device):
    remote(src, src, sem, sem, device).wait_send()


class Chain:
    def __init__(self, S, z, s, own, land, cross, fin, sems, lag=3):
        self.S, self.s, self.lag, self.sems = S, s, lag, sems
        self.own, self.land, self.cross, self.fin = own, land, cross, fin
        low = 1 - (2 * z) // S
        self.depth = low * z + (1 - low) * (S - 1 - z)
        self.inward = (z + 2 * low - 1, s)
        self.outward = (z + 1 - 2 * low, s)
        self.mid = S // 2 - 1
        self.pieces = own.shape[0]
        self.slots = self.pieces + lag * self.mid + lag * max(self.mid - 1, 0)

    def give_out(self, start, stop):
        @pl.when(self.depth == 0)
        def _():
            def step(p, carry):
                remote(
                    self.own.at[p], self.land.at[p], self.sems.at[0, p], self.sems.at[1, p], self.inward
                ).start()
                return carry

            lax.fori_loop(start, stop, step, 0)

    def slot(self, k):
        p = k - self.lag * (self.depth - 1)

        @pl.when((self.depth > 0) & (p >= 0) & (p < self.pieces))
        def _():
            await_recv(self.land.at[p], self.sems.at[1, p], self.outward)
            both = self.own[p].astype(F32) + self.land[p].astype(F32)
            self.own[p] = both.astype(BF16)

            @pl.when(self.depth < self.mid)
            def _():
                remote(
                    self.own.at[p], self.land.at[p], self.sems.at[0, p], self.sems.at[1, p], self.inward
                ).start()

            @pl.when(self.depth == self.mid)
            def _():
                remote(
                    self.own.at[p], self.cross.at[p], self.sems.at[2, p], self.sems.at[3, p], self.inward
                ).start()

        x = k - self.lag * self.mid

        @pl.when((self.depth == self.mid) & (x >= 0) & (x < self.pieces))
        def _():
            await_recv(self.cross.at[x], self.sems.at[3, x], self.inward)
            both = self.own[x].astype(F32) + self.cross[x].astype(F32)
            self.fin[x] = both.astype(BF16)
            remote(
                self.fin.at[x], self.fin.at[x], self.sems.at[4, x], self.sems.at[5, x], self.outward
            ).start()

        b = k - self.lag * self.mid - self.lag * (self.mid - self.depth)

        @pl.when((self.depth < self.mid) & (self.depth > 0) & (b >= 0) & (b < self.pieces))
        def _():
            await_recv(self.fin.at[b], self.sems.at[5, b], self.inward)
            remote(
                self.fin.at[b], self.fin.at[b], self.sems.at[4, b], self.sems.at[5, b], self.outward
            ).start()

    def run(self, start, stop):
        def step(k, carry):
            self.slot(k)
            return carry

        lax.fori_loop(start, stop, step, 0)

    def settle(self):
        def step(p, carry):
            @pl.when(self.depth == 0)
            def _():
                await_recv(self.fin.at[p], self.sems.at[5, p], self.inward)

            @pl.when(self.depth < self.mid)
            def _():
                await_send(self.own.at[p], self.sems.at[0, p], self.inward)

            @pl.when(self.depth == self.mid)
            def _():
                await_send(self.own.at[p], self.sems.at[2, p], self.inward)

            @pl.when(self.depth > 0)
            def _():
                await_send(self.fin.at[p], self.sems.at[4, p], self.outward)

            return carry

        lax.fori_loop(0, self.pieces, step, 0)


def rows_dot(a, b):
    return lax.dot_general(a, b, (((1,), (0,)), ((), ())), preferred_element_type=F32)


def rows_dot_t(a, b):
    return lax.dot_general(a, b, (((1,), (1,)), ((), ())), preferred_element_type=F32)


def cols_dot(a, b):
    return lax.dot_general(a, b, (((0,), (0,)), ((), ())), preferred_element_type=F32)


def entry_kernel(
    dims,
    pos_hbm,
    inp_hbm,
    table_ref,
    wqkv_ref,
    wup_ref,
    wdn_ref,
    wout_ref,
    seg_hbm,
    bup_in_hbm,
    row0_ref,
    row1_ref,
    row2_ref,
    row3_ref,
    row4_ref,
    row5_ref,
    row6_ref,
    row7_ref,
    q_ref,
    kv_ref,
    hid_half_ref,
    hidden_ref,
    wq_ref,
    wup2_ref,
    wdn_o_ref,
    wout_o_ref,
    par_all_ref,
    bup2_ref,
    pos_glob_ref,
    lohi_ref,
    pos_ref,
    inp_ref,
    seg_ref,
    bup_in_ref,
    rows_ref,
    table_v,
    pstage,
    precv,
    cstage,
    crecv,
    qst,
    kvst,
    wup_own,
    par_ref,
    bup_ref,
    pos_ss,
    pos_rs,
    par_ss,
    par_rs,
    posz_ss,
    posz_rs,
    wq_ss,
    wq_rs,
    wqf_ss,
    wqf_rs,
    wup_ss,
    wup_rs,
    wupf_ss,
    wupf_rs,
    misc_ss,
    misc_rs,
    rsp_ss,
    rsp_rs,
    rsc_ss,
    rsc_rs,
    ag_ss,
    ag_rs,
    qx_ss,
    qx_rs,
    zx_ss,
    zx_rs,
    loc,
):
    S, n, C, L, D, hc, R, F2 = dims
    z = lax.axis_index("seq")
    s = lax.axis_index("shard")
    core = lax.rem(s, 2)
    chip = s // 2
    other = 1 - core
    partner = 2 * chip + other
    h2 = 2 * hc
    Dn = D // n

    rows = (row0_ref, row1_ref, row2_ref, row3_ref, row4_ref, row5_ref, row6_ref, row7_ref)
    smalls = [
        pltpu.make_async_copy(pos_hbm, pos_ref, loc.at[6]),
        pltpu.make_async_copy(seg_hbm, seg_ref, loc.at[7]),
        pltpu.make_async_copy(bup_in_hbm, bup_in_ref, loc.at[8]),
    ] + [
        pltpu.make_async_copy(row, rows_ref.at[i], loc.at[9 + i]) for i, row in enumerate(rows)
    ]
    for small in smalls:
        small.start()
    inp_copy = pltpu.make_async_copy(inp_hbm, inp_ref, loc.at[17])
    inp_copy.start()
    table_copy = pltpu.make_async_copy(table_ref, table_v, loc.at[0])
    table_copy.start()
    own_wq = []
    for part in range(3):
        own_wq.append(
            pltpu.make_async_copy(
                wqkv_ref.at[:, pl.ds(pl.multiple_of(part * D + chip * h2, 128), h2)],
                wq_ref.at[s, :, part * h2 : (part + 1) * h2],
                loc.at[1 + part],
            )
        )
        own_wq[-1].start()
    own_wup_in = pltpu.make_async_copy(
        wup_ref.at[:, pl.ds(pl.multiple_of(chip * F2, 128), F2)], wup_own, loc.at[4]
    )
    own_wup_in.start()

    for small in smalls:
        small.wait()
    for i in range(8):
        par_ref[i : i + 1] = rows_ref[i].astype(F32)
    bup_ref[...] = bup_in_ref[...].astype(F32)
    F1 = F2 // 2
    bup_mine = pl.ds(pl.multiple_of(core * F1, 128), F1)
    bup_theirs = pl.ds(pl.multiple_of(other * F1, 128), F1)
    bup2_ref[:, bup_mine] = bup_ref[...]

    barrier = pltpu.get_barrier_semaphore()
    for d in range(1, n):
        pl.semaphore_signal(barrier, inc=1, device_id=(z, flip(s, d, n)), device_id_type=MESH)
    for d in range(1, S):
        pl.semaphore_signal(barrier, inc=1, device_id=(lax.rem(z + d, S), s), device_id_type=MESH)

    for d in (1, S - 1):
        pl.semaphore_signal(
            barrier, inc=1, device_id=(lax.rem(z + d, S), partner), device_id_type=MESH
        )
    pl.semaphore_wait(barrier, n - 1 + S - 1 + 2)

    pos_glob_ref[z, s] = pos_ref[...]
    par_all_ref[s] = par_ref[...]
    for d in range(1, n):
        peer = (z, flip(s, d, n))
        remote(pos_ref, pos_glob_ref.at[z, s], pos_ss.at[d], pos_rs.at[d], peer).start()
        remote(par_ref, par_all_ref.at[s], par_ss.at[d], par_rs.at[d], peer).start()

    for own in own_wq:
        own.wait()

    def wq_src(peer_chip, part):
        return wqkv_ref.at[:, pl.ds(pl.multiple_of(part * D + peer_chip * h2, 128), h2)]

    for j in range(C - 1, 0, -1):
        pc = flip(chip, j, C)
        for part in range(3):
            remote(
                wq_src(pc, part),
                wq_ref.at[s, :, part * h2 : (part + 1) * h2],
                wq_ss.at[j, part],
                wq_rs.at[j, part],
                (z, 2 * pc + core),
            ).start()
    remote(wq_ref.at[s], wq_ref.at[s], wqf_ss.at[0], wqf_rs.at[0], (z, partner)).start()

    own_segs = jnp.concatenate([seg_ref[z * n + i] for i in range(n)], axis=1)

    def count(g, carry):
        low, high = carry
        keys = jnp.broadcast_to(seg_ref[g], (L, L)).T
        lows, highs = [], []
        for i in range(n):
            mine = own_segs[:, i * L : (i + 1) * L]
            lows.append(jnp.sum(jnp.where(keys < mine, 1.0, 0.0), axis=0, keepdims=True))
            highs.append(jnp.sum(jnp.where(keys <= mine, 1.0, 0.0), axis=0, keepdims=True))
        return low + jnp.concatenate(lows, axis=1), high + jnp.concatenate(highs, axis=1)

    none = jnp.zeros((1, n * L), F32)
    low, high = lax.fori_loop(0, S * n, count, (none, none))
    origin = ((z - 1) * n * L).astype(F32)
    lohi_ref[0:1] = low - origin
    lohi_ref[1:2] = high - origin

    for d in range(1, n):
        src = flip(s, d, n)
        await_recv(pos_glob_ref.at[z, src], pos_rs.at[d], (z, src))
    for d in range(1, S):
        remote(
            pos_glob_ref.at[z],
            pos_glob_ref.at[z],
            posz_ss.at[d],
            posz_rs.at[d],
            (lax.rem(z + d, S), s),
        ).start()

    table_copy.wait()
    inp_copy.wait()
    lane_ids = lax.broadcasted_iota(jnp.int32, (L, R), 1) + s * R

    def picked(block):
        ids = jnp.broadcast_to(pos_glob_ref[z, block], (L, L)).T
        ids = jnp.concatenate([ids] * (R // L), axis=1)
        hot = jnp.where(ids == lane_ids, 1.0, 0.0).astype(BF16)
        return rows_dot(hot, table_v[...])

    def send_partner(j):
        pstage[j] = picked(2 * flip(chip, j, C) + other).astype(BF16)
        remote(pstage.at[j], precv.at[j], rsp_ss.at[j], rsp_rs.at[j], (z, partner)).start()

    def combined(j):
        mine = picked(2 * flip(chip, j, C) + core)
        await_recv(precv.at[j], rsp_rs.at[j], (z, partner))
        return mine + precv[j].astype(F32)

    send_partner(C - 1)

    def scatter_step(k, carry):
        j = C - 1 - k
        send_partner(j - 1)
        cstage[j] = combined(j).astype(BF16)
        remote(
            cstage.at[j], crecv.at[j], rsc_ss.at[j], rsc_rs.at[j], (z, 2 * flip(chip, j, C) + core)
        ).start()
        return carry

    lax.fori_loop(0, C - 1, scatter_step, 0)
    hidden = combined(0) + inp_ref[...].astype(F32)

    for j in range(1, C):
        src = 2 * flip(chip, j, C) + core
        for part in range(3):
            await_recv(
                wq_ref.at[src, :, part * h2 : (part + 1) * h2], wq_rs.at[j, part], (z, src)
            )
        remote(wq_ref.at[src], wq_ref.at[src], wqf_ss.at[j], wqf_rs.at[j], (z, partner)).start()

    for j in range(1, C):
        await_recv(crecv.at[j], rsc_rs.at[j], (z, 2 * flip(chip, j, C) + core))
        hidden = hidden + crecv[j].astype(F32)
    hidden_ref[...] = hidden
    hid_half_ref[chip] = hidden.astype(BF16)
    for j in range(C - 1, 0, -1):
        remote(
            hid_half_ref.at[chip],
            hid_half_ref.at[chip],
            ag_ss.at[j],
            ag_rs.at[j],
            (z, 2 * flip(chip, j, C) + core),
        ).start()

    own_wup_in.wait()
    own_wup_out = pltpu.make_async_copy(wup_own, wup2_ref.at[s], loc.at[5])
    own_wup_out.start()
    for j in range(C - 1, 0, -1):
        pc = flip(chip, j, C)
        remote(
            wup_ref.at[:, pl.ds(pl.multiple_of(pc * F2, 128), F2)],
            wup2_ref.at[s],
            wup_ss.at[j],
            wup_rs.at[j],
            (z, 2 * pc + core),
        ).start()
    remote(wup_own, wup2_ref.at[s], wupf_ss.at[0], wupf_rs.at[0], (z, partner)).start()
    remote(wdn_ref, wdn_o_ref, misc_ss.at[0], misc_rs.at[0], (z, partner)).start()
    remote(wout_ref, wout_o_ref, misc_ss.at[1], misc_rs.at[1], (z, partner)).start()
    remote(bup_ref, bup2_ref.at[:, bup_mine], misc_ss.at[2], misc_rs.at[2], (z, partner)).start()

    for j in range(C):
        src = 2 * flip(chip, j, C) + other
        await_recv(wq_ref.at[src], wqf_rs.at[j], (z, partner))
    for d in range(1, n):
        src = flip(s, d, n)
        await_recv(par_all_ref.at[src], par_rs.at[d], (z, src))
    bias = jnp.concatenate([par_all_ref[2 * chip], par_all_ref[2 * chip + 1]], axis=1)
    bias_q, bias_v = bias[6:7], bias[7:8]
    first_core = core == 0

    def project(j, carry):
        c = flip(chip, j, C)

        @pl.when(j > 0)
        def _():
            await_recv(hid_half_ref.at[c], ag_rs.at[j], (z, 2 * c + core))

        res = rows_dot(hid_half_ref[c], wq_ref[...].reshape(D, 3 * h2))
        query = (res[:, :h2] + bias_q).astype(BF16) * score_scale
        key = res[:, h2 : 2 * h2].astype(BF16)
        value = (res[:, 2 * h2 :] + bias_v).astype(BF16)
        q_ref[c, core] = jnp.where(first_core, query[:, :hc], query[:, hc:])
        kv_ref[1, c, core, :, :hc] = jnp.where(first_core, key[:, :hc], key[:, hc:])
        kv_ref[1, c, core, :, hc:] = jnp.where(first_core, value[:, :hc], value[:, hc:])
        qst[j] = jnp.where(first_core, query[:, hc:], query[:, :hc])
        kvst[j, :, :hc] = jnp.where(first_core, key[:, hc:], key[:, :hc])
        kvst[j, :, hc:] = jnp.where(first_core, value[:, hc:], value[:, :hc])
        own_kv = kv_ref.at[1, c, core]

        @pl.when(z < S - 1)
        def _():
            remote(
                own_kv, kv_ref.at[0, c, core], zx_ss.at[j, 0], zx_rs.at[j, 0], (z + 1, s)
            ).start()
            remote(
                kvst.at[j], kv_ref.at[0, c, core], zx_ss.at[j, 1], zx_rs.at[j, 1], (z + 1, partner)
            ).start()

        @pl.when(z > 0)
        def _():
            remote(
                own_kv, kv_ref.at[2, c, core], zx_ss.at[j, 2], zx_rs.at[j, 2], (z - 1, s)
            ).start()
            remote(
                kvst.at[j], kv_ref.at[2, c, core], zx_ss.at[j, 3], zx_rs.at[j, 3], (z - 1, partner)
            ).start()

        remote(qst.at[j], q_ref.at[c, core], qx_ss.at[j, 0], qx_rs.at[j, 0], (z, partner)).start()
        remote(
            kvst.at[j], kv_ref.at[1, c, core], qx_ss.at[j, 1], qx_rs.at[j, 1], (z, partner)
        ).start()
        return carry

    lax.fori_loop(0, C, project, 0)

    for j in range(1, C):
        src = 2 * flip(chip, j, C) + core
        await_recv(wup2_ref.at[src], wup_rs.at[j], (z, src))
        remote(
            wup2_ref.at[src], wup2_ref.at[src], wupf_ss.at[j], wupf_rs.at[j], (z, partner)
        ).start()

    def settle(j, carry):
        c = flip(chip, j, C)
        await_recv(q_ref.at[c, other], qx_rs.at[j, 0], (z, partner))
        await_recv(kv_ref.at[1, c, other], qx_rs.at[j, 1], (z, partner))
        await_send(qst.at[j], qx_ss.at[j, 0], (z, partner))
        await_send(kvst.at[j], qx_ss.at[j, 1], (z, partner))

        @pl.when(z > 0)
        def _():
            await_recv(kv_ref.at[0, c, core], zx_rs.at[j, 0], (z - 1, s))
            await_recv(kv_ref.at[0, c, other], zx_rs.at[j, 1], (z - 1, partner))
            await_send(kvst.at[j], zx_ss.at[j, 2], (z - 1, s))
            await_send(kvst.at[j], zx_ss.at[j, 3], (z - 1, partner))

        @pl.when(z < S - 1)
        def _():
            await_recv(kv_ref.at[2, c, core], zx_rs.at[j, 2], (z + 1, s))
            await_recv(kv_ref.at[2, c, other], zx_rs.at[j, 3], (z + 1, partner))
            await_send(kvst.at[j], zx_ss.at[j, 0], (z + 1, s))
            await_send(kvst.at[j], zx_ss.at[j, 1], (z + 1, partner))

        await_send(pstage.at[j], rsp_ss.at[j], (z, partner))
        await_send(wq_ref.at[s], wqf_ss.at[j], (z, partner))
        await_recv(wup2_ref.at[2 * c + other], wupf_rs.at[j], (z, partner))
        await_send(wup2_ref.at[s], wupf_ss.at[j], (z, partner))
        return carry

    lax.fori_loop(0, C, settle, 0)
    for j in range(1, C):
        peer = (z, 2 * flip(chip, j, C) + core)
        await_send(cstage.at[j], rsc_ss.at[j], peer)
        await_send(hid_half_ref.at[chip], ag_ss.at[j], peer)
        await_send(wup_own, wup_ss.at[j], peer)
        for part in range(3):
            await_send(
                wq_ref.at[s, :, part * h2 : (part + 1) * h2], wq_ss.at[j, part], peer
            )
    for d in range(1, n):
        peer = (z, flip(s, d, n))
        await_send(pos_ref, pos_ss.at[d], peer)
        await_send(par_ref, par_ss.at[d], peer)
    for d in range(1, S):
        src = lax.rem(z + S - d, S)
        await_recv(pos_glob_ref.at[src], posz_rs.at[d], (src, s))
        await_send(pos_glob_ref.at[z], posz_ss.at[d], (lax.rem(z + d, S), s))
    for i, (mine, got) in enumerate(
        ((wdn_ref, wdn_o_ref), (wout_ref, wout_o_ref), (bup_ref, bup2_ref.at[:, bup_theirs]))
    ):
        await_recv(got, misc_rs.at[i], (z, partner))
        await_send(mine, misc_ss.at[i], (z, partner))
    own_wup_out.wait()


def entry_call(S, n, pos, inp, table, wqkv, wup, wdn, wout, seg, bup, rows):
    C = n // 2
    L, D = inp.shape
    hc = D // n
    R = table.shape[0]
    F = wup.shape[1]
    F1, F2 = F // n, 2 * F // n
    dims = (S, n, C, L, D, hc, R, F2)
    dma = pltpu.SemaphoreType.DMA
    vm = pl.BlockSpec(memory_space=pltpu.VMEM)
    anyw = pl.BlockSpec(memory_space=pl.ANY)
    hbm = pl.BlockSpec(memory_space=pltpu.HBM)
    sds = jax.ShapeDtypeStruct
    return pl.pallas_call(
        functools.partial(entry_kernel, dims),
        out_shape=(
            sds((C, 2, L, hc), BF16),
            sds((3, C, 2, L, 2 * hc), BF16),
            sds((C, L, D), BF16),
            sds((L, D), F32),
            sds((n, D // n, 6 * hc), BF16),
            sds((n, D // n, F2), BF16),
            sds((F1, D), BF16),
            sds((D // n, D), BF16),
            sds((n, 8, hc), F32),
            sds((1, F2), F32),
            sds((S, n, 1, L), jnp.int32),
            sds((2, n * L), F32),
        ),
        in_specs=[hbm] * 17,
        out_specs=(vm, vm, vm, vm, vm, anyw, anyw, anyw, vm, vm, vm, vm),
        scratch_shapes=[
            pltpu.VMEM((1, L), jnp.int32),
            pltpu.VMEM((L, D), BF16),
            pltpu.VMEM((S * n, 1, L), jnp.int32),
            pltpu.VMEM((1, F1), BF16),
            pltpu.VMEM((8, 1, hc), BF16),
            pltpu.VMEM((R, D), BF16),
            pltpu.VMEM((C, L, D), BF16),
            pltpu.VMEM((C, L, D), BF16),
            pltpu.VMEM((C, L, D), BF16),
            pltpu.VMEM((C, L, D), BF16),
            pltpu.VMEM((C, L, hc), BF16),
            pltpu.VMEM((C, L, 2 * hc), BF16),
            pltpu.VMEM((D // n, F2), BF16),
            pltpu.VMEM((8, hc), F32),
            pltpu.VMEM((1, F1), F32),
            dma((n,)),
            dma((n,)),
            dma((n,)),
            dma((n,)),
            dma((S,)),
            dma((S,)),
            dma((C, 3)),
            dma((C, 3)),
            dma((C,)),
            dma((C,)),
            dma((C,)),
            dma((C,)),
            dma((C,)),
            dma((C,)),
            dma((3,)),
            dma((3,)),
            dma((C,)),
            dma((C,)),
            dma((C,)),
            dma((C,)),
            dma((C,)),
            dma((C,)),
            dma((C, 2)),
            dma((C, 2)),
            dma((C, 4)),
            dma((C, 4)),
            dma((18,)),
        ],
        compiler_params=pltpu.CompilerParams(
            collective_id=0, has_side_effects=True, vmem_limit_bytes=ENTRY_VMEM * MIB
        ),
        name="entry_stage",
    )(*[
        pltpu.with_memory_space_constraint(v, pltpu.HBM)
        for v in (pos, inp, table, wqkv, wup, wdn, wout, seg, bup, *rows)
    ])


def key_blocks(lohi_ref, rows, bk):
    first = jnp.min(lohi_ref[0:1, rows]).astype(jnp.int32)
    last = jnp.max(lohi_ref[1:2, rows]).astype(jnp.int32)
    return first // bk, (last + bk - 1) // bk


def attend_kernel(dims, q_ref, kv_ref, lohi_ref, att_ref, lse_ref, vt_ref):
    P_, hc, hh, bq, bk = dims
    lanes = lax.broadcasted_iota(jnp.int32, (bq, hc), 1) // HEAD_DIM
    nq = P_ // bq

    def flip_value(kb, carry):
        at = pl.multiple_of(kb * bk, bk)
        vt_ref[kb] = kv_ref[pl.ds(at, bk), hc:].T
        return carry

    first, last = key_blocks(lohi_ref, pl.ds(0, P_), bk)
    lax.fori_loop(first, last, flip_value, 0)

    def one_query_block(qi, carry):
        rows = pl.ds(pl.multiple_of(qi * bq, bq), bq)
        query = q_ref[rows, :]
        heads_q = [jnp.where(lanes == h, query, jnp.zeros_like(query)) for h in range(hh)]
        low = lohi_ref[0:1, rows].astype(jnp.int32)
        high = lohi_ref[1:2, rows].astype(jnp.int32)
        first, last = key_blocks(lohi_ref, rows, bk)

        def one_key_block(kb, state):
            at = pl.multiple_of(kb * bk, bk)
            keys = kv_ref[pl.ds(at, bk), :hc]
            ids = lax.broadcasted_iota(jnp.int32, (bk, bq), 0) + kb * bk
            keep = (ids >= low) & (ids < high)
            fresh = []
            for h in range(hh):
                top, total, acc = state[h]
                scores = jnp.where(keep, rows_dot_t(keys, heads_q[h]), neg_large)
                new_top = jnp.maximum(top, jnp.max(scores, axis=0, keepdims=True))
                weights = jnp.exp(scores - new_top)
                shrink = jnp.exp(top - new_top)
                total = total * shrink + jnp.sum(weights, axis=0, keepdims=True)
                values = vt_ref[kb, h * HEAD_DIM : (h + 1) * HEAD_DIM, :]
                acc = acc * shrink + rows_dot(values, weights.astype(BF16))
                fresh.append((new_top, total, acc))
            return tuple(fresh)

        start = tuple(
            (
                jnp.full((1, bq), neg_large, F32),
                jnp.zeros((1, bq), F32),
                jnp.zeros((HEAD_DIM, bq), F32),
            )
            for _ in range(hh)
        )
        state = lax.fori_loop(first, last, one_key_block, start)
        mixed = jnp.concatenate([acc / total for _, total, acc in state], axis=0)
        att_ref[rows, :] = mixed.T.astype(BF16)
        for h in range(hh):
            lse_ref[h : h + 1, rows] = state[h][0] + jnp.log(state[h][1])
        return carry

    lax.fori_loop(0, nq, one_query_block, 0)


def attend_call(q, kv, lohi, bq, bk):
    P_, hc = q.shape
    hh = hc // HEAD_DIM
    vm = pl.BlockSpec(memory_space=pltpu.VMEM)
    return pl.pallas_call(
        functools.partial(attend_kernel, (P_, hc, hh, bq, bk)),
        out_shape=(
            jax.ShapeDtypeStruct((P_, hc), BF16),
            jax.ShapeDtypeStruct((hh, P_), F32),
        ),
        in_specs=[vm, vm, vm],
        out_specs=(vm, vm),
        scratch_shapes=[pltpu.VMEM((3 * P_ // bk, hc, bk), BF16)],
        compiler_params=pltpu.CompilerParams(vmem_limit_bytes=ATTEND_VMEM * MIB),
        name="attend_stage",
    )(q, kv, lohi)


def attend_back_kernel(
    dims, q_ref, kv_ref, lohi_ref, att_ref, datt_ref, lse_ref, dq_ref, dkv_ref, kt_ref, acc_ref
):
    P_, hc, hh, bq, bk = dims
    lanes = lax.broadcasted_iota(jnp.int32, (bq, hc), 1) // HEAD_DIM
    nq = P_ // bq
    acc_ref[...] = jnp.zeros_like(acc_ref)

    def flip_key(kb, carry):
        at = pl.multiple_of(kb * bk, bk)
        kt_ref[kb] = kv_ref[pl.ds(at, bk), :hc].T
        return carry

    first, last = key_blocks(lohi_ref, pl.ds(0, P_), bk)
    lax.fori_loop(first, last, flip_key, 0)

    def one_query_block(qi, carry):
        rows = pl.ds(pl.multiple_of(qi * bq, bq), bq)
        query, grad = q_ref[rows, :], datt_ref[rows, :]
        zero = jnp.zeros_like(query)
        heads_q = [jnp.where(lanes == h, query, zero) for h in range(hh)]
        heads_g = [jnp.where(lanes == h, grad, zero) for h in range(hh)]
        stack_q = jnp.concatenate(heads_q, axis=0)
        stack_g = jnp.concatenate(heads_g, axis=0)
        product = (grad.astype(F32) * att_ref[rows, :].astype(F32)).T
        delta = [
            jnp.sum(product[h * HEAD_DIM : (h + 1) * HEAD_DIM], axis=0, keepdims=True)
            for h in range(hh)
        ]
        logs = [lse_ref[h : h + 1, rows] for h in range(hh)]
        low = lohi_ref[0:1, rows].astype(jnp.int32)
        high = lohi_ref[1:2, rows].astype(jnp.int32)
        first, last = key_blocks(lohi_ref, rows, bk)

        def one_key_block(kb, state):
            at = pl.multiple_of(kb * bk, bk)
            keys = kv_ref[pl.ds(at, bk), :hc]
            values = kv_ref[pl.ds(at, bk), hc:]
            ids = lax.broadcasted_iota(jnp.int32, (bk, bq), 0) + kb * bk
            keep = (ids >= low) & (ids < high)
            fresh, all_p, all_s = [], [], []
            for h in range(hh):
                scores = rows_dot_t(keys, heads_q[h])
                probs = jnp.where(keep, jnp.exp(scores - logs[h]), 0.0)
                grad_probs = rows_dot_t(values, heads_g[h])
                grad_scores = (probs * (grad_probs - delta[h])).astype(BF16)
                all_p.append(probs.astype(BF16))
                all_s.append(grad_scores)
                key_cols = kt_ref[kb, h * HEAD_DIM : (h + 1) * HEAD_DIM, :]
                fresh.append(state[h] + rows_dot(key_cols, grad_scores))
            acc_ref[pl.ds(at, bk), :hc] += rows_dot(jnp.concatenate(all_s, axis=1), stack_q)
            acc_ref[pl.ds(at, bk), hc:] += rows_dot(jnp.concatenate(all_p, axis=1), stack_g)
            return tuple(fresh)

        start = tuple(jnp.zeros((HEAD_DIM, bq), F32) for _ in range(hh))
        state = lax.fori_loop(first, last, one_key_block, start)
        dq_ref[rows, :] = (jnp.concatenate(state, axis=0).T * score_scale).astype(BF16)
        return carry

    lax.fori_loop(0, nq, one_query_block, 0)
    dkv_ref[...] = acc_ref[...].astype(BF16)


def attend_back_call(q, kv, lohi, att, datt, lse, bq, bk):
    P_, hc = q.shape
    hh = hc // HEAD_DIM
    vm = pl.BlockSpec(memory_space=pltpu.VMEM)
    return pl.pallas_call(
        functools.partial(attend_back_kernel, (P_, hc, hh, bq, bk)),
        out_shape=(
            jax.ShapeDtypeStruct((P_, hc), BF16),
            jax.ShapeDtypeStruct((3 * P_, 2 * hc), BF16),
        ),
        in_specs=[vm, vm, vm, vm, vm, vm],
        out_specs=(vm, vm),
        scratch_shapes=[
            pltpu.VMEM((3 * P_ // bk, hc, bk), BF16),
            pltpu.VMEM((3 * P_, 2 * hc), F32),
        ],
        compiler_params=pltpu.CompilerParams(vmem_limit_bytes=BACK_VMEM * MIB),
        name="attend_back_stage",
    )(q, kv, lohi, att, datt, lse)


def layer_stats(summed):
    center = summed - jnp.mean(summed, axis=1, keepdims=True)
    inverse = lax.rsqrt(jnp.mean(center * center, axis=1, keepdims=True) + epsilon)
    return center * inverse, inverse


def layer_back(grad, normed, inverse):
    first = jnp.mean(grad, axis=1, keepdims=True)
    second = jnp.mean(grad * normed, axis=1, keepdims=True)
    return inverse * (grad - first - normed * second)


def col_sum(x):
    return jnp.sum(x, axis=0, keepdims=True)


def middle_kernel(
    dims,
    att_ref,
    hidden_ref,
    cot_ref,
    par_ref,
    wout_ref,
    wout_o_ref,
    wup_ref,
    wdn_ref,
    wdn_o_ref,
    bup_ref,
    result_ref,
    dfirst_ref,
    datt_ref,
    gdn_ref,
    gup_ref,
    gout_ref,
    stats_ref,
    gbup_ref,
    gdn_done_ref,
    wout_v,
    wup_v,
    wdn_v,
    attp,
    fa,
    da,
    dfa,
    act,
    slope,
    dup,
    stage,
    recv,
    normed_v,
    first_v,
    dnorm_v,
    gdn_v,
    gdn_r,
    gdn_h,
    gdn_l,
    gdn_x,
    gdn_f,
    gup_v,
    gup_r,
    gout_v,
    gout_r,
    gb_v,
    gb_r,
    dattst,
    ap_ss,
    ap_rs,
    sc_ss,
    sc_rs,
    ag_ss,
    ag_rs,
    gx_ss,
    gx_rs,
    dx_ss,
    dx_rs,
    zsem,
    loc,
):
    S, n, C, L, D, hc, F1 = dims
    Dn, F2, Ph = D // n, 2 * F1, C * L
    z = lax.axis_index("seq")
    s = lax.axis_index("shard")
    core = lax.rem(s, 2)
    chip = s // 2
    other = 1 - core
    partner = (z, 2 * chip + other)

    loads = [
        pltpu.make_async_copy(wout_ref, wout_v.at[core], loc.at[0]),
        pltpu.make_async_copy(wout_o_ref, wout_v.at[other], loc.at[1]),
        pltpu.make_async_copy(wup_ref, wup_v, loc.at[2]),
        pltpu.make_async_copy(wdn_ref, wdn_v.at[core], loc.at[3]),
        pltpu.make_async_copy(wdn_o_ref, wdn_v.at[other], loc.at[4]),
    ]
    for load in loads:
        load.start()

    def peer(j):
        return (z, 2 * flip(chip, j, C) + core)

    barrier = pltpu.get_barrier_semaphore()
    pl.semaphore_signal(barrier, inc=1, device_id=partner, device_id_type=MESH)
    for j in range(1, C):
        pl.semaphore_signal(barrier, inc=1, device_id=peer(j), device_id_type=MESH)
    for d in (1, S - 1):
        pl.semaphore_signal(barrier, inc=1, device_id=(lax.rem(z + d, S), s), device_id_type=MESH)
    pl.semaphore_wait(barrier, C + 2)

    def put_stat(row, value):
        for i in range(n):
            stats_ref[i, row : row + 1] = value[:, i * hc : (i + 1) * hc]

    def give(i, src, dst):
        remote(src, dst, gx_ss.at[i], gx_rs.at[i], partner).start()

    def taken(i, src, dst):
        await_recv(dst, gx_rs.at[i], partner)

    def spread(r, buf):
        for j in range(C - 1, 0, -1):
            remote(buf.at[chip], buf.at[chip], ag_ss.at[r, j], ag_rs.at[r, j], peer(j)).start()

    def arrived(r, buf, j):
        @pl.when(j > 0)
        def _():
            c = flip(chip, j, C)
            await_recv(buf.at[c], ag_rs.at[r, j], (z, 2 * c + core))

    def hand(r, j, part):
        stage[r, j] = part.astype(BF16)
        remote(stage.at[r, j], recv.at[r, j], sc_ss.at[r, j], sc_rs.at[r, j], peer(j)).start()

    def collected(r, total):
        for j in range(1, C):
            await_recv(recv.at[r, j], sc_rs.at[r, j], peer(j))
            total = total + recv[r, j].astype(F32)
        return total

    par = jnp.concatenate([par_ref[i] for i in range(n)], axis=1)
    b_out, gain1, shift1 = par[0:1], par[1:2], par[2:3]
    b_down, gain2, shift2 = par[3:4], par[4:5], par[5:6]

    remote(att_ref.at[:, other], attp, ap_ss.at[0], ap_rs.at[0], partner).start()
    loads[0].wait()
    loads[1].wait()
    await_recv(attp, ap_rs.at[0], partner)

    def out_part(j):
        c = flip(chip, j, C)
        return rows_dot(att_ref[c, core], wout_v[core]) + rows_dot(attp[c], wout_v[other])

    def out_step(k, carry):
        hand(0, C - 1 - k, out_part(C - 1 - k))
        return carry

    lax.fori_loop(0, C - 1, out_step, 0)
    first_sum = collected(0, out_part(0) + hidden_ref[...] + b_out)
    normed_one, inverse_one = layer_stats(first_sum)
    normed_v[...] = normed_one
    first_norm = normed_one * gain1 + shift1
    first_v[...] = first_norm
    fa[chip] = first_norm.astype(BF16)
    spread(0, fa)

    loads[2].wait()
    loads[3].wait()
    loads[4].wait()
    first_core = core == 0
    bias_up = bup_ref[...]

    def up_part(j):
        c = flip(chip, j, C)
        pre = rows_dot(fa[c], wup_v[...].reshape(D, F2)) + bias_up
        half = 0.5 * (1.0 + lax.erf(pre * root_half))
        act[c] = (pre * half).astype(BF16)
        slope[c] = half + pre * jnp.exp(-0.5 * pre * pre) * inv_root_two_pi
        return rows_dot(act[c], wdn_v[...].reshape(F2, D))

    own = up_part(0)

    def up_step(j, carry):
        arrived(0, fa, j)
        hand(1, j, up_part(j))
        return carry

    lax.fori_loop(1, C, up_step, 0)
    second_sum = collected(1, own + first_v[...] + b_down)
    normed_two, inverse_two = layer_stats(second_sum)
    result_ref[...] = (normed_two * gain2 + shift2).astype(BF16)
    grad_rows = cot_ref[...].astype(F32)
    put_stat(0, col_sum(grad_rows * normed_two))
    put_stat(1, col_sum(grad_rows))
    d_second = layer_back(grad_rows * gain2, normed_two, inverse_two)
    put_stat(2, col_sum(d_second))
    dnorm_v[...] = d_second
    da[chip] = d_second.astype(BF16)
    spread(1, da)

    def down_back(j):
        c = flip(chip, j, C)
        d_up = rows_dot_t(da[c], wdn_v[...].reshape(F2, D)) * slope[c]
        gb_v[...] += col_sum(d_up)
        dup[c] = d_up.astype(BF16)
        return rows_dot_t(dup[c], wup_v[...].reshape(D, F2))

    gb_v[...] = jnp.zeros_like(gb_v)
    own = down_back(0)

    def back_step(j, carry):
        arrived(1, da, j)
        hand(2, j, down_back(j))
        return carry

    lax.fori_loop(1, C, back_step, 0)
    dnorm_v[...] = dnorm_v[...] + own

    tile = 256
    da_all = da[...].reshape(Ph, D)

    per_half = F1 // tile
    per_tile = gdn_v.shape[1] // per_half

    def down_grad(i, carry):
        t = lax.rem(i + other * per_half, 2 * per_half)
        cols = pl.ds(pl.multiple_of(t * tile, tile), tile)
        res = cols_dot(act[:, :, cols].reshape(Ph, tile), da_all).astype(BF16)
        gdn_v[t // per_half, pl.ds(lax.rem(t, per_half) * per_tile, per_tile)] = res.reshape(
            per_tile, tile // per_tile, D
        )
        return carry

    lax.fori_loop(0, per_half, down_grad, 0)
    give(0, gdn_v.at[other], gdn_r)
    lax.fori_loop(per_half, 2 * per_half, down_grad, 0)

    def up_grad(c, carry):
        cols = pl.ds(pl.multiple_of(c * 2 * Dn, 128), 2 * Dn)
        res = cols_dot(fa[:, :, cols].reshape(Ph, 2 * Dn), dup[...].reshape(Ph, F2)).astype(BF16)
        gup_v[c, 0] = res[:Dn]
        gup_v[c, 1] = res[Dn:]
        return carry

    early = gdn_h.shape[0]
    taken(0, None, gdn_r)
    gdn_h[...] = (gdn_v[core, :early].astype(F32) + gdn_r[:early].astype(F32)).astype(BF16)
    gdn_ref[...] = (gdn_v[core, early:].astype(F32) + gdn_r[early:].astype(F32)).astype(BF16)
    chain = Chain(S, z, s, gdn_h, gdn_l, gdn_x, gdn_f, zsem)
    chain.give_out(0, early)

    lax.fori_loop(0, C, up_grad, 0)
    give(1, gup_v.at[:, other], gup_r)
    gb_r[0] = jnp.where(first_core, gb_v[:, F1:], gb_v[:, :F1])
    give(2, gb_r.at[0], gb_r.at[1])
    chain.run(0, 2)
    d_first_norm = collected(2, dnorm_v[...])
    normed_one = normed_v[...]
    put_stat(3, col_sum(d_first_norm * normed_one))
    put_stat(4, col_sum(d_first_norm))
    d_first = layer_back(d_first_norm * gain1, normed_one, inverse_one)
    put_stat(5, col_sum(d_first))
    stats_ref[:, 6:8] = jnp.zeros((n, 2, hc), F32)
    dfirst_ref[...] = d_first
    dfa[chip] = d_first.astype(BF16)
    spread(2, dfa)

    def att_back(j, carry):
        chain.run(2 * j + 2, 2 * j + 4)
        arrived(2, dfa, j)
        c = flip(chip, j, C)
        datt_ref[c, core] = rows_dot_t(dfa[c], wout_v[core]).astype(BF16)
        dattst[j] = rows_dot_t(dfa[c], wout_v[other]).astype(BF16)
        remote(dattst.at[j], datt_ref.at[c, core], dx_ss.at[j], dx_rs.at[j], partner).start()
        return carry

    lax.fori_loop(0, C, att_back, 0)
    dfa_all = dfa[...].reshape(Ph, D)
    gout_v[0] = cols_dot(attp[...].reshape(Ph, hc), dfa_all).astype(BF16)
    give(3, gout_v.at[0], gout_r)
    gout_v[1] = cols_dot(att_ref[:, core].reshape(Ph, hc), dfa_all).astype(BF16)

    chain.run(2 * C + 2, chain.slots)
    taken(1, None, gup_r)
    gup_ref[...] = (gup_v[:, core].astype(F32) + gup_r[...].astype(F32)).astype(BF16)
    taken(2, None, gb_r.at[1])
    gbup_ref[...] = jnp.where(first_core, gb_v[:, :F1], gb_v[:, F1:]) + gb_r[1]
    taken(3, None, gout_r)
    gout_ref[...] = (gout_v[1].astype(F32) + gout_r[...].astype(F32)).astype(BF16)

    chain.settle()
    gdn_done_ref[...] = gdn_f[...]
    await_send(attp, ap_ss.at[0], partner)
    await_send(gdn_r, gx_ss.at[0], partner)
    await_send(gup_r, gx_ss.at[1], partner)
    await_send(gb_r.at[0], gx_ss.at[2], partner)
    await_send(gout_r, gx_ss.at[3], partner)

    def settle(j, carry):
        c = flip(chip, j, C)
        await_recv(datt_ref.at[c, other], dx_rs.at[j], partner)
        await_send(dattst.at[j], dx_ss.at[j], partner)

        @pl.when(j > 0)
        def _():
            for r in range(3):
                await_send(stage.at[r, j], sc_ss.at[r, j], peer(j))
            await_send(fa.at[chip], ag_ss.at[0, j], peer(j))
            await_send(da.at[chip], ag_ss.at[1, j], peer(j))
            await_send(dfa.at[chip], ag_ss.at[2, j], peer(j))

        return carry

    lax.fori_loop(0, C, settle, 0)


def middle_call(S, n, att, hidden, cot, par, wout, wout_o, wup2, wdn, wdn_o, bup):
    C = n // 2
    L, D = hidden.shape
    hc = D // n
    F1 = wdn.shape[0]
    F2 = 2 * F1
    dims = (S, n, C, L, D, hc, F1)
    dma = pltpu.SemaphoreType.DMA
    vm = pl.BlockSpec(memory_space=pltpu.VMEM)
    anyw = pl.BlockSpec(memory_space=pl.ANY)
    sds = jax.ShapeDtypeStruct
    Dn = D // n
    pc, early = 16, EARLY_PIECES
    return pl.pallas_call(
        functools.partial(middle_kernel, dims),
        out_shape=(
            sds((L, D), BF16),
            sds((L, D), F32),
            sds((C, 2, L, hc), BF16),
            sds((pc - early, F1 // pc, D), BF16),
            sds((C, Dn, F2), BF16),
            sds((hc, D), BF16),
            sds((n, 8, hc), F32),
            sds((1, F1), F32),
            sds((early, F1 // pc, D), BF16),
        ),
        in_specs=[vm, vm, vm, vm, anyw, anyw, anyw, anyw, anyw, vm],
        out_specs=(vm,) * 9,
        scratch_shapes=[
            pltpu.VMEM((2, hc, D), BF16),
            pltpu.VMEM((n, Dn, F2), BF16),
            pltpu.VMEM((2, F1, D), BF16),
            pltpu.VMEM((C, L, hc), BF16),
            pltpu.VMEM((C, L, D), BF16),
            pltpu.VMEM((C, L, D), BF16),
            pltpu.VMEM((C, L, D), BF16),
            pltpu.VMEM((C, L, F2), BF16),
            pltpu.VMEM((C, L, F2), F32),
            pltpu.VMEM((C, L, F2), BF16),
            pltpu.VMEM((3, C, L, D), BF16),
            pltpu.VMEM((3, C, L, D), BF16),
            pltpu.VMEM((L, D), F32),
            pltpu.VMEM((L, D), F32),
            pltpu.VMEM((L, D), F32),
            pltpu.VMEM((2, pc, F1 // pc, D), BF16),
            pltpu.VMEM((pc, F1 // pc, D), BF16),
            pltpu.VMEM((early, F1 // pc, D), BF16),
            pltpu.VMEM((early, F1 // pc, D), BF16),
            pltpu.VMEM((early, F1 // pc, D), BF16),
            pltpu.VMEM((early, F1 // pc, D), BF16),
            pltpu.VMEM((C, 2, Dn, F2), BF16),
            pltpu.VMEM((C, Dn, F2), BF16),
            pltpu.VMEM((2, hc, D), BF16),
            pltpu.VMEM((hc, D), BF16),
            pltpu.VMEM((1, F2), F32),
            pltpu.VMEM((2, 1, F1), F32),
            pltpu.VMEM((C, L, hc), BF16),
            dma((1,)),
            dma((1,)),
            dma((3, C)),
            dma((3, C)),
            dma((3, C)),
            dma((3, C)),
            dma((4,)),
            dma((4,)),
            dma((C,)),
            dma((C,)),
            dma((6, early)),
            dma((5,)),
        ],
        compiler_params=pltpu.CompilerParams(
            collective_id=1, has_side_effects=True, vmem_limit_bytes=MIDDLE_VMEM * MIB
        ),
        name="middle_stage",
    )(att, hidden, cot, par, wout, wout_o, wup2, wdn, wdn_o, bup)


def exit_kernel(
    dims,
    dq_ref,
    dkv_ref,
    hid_ref,
    wq_ref,
    dfirst_ref,
    stats_ref,
    gbup_ref,
    pos_ref,
    gupc_ref,
    goutc_ref,
    gdnc_ref,
    ginp_ref,
    dh_ref,
    gq_f,
    up_f,
    out_f,
    dn_f,
    gtable_ref,
    small_ref,
    gbo_ref,
    zr,
    own3,
    got3,
    x6,
    stage,
    recv,
    dhb,
    gq_v,
    gq_r,
    gq_s,
    gq_o,
    gq_l,
    gq_x,
    up_o,
    up_l,
    up_x,
    out_o,
    out_l,
    out_x,
    dn_o,
    dn_l,
    dn_x,
    plane,
    prod,
    st_r,
    st_v,
    zst,
    zgb,
    zk_ss,
    zk_rs,
    x_ss,
    x_rs,
    sc_ss,
    sc_rs,
    st_ss,
    st_rs,
    zs_ss,
    zs_rs,
    gq_ss,
    gq_rs,
    gx_ss,
    gx_rs,
    ua_ss,
    ua_rs,
    qc,
    uc,
    oc,
    dc,
    zl_ss,
    zl_rs,
    ag_ss,
    ag_rs,
    pf_ss,
    pf_rs,
    loc,
):
    S, n, C, L, D, hc, F1, R, rt = dims
    Dn, Ph = D // n, C * L
    z = lax.axis_index("seq")
    s = lax.axis_index("shard")
    core = lax.rem(s, 2)
    chip = s // 2
    other = 1 - core
    twin = 2 * chip + other
    partner = (z, twin)
    first_core = core == 0

    def peer(j):
        return (z, 2 * flip(chip, j, C) + core)

    barrier = pltpu.get_barrier_semaphore()
    for d in range(1, n):
        pl.semaphore_signal(barrier, inc=1, device_id=(z, flip(s, d, n)), device_id_type=MESH)
    for d in range(1, S):
        pl.semaphore_signal(barrier, inc=1, device_id=(lax.rem(z + d, S), s), device_id_type=MESH)
    pl.semaphore_wait(barrier, n - 1 + S - 1)

    for j in range(C - 1, -1, -1):
        c = flip(chip, j, C)

        @pl.when(z > 0)
        def _():
            remote(
                dkv_ref.at[0, c], zr.at[1, c], zk_ss.at[j, 0], zk_rs.at[j, 1], (z - 1, s)
            ).start()

        @pl.when(z < S - 1)
        def _():
            remote(
                dkv_ref.at[2, c], zr.at[0, c], zk_ss.at[j, 1], zk_rs.at[j, 0], (z + 1, s)
            ).start()

    quarter = Dn // 4
    mine = pl.ds(4 * chip, 4)

    def block_of(j):
        return pl.ds(4 * flip(chip, j, C), 4)

    for j in range(C - 1, 0, -1):
        remote(
            gupc_ref.at[flip(chip, j, C)], up_o.at[mine], ua_ss.at[j], ua_rs.at[j], peer(j)
        ).start()
    up_o[mine] = gupc_ref[chip]
    out_o[...] = goutc_ref[...].reshape(4, quarter, D)
    dn_o[...] = gdnc_ref[...]
    wide = Chain(S, z, s, up_o, up_l, up_x, up_f, uc)
    square = Chain(S, z, s, out_o, out_l, out_x, out_f, oc)
    late = Chain(S, z, s, dn_o, dn_l, dn_x, dn_f, dc)
    inner = Chain(S, z, s, gq_o, gq_l, gq_x, gq_f, qc)
    late.give_out(0, late.pieces)
    square.give_out(0, square.pieces)

    st_r[s] = stats_ref[s]
    for d in range(1, n):
        to = flip(s, d, n)
        remote(stats_ref.at[to], st_r.at[s], st_ss.at[d], st_rs.at[d], (z, to)).start()

    def fold(k, carry):
        j = C - 1 - k
        c = flip(chip, j, C)
        whole = dkv_ref[1, c].astype(F32)

        @pl.when(z > 0)
        def _():
            await_recv(zr.at[0, c], zk_rs.at[j, 0], (z - 1, s))

        @pl.when(z < S - 1)
        def _():
            await_recv(zr.at[1, c], zk_rs.at[j, 1], (z + 1, s))

        whole = whole + jnp.where(z > 0, zr[0, c].astype(F32), 0.0)
        whole = whole + jnp.where(z < S - 1, zr[1, c].astype(F32), 0.0)
        whole = whole.astype(BF16)
        own3[c, :, :, :hc] = dq_ref[c]
        own3[c, :, :, hc:] = whole
        remote(own3.at[c, other], got3.at[c], x_ss.at[j], x_rs.at[j], partner).start()
        sums = jnp.sum(own3[c].astype(F32), axis=(0, 1), keepdims=False)
        st_v[0:1] += sums[None, :hc]
        st_v[1:2] += sums[None, 2 * hc :]
        return carry

    st_v[...] = jnp.zeros_like(st_v)
    lax.fori_loop(0, C, fold, 0)

    def partial(j):
        c = flip(chip, j, C)
        await_recv(got3.at[c], x_rs.at[j], partner)
        mine, theirs = own3[c, core], got3[c]
        low = jnp.where(first_core, mine, theirs)
        high = jnp.where(first_core, theirs, mine)
        pieces = []
        for part in range(3):
            pieces += [low[:, part * hc : (part + 1) * hc], high[:, part * hc : (part + 1) * hc]]
        x6[c] = jnp.concatenate(pieces, axis=1)
        return rows_dot_t(x6[c], wq_ref[...].reshape(D, 6 * hc))

    def scatter(k, carry):
        j = C - 1 - k
        stage[j] = partial(j).astype(BF16)
        remote(stage.at[j], recv.at[j], sc_ss.at[j], sc_rs.at[j], peer(j)).start()
        return carry

    lax.fori_loop(0, C - 1, scatter, 0)
    total = partial(0) + dfirst_ref[...]

    def qkv_grad(c, carry):
        late.slot(c)
        cols = pl.ds(pl.multiple_of(c * 2 * Dn, 128), 2 * Dn)
        res = cols_dot(hid_ref[:, :, cols].reshape(Ph, 2 * Dn), x6[...].reshape(Ph, 6 * hc))
        gq_v[c] = res.astype(BF16).reshape(2, 4, quarter, 6 * hc)
        return carry

    lax.fori_loop(0, C, qkv_grad, 0)
    remote(gq_v.at[:, other], gq_r, gq_ss.at[0], gq_rs.at[0], partner).start()

    sums = st_r[s]
    for d in range(1, n):
        src = flip(s, d, n)
        await_recv(st_r.at[src], st_rs.at[d], (z, src))
    sums = st_r[0]
    for i in range(1, n):
        sums = sums + st_r[i]
    zst[z] = sums
    zst[z, 6:8] = st_v[...]
    zgb[z] = gbup_ref[...]
    for d in range(1, S):
        to = (lax.rem(z + d, S), s)
        remote(zst.at[z], zst.at[z], zs_ss.at[d, 0], zs_rs.at[d, 0], to).start()
        remote(zgb.at[z], zgb.at[z], zs_ss.at[d, 1], zs_rs.at[d, 1], to).start()

    for j in range(1, C):
        await_recv(up_o.at[block_of(j)], ua_rs.at[j], peer(j))
    late.run(C, C + 2)
    await_recv(gq_r, gq_rs.at[0], partner)
    gq_s[...] = (gq_v[:, core].astype(F32) + gq_r[...].astype(F32)).astype(BF16)
    for j in range(C - 1, 0, -1):
        remote(
            gq_s.at[flip(chip, j, C)], gq_o.at[mine], gx_ss.at[j], gx_rs.at[j], peer(j)
        ).start()
    gq_o[mine] = gq_s[chip]

    for j in range(1, C):
        await_recv(recv.at[j], sc_rs.at[j], peer(j))
        total = total + recv[j].astype(F32)
    ginp = total.astype(BF16)
    ginp_ref[...] = ginp
    dhb[...] = ginp
    keep = pltpu.make_async_copy(dhb, dh_ref.at[z, s], loc.at[0])
    keep.start()

    def broadcast(src, at):
        for j in range(C - 1, 0, -1):
            remote(src, dh_ref.at[at, s], ag_ss.at[at, j], ag_rs.at[at, j], peer(j)).start()
        remote(src, dh_ref.at[at, s], pf_ss.at[at, 0], pf_rs.at[at, 0], partner).start()

    @pl.when(z < S - 1)
    def _():
        remote(dhb, dh_ref.at[z, s], zl_ss.at[z, 0], zl_rs.at[z, 0], (z + 1, s)).start()

    @pl.when(z > 0)
    def _():
        remote(dhb, dh_ref.at[z, s], zl_ss.at[z, 1], zl_rs.at[z, 1], (z - 1, s)).start()

    broadcast(dhb, z)
    wide.give_out(0, wide.pieces)
    late.run(C + 2, late.slots)
    square.run(0, square.slots)
    for d in range(1, S):

        @pl.when(z - d >= 0)
        def _():
            at = z - d
            await_recv(dh_ref.at[at, s], zl_rs.at[at, 0], (z - 1, s))

            @pl.when(z < S - 1)
            def _():
                remote(
                    dh_ref.at[at, s], dh_ref.at[at, s], zl_ss.at[at, 0], zl_rs.at[at, 0], (z + 1, s)
                ).start()

            broadcast(dh_ref.at[at, s], at)

        @pl.when(z + d <= S - 1)
        def _():
            at = z + d
            await_recv(dh_ref.at[at, s], zl_rs.at[at, 1], (z + 1, s))

            @pl.when(z > 0)
            def _():
                remote(
                    dh_ref.at[at, s], dh_ref.at[at, s], zl_ss.at[at, 1], zl_rs.at[at, 1], (z - 1, s)
                ).start()

            broadcast(dh_ref.at[at, s], at)

        if d == 2:
            for j in range(1, C):
                await_recv(gq_o.at[block_of(j)], gx_rs.at[j], peer(j))
            inner.give_out(0, inner.pieces)
        wide.run(3 * (d - 1), 3 * d)

    def relay(at):
        for j in range(1, C):
            src = 2 * flip(chip, j, C) + core
            await_recv(dh_ref.at[at, src], ag_rs.at[at, j], (z, src))
            remote(
                dh_ref.at[at, src], dh_ref.at[at, src], pf_ss.at[at, j], pf_rs.at[at, j], partner
            ).start()

    seen = 3 * (S - 1)

    def plane_sum(t, carry):
        at = flip(z, t, S)
        relay(at)

        wide.run(seen + 5 * t, seen + 5 * t + 5)
        inner.run(6 * (t - 2), 6 * (t - 1))

        for j in range(C):
            src = 2 * flip(chip, j, C) + other
            await_recv(dh_ref.at[at, src], pf_rs.at[at, j], partner)

        @pl.when(t == 0)
        def _():
            keep.wait()

        load = pltpu.make_async_copy(dh_ref.at[at], plane, loc.at[1])
        load.start()
        load.wait()

        def rows_tile(r, inner):
            start = pl.multiple_of(r * rt, rt)
            ids = lax.broadcasted_iota(jnp.int32, (rt, L), 0) + (start + s * R)
            hot = jnp.concatenate(
                [jnp.where(ids == pos_ref[at, i], 1.0, 0.0).astype(BF16) for i in range(n)], axis=1
            )
            prod[at, pl.ds(start, rt), :] = rows_dot(hot, plane[...].reshape(n * L, D))
            return inner

        lax.fori_loop(0, R // rt, rows_tile, 0)
        return carry

    lax.fori_loop(0, S, plane_sum, 0)

    def add_tile(r, carry):
        at = pl.ds(pl.multiple_of(r * rt, rt), rt)
        rows = prod[0, at]
        for i in range(1, S):
            rows = rows + prod[i, at]
        gtable_ref[at] = rows.astype(BF16)
        return carry

    lax.fori_loop(0, R // rt, add_tile, 0)

    wide.run(seen + 5 * S, wide.slots)
    inner.run(6 * (S - 2), inner.slots)
    for d in range(1, S):
        src = lax.rem(z + S - d, S)
        await_recv(zst.at[src], zs_rs.at[d, 0], (src, s))
        await_recv(zgb.at[src], zs_rs.at[d, 1], (src, s))
    small, big = zst[0], zgb[0]
    for i in range(1, S):
        small = small + zst[i]
        big = big + zgb[i]
    small_ref[...] = small
    gbo_ref[...] = big

    def settle_plane(at, carry):
        for j in range(C):
            await_send(dhb, pf_ss.at[at, j], partner)
            if j > 0:
                await_send(dhb, ag_ss.at[at, j], peer(j))
        return carry

    lax.fori_loop(0, S, settle_plane, 0)
    for at in range(S):

        @pl.when((z >= at) & (z < S - 1))
        def _():
            await_send(dhb, zl_ss.at[at, 0], (z + 1, s))

        @pl.when((z <= at) & (z > 0))
        def _():
            await_send(dhb, zl_ss.at[at, 1], (z - 1, s))

    for j in range(C):

        @pl.when(z > 0)
        def _():
            await_send(zr.at[0, 0], zk_ss.at[j, 0], (z - 1, s))

        @pl.when(z < S - 1)
        def _():
            await_send(zr.at[0, 0], zk_ss.at[j, 1], (z + 1, s))

        await_send(got3.at[0], x_ss.at[j], partner)
        if j > 0:
            await_send(stage.at[j], sc_ss.at[j], peer(j))
    for d in range(1, n):
        await_send(st_r.at[s], st_ss.at[d], (z, flip(s, d, n)))
    for d in range(1, S):
        to = (lax.rem(z + d, S), s)
        await_send(zst.at[z], zs_ss.at[d, 0], to)
        await_send(zgb.at[z], zs_ss.at[d, 1], to)
    for j in range(1, C):
        await_send(gq_s.at[chip], gx_ss.at[j], peer(j))
        await_send(gupc_ref.at[chip], ua_ss.at[j], peer(j))
    wide.settle()
    square.settle()
    late.settle()
    inner.settle()
    await_send(gq_r, gq_ss.at[0], partner)


def exit_call(S, n, R, dq, dkv, hid_half, wq, dfirst, stats, gbup, pos, gupc, goutc, gdnc):
    C = n // 2
    L, D = dfirst.shape
    hc = D // n
    F1 = gbup.shape[1]
    Dn = D // n
    F2 = gupc.shape[3]
    dims = (S, n, C, L, D, hc, F1, R, 256)
    dma = pltpu.SemaphoreType.DMA
    vm = pl.BlockSpec(memory_space=pltpu.VMEM)
    anyw = pl.BlockSpec(memory_space=pl.ANY)
    sds = jax.ShapeDtypeStruct
    return pl.pallas_call(
        functools.partial(exit_kernel, dims),
        out_shape=(
            sds((L, D), BF16),
            sds((S, n, L, D), BF16),
            sds((4 * C, Dn // 4, 6 * hc), BF16),
            sds((4 * C, Dn // 4, F2), BF16),
            sds((4, Dn // 4, D), BF16),
            sds(gdnc.shape, BF16),
            sds((R, D), BF16),
            sds((8, hc), F32),
            sds((1, F1), F32),
        ),
        in_specs=[vm] * 11,
        out_specs=(vm, anyw) + (vm,) * 7,
        scratch_shapes=[
            pltpu.VMEM((2, C, 2, L, 2 * hc), BF16),
            pltpu.VMEM((C, 2, L, 3 * hc), BF16),
            pltpu.VMEM((C, L, 3 * hc), BF16),
            pltpu.VMEM((C, L, 6 * hc), BF16),
            pltpu.VMEM((C, L, D), BF16),
            pltpu.VMEM((C, L, D), BF16),
            pltpu.VMEM((L, D), BF16),
            pltpu.VMEM((C, 2, 4, Dn // 4, 6 * hc), BF16),
            pltpu.VMEM((C, 4, Dn // 4, 6 * hc), BF16),
            pltpu.VMEM((C, 4, Dn // 4, 6 * hc), BF16),
            pltpu.VMEM((4 * C, Dn // 4, 6 * hc), BF16),
            pltpu.VMEM((4 * C, Dn // 4, 6 * hc), BF16),
            pltpu.VMEM((4 * C, Dn // 4, 6 * hc), BF16),
            pltpu.VMEM((4 * C, Dn // 4, F2), BF16),
            pltpu.VMEM((4 * C, Dn // 4, F2), BF16),
            pltpu.VMEM((4 * C, Dn // 4, F2), BF16),
            pltpu.VMEM((4, Dn // 4, D), BF16),
            pltpu.VMEM((4, Dn // 4, D), BF16),
            pltpu.VMEM((4, Dn // 4, D), BF16),
            pltpu.VMEM(gdnc.shape, BF16),
            pltpu.VMEM(gdnc.shape, BF16),
            pltpu.VMEM(gdnc.shape, BF16),
            pltpu.VMEM((n, L, D), BF16),
            pltpu.VMEM((S, R, D), F32),
            pltpu.VMEM((n, 8, hc), F32),
            pltpu.VMEM((2, hc), F32),
            pltpu.VMEM((S, 8, hc), F32),
            pltpu.VMEM((S, 1, F1), F32),
            dma((C, 2)),
            dma((C, 2)),
            dma((C,)),
            dma((C,)),
            dma((C,)),
            dma((C,)),
            dma((n,)),
            dma((n,)),
            dma((S, 2)),
            dma((S, 2)),
            dma((1,)),
            dma((1,)),
            dma((C,)),
            dma((C,)),
            dma((C,)),
            dma((C,)),
            dma((6, 4 * C)),
            dma((6, 4 * C)),
            dma((6, 4)),
            dma((6, gdnc.shape[0])),
            dma((S, 2)),
            dma((S, 2)),
            dma((S, C)),
            dma((S, C)),
            dma((S, C)),
            dma((S, C)),
            dma((2,)),
        ],
        compiler_params=pltpu.CompilerParams(
            collective_id=2, has_side_effects=True, vmem_limit_bytes=EXIT_VMEM * MIB
        ),
        name="exit_stage",
    )(dq, dkv, hid_half, wq, dfirst, stats, gbup, pos, gupc, goutc, gdnc)


def finish_kernel(
    dims,
    table_ref,
    gq_ref,
    up_ref,
    out_ref,
    early_ref,
    late_ref,
    res_ref,
    inp_ref,
    small_ref,
    gb_ref,
    table_o,
    gq_o,
    up_o,
    out_o,
    dn_o,
    res_o,
    inp_o,
    gb_o,
    *small_o,
):
    C, D, hc = dims
    i = pl.program_id(0)
    h2 = 2 * hc
    F2 = up_ref.shape[3]
    table_o[...] = table_ref[...].astype(F32)
    for c in range(C):
        up_o[:, c * F2 : (c + 1) * F2] = up_ref[c, 0].astype(F32)
        for part in range(3):
            gq_o[:, part * D + c * h2 : part * D + (c + 1) * h2] = gq_ref[
                c, 0, :, part * h2 : (part + 1) * h2
            ].astype(F32)
    out_o[...] = out_ref[0].astype(F32)
    piece = early_ref.shape[0] * early_ref.shape[1]
    dn_o[...] = jnp.where(i < 4, early_ref[...], late_ref[...]).reshape(piece, D).astype(F32)
    res_o[...] = res_ref[...]
    inp_o[...] = inp_ref[...]
    gb_o[...] = gb_ref[...]
    for r, o in enumerate(small_o):
        o[...] = small_ref[r : r + 1]


def finish_call(n, table, gq, up, out, early, late, res, inp, small, gb):
    C = n // 2
    R, D = table.shape
    L = res.shape[0]
    Dn = D // n
    hc = Dn
    q, F2 = up.shape[1:]
    h = q // 2
    piece = early.shape[1]
    F1 = gb.shape[1]
    sds = jax.ShapeDtypeStruct
    steps = 8
    two = lambda rows, cols: pl.BlockSpec((rows, cols), lambda i: (i, 0))
    quad = lambda cols: pl.BlockSpec((C, 1, h, cols), lambda i: (0, i // 2, i % 2, 0))
    fixed = lambda rows, cols: pl.BlockSpec((rows, cols), lambda i: (0, 0))
    return pl.pallas_call(
        functools.partial(finish_kernel, (C, D, hc)),
        grid=(steps,),
        out_shape=(
            sds((R, D), F32),
            sds((Dn, 3 * D), F32),
            sds((Dn, C * F2), F32),
            sds((Dn, D), F32),
            sds((F1, D), F32),
            sds((L, D), BF16),
            sds((L, D), BF16),
            sds((1, F1), F32),
        )
        + (sds((1, hc), F32),) * 8,
        in_specs=[
            two(R // steps, D),
            quad(6 * hc),
            quad(F2),
            pl.BlockSpec((1, h, D), lambda i: (i // 2, i % 2, 0)),
            pl.BlockSpec((2, piece, D), lambda i: (jnp.minimum(i, 3), 0, 0)),
            pl.BlockSpec((2, piece, D), lambda i: (jnp.maximum(i - 4, 0), 0, 0)),
            two(L // steps, D),
            two(L // steps, D),
            fixed(8, hc),
            fixed(1, F1),
        ],
        out_specs=(
            two(R // steps, D),
            two(h, 3 * D),
            two(h, C * F2),
            two(h, D),
            two(2 * piece, D),
            two(L // steps, D),
            two(L // steps, D),
            fixed(1, F1),
        )
        + (fixed(1, hc),) * 8,
        compiler_params=pltpu.CompilerParams(vmem_limit_bytes=ATTEND_VMEM * MIB),
        name="finish_stage",
    )(
        table,
        gq.reshape(C, 4, q, 6 * hc),
        up.reshape(C, 4, q, F2),
        out,
        early,
        late,
        res,
        inp,
        small,
        gb,
    )


QUERY_BLOCK = 512
KEY_BLOCK = 512
BACK_KEY_BLOCK = 256
EARLY_PIECES = 8


def local(
    inputs,
    positions,
    segments,
    pos_table,
    w_qkv,
    b_query,
    b_value,
    w_out,
    b_out,
    ln1_gain,
    ln1_bias,
    w_up,
    b_up,
    w_down,
    b_down,
    ln2_gain,
    ln2_bias,
    cotangent,
):
    S, n = lax.axis_size("seq"), lax.axis_size("shard")
    L, D = inputs.shape
    P_, hc, C = L * n, D // n, n // 2
    R = pos_table.shape[0]
    row = lambda v: v.reshape(1, -1)
    rows = [row(v) for v in (b_out, ln1_gain, ln1_bias, b_down, ln2_gain, ln2_bias, b_query, b_value)]
    q, kv, hid_half, hidden, wq, wup2, wdn_o, wout_o, par_all, bup2, pos_glob, lohi = entry_call(
        S,
        n,
        row(positions),
        inputs,
        pos_table,
        w_qkv,
        w_up,
        w_down,
        w_out,
        segments.reshape(S * n, 1, L),
        row(b_up),
        rows,
    )
    q = q.reshape(P_, hc)
    kv = kv.reshape(3 * P_, 2 * hc)
    att, lse = attend_call(q, kv, lohi, QUERY_BLOCK, KEY_BLOCK)
    result, dfirst, datt, gdn_late, gup, gout, stats, gbup, gdn_early = middle_call(
        S,
        n,
        att.reshape(C, 2, L, hc),
        hidden,
        cotangent,
        par_all,
        w_out,
        wout_o,
        wup2,
        w_down,
        wdn_o,
        bup2,
    )
    dq, dkv = attend_back_call(
        q, kv, lohi, att, datt.reshape(P_, hc), lse, QUERY_BLOCK, BACK_KEY_BLOCK
    )
    ginp, dh, gqkv, gup, gout, gdn_late, gtable, small, gbo = exit_call(
        S,
        n,
        R,
        dq.reshape(C, 2, L, hc),
        dkv.reshape(3, C, 2, L, 2 * hc),
        hid_half,
        wq,
        dfirst,
        stats,
        gbup,
        pos_glob,
        gup.reshape(C, 4, D // n // 4, gup.shape[2]),
        gout,
        gdn_late,
    )
    gtable, gqkv, gup, gout, gdn, result, ginp, gbo, *small = finish_call(
        n, gtable, gqkv, gup, gout, gdn_early, gdn_late, result, ginp, small, gbo
    )
    small = [v[0] for v in small]
    return (
        result,
        ginp,
        gtable,
        gqkv,
        small[6],
        small[7],
        gout,
        small[5],
        small[3],
        small[4],
        gup,
        gbo[0],
        gdn,
        small[2],
        small[0],
        small[1],
    )


def solution(mesh):
    in_specs = (
        P(("seq", "shard"), None),
        P(("seq", "shard")),
        P(),
        P("shard", None),
        P("shard", None),
        P("shard"),
        P("shard"),
        P("shard", None),
        P("shard"),
        P("shard"),
        P("shard"),
        P("shard", None),
        P("shard"),
        P("shard", None),
        P("shard"),
        P("shard"),
        P("shard"),
        P(("seq", "shard"), None),
    )
    out_specs = (
        P(("seq", "shard"), None),
        P(("seq", "shard"), None),
        P("shard", None),
        P("shard", None),
        P("shard"),
        P("shard"),
        P("shard", None),
        P("shard"),
        P("shard"),
        P("shard"),
        P("shard", None),
        P("shard"),
        P("shard", None),
        P("shard"),
        P("shard"),
        P("shard"),
    )
    return jax.shard_map(local, mesh=mesh, in_specs=in_specs, out_specs=out_specs, check_vma=False)
```

```python
import functools
import math

import jax
import jax.numpy as jnp
from jax import lax
from jax.experimental import pallas as pl
from jax.experimental.pallas import tpu as pltpu
from jax.sharding import PartitionSpec as P

HEADS = 16
HEAD_DIM = 64
score_scale = 0.125
neg_large = -1e30
epsilon = 1e-06
root_half = 0.7071067811865476
inv_root_two_pi = 0.3989422804014327
MESH = pl.DeviceIdType.MESH
F32 = jnp.float32
BF16 = jnp.bfloat16
MIB = 1024 * 1024
ENTRY_VMEM, ATTEND_VMEM, MIDDLE_VMEM, BACK_VMEM, EXIT_VMEM = 24, 16, 44, 20, 48


def flip(value, mask, width):
    total, bit = 0, 1
    while bit < width:
        a = lax.rem(value // bit, 2)
        b = (mask // bit) % 2 if isinstance(mask, int) else lax.rem(mask // bit, 2)
        total = total + lax.rem(a + b, 2) * bit
        bit *= 2
    return total


def remote(src, dst, send_sem, recv_sem, device):
    return pltpu.make_async_remote_copy(
        src_ref=src,
        dst_ref=dst,
        send_sem=send_sem,
        recv_sem=recv_sem,
        device_id=device,
        device_id_type=MESH,
    )


def await_recv(dst, sem, device):
    remote(dst, dst, sem, sem, device).wait_recv()


def await_send(src, sem, device):
    remote(src, src, sem, sem, device).wait_send()


class Chain:
    def __init__(self, S, z, s, own, land, cross, fin, sems, lag=3):
        self.S, self.s, self.lag, self.sems = S, s, lag, sems
        self.own, self.land, self.cross, self.fin = own, land, cross, fin
        low = 1 - (2 * z) // S
        self.depth = low * z + (1 - low) * (S - 1 - z)
        self.inward = (z + 2 * low - 1, s)
        self.outward = (z + 1 - 2 * low, s)
        self.mid = S // 2 - 1
        self.pieces = own.shape[0]
        self.slots = self.pieces + lag * self.mid + lag * max(self.mid - 1, 0)

    def give_out(self, start, stop):
        @pl.when(self.depth == 0)
        def _():
            def step(p, carry):
                remote(
                    self.own.at[p], self.land.at[p], self.sems.at[0, p], self.sems.at[1, p], self.inward
                ).start()
                return carry

            lax.fori_loop(start, stop, step, 0)

    def slot(self, k):
        p = k - self.lag * (self.depth - 1)

        @pl.when((self.depth > 0) & (p >= 0) & (p < self.pieces))
        def _():
            await_recv(self.land.at[p], self.sems.at[1, p], self.outward)
            both = self.own[p].astype(F32) + self.land[p].astype(F32)
            self.own[p] = both.astype(BF16)

            @pl.when(self.depth < self.mid)
            def _():
                remote(
                    self.own.at[p], self.land.at[p], self.sems.at[0, p], self.sems.at[1, p], self.inward
                ).start()

            @pl.when(self.depth == self.mid)
            def _():
                remote(
                    self.own.at[p], self.cross.at[p], self.sems.at[2, p], self.sems.at[3, p], self.inward
                ).start()

        x = k - self.lag * self.mid

        @pl.when((self.depth == self.mid) & (x >= 0) & (x < self.pieces))
        def _():
            await_recv(self.cross.at[x], self.sems.at[3, x], self.inward)
            both = self.own[x].astype(F32) + self.cross[x].astype(F32)
            self.fin[x] = both.astype(BF16)
            remote(
                self.fin.at[x], self.fin.at[x], self.sems.at[4, x], self.sems.at[5, x], self.outward
            ).start()

        b = k - self.lag * self.mid - self.lag * (self.mid - self.depth)

        @pl.when((self.depth < self.mid) & (self.depth > 0) & (b >= 0) & (b < self.pieces))
        def _():
            await_recv(self.fin.at[b], self.sems.at[5, b], self.inward)
            remote(
                self.fin.at[b], self.fin.at[b], self.sems.at[4, b], self.sems.at[5, b], self.outward
            ).start()

    def run(self, start, stop):
        def step(k, carry):
            self.slot(k)
            return carry

        lax.fori_loop(start, stop, step, 0)

    def settle(self):
        def step(p, carry):
            @pl.when(self.depth == 0)
            def _():
                await_recv(self.fin.at[p], self.sems.at[5, p], self.inward)

            @pl.when(self.depth < self.mid)
            def _():
                await_send(self.own.at[p], self.sems.at[0, p], self.inward)

            @pl.when(self.depth == self.mid)
            def _():
                await_send(self.own.at[p], self.sems.at[2, p], self.inward)

            @pl.when(self.depth > 0)
            def _():
                await_send(self.fin.at[p], self.sems.at[4, p], self.outward)

            return carry

        lax.fori_loop(0, self.pieces, step, 0)


class Gather:
    def __init__(self, C, chip, peer, rows, slot, ss, rs):
        self.C, self.chip, self.peer, self.rows, self.slot = C, chip, peer, rows, slot
        self.ss, self.rs = ss, rs

    def half(self, ref, h):
        return ref.at[pl.ds(h * (self.rows // 2), self.rows // 2)]

    def block(self, j):
        return self.slot(flip(self.chip, j, self.C))

    def send(self, src):
        dst = self.slot(self.chip)
        if self.C == 4:
            for j, first in ((1, 0), (2, 1)):
                for h in (first, 1 - first):
                    remote(
                        self.half(src, h), self.half(dst, h), self.ss.at[j, h], self.rs.at[j, h], self.peer(j)
                    ).start()
        else:
            for j in range(self.C - 1, 0, -1):
                remote(src, dst, self.ss.at[j, 0], self.rs.at[j, 0], self.peer(j)).start()

    def relay(self):
        if self.C == 4:
            for j, h, to in ((1, 0, 2), (2, 1, 1)):
                part = self.half(self.block(j), h)
                await_recv(part, self.rs.at[j, h], self.peer(j))
                remote(part, part, self.ss.at[3, h], self.rs.at[3, h], self.peer(to)).start()

    def arrived(self, j):
        if self.C == 4:
            for want, h in ((1, 1), (2, 0), (3, 0), (3, 1)):

                @pl.when(j == want)
                def _(want=want, h=h):
                    await_recv(self.half(self.block(want), h), self.rs.at[want, h], self.peer(want))
        else:

            @pl.when(j > 0)
            def _():
                await_recv(self.block(j), self.rs.at[j, 0], self.peer(j))

    def settle(self):
        own = self.slot(self.chip)
        if self.C == 4:
            for j in range(1, 4):
                for h in range(2):
                    await_send(self.half(own, h), self.ss.at[j, h], self.peer(j))
        else:
            for j in range(1, self.C):
                await_send(own, self.ss.at[j, 0], self.peer(j))


class Scatter:
    def __init__(self, C, peer, rows, stage, recv, ss, rs):
        self.C, self.peer, self.rows = C, peer, rows
        self.stage, self.recv, self.ss, self.rs = stage, recv, ss, rs

    def give(self, j, h, to):
        part = pl.ds(h * (self.rows // 2), self.rows // 2)
        remote(
            self.stage.at[j, part], self.recv.at[j, part], self.ss.at[j, h], self.rs.at[j, h], self.peer(to)
        ).start()

    def take(self, j, h, source):
        part = pl.ds(h * (self.rows // 2), self.rows // 2)
        await_recv(self.recv.at[j, part], self.rs.at[j, h], self.peer(source))
        return part

    def send(self, make):
        if self.C != 4:

            def step(k, carry):
                j = self.C - 1 - k
                self.stage[j] = make(j).astype(BF16)
                remote(
                    self.stage.at[j], self.recv.at[j], self.ss.at[j, 0], self.rs.at[j, 0], self.peer(j)
                ).start()
                return carry

            lax.fori_loop(0, self.C - 1, step, 0)
            return make(0)
        self.stage[3] = make(3).astype(BF16)
        self.give(3, 0, 2)
        self.give(3, 1, 1)
        self.stage[1] = make(1).astype(BF16)
        self.give(1, 1, 1)
        self.stage[2] = make(2).astype(BF16)
        self.give(2, 0, 2)
        own = make(0)
        for h, source, j in ((0, 2, 1), (1, 1, 2)):
            part = self.take(3, h, source)
            both = self.stage[j, part].astype(F32) + self.recv[3, part].astype(F32)
            self.stage[j, part] = both.astype(BF16)
            self.give(j, h, j)
        return own

    def collect(self, total):
        if self.C != 4:
            for j in range(1, self.C):
                await_recv(self.recv.at[j], self.rs.at[j, 0], self.peer(j))
                total = total + self.recv[j].astype(F32)
            return total
        for j in (1, 2):
            self.take(j, 2 - j, j)
            self.take(j, j - 1, j)
            total = total + self.recv[j].astype(F32)
        return total

    def settle(self):
        for j in range(1, self.C):
            if self.C == 4:
                for h in range(2):
                    part = pl.ds(h * (self.rows // 2), self.rows // 2)
                    await_send(self.stage.at[j, part], self.ss.at[j, h], self.peer(j))
            else:
                await_send(self.stage.at[j], self.ss.at[j, 0], self.peer(j))


def rows_dot(a, b):
    return lax.dot_general(a, b, (((1,), (0,)), ((), ())), preferred_element_type=F32)


def rows_dot_t(a, b):
    return lax.dot_general(a, b, (((1,), (1,)), ((), ())), preferred_element_type=F32)


def cols_dot(a, b):
    return lax.dot_general(a, b, (((0,), (0,)), ((), ())), preferred_element_type=F32)


def entry_kernel(
    dims,
    pos_hbm,
    inp_hbm,
    table_ref,
    wqkv_ref,
    wup_ref,
    wdn_ref,
    wout_ref,
    seg_hbm,
    bup_in_hbm,
    row0_ref,
    row1_ref,
    row2_ref,
    row3_ref,
    row4_ref,
    row5_ref,
    row6_ref,
    row7_ref,
    q_ref,
    kv_ref,
    hid_half_ref,
    hidden_ref,
    wq_ref,
    wup2_ref,
    wdn_o_ref,
    wout_o_ref,
    par_all_ref,
    bup2_ref,
    pos_glob_ref,
    lohi_ref,
    pos_ref,
    inp_ref,
    seg_ref,
    bup_in_ref,
    rows_ref,
    table_v,
    pstage,
    precv,
    cstage,
    crecv,
    qst,
    kvst,
    wup_own,
    par_ref,
    bup_ref,
    pos_ss,
    pos_rs,
    par_ss,
    par_rs,
    posz_ss,
    posz_rs,
    wq_ss,
    wq_rs,
    wqf_ss,
    wqf_rs,
    wup_ss,
    wup_rs,
    wupf_ss,
    wupf_rs,
    misc_ss,
    misc_rs,
    rsp_ss,
    rsp_rs,
    rsc_ss,
    rsc_rs,
    ag_ss,
    ag_rs,
    qx_ss,
    qx_rs,
    zx_ss,
    zx_rs,
    loc,
):
    S, n, C, L, D, hc, R, F2 = dims
    z = lax.axis_index("seq")
    s = lax.axis_index("shard")
    core = lax.rem(s, 2)
    chip = s // 2
    other = 1 - core
    partner = 2 * chip + other
    h2 = 2 * hc
    Dn = D // n

    rows = (row0_ref, row1_ref, row2_ref, row3_ref, row4_ref, row5_ref, row6_ref, row7_ref)
    smalls = [
        pltpu.make_async_copy(pos_hbm, pos_ref, loc.at[6]),
        pltpu.make_async_copy(seg_hbm, seg_ref, loc.at[7]),
        pltpu.make_async_copy(bup_in_hbm, bup_in_ref, loc.at[8]),
    ] + [
        pltpu.make_async_copy(row, rows_ref.at[i], loc.at[9 + i]) for i, row in enumerate(rows)
    ]
    for small in smalls:
        small.start()
    inp_copy = pltpu.make_async_copy(inp_hbm, inp_ref, loc.at[17])
    inp_copy.start()
    table_copy = pltpu.make_async_copy(table_ref, table_v, loc.at[0])
    table_copy.start()
    own_wq = []
    for part in range(3):
        own_wq.append(
            pltpu.make_async_copy(
                wqkv_ref.at[:, pl.ds(pl.multiple_of(part * D + chip * h2, 128), h2)],
                wq_ref.at[s, :, part * h2 : (part + 1) * h2],
                loc.at[1 + part],
            )
        )
        own_wq[-1].start()
    own_wup_in = pltpu.make_async_copy(
        wup_ref.at[:, pl.ds(pl.multiple_of(chip * F2, 128), F2)], wup_own, loc.at[4]
    )
    own_wup_in.start()

    for small in smalls:
        small.wait()
    for i in range(8):
        par_ref[i : i + 1] = rows_ref[i].astype(F32)
    bup_ref[...] = bup_in_ref[...].astype(F32)
    F1 = F2 // 2
    bup_mine = pl.ds(pl.multiple_of(core * F1, 128), F1)
    bup_theirs = pl.ds(pl.multiple_of(other * F1, 128), F1)
    bup2_ref[:, bup_mine] = bup_ref[...]

    barrier = pltpu.get_barrier_semaphore()
    for d in range(1, n):
        pl.semaphore_signal(barrier, inc=1, device_id=(z, flip(s, d, n)), device_id_type=MESH)
    for d in range(1, S):
        pl.semaphore_signal(barrier, inc=1, device_id=(lax.rem(z + d, S), s), device_id_type=MESH)

    for d in (1, S - 1):
        pl.semaphore_signal(
            barrier, inc=1, device_id=(lax.rem(z + d, S), partner), device_id_type=MESH
        )
    pl.semaphore_wait(barrier, n - 1 + S - 1 + 2)

    pos_glob_ref[z, s] = pos_ref[...]
    par_all_ref[s] = par_ref[...]
    for d in range(1, n):
        peer = (z, flip(s, d, n))
        remote(pos_ref, pos_glob_ref.at[z, s], pos_ss.at[d], pos_rs.at[d], peer).start()
        remote(par_ref, par_all_ref.at[s], par_ss.at[d], par_rs.at[d], peer).start()

    for own in own_wq:
        own.wait()

    def wq_src(peer_chip, part):
        return wqkv_ref.at[:, pl.ds(pl.multiple_of(part * D + peer_chip * h2, 128), h2)]

    for j in range(C - 1, 0, -1):
        pc = flip(chip, j, C)
        for part in range(3):
            remote(
                wq_src(pc, part),
                wq_ref.at[s, :, part * h2 : (part + 1) * h2],
                wq_ss.at[j, part],
                wq_rs.at[j, part],
                (z, 2 * pc + core),
            ).start()
    remote(wq_ref.at[s], wq_ref.at[s], wqf_ss.at[0], wqf_rs.at[0], (z, partner)).start()

    own_segs = jnp.concatenate([seg_ref[z * n + i] for i in range(n)], axis=1)

    def count(g, carry):
        low, high = carry
        keys = jnp.broadcast_to(seg_ref[g], (L, L)).T
        lows, highs = [], []
        for i in range(n):
            mine = own_segs[:, i * L : (i + 1) * L]
            lows.append(jnp.sum(jnp.where(keys < mine, 1.0, 0.0), axis=0, keepdims=True))
            highs.append(jnp.sum(jnp.where(keys <= mine, 1.0, 0.0), axis=0, keepdims=True))
        return low + jnp.concatenate(lows, axis=1), high + jnp.concatenate(highs, axis=1)

    none = jnp.zeros((1, n * L), F32)
    low, high = lax.fori_loop(0, S * n, count, (none, none))
    origin = ((z - 1) * n * L).astype(F32)
    lohi_ref[0:1] = low - origin
    lohi_ref[1:2] = high - origin

    for d in range(1, n):
        src = flip(s, d, n)
        await_recv(pos_glob_ref.at[z, src], pos_rs.at[d], (z, src))
    for d in range(1, S):
        remote(
            pos_glob_ref.at[z],
            pos_glob_ref.at[z],
            posz_ss.at[d],
            posz_rs.at[d],
            (lax.rem(z + d, S), s),
        ).start()

    table_copy.wait()
    inp_copy.wait()
    lane_ids = lax.broadcasted_iota(jnp.int32, (L, R), 1) + s * R

    def picked(block):
        ids = jnp.broadcast_to(pos_glob_ref[z, block], (L, L)).T
        ids = jnp.concatenate([ids] * (R // L), axis=1)
        hot = jnp.where(ids == lane_ids, 1.0, 0.0).astype(BF16)
        return rows_dot(hot, table_v[...])

    def send_partner(j):
        pstage[j] = picked(2 * flip(chip, j, C) + other).astype(BF16)
        remote(pstage.at[j], precv.at[j], rsp_ss.at[j], rsp_rs.at[j], (z, partner)).start()

    def combined(j):
        mine = picked(2 * flip(chip, j, C) + core)
        await_recv(precv.at[j], rsp_rs.at[j], (z, partner))
        return mine + precv[j].astype(F32)

    def peer(j):
        return (z, 2 * flip(chip, j, C) + core)

    def partner_step(k, carry):
        send_partner(C - 1 - k)
        return carry

    lax.fori_loop(0, C, partner_step, 0)
    rows_sum = Scatter(C, peer, L, cstage, crecv, rsc_ss, rsc_rs)
    hidden = rows_sum.send(combined) + inp_ref[...].astype(F32)

    for j in range(1, C):
        src = 2 * flip(chip, j, C) + core
        for part in range(3):
            await_recv(
                wq_ref.at[src, :, part * h2 : (part + 1) * h2], wq_rs.at[j, part], (z, src)
            )
        remote(wq_ref.at[src], wq_ref.at[src], wqf_ss.at[j], wqf_rs.at[j], (z, partner)).start()

    hidden = rows_sum.collect(hidden)
    hidden_ref[...] = hidden
    hid_half_ref[chip] = hidden.astype(BF16)
    gather = Gather(C, chip, peer, L, lambda c: hid_half_ref.at[c], ag_ss, ag_rs)
    gather.send(hid_half_ref.at[chip])

    own_wup_in.wait()
    own_wup_out = pltpu.make_async_copy(wup_own, wup2_ref.at[s], loc.at[5])
    own_wup_out.start()
    for j in range(C - 1, 0, -1):
        pc = flip(chip, j, C)
        remote(
            wup_ref.at[:, pl.ds(pl.multiple_of(pc * F2, 128), F2)],
            wup2_ref.at[s],
            wup_ss.at[j],
            wup_rs.at[j],
            (z, 2 * pc + core),
        ).start()
    remote(wup_own, wup2_ref.at[s], wupf_ss.at[0], wupf_rs.at[0], (z, partner)).start()
    remote(wdn_ref, wdn_o_ref, misc_ss.at[0], misc_rs.at[0], (z, partner)).start()
    remote(wout_ref, wout_o_ref, misc_ss.at[1], misc_rs.at[1], (z, partner)).start()
    remote(bup_ref, bup2_ref.at[:, bup_mine], misc_ss.at[2], misc_rs.at[2], (z, partner)).start()

    for j in range(C):
        src = 2 * flip(chip, j, C) + other
        await_recv(wq_ref.at[src], wqf_rs.at[j], (z, partner))
    for d in range(1, n):
        src = flip(s, d, n)
        await_recv(par_all_ref.at[src], par_rs.at[d], (z, src))
    bias = jnp.concatenate([par_all_ref[2 * chip], par_all_ref[2 * chip + 1]], axis=1)
    bias_q, bias_v = bias[6:7], bias[7:8]
    first_core = core == 0

    def project(j, carry):
        c = flip(chip, j, C)

        gather.arrived(j)
        res = rows_dot(hid_half_ref[c], wq_ref[...].reshape(D, 3 * h2))
        query = (res[:, :h2] + bias_q).astype(BF16) * score_scale
        key = res[:, h2 : 2 * h2].astype(BF16)
        value = (res[:, 2 * h2 :] + bias_v).astype(BF16)
        q_ref[c, core] = jnp.where(first_core, query[:, :hc], query[:, hc:])
        kv_ref[1, c, core, :, :hc] = jnp.where(first_core, key[:, :hc], key[:, hc:])
        kv_ref[1, c, core, :, hc:] = jnp.where(first_core, value[:, :hc], value[:, hc:])
        qst[j] = jnp.where(first_core, query[:, hc:], query[:, :hc])
        kvst[j, :, :hc] = jnp.where(first_core, key[:, hc:], key[:, :hc])
        kvst[j, :, hc:] = jnp.where(first_core, value[:, hc:], value[:, :hc])
        own_kv = kv_ref.at[1, c, core]

        @pl.when(z < S - 1)
        def _():
            remote(
                own_kv, kv_ref.at[0, c, core], zx_ss.at[j, 0], zx_rs.at[j, 0], (z + 1, s)
            ).start()
            remote(
                kvst.at[j], kv_ref.at[0, c, core], zx_ss.at[j, 1], zx_rs.at[j, 1], (z + 1, partner)
            ).start()

        @pl.when(z > 0)
        def _():
            remote(
                own_kv, kv_ref.at[2, c, core], zx_ss.at[j, 2], zx_rs.at[j, 2], (z - 1, s)
            ).start()
            remote(
                kvst.at[j], kv_ref.at[2, c, core], zx_ss.at[j, 3], zx_rs.at[j, 3], (z - 1, partner)
            ).start()

        remote(qst.at[j], q_ref.at[c, core], qx_ss.at[j, 0], qx_rs.at[j, 0], (z, partner)).start()
        remote(
            kvst.at[j], kv_ref.at[1, c, core], qx_ss.at[j, 1], qx_rs.at[j, 1], (z, partner)
        ).start()
        return carry

    gather.relay()
    lax.fori_loop(0, C, project, 0)

    for j in range(1, C):
        src = 2 * flip(chip, j, C) + core
        await_recv(wup2_ref.at[src], wup_rs.at[j], (z, src))
        remote(
            wup2_ref.at[src], wup2_ref.at[src], wupf_ss.at[j], wupf_rs.at[j], (z, partner)
        ).start()

    def settle(j, carry):
        c = flip(chip, j, C)
        await_recv(q_ref.at[c, other], qx_rs.at[j, 0], (z, partner))
        await_recv(kv_ref.at[1, c, other], qx_rs.at[j, 1], (z, partner))
        await_send(qst.at[j], qx_ss.at[j, 0], (z, partner))
        await_send(kvst.at[j], qx_ss.at[j, 1], (z, partner))

        @pl.when(z > 0)
        def _():
            await_recv(kv_ref.at[0, c, core], zx_rs.at[j, 0], (z - 1, s))
            await_recv(kv_ref.at[0, c, other], zx_rs.at[j, 1], (z - 1, partner))
            await_send(kvst.at[j], zx_ss.at[j, 2], (z - 1, s))
            await_send(kvst.at[j], zx_ss.at[j, 3], (z - 1, partner))

        @pl.when(z < S - 1)
        def _():
            await_recv(kv_ref.at[2, c, core], zx_rs.at[j, 2], (z + 1, s))
            await_recv(kv_ref.at[2, c, other], zx_rs.at[j, 3], (z + 1, partner))
            await_send(kvst.at[j], zx_ss.at[j, 0], (z + 1, s))
            await_send(kvst.at[j], zx_ss.at[j, 1], (z + 1, partner))

        await_send(pstage.at[j], rsp_ss.at[j], (z, partner))
        await_send(wq_ref.at[s], wqf_ss.at[j], (z, partner))
        await_recv(wup2_ref.at[2 * c + other], wupf_rs.at[j], (z, partner))
        await_send(wup2_ref.at[s], wupf_ss.at[j], (z, partner))
        return carry

    lax.fori_loop(0, C, settle, 0)
    gather.settle()
    rows_sum.settle()
    for j in range(1, C):
        await_send(wup_own, wup_ss.at[j], peer(j))
        for part in range(3):
            await_send(
                wq_ref.at[s, :, part * h2 : (part + 1) * h2], wq_ss.at[j, part], peer(j)
            )
    for d in range(1, n):
        peer = (z, flip(s, d, n))
        await_send(pos_ref, pos_ss.at[d], peer)
        await_send(par_ref, par_ss.at[d], peer)
    for d in range(1, S):
        src = lax.rem(z + S - d, S)
        await_recv(pos_glob_ref.at[src], posz_rs.at[d], (src, s))
        await_send(pos_glob_ref.at[z], posz_ss.at[d], (lax.rem(z + d, S), s))
    for i, (mine, got) in enumerate(
        ((wdn_ref, wdn_o_ref), (wout_ref, wout_o_ref), (bup_ref, bup2_ref.at[:, bup_theirs]))
    ):
        await_recv(got, misc_rs.at[i], (z, partner))
        await_send(mine, misc_ss.at[i], (z, partner))
    own_wup_out.wait()


def entry_call(S, n, pos, inp, table, wqkv, wup, wdn, wout, seg, bup, rows):
    C = n // 2
    L, D = inp.shape
    hc = D // n
    R = table.shape[0]
    F = wup.shape[1]
    F1, F2 = F // n, 2 * F // n
    dims = (S, n, C, L, D, hc, R, F2)
    dma = pltpu.SemaphoreType.DMA
    vm = pl.BlockSpec(memory_space=pltpu.VMEM)
    anyw = pl.BlockSpec(memory_space=pl.ANY)
    hbm = pl.BlockSpec(memory_space=pltpu.HBM)
    sds = jax.ShapeDtypeStruct
    return pl.pallas_call(
        functools.partial(entry_kernel, dims),
        out_shape=(
            sds((C, 2, L, hc), BF16),
            sds((3, C, 2, L, 2 * hc), BF16),
            sds((C, L, D), BF16),
            sds((L, D), F32),
            sds((n, D // n, 6 * hc), BF16),
            sds((n, D // n, F2), BF16),
            sds((F1, D), BF16),
            sds((D // n, D), BF16),
            sds((n, 8, hc), F32),
            sds((1, F2), F32),
            sds((S, n, 1, L), jnp.int32),
            sds((2, n * L), F32),
        ),
        in_specs=[hbm] * 17,
        out_specs=(vm, vm, vm, vm, vm, anyw, anyw, anyw, vm, vm, vm, vm),
        scratch_shapes=[
            pltpu.VMEM((1, L), jnp.int32),
            pltpu.VMEM((L, D), BF16),
            pltpu.VMEM((S * n, 1, L), jnp.int32),
            pltpu.VMEM((1, F1), BF16),
            pltpu.VMEM((8, 1, hc), BF16),
            pltpu.VMEM((R, D), BF16),
            pltpu.VMEM((C, L, D), BF16),
            pltpu.VMEM((C, L, D), BF16),
            pltpu.VMEM((C, L, D), BF16),
            pltpu.VMEM((C, L, D), BF16),
            pltpu.VMEM((C, L, hc), BF16),
            pltpu.VMEM((C, L, 2 * hc), BF16),
            pltpu.VMEM((D // n, F2), BF16),
            pltpu.VMEM((8, hc), F32),
            pltpu.VMEM((1, F1), F32),
            dma((n,)),
            dma((n,)),
            dma((n,)),
            dma((n,)),
            dma((S,)),
            dma((S,)),
            dma((C, 3)),
            dma((C, 3)),
            dma((C,)),
            dma((C,)),
            dma((C,)),
            dma((C,)),
            dma((C,)),
            dma((C,)),
            dma((3,)),
            dma((3,)),
            dma((C,)),
            dma((C,)),
            dma((C, 2)),
            dma((C, 2)),
            dma((C, 2)),
            dma((C, 2)),
            dma((C, 2)),
            dma((C, 2)),
            dma((C, 4)),
            dma((C, 4)),
            dma((18,)),
        ],
        compiler_params=pltpu.CompilerParams(
            collective_id=0, has_side_effects=True, vmem_limit_bytes=ENTRY_VMEM * MIB
        ),
        name="entry_stage",
    )(*[
        pltpu.with_memory_space_constraint(v, pltpu.HBM)
        for v in (pos, inp, table, wqkv, wup, wdn, wout, seg, bup, *rows)
    ])


def key_blocks(lohi_ref, rows, bk):
    first = jnp.min(lohi_ref[0:1, rows]).astype(jnp.int32)
    last = jnp.max(lohi_ref[1:2, rows]).astype(jnp.int32)
    return first // bk, (last + bk - 1) // bk


def attend_kernel(dims, q_ref, kv_ref, lohi_ref, att_ref, lse_ref, vt_ref):
    P_, hc, hh, bq, bk = dims
    lanes = lax.broadcasted_iota(jnp.int32, (bq, hc), 1) // HEAD_DIM
    nq = P_ // bq

    def flip_value(kb, carry):
        at = pl.multiple_of(kb * bk, bk)
        vt_ref[kb] = kv_ref[pl.ds(at, bk), hc:].T
        return carry

    first, last = key_blocks(lohi_ref, pl.ds(0, P_), bk)
    lax.fori_loop(first, last, flip_value, 0)

    def one_query_block(qi, carry):
        rows = pl.ds(pl.multiple_of(qi * bq, bq), bq)
        query = q_ref[rows, :]
        heads_q = [jnp.where(lanes == h, query, jnp.zeros_like(query)) for h in range(hh)]
        low = lohi_ref[0:1, rows].astype(jnp.int32)
        high = lohi_ref[1:2, rows].astype(jnp.int32)
        first, last = key_blocks(lohi_ref, rows, bk)

        def one_key_block(kb, state):
            at = pl.multiple_of(kb * bk, bk)
            keys = kv_ref[pl.ds(at, bk), :hc]
            ids = lax.broadcasted_iota(jnp.int32, (bk, bq), 0) + kb * bk
            keep = (ids >= low) & (ids < high)
            fresh = []
            for h in range(hh):
                top, total, acc = state[h]
                scores = jnp.where(keep, rows_dot_t(keys, heads_q[h]), neg_large)
                new_top = jnp.maximum(top, jnp.max(scores, axis=0, keepdims=True))
                weights = jnp.exp(scores - new_top)
                shrink = jnp.exp(top - new_top)
                total = total * shrink + jnp.sum(weights, axis=0, keepdims=True)
                values = vt_ref[kb, h * HEAD_DIM : (h + 1) * HEAD_DIM, :]
                acc = acc * shrink + rows_dot(values, weights.astype(BF16))
                fresh.append((new_top, total, acc))
            return tuple(fresh)

        start = tuple(
            (
                jnp.full((1, bq), neg_large, F32),
                jnp.zeros((1, bq), F32),
                jnp.zeros((HEAD_DIM, bq), F32),
            )
            for _ in range(hh)
        )
        state = lax.fori_loop(first, last, one_key_block, start)
        mixed = jnp.concatenate([acc / total for _, total, acc in state], axis=0)
        att_ref[rows, :] = mixed.T.astype(BF16)
        for h in range(hh):
            lse_ref[h : h + 1, rows] = state[h][0] + jnp.log(state[h][1])
        return carry

    lax.fori_loop(0, nq, one_query_block, 0)


def attend_call(q, kv, lohi, bq, bk):
    P_, hc = q.shape
    hh = hc // HEAD_DIM
    vm = pl.BlockSpec(memory_space=pltpu.VMEM)
    return pl.pallas_call(
        functools.partial(attend_kernel, (P_, hc, hh, bq, bk)),
        out_shape=(
            jax.ShapeDtypeStruct((P_, hc), BF16),
            jax.ShapeDtypeStruct((hh, P_), F32),
        ),
        in_specs=[vm, vm, vm],
        out_specs=(vm, vm),
        scratch_shapes=[pltpu.VMEM((3 * P_ // bk, hc, bk), BF16)],
        compiler_params=pltpu.CompilerParams(vmem_limit_bytes=ATTEND_VMEM * MIB),
        name="attend_stage",
    )(q, kv, lohi)


def attend_back_kernel(
    dims, q_ref, kv_ref, lohi_ref, att_ref, datt_ref, lse_ref, dq_ref, dkv_ref, kt_ref, acc_ref
):
    P_, hc, hh, bq, bk = dims
    lanes = lax.broadcasted_iota(jnp.int32, (bq, hc), 1) // HEAD_DIM
    nq = P_ // bq
    acc_ref[...] = jnp.zeros_like(acc_ref)

    def flip_key(kb, carry):
        at = pl.multiple_of(kb * bk, bk)
        kt_ref[kb] = kv_ref[pl.ds(at, bk), :hc].T
        return carry

    first, last = key_blocks(lohi_ref, pl.ds(0, P_), bk)
    lax.fori_loop(first, last, flip_key, 0)

    def one_query_block(qi, carry):
        rows = pl.ds(pl.multiple_of(qi * bq, bq), bq)
        query, grad = q_ref[rows, :], datt_ref[rows, :]
        zero = jnp.zeros_like(query)
        heads_q = [jnp.where(lanes == h, query, zero) for h in range(hh)]
        heads_g = [jnp.where(lanes == h, grad, zero) for h in range(hh)]
        stack_q = jnp.concatenate(heads_q, axis=0)
        stack_g = jnp.concatenate(heads_g, axis=0)
        product = (grad.astype(F32) * att_ref[rows, :].astype(F32)).T
        delta = [
            jnp.sum(product[h * HEAD_DIM : (h + 1) * HEAD_DIM], axis=0, keepdims=True)
            for h in range(hh)
        ]
        logs = [lse_ref[h : h + 1, rows] for h in range(hh)]
        low = lohi_ref[0:1, rows].astype(jnp.int32)
        high = lohi_ref[1:2, rows].astype(jnp.int32)
        first, last = key_blocks(lohi_ref, rows, bk)

        def one_key_block(kb, state):
            at = pl.multiple_of(kb * bk, bk)
            keys = kv_ref[pl.ds(at, bk), :hc]
            values = kv_ref[pl.ds(at, bk), hc:]
            ids = lax.broadcasted_iota(jnp.int32, (bk, bq), 0) + kb * bk
            keep = (ids >= low) & (ids < high)
            fresh, all_p, all_s = [], [], []
            for h in range(hh):
                scores = rows_dot_t(keys, heads_q[h])
                probs = jnp.where(keep, jnp.exp(scores - logs[h]), 0.0)
                grad_probs = rows_dot_t(values, heads_g[h])
                grad_scores = (probs * (grad_probs - delta[h])).astype(BF16)
                all_p.append(probs.astype(BF16))
                all_s.append(grad_scores)
                key_cols = kt_ref[kb, h * HEAD_DIM : (h + 1) * HEAD_DIM, :]
                fresh.append(state[h] + rows_dot(key_cols, grad_scores))
            acc_ref[pl.ds(at, bk), :hc] += rows_dot(jnp.concatenate(all_s, axis=1), stack_q)
            acc_ref[pl.ds(at, bk), hc:] += rows_dot(jnp.concatenate(all_p, axis=1), stack_g)
            return tuple(fresh)

        start = tuple(jnp.zeros((HEAD_DIM, bq), F32) for _ in range(hh))
        state = lax.fori_loop(first, last, one_key_block, start)
        dq_ref[rows, :] = (jnp.concatenate(state, axis=0).T * score_scale).astype(BF16)
        return carry

    lax.fori_loop(0, nq, one_query_block, 0)
    dkv_ref[...] = acc_ref[...].astype(BF16)


def attend_back_call(q, kv, lohi, att, datt, lse, bq, bk):
    P_, hc = q.shape
    hh = hc // HEAD_DIM
    vm = pl.BlockSpec(memory_space=pltpu.VMEM)
    return pl.pallas_call(
        functools.partial(attend_back_kernel, (P_, hc, hh, bq, bk)),
        out_shape=(
            jax.ShapeDtypeStruct((P_, hc), BF16),
            jax.ShapeDtypeStruct((3 * P_, 2 * hc), BF16),
        ),
        in_specs=[vm, vm, vm, vm, vm, vm],
        out_specs=(vm, vm),
        scratch_shapes=[
            pltpu.VMEM((3 * P_ // bk, hc, bk), BF16),
            pltpu.VMEM((3 * P_, 2 * hc), F32),
        ],
        compiler_params=pltpu.CompilerParams(vmem_limit_bytes=BACK_VMEM * MIB),
        name="attend_back_stage",
    )(q, kv, lohi, att, datt, lse)


def layer_stats(summed):
    center = summed - jnp.mean(summed, axis=1, keepdims=True)
    inverse = lax.rsqrt(jnp.mean(center * center, axis=1, keepdims=True) + epsilon)
    return center * inverse, inverse


def layer_back(grad, normed, inverse):
    first = jnp.mean(grad, axis=1, keepdims=True)
    second = jnp.mean(grad * normed, axis=1, keepdims=True)
    return inverse * (grad - first - normed * second)


def col_sum(x):
    return jnp.sum(x, axis=0, keepdims=True)


def middle_kernel(
    dims,
    att_ref,
    hidden_ref,
    cot_ref,
    par_ref,
    wout_ref,
    wout_o_ref,
    wup_ref,
    wdn_ref,
    wdn_o_ref,
    bup_ref,
    result_ref,
    dfirst_ref,
    datt_ref,
    gdn_ref,
    gup_ref,
    gout_ref,
    stats_ref,
    gbup_ref,
    gdn_done_ref,
    wout_v,
    wup_v,
    wdn_v,
    attp,
    fa,
    da,
    dfa,
    act,
    slope,
    dup,
    stage,
    recv,
    normed_v,
    first_v,
    dnorm_v,
    gdn_v,
    gdn_r,
    gdn_h,
    gdn_l,
    gdn_x,
    gdn_f,
    gup_v,
    gup_r,
    gout_v,
    gout_r,
    gb_v,
    gb_r,
    dattst,
    ap_ss,
    ap_rs,
    sc_ss,
    sc_rs,
    ag_ss,
    ag_rs,
    gx_ss,
    gx_rs,
    dx_ss,
    dx_rs,
    zsem,
    loc,
):
    S, n, C, L, D, hc, F1 = dims
    Dn, F2, Ph = D // n, 2 * F1, C * L
    z = lax.axis_index("seq")
    s = lax.axis_index("shard")
    core = lax.rem(s, 2)
    chip = s // 2
    other = 1 - core
    partner = (z, 2 * chip + other)

    loads = [
        pltpu.make_async_copy(wout_ref, wout_v.at[core], loc.at[0]),
        pltpu.make_async_copy(wout_o_ref, wout_v.at[other], loc.at[1]),
        pltpu.make_async_copy(wup_ref, wup_v, loc.at[2]),
        pltpu.make_async_copy(wdn_ref, wdn_v.at[core], loc.at[3]),
        pltpu.make_async_copy(wdn_o_ref, wdn_v.at[other], loc.at[4]),
    ]
    for load in loads:
        load.start()

    def peer(j):
        return (z, 2 * flip(chip, j, C) + core)

    barrier = pltpu.get_barrier_semaphore()
    pl.semaphore_signal(barrier, inc=1, device_id=partner, device_id_type=MESH)
    for j in range(1, C):
        pl.semaphore_signal(barrier, inc=1, device_id=peer(j), device_id_type=MESH)
    for d in (1, S - 1):
        pl.semaphore_signal(barrier, inc=1, device_id=(lax.rem(z + d, S), s), device_id_type=MESH)
    pl.semaphore_wait(barrier, C + 2)

    def put_stat(row, value):
        for i in range(n):
            stats_ref[i, row : row + 1] = value[:, i * hc : (i + 1) * hc]

    def give(i, src, dst):
        remote(src, dst, gx_ss.at[i], gx_rs.at[i], partner).start()

    def taken(i, src, dst):
        await_recv(dst, gx_rs.at[i], partner)

    def gather_of(r, buf):
        return Gather(C, chip, peer, L, lambda c: buf.at[c], ag_ss.at[r], ag_rs.at[r])

    gathers = [gather_of(0, fa), gather_of(1, da), gather_of(2, dfa)]
    out_sum = Scatter(C, peer, L, stage.at[0], recv.at[0], sc_ss.at[0], sc_rs.at[0])

    def hand(r, j, part):
        stage[r, j] = part.astype(BF16)
        remote(
            stage.at[r, j], recv.at[r, j], sc_ss.at[r, j, 0], sc_rs.at[r, j, 0], peer(j)
        ).start()

    def collected(r, total):
        for j in range(1, C):
            await_recv(recv.at[r, j], sc_rs.at[r, j, 0], peer(j))
            total = total + recv[r, j].astype(F32)
        return total

    par = jnp.concatenate([par_ref[i] for i in range(n)], axis=1)
    b_out, gain1, shift1 = par[0:1], par[1:2], par[2:3]
    b_down, gain2, shift2 = par[3:4], par[4:5], par[5:6]

    remote(att_ref.at[:, other], attp, ap_ss.at[0], ap_rs.at[0], partner).start()
    loads[0].wait()
    loads[1].wait()
    await_recv(attp, ap_rs.at[0], partner)

    def out_part(j):
        c = flip(chip, j, C)
        return rows_dot(att_ref[c, core], wout_v[core]) + rows_dot(attp[c], wout_v[other])

    first_sum = out_sum.collect(out_sum.send(out_part) + hidden_ref[...] + b_out)
    normed_one, inverse_one = layer_stats(first_sum)
    normed_v[...] = normed_one
    first_norm = normed_one * gain1 + shift1
    first_v[...] = first_norm
    fa[chip] = first_norm.astype(BF16)
    gathers[0].send(fa.at[chip])

    loads[2].wait()
    loads[3].wait()
    loads[4].wait()
    first_core = core == 0
    bias_up = bup_ref[...]

    def up_part(j):
        c = flip(chip, j, C)
        pre = rows_dot(fa[c], wup_v[...].reshape(D, F2)) + bias_up
        half = 0.5 * (1.0 + lax.erf(pre * root_half))
        act[c] = (pre * half).astype(BF16)
        slope[c] = half + pre * jnp.exp(-0.5 * pre * pre) * inv_root_two_pi
        return rows_dot(act[c], wdn_v[...].reshape(F2, D))

    own = up_part(0)
    gathers[0].relay()

    def up_step(j, carry):
        gathers[0].arrived(j)
        hand(1, j, up_part(j))
        return carry

    lax.fori_loop(1, C, up_step, 0)
    second_sum = collected(1, own + first_v[...] + b_down)
    normed_two, inverse_two = layer_stats(second_sum)
    result_ref[...] = (normed_two * gain2 + shift2).astype(BF16)
    grad_rows = cot_ref[...].astype(F32)
    put_stat(0, col_sum(grad_rows * normed_two))
    put_stat(1, col_sum(grad_rows))
    d_second = layer_back(grad_rows * gain2, normed_two, inverse_two)
    put_stat(2, col_sum(d_second))
    dnorm_v[...] = d_second
    da[chip] = d_second.astype(BF16)
    gathers[1].send(da.at[chip])

    def down_back(j):
        c = flip(chip, j, C)
        d_up = rows_dot_t(da[c], wdn_v[...].reshape(F2, D)) * slope[c]
        gb_v[...] += col_sum(d_up)
        dup[c] = d_up.astype(BF16)
        return rows_dot_t(dup[c], wup_v[...].reshape(D, F2))

    gb_v[...] = jnp.zeros_like(gb_v)
    own = down_back(0)
    gathers[1].relay()

    def back_step(j, carry):
        gathers[1].arrived(j)
        hand(2, j, down_back(j))
        return carry

    lax.fori_loop(1, C, back_step, 0)
    dnorm_v[...] = dnorm_v[...] + own

    tile = 256
    da_all = da[...].reshape(Ph, D)

    per_half = F1 // tile
    per_tile = gdn_v.shape[1] // per_half

    def down_grad(i, carry):
        t = lax.rem(i + other * per_half, 2 * per_half)
        cols = pl.ds(pl.multiple_of(t * tile, tile), tile)
        res = cols_dot(act[:, :, cols].reshape(Ph, tile), da_all).astype(BF16)
        gdn_v[t // per_half, pl.ds(lax.rem(t, per_half) * per_tile, per_tile)] = res.reshape(
            per_tile, tile // per_tile, D
        )
        return carry

    lax.fori_loop(0, per_half, down_grad, 0)
    give(0, gdn_v.at[other], gdn_r)
    lax.fori_loop(per_half, 2 * per_half, down_grad, 0)

    def up_grad(c, carry):
        cols = pl.ds(pl.multiple_of(c * 2 * Dn, 128), 2 * Dn)
        res = cols_dot(fa[:, :, cols].reshape(Ph, 2 * Dn), dup[...].reshape(Ph, F2)).astype(BF16)
        gup_v[c, 0] = res[:Dn]
        gup_v[c, 1] = res[Dn:]
        return carry

    early = gdn_h.shape[0]
    taken(0, None, gdn_r)
    gdn_h[...] = (gdn_v[core, :early].astype(F32) + gdn_r[:early].astype(F32)).astype(BF16)
    gdn_ref[...] = (gdn_v[core, early:].astype(F32) + gdn_r[early:].astype(F32)).astype(BF16)
    chain = Chain(S, z, s, gdn_h, gdn_l, gdn_x, gdn_f, zsem)
    chain.give_out(0, early)

    lax.fori_loop(0, C, up_grad, 0)
    give(1, gup_v.at[:, other], gup_r)
    gb_r[0] = jnp.where(first_core, gb_v[:, F1:], gb_v[:, :F1])
    give(2, gb_r.at[0], gb_r.at[1])
    chain.run(0, 2)
    d_first_norm = collected(2, dnorm_v[...])
    normed_one = normed_v[...]
    put_stat(3, col_sum(d_first_norm * normed_one))
    put_stat(4, col_sum(d_first_norm))
    d_first = layer_back(d_first_norm * gain1, normed_one, inverse_one)
    put_stat(5, col_sum(d_first))
    stats_ref[:, 6:8] = jnp.zeros((n, 2, hc), F32)
    dfirst_ref[...] = d_first
    dfa[chip] = d_first.astype(BF16)
    gathers[2].send(dfa.at[chip])

    def att_back(j, carry):
        chain.run(2 * j + 2, 2 * j + 4)

        @pl.when(j == 1)
        def _():
            gathers[2].relay()

        gathers[2].arrived(j)
        c = flip(chip, j, C)
        datt_ref[c, core] = rows_dot_t(dfa[c], wout_v[core]).astype(BF16)
        dattst[j] = rows_dot_t(dfa[c], wout_v[other]).astype(BF16)
        remote(dattst.at[j], datt_ref.at[c, core], dx_ss.at[j], dx_rs.at[j], partner).start()
        return carry

    lax.fori_loop(0, C, att_back, 0)
    dfa_all = dfa[...].reshape(Ph, D)
    gout_v[0] = cols_dot(attp[...].reshape(Ph, hc), dfa_all).astype(BF16)
    give(3, gout_v.at[0], gout_r)
    gout_v[1] = cols_dot(att_ref[:, core].reshape(Ph, hc), dfa_all).astype(BF16)

    chain.run(2 * C + 2, chain.slots)
    taken(1, None, gup_r)
    gup_ref[...] = (gup_v[:, core].astype(F32) + gup_r[...].astype(F32)).astype(BF16)
    taken(2, None, gb_r.at[1])
    gbup_ref[...] = jnp.where(first_core, gb_v[:, :F1], gb_v[:, F1:]) + gb_r[1]
    taken(3, None, gout_r)
    gout_ref[...] = (gout_v[1].astype(F32) + gout_r[...].astype(F32)).astype(BF16)

    chain.settle()
    out_sum.settle()
    for gather in gathers:
        gather.settle()
    gdn_done_ref[...] = gdn_f[...]
    await_send(attp, ap_ss.at[0], partner)
    await_send(gdn_r, gx_ss.at[0], partner)
    await_send(gup_r, gx_ss.at[1], partner)
    await_send(gb_r.at[0], gx_ss.at[2], partner)
    await_send(gout_r, gx_ss.at[3], partner)

    def settle(j, carry):
        c = flip(chip, j, C)
        await_recv(datt_ref.at[c, other], dx_rs.at[j], partner)
        await_send(dattst.at[j], dx_ss.at[j], partner)

        @pl.when(j > 0)
        def _():
            for r in range(1, 3):
                await_send(stage.at[r, j], sc_ss.at[r, j, 0], peer(j))

        return carry

    lax.fori_loop(0, C, settle, 0)


def middle_call(S, n, att, hidden, cot, par, wout, wout_o, wup2, wdn, wdn_o, bup):
    C = n // 2
    L, D = hidden.shape
    hc = D // n
    F1 = wdn.shape[0]
    F2 = 2 * F1
    dims = (S, n, C, L, D, hc, F1)
    dma = pltpu.SemaphoreType.DMA
    vm = pl.BlockSpec(memory_space=pltpu.VMEM)
    anyw = pl.BlockSpec(memory_space=pl.ANY)
    sds = jax.ShapeDtypeStruct
    Dn = D // n
    pc, early = 16, EARLY_PIECES
    return pl.pallas_call(
        functools.partial(middle_kernel, dims),
        out_shape=(
            sds((L, D), BF16),
            sds((L, D), F32),
            sds((C, 2, L, hc), BF16),
            sds((pc - early, F1 // pc, D), BF16),
            sds((C, Dn, F2), BF16),
            sds((hc, D), BF16),
            sds((n, 8, hc), F32),
            sds((1, F1), F32),
            sds((early, F1 // pc, D), BF16),
        ),
        in_specs=[vm, vm, vm, vm, anyw, anyw, anyw, anyw, anyw, vm],
        out_specs=(vm,) * 9,
        scratch_shapes=[
            pltpu.VMEM((2, hc, D), BF16),
            pltpu.VMEM((n, Dn, F2), BF16),
            pltpu.VMEM((2, F1, D), BF16),
            pltpu.VMEM((C, L, hc), BF16),
            pltpu.VMEM((C, L, D), BF16),
            pltpu.VMEM((C, L, D), BF16),
            pltpu.VMEM((C, L, D), BF16),
            pltpu.VMEM((C, L, F2), BF16),
            pltpu.VMEM((C, L, F2), F32),
            pltpu.VMEM((C, L, F2), BF16),
            pltpu.VMEM((3, C, L, D), BF16),
            pltpu.VMEM((3, C, L, D), BF16),
            pltpu.VMEM((L, D), F32),
            pltpu.VMEM((L, D), F32),
            pltpu.VMEM((L, D), F32),
            pltpu.VMEM((2, pc, F1 // pc, D), BF16),
            pltpu.VMEM((pc, F1 // pc, D), BF16),
            pltpu.VMEM((early, F1 // pc, D), BF16),
            pltpu.VMEM((early, F1 // pc, D), BF16),
            pltpu.VMEM((early, F1 // pc, D), BF16),
            pltpu.VMEM((early, F1 // pc, D), BF16),
            pltpu.VMEM((C, 2, Dn, F2), BF16),
            pltpu.VMEM((C, Dn, F2), BF16),
            pltpu.VMEM((2, hc, D), BF16),
            pltpu.VMEM((hc, D), BF16),
            pltpu.VMEM((1, F2), F32),
            pltpu.VMEM((2, 1, F1), F32),
            pltpu.VMEM((C, L, hc), BF16),
            dma((1,)),
            dma((1,)),
            dma((3, C, 2)),
            dma((3, C, 2)),
            dma((3, C, 2)),
            dma((3, C, 2)),
            dma((4,)),
            dma((4,)),
            dma((C,)),
            dma((C,)),
            dma((6, early)),
            dma((5,)),
        ],
        compiler_params=pltpu.CompilerParams(
            collective_id=1, has_side_effects=True, vmem_limit_bytes=MIDDLE_VMEM * MIB
        ),
        name="middle_stage",
    )(att, hidden, cot, par, wout, wout_o, wup2, wdn, wdn_o, bup)


def exit_kernel(
    dims,
    dq_ref,
    dkv_ref,
    hid_ref,
    wq_ref,
    dfirst_ref,
    stats_ref,
    gbup_ref,
    pos_ref,
    gupc_ref,
    goutc_ref,
    gdnc_ref,
    ginp_ref,
    dh_ref,
    gq_f,
    up_f,
    out_f,
    dn_f,
    gtable_ref,
    small_ref,
    gbo_ref,
    zr,
    own3,
    got3,
    x6,
    stage,
    recv,
    dhb,
    gq_v,
    gq_r,
    gq_s,
    gq_o,
    gq_l,
    gq_x,
    up_o,
    up_l,
    up_x,
    out_o,
    out_l,
    out_x,
    dn_o,
    dn_l,
    dn_x,
    plane,
    prod,
    st_r,
    st_v,
    zst,
    zgb,
    zk_ss,
    zk_rs,
    x_ss,
    x_rs,
    sc_ss,
    sc_rs,
    st_ss,
    st_rs,
    zs_ss,
    zs_rs,
    gq_ss,
    gq_rs,
    gx_ss,
    gx_rs,
    ua_ss,
    ua_rs,
    qc,
    uc,
    oc,
    dc,
    zl_ss,
    zl_rs,
    ag_ss,
    ag_rs,
    pf_ss,
    pf_rs,
    loc,
):
    S, n, C, L, D, hc, F1, R, rt = dims
    Dn, Ph = D // n, C * L
    z = lax.axis_index("seq")
    s = lax.axis_index("shard")
    core = lax.rem(s, 2)
    chip = s // 2
    other = 1 - core
    twin = 2 * chip + other
    partner = (z, twin)
    first_core = core == 0

    def peer(j):
        return (z, 2 * flip(chip, j, C) + core)

    barrier = pltpu.get_barrier_semaphore()
    for d in range(1, n):
        pl.semaphore_signal(barrier, inc=1, device_id=(z, flip(s, d, n)), device_id_type=MESH)
    for d in range(1, S):
        pl.semaphore_signal(barrier, inc=1, device_id=(lax.rem(z + d, S), s), device_id_type=MESH)
    pl.semaphore_wait(barrier, n - 1 + S - 1)

    for j in range(C - 1, -1, -1):
        c = flip(chip, j, C)

        @pl.when(z > 0)
        def _():
            remote(
                dkv_ref.at[0, c], zr.at[1, c], zk_ss.at[j, 0], zk_rs.at[j, 1], (z - 1, s)
            ).start()

        @pl.when(z < S - 1)
        def _():
            remote(
                dkv_ref.at[2, c], zr.at[0, c], zk_ss.at[j, 1], zk_rs.at[j, 0], (z + 1, s)
            ).start()

    quarter = Dn // 4
    mine = pl.ds(4 * chip, 4)

    def block_of(j):
        return pl.ds(4 * flip(chip, j, C), 4)

    for j in range(C - 1, 0, -1):
        remote(
            gupc_ref.at[flip(chip, j, C)], up_o.at[mine], ua_ss.at[j], ua_rs.at[j], peer(j)
        ).start()
    up_o[mine] = gupc_ref[chip]
    out_o[...] = goutc_ref[...].reshape(4, quarter, D)
    dn_o[...] = gdnc_ref[...]
    wide = Chain(S, z, s, up_o, up_l, up_x, up_f, uc)
    square = Chain(S, z, s, out_o, out_l, out_x, out_f, oc)
    late = Chain(S, z, s, dn_o, dn_l, dn_x, dn_f, dc)
    inner = Chain(S, z, s, gq_o, gq_l, gq_x, gq_f, qc)
    late.give_out(0, late.pieces)
    square.give_out(0, square.pieces)
    starts = [0, late.pieces, late.pieces + square.pieces]
    starts.append(starts[2] + wide.pieces)
    last_step = starts[3] + inner.slots

    def chain_step(m, carry=0):
        for chain, begin in zip((late, square, wide, inner), starts):
            chain.slot(m - begin)
        return carry

    def chain_steps(begin, end):
        lax.fori_loop(begin, end, chain_step, 0)

    st_r[s] = stats_ref[s]
    for d in range(1, n):
        to = flip(s, d, n)
        remote(stats_ref.at[to], st_r.at[s], st_ss.at[d], st_rs.at[d], (z, to)).start()

    def fold(k, carry):
        j = C - 1 - k
        c = flip(chip, j, C)
        whole = dkv_ref[1, c].astype(F32)

        @pl.when(z > 0)
        def _():
            await_recv(zr.at[0, c], zk_rs.at[j, 0], (z - 1, s))

        @pl.when(z < S - 1)
        def _():
            await_recv(zr.at[1, c], zk_rs.at[j, 1], (z + 1, s))

        whole = whole + jnp.where(z > 0, zr[0, c].astype(F32), 0.0)
        whole = whole + jnp.where(z < S - 1, zr[1, c].astype(F32), 0.0)
        whole = whole.astype(BF16)
        own3[c, :, :, :hc] = dq_ref[c]
        own3[c, :, :, hc:] = whole
        remote(own3.at[c, other], got3.at[c], x_ss.at[j], x_rs.at[j], partner).start()
        sums = jnp.sum(own3[c].astype(F32), axis=(0, 1), keepdims=False)
        st_v[0:1] += sums[None, :hc]
        st_v[1:2] += sums[None, 2 * hc :]
        return carry

    st_v[...] = jnp.zeros_like(st_v)
    lax.fori_loop(0, C, fold, 0)

    def partial(j):
        c = flip(chip, j, C)
        await_recv(got3.at[c], x_rs.at[j], partner)
        mine, theirs = own3[c, core], got3[c]
        low = jnp.where(first_core, mine, theirs)
        high = jnp.where(first_core, theirs, mine)
        pieces = []
        for part in range(3):
            pieces += [low[:, part * hc : (part + 1) * hc], high[:, part * hc : (part + 1) * hc]]
        x6[c] = jnp.concatenate(pieces, axis=1)
        return rows_dot_t(x6[c], wq_ref[...].reshape(D, 6 * hc))

    tokens_sum = Scatter(C, peer, L, stage, recv, sc_ss, sc_rs)
    total = tokens_sum.send(partial) + dfirst_ref[...]
    chain_steps(0, 2)

    def qkv_grad(c, carry):
        chain_step(2 + c)
        cols = pl.ds(pl.multiple_of(c * 2 * Dn, 128), 2 * Dn)
        res = cols_dot(hid_ref[:, :, cols].reshape(Ph, 2 * Dn), x6[...].reshape(Ph, 6 * hc))
        gq_v[c] = res.astype(BF16).reshape(2, 4, quarter, 6 * hc)
        return carry

    lax.fori_loop(0, C, qkv_grad, 0)
    remote(gq_v.at[:, other], gq_r, gq_ss.at[0], gq_rs.at[0], partner).start()

    sums = st_r[s]
    for d in range(1, n):
        src = flip(s, d, n)
        await_recv(st_r.at[src], st_rs.at[d], (z, src))
    sums = st_r[0]
    for i in range(1, n):
        sums = sums + st_r[i]
    zst[z] = sums
    zst[z, 6:8] = st_v[...]
    zgb[z] = gbup_ref[...]
    for d in range(1, S):
        to = (lax.rem(z + d, S), s)
        remote(zst.at[z], zst.at[z], zs_ss.at[d, 0], zs_rs.at[d, 0], to).start()
        remote(zgb.at[z], zgb.at[z], zs_ss.at[d, 1], zs_rs.at[d, 1], to).start()

    for j in range(1, C):
        await_recv(up_o.at[block_of(j)], ua_rs.at[j], peer(j))
    wide.give_out(0, 4)
    chain_steps(C + 2, C + 4)
    await_recv(gq_r, gq_rs.at[0], partner)
    gq_s[...] = (gq_v[:, core].astype(F32) + gq_r[...].astype(F32)).astype(BF16)
    for j in range(C - 1, 0, -1):
        remote(
            gq_s.at[flip(chip, j, C)], gq_o.at[mine], gx_ss.at[j], gx_rs.at[j], peer(j)
        ).start()
    gq_o[mine] = gq_s[chip]

    total = tokens_sum.collect(total)
    ginp = total.astype(BF16)
    ginp_ref[...] = ginp
    dhb[...] = ginp
    keep = pltpu.make_async_copy(dhb, dh_ref.at[z, s], loc.at[0])
    keep.start()

    def gather_of(at):
        return Gather(
            C, chip, peer, L, lambda c: dh_ref.at[at, 2 * c + core], ag_ss.at[at], ag_rs.at[at]
        )

    def broadcast(src, at):
        gather_of(at).send(src)
        remote(src, dh_ref.at[at, s], pf_ss.at[at, 0], pf_rs.at[at, 0], partner).start()

    def pass_on(d):
        @pl.when(z - d >= 0)
        def _():
            gather_of(z - d).relay()

        if d:

            @pl.when(z + d <= S - 1)
            def _():
                gather_of(z + d).relay()

    @pl.when(z < S - 1)
    def _():
        remote(dhb, dh_ref.at[z, s], zl_ss.at[z, 0], zl_rs.at[z, 0], (z + 1, s)).start()

    @pl.when(z > 0)
    def _():
        remote(dhb, dh_ref.at[z, s], zl_ss.at[z, 1], zl_rs.at[z, 1], (z - 1, s)).start()

    broadcast(dhb, z)
    wide.give_out(4, wide.pieces)
    chain_steps(C + 4, C + 7)
    for d in range(1, S):

        @pl.when(z - d >= 0)
        def _():
            at = z - d
            await_recv(dh_ref.at[at, s], zl_rs.at[at, 0], (z - 1, s))

            @pl.when(z < S - 1)
            def _():
                remote(
                    dh_ref.at[at, s], dh_ref.at[at, s], zl_ss.at[at, 0], zl_rs.at[at, 0], (z + 1, s)
                ).start()

            broadcast(dh_ref.at[at, s], at)

        @pl.when(z + d <= S - 1)
        def _():
            at = z + d
            await_recv(dh_ref.at[at, s], zl_rs.at[at, 1], (z + 1, s))

            @pl.when(z > 0)
            def _():
                remote(
                    dh_ref.at[at, s], dh_ref.at[at, s], zl_ss.at[at, 1], zl_rs.at[at, 1], (z - 1, s)
                ).start()

            broadcast(dh_ref.at[at, s], at)

        if d == 2:
            for j in range(1, C):
                await_recv(gq_o.at[block_of(j)], gx_rs.at[j], peer(j))
            inner.give_out(0, inner.pieces)
        pass_on(d - 1)
        chain_steps(C + 3 + 4 * d, C + 7 + 4 * d)

    def relay(at):
        for j in range(1, C):
            src = 2 * flip(chip, j, C) + core
            gather_of(at).arrived(j)
            remote(
                dh_ref.at[at, src], dh_ref.at[at, src], pf_ss.at[at, j], pf_rs.at[at, j], partner
            ).start()

    pass_on(S - 1)
    seen = C + 3 + 4 * S

    def plane_sum(t, carry):
        at = flip(z, t, S)
        chain_step(seen + 6 * t)
        relay(at)
        chain_step(seen + 6 * t + 1)

        for j in range(C):
            src = 2 * flip(chip, j, C) + other
            await_recv(dh_ref.at[at, src], pf_rs.at[at, j], partner)

        @pl.when(t == 0)
        def _():
            keep.wait()

        load = pltpu.make_async_copy(dh_ref.at[at], plane, loc.at[1])
        load.start()
        load.wait()

        def rows_tile(r, carry):
            chain_step(seen + 6 * t + 2 + r)
            start = pl.multiple_of(r * rt, rt)
            ids = lax.broadcasted_iota(jnp.int32, (rt, L), 0) + (start + s * R)
            hot = jnp.concatenate(
                [jnp.where(ids == pos_ref[at, i], 1.0, 0.0).astype(BF16) for i in range(n)], axis=1
            )
            prod[at, pl.ds(start, rt), :] = rows_dot(hot, plane[...].reshape(n * L, D))
            return carry

        lax.fori_loop(0, R // rt, rows_tile, 0)
        return carry

    lax.fori_loop(0, S, plane_sum, 0)

    def add_tile(r, carry):
        at = pl.ds(pl.multiple_of(r * rt, rt), rt)
        rows = prod[0, at]
        for i in range(1, S):
            rows = rows + prod[i, at]
        gtable_ref[at] = rows.astype(BF16)
        return carry

    lax.fori_loop(0, R // rt, add_tile, 0)

    chain_steps(seen + 6 * S, last_step)
    for d in range(1, S):
        src = lax.rem(z + S - d, S)
        await_recv(zst.at[src], zs_rs.at[d, 0], (src, s))
        await_recv(zgb.at[src], zs_rs.at[d, 1], (src, s))
    small, big = zst[0], zgb[0]
    for i in range(1, S):
        small = small + zst[i]
        big = big + zgb[i]
    small_ref[...] = small
    gbo_ref[...] = big

    def settle_plane(at, carry):
        for j in range(C):
            await_send(dhb, pf_ss.at[at, j], partner)
        gather_of(at).settle()
        return carry

    lax.fori_loop(0, S, settle_plane, 0)
    for at in range(S):

        @pl.when((z >= at) & (z < S - 1))
        def _():
            await_send(dhb, zl_ss.at[at, 0], (z + 1, s))

        @pl.when((z <= at) & (z > 0))
        def _():
            await_send(dhb, zl_ss.at[at, 1], (z - 1, s))

    for j in range(C):

        @pl.when(z > 0)
        def _():
            await_send(zr.at[0, 0], zk_ss.at[j, 0], (z - 1, s))

        @pl.when(z < S - 1)
        def _():
            await_send(zr.at[0, 0], zk_ss.at[j, 1], (z + 1, s))

        await_send(got3.at[0], x_ss.at[j], partner)
    for d in range(1, n):
        await_send(st_r.at[s], st_ss.at[d], (z, flip(s, d, n)))
    for d in range(1, S):
        to = (lax.rem(z + d, S), s)
        await_send(zst.at[z], zs_ss.at[d, 0], to)
        await_send(zgb.at[z], zs_ss.at[d, 1], to)
    for j in range(1, C):
        await_send(gq_s.at[chip], gx_ss.at[j], peer(j))
        await_send(gupc_ref.at[chip], ua_ss.at[j], peer(j))
    tokens_sum.settle()
    wide.settle()
    square.settle()
    late.settle()
    inner.settle()
    await_send(gq_r, gq_ss.at[0], partner)


def exit_call(S, n, R, dq, dkv, hid_half, wq, dfirst, stats, gbup, pos, gupc, goutc, gdnc):
    C = n // 2
    L, D = dfirst.shape
    hc = D // n
    F1 = gbup.shape[1]
    Dn = D // n
    F2 = gupc.shape[3]
    dims = (S, n, C, L, D, hc, F1, R, 256)
    dma = pltpu.SemaphoreType.DMA
    vm = pl.BlockSpec(memory_space=pltpu.VMEM)
    anyw = pl.BlockSpec(memory_space=pl.ANY)
    sds = jax.ShapeDtypeStruct
    return pl.pallas_call(
        functools.partial(exit_kernel, dims),
        out_shape=(
            sds((L, D), BF16),
            sds((S, n, L, D), BF16),
            sds((4 * C, Dn // 4, 6 * hc), BF16),
            sds((4 * C, Dn // 4, F2), BF16),
            sds((4, Dn // 4, D), BF16),
            sds(gdnc.shape, BF16),
            sds((R, D), BF16),
            sds((8, hc), F32),
            sds((1, F1), F32),
        ),
        in_specs=[vm] * 11,
        out_specs=(vm, anyw) + (vm,) * 7,
        scratch_shapes=[
            pltpu.VMEM((2, C, 2, L, 2 * hc), BF16),
            pltpu.VMEM((C, 2, L, 3 * hc), BF16),
            pltpu.VMEM((C, L, 3 * hc), BF16),
            pltpu.VMEM((C, L, 6 * hc), BF16),
            pltpu.VMEM((C, L, D), BF16),
            pltpu.VMEM((C, L, D), BF16),
            pltpu.VMEM((L, D), BF16),
            pltpu.VMEM((C, 2, 4, Dn // 4, 6 * hc), BF16),
            pltpu.VMEM((C, 4, Dn // 4, 6 * hc), BF16),
            pltpu.VMEM((C, 4, Dn // 4, 6 * hc), BF16),
            pltpu.VMEM((4 * C, Dn // 4, 6 * hc), BF16),
            pltpu.VMEM((4 * C, Dn // 4, 6 * hc), BF16),
            pltpu.VMEM((4 * C, Dn // 4, 6 * hc), BF16),
            pltpu.VMEM((4 * C, Dn // 4, F2), BF16),
            pltpu.VMEM((4 * C, Dn // 4, F2), BF16),
            pltpu.VMEM((4 * C, Dn // 4, F2), BF16),
            pltpu.VMEM((4, Dn // 4, D), BF16),
            pltpu.VMEM((4, Dn // 4, D), BF16),
            pltpu.VMEM((4, Dn // 4, D), BF16),
            pltpu.VMEM(gdnc.shape, BF16),
            pltpu.VMEM(gdnc.shape, BF16),
            pltpu.VMEM(gdnc.shape, BF16),
            pltpu.VMEM((n, L, D), BF16),
            pltpu.VMEM((S, R, D), F32),
            pltpu.VMEM((n, 8, hc), F32),
            pltpu.VMEM((2, hc), F32),
            pltpu.VMEM((S, 8, hc), F32),
            pltpu.VMEM((S, 1, F1), F32),
            dma((C, 2)),
            dma((C, 2)),
            dma((C,)),
            dma((C,)),
            dma((C, 2)),
            dma((C, 2)),
            dma((n,)),
            dma((n,)),
            dma((S, 2)),
            dma((S, 2)),
            dma((1,)),
            dma((1,)),
            dma((C,)),
            dma((C,)),
            dma((C,)),
            dma((C,)),
            dma((6, 4 * C)),
            dma((6, 4 * C)),
            dma((6, 4)),
            dma((6, gdnc.shape[0])),
            dma((S, 2)),
            dma((S, 2)),
            dma((S, C, 2)),
            dma((S, C, 2)),
            dma((S, C)),
            dma((S, C)),
            dma((2,)),
        ],
        compiler_params=pltpu.CompilerParams(
            collective_id=2, has_side_effects=True, vmem_limit_bytes=EXIT_VMEM * MIB
        ),
        name="exit_stage",
    )(dq, dkv, hid_half, wq, dfirst, stats, gbup, pos, gupc, goutc, gdnc)


def finish_kernel(
    dims,
    table_ref,
    gq_ref,
    up_ref,
    out_ref,
    early_ref,
    late_ref,
    res_ref,
    inp_ref,
    small_ref,
    gb_ref,
    table_o,
    gq_o,
    up_o,
    out_o,
    dn_o,
    res_o,
    inp_o,
    gb_o,
    *small_o,
):
    C, D, hc = dims
    i = pl.program_id(0)
    h2 = 2 * hc
    F2 = up_ref.shape[3]
    table_o[...] = table_ref[...].astype(F32)
    for c in range(C):
        up_o[:, c * F2 : (c + 1) * F2] = up_ref[c, 0].astype(F32)
        for part in range(3):
            gq_o[:, part * D + c * h2 : part * D + (c + 1) * h2] = gq_ref[
                c, 0, :, part * h2 : (part + 1) * h2
            ].astype(F32)
    out_o[...] = out_ref[0].astype(F32)
    piece = early_ref.shape[0] * early_ref.shape[1]
    dn_o[...] = jnp.where(i < 4, early_ref[...], late_ref[...]).reshape(piece, D).astype(F32)
    res_o[...] = res_ref[...]
    inp_o[...] = inp_ref[...]
    gb_o[...] = gb_ref[...]
    for r, o in enumerate(small_o):
        o[...] = small_ref[r : r + 1]


def finish_call(n, table, gq, up, out, early, late, res, inp, small, gb):
    C = n // 2
    R, D = table.shape
    L = res.shape[0]
    Dn = D // n
    hc = Dn
    q, F2 = up.shape[1:]
    h = q // 2
    piece = early.shape[1]
    F1 = gb.shape[1]
    sds = jax.ShapeDtypeStruct
    steps = 8
    two = lambda rows, cols: pl.BlockSpec((rows, cols), lambda i: (i, 0))
    quad = lambda cols: pl.BlockSpec((C, 1, h, cols), lambda i: (0, i // 2, i % 2, 0))
    fixed = lambda rows, cols: pl.BlockSpec((rows, cols), lambda i: (0, 0))
    return pl.pallas_call(
        functools.partial(finish_kernel, (C, D, hc)),
        grid=(steps,),
        out_shape=(
            sds((R, D), F32),
            sds((Dn, 3 * D), F32),
            sds((Dn, C * F2), F32),
            sds((Dn, D), F32),
            sds((F1, D), F32),
            sds((L, D), BF16),
            sds((L, D), BF16),
            sds((1, F1), F32),
        )
        + (sds((1, hc), F32),) * 8,
        in_specs=[
            two(R // steps, D),
            quad(6 * hc),
            quad(F2),
            pl.BlockSpec((1, h, D), lambda i: (i // 2, i % 2, 0)),
            pl.BlockSpec((2, piece, D), lambda i: (jnp.minimum(i, 3), 0, 0)),
            pl.BlockSpec((2, piece, D), lambda i: (jnp.maximum(i - 4, 0), 0, 0)),
            two(L // steps, D),
            two(L // steps, D),
            fixed(8, hc),
            fixed(1, F1),
        ],
        out_specs=(
            two(R // steps, D),
            two(h, 3 * D),
            two(h, C * F2),
            two(h, D),
            two(2 * piece, D),
            two(L // steps, D),
            two(L // steps, D),
            fixed(1, F1),
        )
        + (fixed(1, hc),) * 8,
        compiler_params=pltpu.CompilerParams(vmem_limit_bytes=ATTEND_VMEM * MIB),
        name="finish_stage",
    )(
        table,
        gq.reshape(C, 4, q, 6 * hc),
        up.reshape(C, 4, q, F2),
        out,
        early,
        late,
        res,
        inp,
        small,
        gb,
    )


QUERY_BLOCK = 512
KEY_BLOCK = 512
BACK_KEY_BLOCK = 256
EARLY_PIECES = 8


def local(
    inputs,
    positions,
    segments,
    pos_table,
    w_qkv,
    b_query,
    b_value,
    w_out,
    b_out,
    ln1_gain,
    ln1_bias,
    w_up,
    b_up,
    w_down,
    b_down,
    ln2_gain,
    ln2_bias,
    cotangent,
):
    S, n = lax.axis_size("seq"), lax.axis_size("shard")
    L, D = inputs.shape
    P_, hc, C = L * n, D // n, n // 2
    R = pos_table.shape[0]
    row = lambda v: v.reshape(1, -1)
    rows = [row(v) for v in (b_out, ln1_gain, ln1_bias, b_down, ln2_gain, ln2_bias, b_query, b_value)]
    q, kv, hid_half, hidden, wq, wup2, wdn_o, wout_o, par_all, bup2, pos_glob, lohi = entry_call(
        S,
        n,
        row(positions),
        inputs,
        pos_table,
        w_qkv,
        w_up,
        w_down,
        w_out,
        segments.reshape(S * n, 1, L),
        row(b_up),
        rows,
    )
    q = q.reshape(P_, hc)
    kv = kv.reshape(3 * P_, 2 * hc)
    att, lse = attend_call(q, kv, lohi, QUERY_BLOCK, KEY_BLOCK)
    result, dfirst, datt, gdn_late, gup, gout, stats, gbup, gdn_early = middle_call(
        S,
        n,
        att.reshape(C, 2, L, hc),
        hidden,
        cotangent,
        par_all,
        w_out,
        wout_o,
        wup2,
        w_down,
        wdn_o,
        bup2,
    )
    dq, dkv = attend_back_call(
        q, kv, lohi, att, datt.reshape(P_, hc), lse, QUERY_BLOCK, BACK_KEY_BLOCK
    )
    ginp, dh, gqkv, gup, gout, gdn_late, gtable, small, gbo = exit_call(
        S,
        n,
        R,
        dq.reshape(C, 2, L, hc),
        dkv.reshape(3, C, 2, L, 2 * hc),
        hid_half,
        wq,
        dfirst,
        stats,
        gbup,
        pos_glob,
        gup.reshape(C, 4, D // n // 4, gup.shape[2]),
        gout,
        gdn_late,
    )
    gtable, gqkv, gup, gout, gdn, result, ginp, gbo, *small = finish_call(
        n, gtable, gqkv, gup, gout, gdn_early, gdn_late, result, ginp, small, gbo
    )
    small = [v[0] for v in small]
    return (
        result,
        ginp,
        gtable,
        gqkv,
        small[6],
        small[7],
        gout,
        small[5],
        small[3],
        small[4],
        gup,
        gbo[0],
        gdn,
        small[2],
        small[0],
        small[1],
    )


def solution(mesh):
    in_specs = (
        P(("seq", "shard"), None),
        P(("seq", "shard")),
        P(),
        P("shard", None),
        P("shard", None),
        P("shard"),
        P("shard"),
        P("shard", None),
        P("shard"),
        P("shard"),
        P("shard"),
        P("shard", None),
        P("shard"),
        P("shard", None),
        P("shard"),
        P("shard"),
        P("shard"),
        P(("seq", "shard"), None),
    )
    out_specs = (
        P(("seq", "shard"), None),
        P(("seq", "shard"), None),
        P("shard", None),
        P("shard", None),
        P("shard"),
        P("shard"),
        P("shard", None),
        P("shard"),
        P("shard"),
        P("shard"),
        P("shard", None),
        P("shard"),
        P("shard", None),
        P("shard"),
        P("shard"),
        P("shard"),
    )
    return jax.shard_map(local, mesh=mesh, in_specs=in_specs, out_specs=out_specs, check_vma=False)
```

```python
import functools
import math

import jax
import jax.numpy as jnp
from jax import lax
from jax.experimental import pallas as pl
from jax.experimental.pallas import tpu as pltpu
from jax.sharding import PartitionSpec as P

HEADS = 16
HEAD_DIM = 64
score_scale = 0.125
neg_large = -1e30
epsilon = 1e-06
root_half = 0.7071067811865476
inv_root_two_pi = 0.3989422804014327
MESH = pl.DeviceIdType.MESH
F32 = jnp.float32
BF16 = jnp.bfloat16
MIB = 1024 * 1024
ENTRY_VMEM, ATTEND_VMEM, MIDDLE_VMEM, BACK_VMEM, EXIT_VMEM = 24, 16, 40, 20, 42


def flip(value, mask, width):
    total, bit = 0, 1
    while bit < width:
        a = lax.rem(value // bit, 2)
        b = (mask // bit) % 2 if isinstance(mask, int) else lax.rem(mask // bit, 2)
        total = total + lax.rem(a + b, 2) * bit
        bit *= 2
    return total


def remote(src, dst, send_sem, recv_sem, device):
    return pltpu.make_async_remote_copy(
        src_ref=src,
        dst_ref=dst,
        send_sem=send_sem,
        recv_sem=recv_sem,
        device_id=device,
        device_id_type=MESH,
    )


def await_recv(dst, sem, device):
    remote(dst, dst, sem, sem, device).wait_recv()


def await_send(src, sem, device):
    remote(src, src, sem, sem, device).wait_send()


class Chain:
    def __init__(self, S, z, s, own, land, cross, fin, sems, lag=4):
        self.S, self.s, self.lag, self.sems = S, s, lag, sems
        self.own, self.land, self.cross, self.fin = own, land, cross, fin
        low = 1 - (2 * z) // S
        self.depth = low * z + (1 - low) * (S - 1 - z)
        self.inward = (z + 2 * low - 1, s)
        self.outward = (z + 1 - 2 * low, s)
        self.mid = S // 2 - 1
        self.pieces = own.shape[0]
        self.slots = self.pieces + lag * self.mid + lag * max(self.mid - 1, 0)

    def give_out(self, start, stop):
        @pl.when(self.depth == 0)
        def _():
            def step(p, carry):
                remote(
                    self.own.at[p], self.land.at[p], self.sems.at[0, p], self.sems.at[1, p], self.inward
                ).start()
                return carry

            lax.fori_loop(start, stop, step, 0)

    def slot(self, k):
        p = k - self.lag * (self.depth - 1)

        @pl.when((self.depth > 0) & (p >= 0) & (p < self.pieces))
        def _():
            await_recv(self.land.at[p], self.sems.at[1, p], self.outward)
            both = self.own[p].astype(F32) + self.land[p].astype(F32)
            self.own[p] = both.astype(BF16)

            @pl.when(self.depth < self.mid)
            def _():
                remote(
                    self.own.at[p], self.land.at[p], self.sems.at[0, p], self.sems.at[1, p], self.inward
                ).start()

            @pl.when(self.depth == self.mid)
            def _():
                remote(
                    self.own.at[p], self.cross.at[p], self.sems.at[2, p], self.sems.at[3, p], self.inward
                ).start()

        x = k - self.lag * self.mid

        @pl.when((self.depth == self.mid) & (x >= 0) & (x < self.pieces))
        def _():
            await_recv(self.cross.at[x], self.sems.at[3, x], self.inward)
            both = self.own[x].astype(F32) + self.cross[x].astype(F32)
            self.fin[x] = both.astype(BF16)
            remote(
                self.fin.at[x], self.fin.at[x], self.sems.at[4, x], self.sems.at[5, x], self.outward
            ).start()

        b = k - self.lag * self.mid - self.lag * (self.mid - self.depth)

        @pl.when((self.depth < self.mid) & (self.depth > 0) & (b >= 0) & (b < self.pieces))
        def _():
            await_recv(self.fin.at[b], self.sems.at[5, b], self.inward)
            remote(
                self.fin.at[b], self.fin.at[b], self.sems.at[4, b], self.sems.at[5, b], self.outward
            ).start()

    def run(self, start, stop):
        def step(k, carry):
            self.slot(k)
            return carry

        lax.fori_loop(start, stop, step, 0)

    def settle(self):
        def step(p, carry):
            @pl.when(self.depth == 0)
            def _():
                await_recv(self.fin.at[p], self.sems.at[5, p], self.inward)

            @pl.when(self.depth < self.mid)
            def _():
                await_send(self.own.at[p], self.sems.at[0, p], self.inward)

            @pl.when(self.depth == self.mid)
            def _():
                await_send(self.own.at[p], self.sems.at[2, p], self.inward)

            @pl.when(self.depth > 0)
            def _():
                await_send(self.fin.at[p], self.sems.at[4, p], self.outward)

            return carry

        lax.fori_loop(0, self.pieces, step, 0)


class Gather:
    def __init__(self, C, chip, peer, rows, slot, ss, rs):
        self.C, self.chip, self.peer, self.rows, self.slot = C, chip, peer, rows, slot
        self.ss, self.rs = ss, rs

    def half(self, ref, h):
        return ref.at[pl.ds(h * (self.rows // 2), self.rows // 2)]

    def block(self, j):
        return self.slot(flip(self.chip, j, self.C))

    def send(self, src):
        dst = self.slot(self.chip)
        if self.C == 4:
            for j, first in ((1, 0), (2, 1)):
                for h in (first, 1 - first):
                    remote(
                        self.half(src, h), self.half(dst, h), self.ss.at[j, h], self.rs.at[j, h], self.peer(j)
                    ).start()
        else:
            for j in range(self.C - 1, 0, -1):
                remote(src, dst, self.ss.at[j, 0], self.rs.at[j, 0], self.peer(j)).start()

    def relay(self):
        if self.C == 4:
            for j, h, to in ((1, 0, 2), (2, 1, 1)):
                part = self.half(self.block(j), h)
                await_recv(part, self.rs.at[j, h], self.peer(j))
                remote(part, part, self.ss.at[3, h], self.rs.at[3, h], self.peer(to)).start()

    def arrived(self, j):
        if self.C == 4:
            for want, h in ((1, 1), (2, 0), (3, 0), (3, 1)):

                @pl.when(j == want)
                def _(want=want, h=h):
                    await_recv(self.half(self.block(want), h), self.rs.at[want, h], self.peer(want))
        else:

            @pl.when(j > 0)
            def _():
                await_recv(self.block(j), self.rs.at[j, 0], self.peer(j))

    def settle(self):
        own = self.slot(self.chip)
        if self.C == 4:
            for j in range(1, 4):
                for h in range(2):
                    await_send(self.half(own, h), self.ss.at[j, h], self.peer(j))
        else:
            for j in range(1, self.C):
                await_send(own, self.ss.at[j, 0], self.peer(j))


class Scatter:
    def __init__(self, C, peer, rows, stage, recv, ss, rs):
        self.C, self.peer, self.rows = C, peer, rows
        self.stage, self.recv, self.ss, self.rs = stage, recv, ss, rs

    def give(self, j, h, to):
        part = pl.ds(h * (self.rows // 2), self.rows // 2)
        remote(
            self.stage.at[j, part], self.recv.at[j, part], self.ss.at[j, h], self.rs.at[j, h], self.peer(to)
        ).start()

    def take(self, j, h, source):
        part = pl.ds(h * (self.rows // 2), self.rows // 2)
        await_recv(self.recv.at[j, part], self.rs.at[j, h], self.peer(source))
        return part

    def send(self, make):
        if self.C != 4:

            def step(k, carry):
                j = self.C - 1 - k
                self.stage[j] = make(j).astype(BF16)
                remote(
                    self.stage.at[j], self.recv.at[j], self.ss.at[j, 0], self.rs.at[j, 0], self.peer(j)
                ).start()
                return carry

            lax.fori_loop(0, self.C - 1, step, 0)
            return make(0)
        self.stage[3] = make(3).astype(BF16)
        self.give(3, 0, 2)
        self.give(3, 1, 1)
        self.stage[1] = make(1).astype(BF16)
        self.give(1, 1, 1)
        self.stage[2] = make(2).astype(BF16)
        self.give(2, 0, 2)
        own = make(0)
        for h, source, j in ((0, 2, 1), (1, 1, 2)):
            part = self.take(3, h, source)
            both = self.stage[j, part].astype(F32) + self.recv[3, part].astype(F32)
            self.stage[j, part] = both.astype(BF16)
            self.give(j, h, j)
        return own

    def collect(self, total):
        if self.C != 4:
            for j in range(1, self.C):
                await_recv(self.recv.at[j], self.rs.at[j, 0], self.peer(j))
                total = total + self.recv[j].astype(F32)
            return total
        for j in (1, 2):
            self.take(j, 2 - j, j)
            self.take(j, j - 1, j)
            total = total + self.recv[j].astype(F32)
        return total

    def settle(self):
        for j in range(1, self.C):
            if self.C == 4:
                for h in range(2):
                    part = pl.ds(h * (self.rows // 2), self.rows // 2)
                    await_send(self.stage.at[j, part], self.ss.at[j, h], self.peer(j))
            else:
                await_send(self.stage.at[j], self.ss.at[j, 0], self.peer(j))


def rows_dot(a, b):
    return lax.dot_general(a, b, (((1,), (0,)), ((), ())), preferred_element_type=F32)


def rows_dot_t(a, b):
    return lax.dot_general(a, b, (((1,), (1,)), ((), ())), preferred_element_type=F32)


def cols_dot(a, b):
    return lax.dot_general(a, b, (((0,), (0,)), ((), ())), preferred_element_type=F32)


def entry_kernel(
    dims,
    pos_hbm,
    inp_hbm,
    table_ref,
    wqkv_ref,
    wup_ref,
    wdn_ref,
    wout_ref,
    seg_hbm,
    bup_in_hbm,
    row0_ref,
    row1_ref,
    row2_ref,
    row3_ref,
    row4_ref,
    row5_ref,
    row6_ref,
    row7_ref,
    q_ref,
    kv_ref,
    hid_half_ref,
    hidden_ref,
    wq_ref,
    wup2_ref,
    wdn_o_ref,
    wout_o_ref,
    par_all_ref,
    bup2_ref,
    pos_glob_ref,
    lohi_ref,
    pos_ref,
    inp_ref,
    seg_ref,
    bup_in_ref,
    rows_ref,
    table_v,
    pstage,
    precv,
    cstage,
    crecv,
    qst,
    kvst,
    wup_own,
    par_ref,
    bup_ref,
    pos_ss,
    pos_rs,
    par_ss,
    par_rs,
    posz_ss,
    posz_rs,
    wq_ss,
    wq_rs,
    wqf_ss,
    wqf_rs,
    wup_ss,
    wup_rs,
    wupf_ss,
    wupf_rs,
    misc_ss,
    misc_rs,
    rsp_ss,
    rsp_rs,
    rsc_ss,
    rsc_rs,
    ag_ss,
    ag_rs,
    qx_ss,
    qx_rs,
    zx_ss,
    zx_rs,
    loc,
):
    S, n, C, L, D, hc, R, F2 = dims
    z = lax.axis_index("seq")
    s = lax.axis_index("shard")
    core = lax.rem(s, 2)
    chip = s // 2
    other = 1 - core
    partner = 2 * chip + other
    h2 = 2 * hc
    Dn = D // n

    rows = (row0_ref, row1_ref, row2_ref, row3_ref, row4_ref, row5_ref, row6_ref, row7_ref)
    smalls = [
        pltpu.make_async_copy(pos_hbm, pos_ref, loc.at[6]),
        pltpu.make_async_copy(seg_hbm, seg_ref, loc.at[7]),
        pltpu.make_async_copy(bup_in_hbm, bup_in_ref, loc.at[8]),
    ] + [
        pltpu.make_async_copy(row, rows_ref.at[i], loc.at[9 + i]) for i, row in enumerate(rows)
    ]
    for small in smalls:
        small.start()
    inp_copy = pltpu.make_async_copy(inp_hbm, inp_ref, loc.at[17])
    inp_copy.start()
    table_copy = pltpu.make_async_copy(table_ref, table_v, loc.at[0])
    table_copy.start()
    own_wq = []
    for part in range(3):
        own_wq.append(
            pltpu.make_async_copy(
                wqkv_ref.at[:, pl.ds(pl.multiple_of(part * D + chip * h2, 128), h2)],
                wq_ref.at[s, :, part * h2 : (part + 1) * h2],
                loc.at[1 + part],
            )
        )
        own_wq[-1].start()
    own_wup_in = pltpu.make_async_copy(
        wup_ref.at[:, pl.ds(pl.multiple_of(chip * F2, 128), F2)], wup_own, loc.at[4]
    )
    own_wup_in.start()

    for small in smalls:
        small.wait()
    for i in range(8):
        par_ref[i : i + 1] = rows_ref[i].astype(F32)
    bup_ref[...] = bup_in_ref[...].astype(F32)
    F1 = F2 // 2
    bup_mine = pl.ds(pl.multiple_of(core * F1, 128), F1)
    bup_theirs = pl.ds(pl.multiple_of(other * F1, 128), F1)
    bup2_ref[:, bup_mine] = bup_ref[...]

    barrier = pltpu.get_barrier_semaphore()
    for d in range(1, n):
        pl.semaphore_signal(barrier, inc=1, device_id=(z, flip(s, d, n)), device_id_type=MESH)
    for d in range(1, S):
        pl.semaphore_signal(barrier, inc=1, device_id=(lax.rem(z + d, S), s), device_id_type=MESH)

    for d in (1, S - 1):
        pl.semaphore_signal(
            barrier, inc=1, device_id=(lax.rem(z + d, S), partner), device_id_type=MESH
        )
    pl.semaphore_wait(barrier, n - 1 + S - 1 + 2)

    pos_glob_ref[z, s] = pos_ref[...]
    par_all_ref[s] = par_ref[...]
    for d in range(1, n):
        peer = (z, flip(s, d, n))
        remote(pos_ref, pos_glob_ref.at[z, s], pos_ss.at[d], pos_rs.at[d], peer).start()
        remote(par_ref, par_all_ref.at[s], par_ss.at[d], par_rs.at[d], peer).start()

    for own in own_wq:
        own.wait()

    def wq_src(peer_chip, part):
        return wqkv_ref.at[:, pl.ds(pl.multiple_of(part * D + peer_chip * h2, 128), h2)]

    for j in range(C - 1, 0, -1):
        pc = flip(chip, j, C)
        for part in range(3):
            remote(
                wq_src(pc, part),
                wq_ref.at[s, :, part * h2 : (part + 1) * h2],
                wq_ss.at[j, part],
                wq_rs.at[j, part],
                (z, 2 * pc + core),
            ).start()
    remote(wq_ref.at[s], wq_ref.at[s], wqf_ss.at[0], wqf_rs.at[0], (z, partner)).start()

    own_segs = jnp.concatenate([seg_ref[z * n + i] for i in range(n)], axis=1)

    def count(g, carry):
        low, high = carry
        keys = jnp.broadcast_to(seg_ref[g], (L, L)).T
        lows, highs = [], []
        for i in range(n):
            mine = own_segs[:, i * L : (i + 1) * L]
            lows.append(jnp.sum(jnp.where(keys < mine, 1.0, 0.0), axis=0, keepdims=True))
            highs.append(jnp.sum(jnp.where(keys <= mine, 1.0, 0.0), axis=0, keepdims=True))
        return low + jnp.concatenate(lows, axis=1), high + jnp.concatenate(highs, axis=1)

    none = jnp.zeros((1, n * L), F32)
    low, high = lax.fori_loop(0, S * n, count, (none, none))
    origin = ((z - 1) * n * L).astype(F32)
    lohi_ref[0:1] = low - origin
    lohi_ref[1:2] = high - origin

    for d in range(1, n):
        src = flip(s, d, n)
        await_recv(pos_glob_ref.at[z, src], pos_rs.at[d], (z, src))
    for d in range(1, S):
        remote(
            pos_glob_ref.at[z],
            pos_glob_ref.at[z],
            posz_ss.at[d],
            posz_rs.at[d],
            (lax.rem(z + d, S), s),
        ).start()

    table_copy.wait()
    inp_copy.wait()
    lane_ids = lax.broadcasted_iota(jnp.int32, (L, R), 1) + s * R

    def picked(block):
        ids = jnp.broadcast_to(pos_glob_ref[z, block], (L, L)).T
        ids = jnp.concatenate([ids] * (R // L), axis=1)
        hot = jnp.where(ids == lane_ids, 1.0, 0.0).astype(BF16)
        return rows_dot(hot, table_v[...])

    def send_partner(j):
        pstage[j] = picked(2 * flip(chip, j, C) + other).astype(BF16)
        remote(pstage.at[j], precv.at[j], rsp_ss.at[j], rsp_rs.at[j], (z, partner)).start()

    def combined(j):
        mine = picked(2 * flip(chip, j, C) + core)
        await_recv(precv.at[j], rsp_rs.at[j], (z, partner))
        return mine + precv[j].astype(F32)

    def peer(j):
        return (z, 2 * flip(chip, j, C) + core)

    def partner_step(k, carry):
        send_partner(C - 1 - k)
        return carry

    lax.fori_loop(0, C, partner_step, 0)
    rows_sum = Scatter(C, peer, L, cstage, crecv, rsc_ss, rsc_rs)
    hidden = rows_sum.send(combined) + inp_ref[...].astype(F32)

    for j in range(1, C):
        src = 2 * flip(chip, j, C) + core
        for part in range(3):
            await_recv(
                wq_ref.at[src, :, part * h2 : (part + 1) * h2], wq_rs.at[j, part], (z, src)
            )
        remote(wq_ref.at[src], wq_ref.at[src], wqf_ss.at[j], wqf_rs.at[j], (z, partner)).start()

    hidden = rows_sum.collect(hidden)
    hidden_ref[...] = hidden
    hid_half_ref[chip] = hidden.astype(BF16)
    gather = Gather(C, chip, peer, L, lambda c: hid_half_ref.at[c], ag_ss, ag_rs)
    gather.send(hid_half_ref.at[chip])

    own_wup_in.wait()
    own_wup_out = pltpu.make_async_copy(wup_own, wup2_ref.at[s], loc.at[5])
    own_wup_out.start()
    for j in range(C - 1, 0, -1):
        pc = flip(chip, j, C)
        remote(
            wup_ref.at[:, pl.ds(pl.multiple_of(pc * F2, 128), F2)],
            wup2_ref.at[s],
            wup_ss.at[j],
            wup_rs.at[j],
            (z, 2 * pc + core),
        ).start()
    remote(wup_own, wup2_ref.at[s], wupf_ss.at[0], wupf_rs.at[0], (z, partner)).start()
    remote(wdn_ref, wdn_o_ref, misc_ss.at[0], misc_rs.at[0], (z, partner)).start()
    remote(wout_ref, wout_o_ref, misc_ss.at[1], misc_rs.at[1], (z, partner)).start()
    remote(bup_ref, bup2_ref.at[:, bup_mine], misc_ss.at[2], misc_rs.at[2], (z, partner)).start()

    for j in range(C):
        src = 2 * flip(chip, j, C) + other
        await_recv(wq_ref.at[src], wqf_rs.at[j], (z, partner))
    for d in range(1, n):
        src = flip(s, d, n)
        await_recv(par_all_ref.at[src], par_rs.at[d], (z, src))
    bias = jnp.concatenate([par_all_ref[2 * chip], par_all_ref[2 * chip + 1]], axis=1)
    bias_q, bias_v = bias[6:7], bias[7:8]
    first_core = core == 0

    def project(j, carry):
        c = flip(chip, j, C)

        gather.arrived(j)
        res = rows_dot(hid_half_ref[c], wq_ref[...].reshape(D, 3 * h2))
        query = (res[:, :h2] + bias_q).astype(BF16) * score_scale
        key = res[:, h2 : 2 * h2].astype(BF16)
        value = (res[:, 2 * h2 :] + bias_v).astype(BF16)
        q_ref[c, core] = jnp.where(first_core, query[:, :hc], query[:, hc:])
        kv_ref[1, c, core, :, :hc] = jnp.where(first_core, key[:, :hc], key[:, hc:])
        kv_ref[1, c, core, :, hc:] = jnp.where(first_core, value[:, :hc], value[:, hc:])
        qst[j] = jnp.where(first_core, query[:, hc:], query[:, :hc])
        kvst[j, :, :hc] = jnp.where(first_core, key[:, hc:], key[:, :hc])
        kvst[j, :, hc:] = jnp.where(first_core, value[:, hc:], value[:, :hc])
        own_kv = kv_ref.at[1, c, core]

        @pl.when(z < S - 1)
        def _():
            remote(
                own_kv, kv_ref.at[0, c, core], zx_ss.at[j, 0], zx_rs.at[j, 0], (z + 1, s)
            ).start()
            remote(
                kvst.at[j], kv_ref.at[0, c, core], zx_ss.at[j, 1], zx_rs.at[j, 1], (z + 1, partner)
            ).start()

        @pl.when(z > 0)
        def _():
            remote(
                own_kv, kv_ref.at[2, c, core], zx_ss.at[j, 2], zx_rs.at[j, 2], (z - 1, s)
            ).start()
            remote(
                kvst.at[j], kv_ref.at[2, c, core], zx_ss.at[j, 3], zx_rs.at[j, 3], (z - 1, partner)
            ).start()

        remote(qst.at[j], q_ref.at[c, core], qx_ss.at[j, 0], qx_rs.at[j, 0], (z, partner)).start()
        remote(
            kvst.at[j], kv_ref.at[1, c, core], qx_ss.at[j, 1], qx_rs.at[j, 1], (z, partner)
        ).start()
        return carry

    gather.relay()
    lax.fori_loop(0, C, project, 0)

    for j in range(1, C):
        src = 2 * flip(chip, j, C) + core
        await_recv(wup2_ref.at[src], wup_rs.at[j], (z, src))
        remote(
            wup2_ref.at[src], wup2_ref.at[src], wupf_ss.at[j], wupf_rs.at[j], (z, partner)
        ).start()

    def settle(j, carry):
        c = flip(chip, j, C)
        await_recv(q_ref.at[c, other], qx_rs.at[j, 0], (z, partner))
        await_recv(kv_ref.at[1, c, other], qx_rs.at[j, 1], (z, partner))
        await_send(qst.at[j], qx_ss.at[j, 0], (z, partner))
        await_send(kvst.at[j], qx_ss.at[j, 1], (z, partner))

        @pl.when(z > 0)
        def _():
            await_recv(kv_ref.at[0, c, core], zx_rs.at[j, 0], (z - 1, s))
            await_recv(kv_ref.at[0, c, other], zx_rs.at[j, 1], (z - 1, partner))
            await_send(kvst.at[j], zx_ss.at[j, 2], (z - 1, s))
            await_send(kvst.at[j], zx_ss.at[j, 3], (z - 1, partner))

        @pl.when(z < S - 1)
        def _():
            await_recv(kv_ref.at[2, c, core], zx_rs.at[j, 2], (z + 1, s))
            await_recv(kv_ref.at[2, c, other], zx_rs.at[j, 3], (z + 1, partner))
            await_send(kvst.at[j], zx_ss.at[j, 0], (z + 1, s))
            await_send(kvst.at[j], zx_ss.at[j, 1], (z + 1, partner))

        await_send(pstage.at[j], rsp_ss.at[j], (z, partner))
        await_send(wq_ref.at[s], wqf_ss.at[j], (z, partner))
        await_recv(wup2_ref.at[2 * c + other], wupf_rs.at[j], (z, partner))
        await_send(wup2_ref.at[s], wupf_ss.at[j], (z, partner))
        return carry

    lax.fori_loop(0, C, settle, 0)
    gather.settle()
    rows_sum.settle()
    for j in range(1, C):
        await_send(wup_own, wup_ss.at[j], peer(j))
        for part in range(3):
            await_send(
                wq_ref.at[s, :, part * h2 : (part + 1) * h2], wq_ss.at[j, part], peer(j)
            )
    for d in range(1, n):
        peer = (z, flip(s, d, n))
        await_send(pos_ref, pos_ss.at[d], peer)
        await_send(par_ref, par_ss.at[d], peer)
    for d in range(1, S):
        src = lax.rem(z + S - d, S)
        await_recv(pos_glob_ref.at[src], posz_rs.at[d], (src, s))
        await_send(pos_glob_ref.at[z], posz_ss.at[d], (lax.rem(z + d, S), s))
    for i, (mine, got) in enumerate(
        ((wdn_ref, wdn_o_ref), (wout_ref, wout_o_ref), (bup_ref, bup2_ref.at[:, bup_theirs]))
    ):
        await_recv(got, misc_rs.at[i], (z, partner))
        await_send(mine, misc_ss.at[i], (z, partner))
    own_wup_out.wait()


def entry_call(S, n, pos, inp, table, wqkv, wup, wdn, wout, seg, bup, rows):
    C = n // 2
    L, D = inp.shape
    hc = D // n
    R = table.shape[0]
    F = wup.shape[1]
    F1, F2 = F // n, 2 * F // n
    dims = (S, n, C, L, D, hc, R, F2)
    dma = pltpu.SemaphoreType.DMA
    vm = pl.BlockSpec(memory_space=pltpu.VMEM)
    anyw = pl.BlockSpec(memory_space=pl.ANY)
    hbm = pl.BlockSpec(memory_space=pltpu.HBM)
    sds = jax.ShapeDtypeStruct
    return pl.pallas_call(
        functools.partial(entry_kernel, dims),
        out_shape=(
            sds((C, 2, L, hc), BF16),
            sds((3, C, 2, L, 2 * hc), BF16),
            sds((C, L, D), BF16),
            sds((L, D), F32),
            sds((n, D // n, 6 * hc), BF16),
            sds((n, D // n, F2), BF16),
            sds((F1, D), BF16),
            sds((D // n, D), BF16),
            sds((n, 8, hc), F32),
            sds((1, F2), F32),
            sds((S, n, 1, L), jnp.int32),
            sds((2, n * L), F32),
        ),
        in_specs=[hbm] * 17,
        out_specs=(vm, vm, vm, vm, vm, anyw, anyw, anyw, vm, vm, vm, vm),
        scratch_shapes=[
            pltpu.VMEM((1, L), jnp.int32),
            pltpu.VMEM((L, D), BF16),
            pltpu.VMEM((S * n, 1, L), jnp.int32),
            pltpu.VMEM((1, F1), BF16),
            pltpu.VMEM((8, 1, hc), BF16),
            pltpu.VMEM((R, D), BF16),
            pltpu.VMEM((C, L, D), BF16),
            pltpu.VMEM((C, L, D), BF16),
            pltpu.VMEM((C, L, D), BF16),
            pltpu.VMEM((C, L, D), BF16),
            pltpu.VMEM((C, L, hc), BF16),
            pltpu.VMEM((C, L, 2 * hc), BF16),
            pltpu.VMEM((D // n, F2), BF16),
            pltpu.VMEM((8, hc), F32),
            pltpu.VMEM((1, F1), F32),
            dma((n,)),
            dma((n,)),
            dma((n,)),
            dma((n,)),
            dma((S,)),
            dma((S,)),
            dma((C, 3)),
            dma((C, 3)),
            dma((C,)),
            dma((C,)),
            dma((C,)),
            dma((C,)),
            dma((C,)),
            dma((C,)),
            dma((3,)),
            dma((3,)),
            dma((C,)),
            dma((C,)),
            dma((C, 2)),
            dma((C, 2)),
            dma((C, 2)),
            dma((C, 2)),
            dma((C, 2)),
            dma((C, 2)),
            dma((C, 4)),
            dma((C, 4)),
            dma((18,)),
        ],
        compiler_params=pltpu.CompilerParams(
            collective_id=0, has_side_effects=True, vmem_limit_bytes=ENTRY_VMEM * MIB
        ),
        name="entry_stage",
    )(*[
        pltpu.with_memory_space_constraint(v, pltpu.HBM)
        for v in (pos, inp, table, wqkv, wup, wdn, wout, seg, bup, *rows)
    ])


def key_blocks(lohi_ref, rows, bk):
    first = jnp.min(lohi_ref[0:1, rows]).astype(jnp.int32)
    last = jnp.max(lohi_ref[1:2, rows]).astype(jnp.int32)
    return first // bk, (last + bk - 1) // bk


def attend_kernel(dims, q_ref, kv_ref, lohi_ref, att_ref, lse_ref, vt_ref):
    P_, hc, hh, bq, bk = dims
    lanes = lax.broadcasted_iota(jnp.int32, (bq, hc), 1) // HEAD_DIM
    nq = P_ // bq

    def flip_value(kb, carry):
        at = pl.multiple_of(kb * bk, bk)
        vt_ref[kb] = kv_ref[pl.ds(at, bk), hc:].T
        return carry

    first, last = key_blocks(lohi_ref, pl.ds(0, P_), bk)
    lax.fori_loop(first, last, flip_value, 0)

    def one_query_block(qi, carry):
        rows = pl.ds(pl.multiple_of(qi * bq, bq), bq)
        query = q_ref[rows, :]
        heads_q = [jnp.where(lanes == h, query, jnp.zeros_like(query)) for h in range(hh)]
        low = lohi_ref[0:1, rows].astype(jnp.int32)
        high = lohi_ref[1:2, rows].astype(jnp.int32)
        first, last = key_blocks(lohi_ref, rows, bk)

        def one_key_block(kb, state):
            at = pl.multiple_of(kb * bk, bk)
            keys = kv_ref[pl.ds(at, bk), :hc]
            ids = lax.broadcasted_iota(jnp.int32, (bk, bq), 0) + kb * bk
            keep = (ids >= low) & (ids < high)
            fresh = []
            for h in range(hh):
                top, total, acc = state[h]
                scores = jnp.where(keep, rows_dot_t(keys, heads_q[h]), neg_large)
                new_top = jnp.maximum(top, jnp.max(scores, axis=0, keepdims=True))
                weights = jnp.exp(scores - new_top)
                shrink = jnp.exp(top - new_top)
                total = total * shrink + jnp.sum(weights, axis=0, keepdims=True)
                values = vt_ref[kb, h * HEAD_DIM : (h + 1) * HEAD_DIM, :]
                acc = acc * shrink + rows_dot(values, weights.astype(BF16))
                fresh.append((new_top, total, acc))
            return tuple(fresh)

        start = tuple(
            (
                jnp.full((1, bq), neg_large, F32),
                jnp.zeros((1, bq), F32),
                jnp.zeros((HEAD_DIM, bq), F32),
            )
            for _ in range(hh)
        )
        state = lax.fori_loop(first, last, one_key_block, start)
        mixed = jnp.concatenate([acc / total for _, total, acc in state], axis=0)
        att_ref[rows, :] = mixed.T.astype(BF16)
        for h in range(hh):
            lse_ref[h : h + 1, rows] = state[h][0] + jnp.log(state[h][1])
        return carry

    lax.fori_loop(0, nq, one_query_block, 0)


def attend_call(q, kv, lohi, bq, bk):
    P_, hc = q.shape
    hh = hc // HEAD_DIM
    vm = pl.BlockSpec(memory_space=pltpu.VMEM)
    return pl.pallas_call(
        functools.partial(attend_kernel, (P_, hc, hh, bq, bk)),
        out_shape=(
            jax.ShapeDtypeStruct((P_, hc), BF16),
            jax.ShapeDtypeStruct((hh, P_), F32),
        ),
        in_specs=[vm, vm, vm],
        out_specs=(vm, vm),
        scratch_shapes=[pltpu.VMEM((3 * P_ // bk, hc, bk), BF16)],
        compiler_params=pltpu.CompilerParams(vmem_limit_bytes=ATTEND_VMEM * MIB),
        name="attend_stage",
    )(q, kv, lohi)


def attend_back_kernel(
    dims, q_ref, kv_ref, lohi_ref, att_ref, datt_ref, lse_ref, dq_ref, dkv_ref, kt_ref, acc_ref
):
    P_, hc, hh, bq, bk = dims
    lanes = lax.broadcasted_iota(jnp.int32, (bq, hc), 1) // HEAD_DIM
    nq = P_ // bq
    acc_ref[...] = jnp.zeros_like(acc_ref)

    def flip_key(kb, carry):
        at = pl.multiple_of(kb * bk, bk)
        kt_ref[kb] = kv_ref[pl.ds(at, bk), :hc].T
        return carry

    first, last = key_blocks(lohi_ref, pl.ds(0, P_), bk)
    lax.fori_loop(first, last, flip_key, 0)

    def one_query_block(qi, carry):
        rows = pl.ds(pl.multiple_of(qi * bq, bq), bq)
        query, grad = q_ref[rows, :], datt_ref[rows, :]
        zero = jnp.zeros_like(query)
        heads_q = [jnp.where(lanes == h, query, zero) for h in range(hh)]
        heads_g = [jnp.where(lanes == h, grad, zero) for h in range(hh)]
        stack_q = jnp.concatenate(heads_q, axis=0)
        stack_g = jnp.concatenate(heads_g, axis=0)
        product = (grad.astype(F32) * att_ref[rows, :].astype(F32)).T
        delta = [
            jnp.sum(product[h * HEAD_DIM : (h + 1) * HEAD_DIM], axis=0, keepdims=True)
            for h in range(hh)
        ]
        logs = [lse_ref[h : h + 1, rows] for h in range(hh)]
        low = lohi_ref[0:1, rows].astype(jnp.int32)
        high = lohi_ref[1:2, rows].astype(jnp.int32)
        first, last = key_blocks(lohi_ref, rows, bk)

        def one_key_block(kb, state):
            at = pl.multiple_of(kb * bk, bk)
            keys = kv_ref[pl.ds(at, bk), :hc]
            values = kv_ref[pl.ds(at, bk), hc:]
            ids = lax.broadcasted_iota(jnp.int32, (bk, bq), 0) + kb * bk
            keep = (ids >= low) & (ids < high)
            fresh, all_p, all_s = [], [], []
            for h in range(hh):
                scores = rows_dot_t(keys, heads_q[h])
                probs = jnp.where(keep, jnp.exp(scores - logs[h]), 0.0)
                grad_probs = rows_dot_t(values, heads_g[h])
                grad_scores = (probs * (grad_probs - delta[h])).astype(BF16)
                all_p.append(probs.astype(BF16))
                all_s.append(grad_scores)
                key_cols = kt_ref[kb, h * HEAD_DIM : (h + 1) * HEAD_DIM, :]
                fresh.append(state[h] + rows_dot(key_cols, grad_scores))
            acc_ref[pl.ds(at, bk), :hc] += rows_dot(jnp.concatenate(all_s, axis=1), stack_q)
            acc_ref[pl.ds(at, bk), hc:] += rows_dot(jnp.concatenate(all_p, axis=1), stack_g)
            return tuple(fresh)

        start = tuple(jnp.zeros((HEAD_DIM, bq), F32) for _ in range(hh))
        state = lax.fori_loop(first, last, one_key_block, start)
        dq_ref[rows, :] = (jnp.concatenate(state, axis=0).T * score_scale).astype(BF16)
        return carry

    lax.fori_loop(0, nq, one_query_block, 0)
    dkv_ref[...] = acc_ref[...].astype(BF16)


def attend_back_call(q, kv, lohi, att, datt, lse, bq, bk):
    P_, hc = q.shape
    hh = hc // HEAD_DIM
    vm = pl.BlockSpec(memory_space=pltpu.VMEM)
    return pl.pallas_call(
        functools.partial(attend_back_kernel, (P_, hc, hh, bq, bk)),
        out_shape=(
            jax.ShapeDtypeStruct((P_, hc), BF16),
            jax.ShapeDtypeStruct((3 * P_, 2 * hc), BF16),
        ),
        in_specs=[vm, vm, vm, vm, vm, vm],
        out_specs=(vm, vm),
        scratch_shapes=[
            pltpu.VMEM((3 * P_ // bk, hc, bk), BF16),
            pltpu.VMEM((3 * P_, 2 * hc), F32),
        ],
        compiler_params=pltpu.CompilerParams(vmem_limit_bytes=BACK_VMEM * MIB),
        name="attend_back_stage",
    )(q, kv, lohi, att, datt, lse)


def layer_stats(summed):
    center = summed - jnp.mean(summed, axis=1, keepdims=True)
    inverse = lax.rsqrt(jnp.mean(center * center, axis=1, keepdims=True) + epsilon)
    return center * inverse, inverse


def layer_back(grad, normed, inverse):
    first = jnp.mean(grad, axis=1, keepdims=True)
    second = jnp.mean(grad * normed, axis=1, keepdims=True)
    return inverse * (grad - first - normed * second)


def col_sum(x):
    return jnp.sum(x, axis=0, keepdims=True)


def middle_kernel(
    dims,
    att_ref,
    hidden_ref,
    cot_ref,
    par_ref,
    wout_ref,
    wout_o_ref,
    wup_ref,
    wdn_ref,
    wdn_o_ref,
    bup_ref,
    result_ref,
    dfirst_ref,
    datt_ref,
    gdn_ref,
    gup_ref,
    gout_ref,
    stats_ref,
    gbup_ref,
    gdn_done_ref,
    wout_v,
    wup_v,
    wdn_v,
    attp,
    fa,
    da,
    dfa,
    act,
    slope,
    dup,
    stage,
    recv,
    normed_v,
    first_v,
    dnorm_v,
    gdn_v,
    gdn_r,
    gdn_h,
    gdn_l,
    gdn_x,
    gdn_f,
    gup_v,
    gup_r,
    gout_v,
    gout_r,
    gb_v,
    gb_r,
    dattst,
    ap_ss,
    ap_rs,
    sc_ss,
    sc_rs,
    ag_ss,
    ag_rs,
    gx_ss,
    gx_rs,
    dx_ss,
    dx_rs,
    zsem,
    loc,
):
    S, n, C, L, D, hc, F1 = dims
    Dn, F2, Ph = D // n, 2 * F1, C * L
    z = lax.axis_index("seq")
    s = lax.axis_index("shard")
    core = lax.rem(s, 2)
    chip = s // 2
    other = 1 - core
    partner = (z, 2 * chip + other)

    loads = [
        pltpu.make_async_copy(wout_ref, wout_v.at[core], loc.at[0]),
        pltpu.make_async_copy(wout_o_ref, wout_v.at[other], loc.at[1]),
        pltpu.make_async_copy(wup_ref, wup_v, loc.at[2]),
        pltpu.make_async_copy(wdn_ref, wdn_v.at[core], loc.at[3]),
        pltpu.make_async_copy(wdn_o_ref, wdn_v.at[other], loc.at[4]),
    ]
    for load in loads:
        load.start()

    def peer(j):
        return (z, 2 * flip(chip, j, C) + core)

    barrier = pltpu.get_barrier_semaphore()
    pl.semaphore_signal(barrier, inc=1, device_id=partner, device_id_type=MESH)
    for j in range(1, C):
        pl.semaphore_signal(barrier, inc=1, device_id=peer(j), device_id_type=MESH)
    for d in (1, S - 1):
        pl.semaphore_signal(barrier, inc=1, device_id=(lax.rem(z + d, S), s), device_id_type=MESH)
    pl.semaphore_wait(barrier, C + 2)

    def put_stat(row, value):
        for i in range(n):
            stats_ref[i, row : row + 1] = value[:, i * hc : (i + 1) * hc]

    def give(i, src, dst):
        remote(src, dst, gx_ss.at[i], gx_rs.at[i], partner).start()

    def taken(i, src, dst):
        await_recv(dst, gx_rs.at[i], partner)

    def gather_of(r, buf):
        return Gather(C, chip, peer, L, lambda c: buf.at[c], ag_ss.at[r], ag_rs.at[r])

    gathers = [gather_of(0, fa), gather_of(1, da), gather_of(2, dfa)]
    out_sum = Scatter(C, peer, L, stage.at[0], recv.at[0], sc_ss.at[0], sc_rs.at[0])

    def hand(r, j, part):
        stage[r, j] = part.astype(BF16)
        remote(
            stage.at[r, j], recv.at[r, j], sc_ss.at[r, j, 0], sc_rs.at[r, j, 0], peer(j)
        ).start()

    def collected(r, total):
        for j in range(1, C):
            await_recv(recv.at[r, j], sc_rs.at[r, j, 0], peer(j))
            total = total + recv[r, j].astype(F32)
        return total

    par = jnp.concatenate([par_ref[i] for i in range(n)], axis=1)
    b_out, gain1, shift1 = par[0:1], par[1:2], par[2:3]
    b_down, gain2, shift2 = par[3:4], par[4:5], par[5:6]

    remote(att_ref.at[:, other], attp, ap_ss.at[0], ap_rs.at[0], partner).start()
    loads[0].wait()
    loads[1].wait()
    await_recv(attp, ap_rs.at[0], partner)

    def out_part(j):
        c = flip(chip, j, C)
        return rows_dot(att_ref[c, core], wout_v[core]) + rows_dot(attp[c], wout_v[other])

    first_sum = out_sum.collect(out_sum.send(out_part) + hidden_ref[...] + b_out)
    normed_one, inverse_one = layer_stats(first_sum)
    normed_v[...] = normed_one
    first_norm = normed_one * gain1 + shift1
    first_v[...] = first_norm
    fa[chip] = first_norm.astype(BF16)
    gathers[0].send(fa.at[chip])

    loads[2].wait()
    loads[3].wait()
    loads[4].wait()
    first_core = core == 0
    bias_up = bup_ref[...]

    def up_part(j):
        c = flip(chip, j, C)
        pre = rows_dot(fa[c], wup_v[...].reshape(D, F2)) + bias_up
        half = 0.5 * (1.0 + lax.erf(pre * root_half))
        act[c] = (pre * half).astype(BF16)
        slope[c] = half + pre * jnp.exp(-0.5 * pre * pre) * inv_root_two_pi
        return rows_dot(act[c], wdn_v[...].reshape(F2, D))

    own = up_part(0)
    gathers[0].relay()

    def up_step(j, carry):
        gathers[0].arrived(j)
        hand(1, j, up_part(j))
        return carry

    lax.fori_loop(1, C, up_step, 0)
    second_sum = collected(1, own + first_v[...] + b_down)
    normed_two, inverse_two = layer_stats(second_sum)
    result_ref[...] = (normed_two * gain2 + shift2).astype(BF16)
    grad_rows = cot_ref[...].astype(F32)
    put_stat(0, col_sum(grad_rows * normed_two))
    put_stat(1, col_sum(grad_rows))
    d_second = layer_back(grad_rows * gain2, normed_two, inverse_two)
    put_stat(2, col_sum(d_second))
    dnorm_v[...] = d_second
    da[chip] = d_second.astype(BF16)
    gathers[1].send(da.at[chip])

    def down_back(j):
        c = flip(chip, j, C)
        d_up = rows_dot_t(da[c], wdn_v[...].reshape(F2, D)) * slope[c]
        gb_v[...] += col_sum(d_up)
        dup[c] = d_up.astype(BF16)
        return rows_dot_t(dup[c], wup_v[...].reshape(D, F2))

    gb_v[...] = jnp.zeros_like(gb_v)
    own = down_back(0)
    gathers[1].relay()

    def back_step(j, carry):
        gathers[1].arrived(j)
        hand(2, j, down_back(j))
        return carry

    lax.fori_loop(1, C, back_step, 0)
    dnorm_v[...] = dnorm_v[...] + own

    tile = 256
    da_all = da[...].reshape(Ph, D)

    per_half = F1 // tile
    per_tile = gdn_v.shape[1] // per_half

    def down_grad(i, carry):
        t = lax.rem(i + other * per_half, 2 * per_half)
        cols = pl.ds(pl.multiple_of(t * tile, tile), tile)
        res = cols_dot(act[:, :, cols].reshape(Ph, tile), da_all).astype(BF16)
        gdn_v[t // per_half, pl.ds(lax.rem(t, per_half) * per_tile, per_tile)] = res.reshape(
            per_tile, tile // per_tile, D
        )
        return carry

    lax.fori_loop(0, per_half, down_grad, 0)
    give(0, gdn_v.at[other], gdn_r)
    lax.fori_loop(per_half, 2 * per_half, down_grad, 0)

    def up_grad(c, carry):
        cols = pl.ds(pl.multiple_of(c * 2 * Dn, 128), 2 * Dn)
        res = cols_dot(fa[:, :, cols].reshape(Ph, 2 * Dn), dup[...].reshape(Ph, F2)).astype(BF16)
        gup_v[c, 0] = res[:Dn]
        gup_v[c, 1] = res[Dn:]
        return carry

    early = gdn_h.shape[0]
    taken(0, None, gdn_r)
    gdn_h[...] = (gdn_v[core, :early].astype(F32) + gdn_r[:early].astype(F32)).astype(BF16)
    gdn_ref[...] = (gdn_v[core, early:].astype(F32) + gdn_r[early:].astype(F32)).astype(BF16)
    chain = Chain(S, z, s, gdn_h, gdn_l, gdn_x, gdn_f, zsem, 2)
    chain.give_out(0, early)

    lax.fori_loop(0, C, up_grad, 0)
    give(1, gup_v.at[:, other], gup_r)
    gb_r[0] = jnp.where(first_core, gb_v[:, F1:], gb_v[:, :F1])
    give(2, gb_r.at[0], gb_r.at[1])
    chain.run(0, 2)
    d_first_norm = collected(2, dnorm_v[...])
    normed_one = normed_v[...]
    put_stat(3, col_sum(d_first_norm * normed_one))
    put_stat(4, col_sum(d_first_norm))
    d_first = layer_back(d_first_norm * gain1, normed_one, inverse_one)
    put_stat(5, col_sum(d_first))
    stats_ref[:, 6:8] = jnp.zeros((n, 2, hc), F32)
    dfirst_ref[...] = d_first
    dfa[chip] = d_first.astype(BF16)
    gathers[2].send(dfa.at[chip])

    def att_back(j, carry):
        chain.run(2 * j + 2, 2 * j + 4)

        @pl.when(j == 1)
        def _():
            gathers[2].relay()

        gathers[2].arrived(j)
        c = flip(chip, j, C)
        datt_ref[c, core] = rows_dot_t(dfa[c], wout_v[core]).astype(BF16)
        dattst[j] = rows_dot_t(dfa[c], wout_v[other]).astype(BF16)
        remote(dattst.at[j], datt_ref.at[c, core], dx_ss.at[j], dx_rs.at[j], partner).start()
        return carry

    lax.fori_loop(0, C, att_back, 0)
    dfa_all = dfa[...].reshape(Ph, D)
    gout_v[0] = cols_dot(attp[...].reshape(Ph, hc), dfa_all).astype(BF16)
    give(3, gout_v.at[0], gout_r)
    gout_v[1] = cols_dot(att_ref[:, core].reshape(Ph, hc), dfa_all).astype(BF16)

    chain.run(2 * C + 2, chain.slots)
    taken(1, None, gup_r)
    gup_ref[...] = (gup_v[:, core].astype(F32) + gup_r[...].astype(F32)).astype(BF16)
    taken(2, None, gb_r.at[1])
    gbup_ref[...] = jnp.where(first_core, gb_v[:, :F1], gb_v[:, F1:]) + gb_r[1]
    taken(3, None, gout_r)
    gout_ref[...] = (gout_v[1].astype(F32) + gout_r[...].astype(F32)).astype(BF16)

    chain.settle()
    out_sum.settle()
    for gather in gathers:
        gather.settle()
    gdn_done_ref[...] = gdn_f[...]
    await_send(attp, ap_ss.at[0], partner)
    await_send(gdn_r, gx_ss.at[0], partner)
    await_send(gup_r, gx_ss.at[1], partner)
    await_send(gb_r.at[0], gx_ss.at[2], partner)
    await_send(gout_r, gx_ss.at[3], partner)

    def settle(j, carry):
        c = flip(chip, j, C)
        await_recv(datt_ref.at[c, other], dx_rs.at[j], partner)
        await_send(dattst.at[j], dx_ss.at[j], partner)

        @pl.when(j > 0)
        def _():
            for r in range(1, 3):
                await_send(stage.at[r, j], sc_ss.at[r, j, 0], peer(j))

        return carry

    lax.fori_loop(0, C, settle, 0)


def middle_call(S, n, att, hidden, cot, par, wout, wout_o, wup2, wdn, wdn_o, bup):
    C = n // 2
    L, D = hidden.shape
    hc = D // n
    F1 = wdn.shape[0]
    F2 = 2 * F1
    dims = (S, n, C, L, D, hc, F1)
    dma = pltpu.SemaphoreType.DMA
    vm = pl.BlockSpec(memory_space=pltpu.VMEM)
    anyw = pl.BlockSpec(memory_space=pl.ANY)
    sds = jax.ShapeDtypeStruct
    Dn = D // n
    pc, early = 16, EARLY_PIECES
    return pl.pallas_call(
        functools.partial(middle_kernel, dims),
        out_shape=(
            sds((L, D), BF16),
            sds((L, D), F32),
            sds((C, 2, L, hc), BF16),
            sds((pc - early, F1 // pc, D), BF16),
            sds((C, Dn, F2), BF16),
            sds((hc, D), BF16),
            sds((n, 8, hc), F32),
            sds((1, F1), F32),
            sds((early, F1 // pc, D), BF16),
        ),
        in_specs=[vm, vm, vm, vm, anyw, anyw, anyw, anyw, anyw, vm],
        out_specs=(vm,) * 9,
        scratch_shapes=[
            pltpu.VMEM((2, hc, D), BF16),
            pltpu.VMEM((n, Dn, F2), BF16),
            pltpu.VMEM((2, F1, D), BF16),
            pltpu.VMEM((C, L, hc), BF16),
            pltpu.VMEM((C, L, D), BF16),
            pltpu.VMEM((C, L, D), BF16),
            pltpu.VMEM((C, L, D), BF16),
            pltpu.VMEM((C, L, F2), BF16),
            pltpu.VMEM((C, L, F2), F32),
            pltpu.VMEM((C, L, F2), BF16),
            pltpu.VMEM((3, C, L, D), BF16),
            pltpu.VMEM((3, C, L, D), BF16),
            pltpu.VMEM((L, D), F32),
            pltpu.VMEM((L, D), F32),
            pltpu.VMEM((L, D), F32),
            pltpu.VMEM((2, pc, F1 // pc, D), BF16),
            pltpu.VMEM((pc, F1 // pc, D), BF16),
            pltpu.VMEM((early, F1 // pc, D), BF16),
            pltpu.VMEM((early, F1 // pc, D), BF16),
            pltpu.VMEM((early, F1 // pc, D), BF16),
            pltpu.VMEM((early, F1 // pc, D), BF16),
            pltpu.VMEM((C, 2, Dn, F2), BF16),
            pltpu.VMEM((C, Dn, F2), BF16),
            pltpu.VMEM((2, hc, D), BF16),
            pltpu.VMEM((hc, D), BF16),
            pltpu.VMEM((1, F2), F32),
            pltpu.VMEM((2, 1, F1), F32),
            pltpu.VMEM((C, L, hc), BF16),
            dma((1,)),
            dma((1,)),
            dma((3, C, 2)),
            dma((3, C, 2)),
            dma((3, C, 2)),
            dma((3, C, 2)),
            dma((4,)),
            dma((4,)),
            dma((C,)),
            dma((C,)),
            dma((6, early)),
            dma((5,)),
        ],
        compiler_params=pltpu.CompilerParams(
            collective_id=1, has_side_effects=True, vmem_limit_bytes=MIDDLE_VMEM * MIB
        ),
        name="middle_stage",
    )(att, hidden, cot, par, wout, wout_o, wup2, wdn, wdn_o, bup)


def exit_kernel(
    dims,
    dq_ref,
    dkv_ref,
    hid_ref,
    wq_ref,
    dfirst_ref,
    stats_ref,
    gbup_ref,
    pos_ref,
    gupc_ref,
    goutc_ref,
    gdnc_ref,
    ginp_ref,
    dh_ref,
    gq_f,
    up_f,
    out_f,
    dn_f,
    gtable_ref,
    small_ref,
    gbo_ref,
    zr,
    own3,
    got3,
    x6,
    stage,
    recv,
    dhb,
    gq_v,
    gq_r,
    gq_s,
    gq_o,
    gq_l,
    gq_x,
    up_o,
    up_l,
    up_x,
    out_o,
    out_l,
    out_x,
    dn_o,
    dn_l,
    dn_x,
    plane,
    prod,
    st_r,
    st_v,
    zst,
    zgb,
    zk_ss,
    zk_rs,
    x_ss,
    x_rs,
    sc_ss,
    sc_rs,
    st_ss,
    st_rs,
    zs_ss,
    zs_rs,
    gq_ss,
    gq_rs,
    gx_ss,
    gx_rs,
    ua_ss,
    ua_rs,
    qc,
    uc,
    oc,
    dc,
    zl_ss,
    zl_rs,
    ag_ss,
    ag_rs,
    pf_ss,
    pf_rs,
    loc,
):
    S, n, C, L, D, hc, F1, R, rt = dims
    Dn, Ph = D // n, C * L
    z = lax.axis_index("seq")
    s = lax.axis_index("shard")
    core = lax.rem(s, 2)
    chip = s // 2
    other = 1 - core
    twin = 2 * chip + other
    partner = (z, twin)
    first_core = core == 0

    def peer(j):
        return (z, 2 * flip(chip, j, C) + core)

    barrier = pltpu.get_barrier_semaphore()
    for d in range(1, n):
        pl.semaphore_signal(barrier, inc=1, device_id=(z, flip(s, d, n)), device_id_type=MESH)
    for d in range(1, S):
        pl.semaphore_signal(barrier, inc=1, device_id=(lax.rem(z + d, S), s), device_id_type=MESH)
    pl.semaphore_wait(barrier, n - 1 + S - 1)

    for j in range(C - 1, -1, -1):
        c = flip(chip, j, C)

        @pl.when(z > 0)
        def _():
            remote(
                dkv_ref.at[0, c], zr.at[1, c], zk_ss.at[j, 0], zk_rs.at[j, 1], (z - 1, s)
            ).start()

        @pl.when(z < S - 1)
        def _():
            remote(
                dkv_ref.at[2, c], zr.at[0, c], zk_ss.at[j, 1], zk_rs.at[j, 0], (z + 1, s)
            ).start()

    quarter = Dn // 4
    mine = pl.ds(4 * chip, 4)

    def block_of(j):
        return pl.ds(4 * flip(chip, j, C), 4)

    for j in range(C - 1, 0, -1):
        remote(
            gupc_ref.at[flip(chip, j, C)], up_o.at[mine], ua_ss.at[j], ua_rs.at[j], peer(j)
        ).start()
    up_o[mine] = gupc_ref[chip]
    out_o[...] = goutc_ref[...].reshape(4, quarter, D)
    dn_o[...] = gdnc_ref[...]
    wide = Chain(S, z, s, up_o, up_l, up_x, up_f, uc)
    square = Chain(S, z, s, out_o, out_l, out_x, out_f, oc)
    late = Chain(S, z, s, dn_o, dn_l, dn_x, dn_f, dc)
    inner = Chain(S, z, s, gq_o, gq_l, gq_x, gq_f, qc)
    late.give_out(0, late.pieces)
    square.give_out(0, square.pieces)
    starts = [0, late.pieces, late.pieces + square.pieces]
    starts.append(starts[2] + wide.pieces)
    last_step = starts[3] + inner.slots

    def chain_step(m, carry=0):
        for chain, begin in zip((late, square, wide, inner), starts):
            chain.slot(m - begin)
        return carry

    def chain_steps(begin, end):
        lax.fori_loop(begin, end, chain_step, 0)

    st_r[s] = stats_ref[s]
    for d in range(1, n):
        to = flip(s, d, n)
        remote(stats_ref.at[to], st_r.at[s], st_ss.at[d], st_rs.at[d], (z, to)).start()

    def fold(k, carry):
        j = C - 1 - k
        c = flip(chip, j, C)
        whole = dkv_ref[1, c].astype(F32)

        @pl.when(z > 0)
        def _():
            await_recv(zr.at[0, c], zk_rs.at[j, 0], (z - 1, s))

        @pl.when(z < S - 1)
        def _():
            await_recv(zr.at[1, c], zk_rs.at[j, 1], (z + 1, s))

        whole = whole + jnp.where(z > 0, zr[0, c].astype(F32), 0.0)
        whole = whole + jnp.where(z < S - 1, zr[1, c].astype(F32), 0.0)
        whole = whole.astype(BF16)
        own3[c, :, :, :hc] = dq_ref[c]
        own3[c, :, :, hc:] = whole
        remote(own3.at[c, other], got3.at[c], x_ss.at[j], x_rs.at[j], partner).start()
        sums = jnp.sum(own3[c].astype(F32), axis=(0, 1), keepdims=False)
        st_v[0:1] += sums[None, :hc]
        st_v[1:2] += sums[None, 2 * hc :]
        return carry

    st_v[...] = jnp.zeros_like(st_v)
    lax.fori_loop(0, C, fold, 0)

    def partial(j):
        c = flip(chip, j, C)
        await_recv(got3.at[c], x_rs.at[j], partner)
        mine, theirs = own3[c, core], got3[c]
        low = jnp.where(first_core, mine, theirs)
        high = jnp.where(first_core, theirs, mine)
        pieces = []
        for part in range(3):
            pieces += [low[:, part * hc : (part + 1) * hc], high[:, part * hc : (part + 1) * hc]]
        x6[c] = jnp.concatenate(pieces, axis=1)
        return rows_dot_t(x6[c], wq_ref[...].reshape(D, 6 * hc))

    tokens_sum = Scatter(C, peer, L, stage, recv, sc_ss, sc_rs)
    total = tokens_sum.send(partial) + dfirst_ref[...]
    chain_steps(0, 2)

    def qkv_grad(c, carry):
        chain_step(2 + c)
        cols = pl.ds(pl.multiple_of(c * 2 * Dn, 128), 2 * Dn)
        res = cols_dot(hid_ref[:, :, cols].reshape(Ph, 2 * Dn), x6[...].reshape(Ph, 6 * hc))
        gq_v[c] = res.astype(BF16).reshape(2, 4, quarter, 6 * hc)
        return carry

    lax.fori_loop(0, C, qkv_grad, 0)
    remote(gq_v.at[:, other], gq_r, gq_ss.at[0], gq_rs.at[0], partner).start()

    sums = st_r[s]
    for d in range(1, n):
        src = flip(s, d, n)
        await_recv(st_r.at[src], st_rs.at[d], (z, src))
    sums = st_r[0]
    for i in range(1, n):
        sums = sums + st_r[i]
    zst[z] = sums
    zst[z, 6:8] = st_v[...]
    zgb[z] = gbup_ref[...]
    for d in range(1, S):
        to = (lax.rem(z + d, S), s)
        remote(zst.at[z], zst.at[z], zs_ss.at[d, 0], zs_rs.at[d, 0], to).start()
        remote(zgb.at[z], zgb.at[z], zs_ss.at[d, 1], zs_rs.at[d, 1], to).start()

    for j in range(1, C):
        await_recv(up_o.at[block_of(j)], ua_rs.at[j], peer(j))
    wide.give_out(0, 2)
    chain_steps(C + 2, C + 4)
    await_recv(gq_r, gq_rs.at[0], partner)
    gq_s[...] = (gq_v[:, core].astype(F32) + gq_r[...].astype(F32)).astype(BF16)
    for j in range(C - 1, 0, -1):
        remote(
            gq_s.at[flip(chip, j, C)], gq_o.at[mine], gx_ss.at[j], gx_rs.at[j], peer(j)
        ).start()
    gq_o[mine] = gq_s[chip]

    total = tokens_sum.collect(total)
    ginp = total.astype(BF16)
    ginp_ref[...] = ginp
    dhb[...] = ginp
    keep = pltpu.make_async_copy(dhb, dh_ref.at[z, s], loc.at[0])
    keep.start()

    def gather_of(at):
        return Gather(
            C, chip, peer, L, lambda c: dh_ref.at[at, 2 * c + core], ag_ss.at[at], ag_rs.at[at]
        )

    def broadcast(src, at):
        gather_of(at).send(src)
        remote(src, dh_ref.at[at, s], pf_ss.at[at, 0], pf_rs.at[at, 0], partner).start()

    def pass_on(d):
        @pl.when(z - d >= 0)
        def _():
            gather_of(z - d).relay()

        if d:

            @pl.when(z + d <= S - 1)
            def _():
                gather_of(z + d).relay()

    @pl.when(z < S - 1)
    def _():
        remote(dhb, dh_ref.at[z, s], zl_ss.at[z, 0], zl_rs.at[z, 0], (z + 1, s)).start()

    @pl.when(z > 0)
    def _():
        remote(dhb, dh_ref.at[z, s], zl_ss.at[z, 1], zl_rs.at[z, 1], (z - 1, s)).start()

    broadcast(dhb, z)
    wide.give_out(2, wide.pieces)
    chain_steps(C + 4, C + 7)
    def next_planes(d):
        @pl.when(z - d >= 0)
        def _():
            at = z - d
            await_recv(dh_ref.at[at, s], zl_rs.at[at, 0], (z - 1, s))

            @pl.when(z < S - 1)
            def _():
                remote(
                    dh_ref.at[at, s], dh_ref.at[at, s], zl_ss.at[at, 0], zl_rs.at[at, 0], (z + 1, s)
                ).start()

            broadcast(dh_ref.at[at, s], at)

        @pl.when(z + d <= S - 1)
        def _():
            at = z + d
            await_recv(dh_ref.at[at, s], zl_rs.at[at, 1], (z + 1, s))

            @pl.when(z > 0)
            def _():
                remote(
                    dh_ref.at[at, s], dh_ref.at[at, s], zl_ss.at[at, 1], zl_rs.at[at, 1], (z - 1, s)
                ).start()

            broadcast(dh_ref.at[at, s], at)

    def relay(at):
        for j in range(1, C):
            src = 2 * flip(chip, j, C) + core
            gather_of(at).arrived(j)
            remote(
                dh_ref.at[at, src], dh_ref.at[at, src], pf_ss.at[at, j], pf_rs.at[at, j], partner
            ).start()

    def plane_sum(t, step):
        at = flip(z, t, S)
        chain_step(step)
        relay(at)
        chain_step(step + 1)

        for j in range(C):
            src = 2 * flip(chip, j, C) + other
            await_recv(dh_ref.at[at, src], pf_rs.at[at, j], partner)

        if t == 0:
            keep.wait()

        load = pltpu.make_async_copy(dh_ref.at[at], plane, loc.at[1])
        load.start()
        load.wait()

        def rows_tile(r, carry):
            chain_step(step + 2 + r)
            start = pl.multiple_of(r * rt, rt)
            ids = lax.broadcasted_iota(jnp.int32, (rt, L), 0) + (start + s * R)
            hot = jnp.concatenate(
                [jnp.where(ids == pos_ref[at, i], 1.0, 0.0).astype(BF16) for i in range(n)], axis=1
            )
            prod[at, pl.ds(start, rt), :] = rows_dot(hot, plane[...].reshape(n * L, D))
            return carry

        lax.fori_loop(0, R // rt, rows_tile, 0)

    next_planes(1)
    pass_on(0)
    chain_steps(C + 7, C + 11)
    step = C + 11
    for t in range(S):
        if t + 2 < S:
            next_planes(t + 2)
        if t + 1 < S:
            pass_on(t + 1)
        if t == 0:
            for j in range(1, C):
                await_recv(gq_o.at[block_of(j)], gx_rs.at[j], peer(j))
            inner.give_out(0, inner.pieces)
        chain_steps(step, step + 2)
        plane_sum(t, step + 2)
        step += 4 + R // rt

    def add_tile(r, carry):
        at = pl.ds(pl.multiple_of(r * rt, rt), rt)
        rows = prod[0, at]
        for i in range(1, S):
            rows = rows + prod[i, at]
        gtable_ref[at] = rows.astype(BF16)
        return carry

    lax.fori_loop(0, R // rt, add_tile, 0)

    chain_steps(step, last_step)
    for d in range(1, S):
        src = lax.rem(z + S - d, S)
        await_recv(zst.at[src], zs_rs.at[d, 0], (src, s))
        await_recv(zgb.at[src], zs_rs.at[d, 1], (src, s))
    small, big = zst[0], zgb[0]
    for i in range(1, S):
        small = small + zst[i]
        big = big + zgb[i]
    small_ref[...] = small
    gbo_ref[...] = big

    def settle_plane(at, carry):
        for j in range(C):
            await_send(dhb, pf_ss.at[at, j], partner)
        gather_of(at).settle()
        return carry

    lax.fori_loop(0, S, settle_plane, 0)
    for at in range(S):

        @pl.when((z >= at) & (z < S - 1))
        def _():
            await_send(dhb, zl_ss.at[at, 0], (z + 1, s))

        @pl.when((z <= at) & (z > 0))
        def _():
            await_send(dhb, zl_ss.at[at, 1], (z - 1, s))

    for j in range(C):

        @pl.when(z > 0)
        def _():
            await_send(zr.at[0, 0], zk_ss.at[j, 0], (z - 1, s))

        @pl.when(z < S - 1)
        def _():
            await_send(zr.at[0, 0], zk_ss.at[j, 1], (z + 1, s))

        await_send(got3.at[0], x_ss.at[j], partner)
    for d in range(1, n):
        await_send(st_r.at[s], st_ss.at[d], (z, flip(s, d, n)))
    for d in range(1, S):
        to = (lax.rem(z + d, S), s)
        await_send(zst.at[z], zs_ss.at[d, 0], to)
        await_send(zgb.at[z], zs_ss.at[d, 1], to)
    for j in range(1, C):
        await_send(gq_s.at[chip], gx_ss.at[j], peer(j))
        await_send(gupc_ref.at[chip], ua_ss.at[j], peer(j))
    tokens_sum.settle()
    wide.settle()
    square.settle()
    late.settle()
    inner.settle()
    await_send(gq_r, gq_ss.at[0], partner)


def exit_call(S, n, R, dq, dkv, hid_half, wq, dfirst, stats, gbup, pos, gupc, goutc, gdnc):
    C = n // 2
    L, D = dfirst.shape
    hc = D // n
    F1 = gbup.shape[1]
    Dn = D // n
    F2 = gupc.shape[3]
    dims = (S, n, C, L, D, hc, F1, R, 256)
    dma = pltpu.SemaphoreType.DMA
    vm = pl.BlockSpec(memory_space=pltpu.VMEM)
    anyw = pl.BlockSpec(memory_space=pl.ANY)
    sds = jax.ShapeDtypeStruct
    return pl.pallas_call(
        functools.partial(exit_kernel, dims),
        out_shape=(
            sds((L, D), BF16),
            sds((S, n, L, D), BF16),
            sds((4 * C, Dn // 4, 6 * hc), BF16),
            sds((4 * C, Dn // 4, F2), BF16),
            sds((4, Dn // 4, D), BF16),
            sds(gdnc.shape, BF16),
            sds((R, D), BF16),
            sds((8, hc), F32),
            sds((1, F1), F32),
        ),
        in_specs=[vm] * 11,
        out_specs=(vm, anyw) + (vm,) * 7,
        scratch_shapes=[
            pltpu.VMEM((2, C, 2, L, 2 * hc), BF16),
            pltpu.VMEM((C, 2, L, 3 * hc), BF16),
            pltpu.VMEM((C, L, 3 * hc), BF16),
            pltpu.VMEM((C, L, 6 * hc), BF16),
            pltpu.VMEM((C, L, D), BF16),
            pltpu.VMEM((C, L, D), BF16),
            pltpu.VMEM((L, D), BF16),
            pltpu.VMEM((C, 2, 4, Dn // 4, 6 * hc), BF16),
            pltpu.VMEM((C, 4, Dn // 4, 6 * hc), BF16),
            pltpu.VMEM((C, 4, Dn // 4, 6 * hc), BF16),
            pltpu.VMEM((4 * C, Dn // 4, 6 * hc), BF16),
            pltpu.VMEM((4 * C, Dn // 4, 6 * hc), BF16),
            pltpu.VMEM((4 * C, Dn // 4, 6 * hc), BF16),
            pltpu.VMEM((4 * C, Dn // 4, F2), BF16),
            pltpu.VMEM((4 * C, Dn // 4, F2), BF16),
            pltpu.VMEM((4 * C, Dn // 4, F2), BF16),
            pltpu.VMEM((4, Dn // 4, D), BF16),
            pltpu.VMEM((4, Dn // 4, D), BF16),
            pltpu.VMEM((4, Dn // 4, D), BF16),
            pltpu.VMEM(gdnc.shape, BF16),
            pltpu.VMEM(gdnc.shape, BF16),
            pltpu.VMEM(gdnc.shape, BF16),
            pltpu.VMEM((n, L, D), BF16),
            pltpu.VMEM((S, R, D), F32),
            pltpu.VMEM((n, 8, hc), F32),
            pltpu.VMEM((2, hc), F32),
            pltpu.VMEM((S, 8, hc), F32),
            pltpu.VMEM((S, 1, F1), F32),
            dma((C, 2)),
            dma((C, 2)),
            dma((C,)),
            dma((C,)),
            dma((C, 2)),
            dma((C, 2)),
            dma((n,)),
            dma((n,)),
            dma((S, 2)),
            dma((S, 2)),
            dma((1,)),
            dma((1,)),
            dma((C,)),
            dma((C,)),
            dma((C,)),
            dma((C,)),
            dma((6, 4 * C)),
            dma((6, 4 * C)),
            dma((6, 4)),
            dma((6, gdnc.shape[0])),
            dma((S, 2)),
            dma((S, 2)),
            dma((S, C, 2)),
            dma((S, C, 2)),
            dma((S, C)),
            dma((S, C)),
            dma((2,)),
        ],
        compiler_params=pltpu.CompilerParams(
            collective_id=2, has_side_effects=True, vmem_limit_bytes=EXIT_VMEM * MIB
        ),
        name="exit_stage",
    )(dq, dkv, hid_half, wq, dfirst, stats, gbup, pos, gupc, goutc, gdnc)


def finish_kernel(
    dims,
    table_ref,
    gq_ref,
    up_ref,
    out_ref,
    early_ref,
    late_ref,
    res_ref,
    inp_ref,
    small_ref,
    gb_ref,
    table_o,
    gq_o,
    up_o,
    out_o,
    dn_o,
    res_o,
    inp_o,
    gb_o,
    *small_o,
):
    C, D, hc = dims
    i = pl.program_id(0)
    h2 = 2 * hc
    F2 = up_ref.shape[3]
    table_o[...] = table_ref[...].astype(F32)
    for c in range(C):
        up_o[:, c * F2 : (c + 1) * F2] = up_ref[c, 0].astype(F32)
        for part in range(3):
            gq_o[:, part * D + c * h2 : part * D + (c + 1) * h2] = gq_ref[
                c, 0, :, part * h2 : (part + 1) * h2
            ].astype(F32)
    out_o[...] = out_ref[0].astype(F32)
    piece = early_ref.shape[0] * early_ref.shape[1]
    dn_o[...] = jnp.where(i < 4, early_ref[...], late_ref[...]).reshape(piece, D).astype(F32)
    res_o[...] = res_ref[...]
    inp_o[...] = inp_ref[...]
    gb_o[...] = gb_ref[...]
    for r, o in enumerate(small_o):
        o[...] = small_ref[r : r + 1]


def finish_call(n, table, gq, up, out, early, late, res, inp, small, gb):
    C = n // 2
    R, D = table.shape
    L = res.shape[0]
    Dn = D // n
    hc = Dn
    q, F2 = up.shape[1:]
    h = q // 2
    piece = early.shape[1]
    F1 = gb.shape[1]
    sds = jax.ShapeDtypeStruct
    steps = 8
    two = lambda rows, cols: pl.BlockSpec((rows, cols), lambda i: (i, 0))
    quad = lambda cols: pl.BlockSpec((C, 1, h, cols), lambda i: (0, i // 2, i % 2, 0))
    fixed = lambda rows, cols: pl.BlockSpec((rows, cols), lambda i: (0, 0))
    return pl.pallas_call(
        functools.partial(finish_kernel, (C, D, hc)),
        grid=(steps,),
        out_shape=(
            sds((R, D), F32),
            sds((Dn, 3 * D), F32),
            sds((Dn, C * F2), F32),
            sds((Dn, D), F32),
            sds((F1, D), F32),
            sds((L, D), BF16),
            sds((L, D), BF16),
            sds((1, F1), F32),
        )
        + (sds((1, hc), F32),) * 8,
        in_specs=[
            two(R // steps, D),
            quad(6 * hc),
            quad(F2),
            pl.BlockSpec((1, h, D), lambda i: (i // 2, i % 2, 0)),
            pl.BlockSpec((2, piece, D), lambda i: (jnp.minimum(i, 3), 0, 0)),
            pl.BlockSpec((2, piece, D), lambda i: (jnp.maximum(i - 4, 0), 0, 0)),
            two(L // steps, D),
            two(L // steps, D),
            fixed(8, hc),
            fixed(1, F1),
        ],
        out_specs=(
            two(R // steps, D),
            two(h, 3 * D),
            two(h, C * F2),
            two(h, D),
            two(2 * piece, D),
            two(L // steps, D),
            two(L // steps, D),
            fixed(1, F1),
        )
        + (fixed(1, hc),) * 8,
        compiler_params=pltpu.CompilerParams(vmem_limit_bytes=ATTEND_VMEM * MIB),
        name="finish_stage",
    )(
        table,
        gq.reshape(C, 4, q, 6 * hc),
        up.reshape(C, 4, q, F2),
        out,
        early,
        late,
        res,
        inp,
        small,
        gb,
    )


QUERY_BLOCK = 512
KEY_BLOCK = 512
BACK_KEY_BLOCK = 256
EARLY_PIECES = 8


def local(
    inputs,
    positions,
    segments,
    pos_table,
    w_qkv,
    b_query,
    b_value,
    w_out,
    b_out,
    ln1_gain,
    ln1_bias,
    w_up,
    b_up,
    w_down,
    b_down,
    ln2_gain,
    ln2_bias,
    cotangent,
):
    S, n = lax.axis_size("seq"), lax.axis_size("shard")
    L, D = inputs.shape
    P_, hc, C = L * n, D // n, n // 2
    R = pos_table.shape[0]
    row = lambda v: v.reshape(1, -1)
    rows = [row(v) for v in (b_out, ln1_gain, ln1_bias, b_down, ln2_gain, ln2_bias, b_query, b_value)]
    q, kv, hid_half, hidden, wq, wup2, wdn_o, wout_o, par_all, bup2, pos_glob, lohi = entry_call(
        S,
        n,
        row(positions),
        inputs,
        pos_table,
        w_qkv,
        w_up,
        w_down,
        w_out,
        segments.reshape(S * n, 1, L),
        row(b_up),
        rows,
    )
    q = q.reshape(P_, hc)
    kv = kv.reshape(3 * P_, 2 * hc)
    att, lse = attend_call(q, kv, lohi, QUERY_BLOCK, KEY_BLOCK)
    result, dfirst, datt, gdn_late, gup, gout, stats, gbup, gdn_early = middle_call(
        S,
        n,
        att.reshape(C, 2, L, hc),
        hidden,
        cotangent,
        par_all,
        w_out,
        wout_o,
        wup2,
        w_down,
        wdn_o,
        bup2,
    )
    dq, dkv = attend_back_call(
        q, kv, lohi, att, datt.reshape(P_, hc), lse, QUERY_BLOCK, BACK_KEY_BLOCK
    )
    ginp, dh, gqkv, gup, gout, gdn_late, gtable, small, gbo = exit_call(
        S,
        n,
        R,
        dq.reshape(C, 2, L, hc),
        dkv.reshape(3, C, 2, L, 2 * hc),
        hid_half,
        wq,
        dfirst,
        stats,
        gbup,
        pos_glob,
        gup.reshape(C, 4, D // n // 4, gup.shape[2]),
        gout,
        gdn_late,
    )
    gtable, gqkv, gup, gout, gdn, result, ginp, gbo, *small = finish_call(
        n, gtable, gqkv, gup, gout, gdn_early, gdn_late, result, ginp, small, gbo
    )
    small = [v[0] for v in small]
    return (
        result,
        ginp,
        gtable,
        gqkv,
        small[6],
        small[7],
        gout,
        small[5],
        small[3],
        small[4],
        gup,
        gbo[0],
        gdn,
        small[2],
        small[0],
        small[1],
    )


def solution(mesh):
    in_specs = (
        P(("seq", "shard"), None),
        P(("seq", "shard")),
        P(),
        P("shard", None),
        P("shard", None),
        P("shard"),
        P("shard"),
        P("shard", None),
        P("shard"),
        P("shard"),
        P("shard"),
        P("shard", None),
        P("shard"),
        P("shard", None),
        P("shard"),
        P("shard"),
        P("shard"),
        P(("seq", "shard"), None),
    )
    out_specs = (
        P(("seq", "shard"), None),
        P(("seq", "shard"), None),
        P("shard", None),
        P("shard", None),
        P("shard"),
        P("shard"),
        P("shard", None),
        P("shard"),
        P("shard"),
        P("shard"),
        P("shard", None),
        P("shard"),
        P("shard", None),
        P("shard"),
        P("shard"),
        P("shard"),
    )
    return jax.shard_map(local, mesh=mesh, in_specs=in_specs, out_specs=out_specs, check_vma=False)
```

```python
import functools
import math

import jax
import jax.numpy as jnp
from jax import lax
from jax.experimental import pallas as pl
from jax.experimental.pallas import tpu as pltpu
from jax.sharding import PartitionSpec as P

HEADS = 16
HEAD_DIM = 64
score_scale = 0.125
neg_large = -1e30
epsilon = 1e-06
root_half = 0.7071067811865476
inv_root_two_pi = 0.3989422804014327
MESH = pl.DeviceIdType.MESH
F32 = jnp.float32
BF16 = jnp.bfloat16
MIB = 1024 * 1024
ENTRY_VMEM, ATTEND_VMEM, MIDDLE_VMEM, BACK_VMEM, EXIT_VMEM = 24, 16, 40, 20, 42


def flip(value, mask, width):
    total, bit = 0, 1
    while bit < width:
        a = lax.rem(value // bit, 2)
        b = (mask // bit) % 2 if isinstance(mask, int) else lax.rem(mask // bit, 2)
        total = total + lax.rem(a + b, 2) * bit
        bit *= 2
    return total


def remote(src, dst, send_sem, recv_sem, device):
    return pltpu.make_async_remote_copy(
        src_ref=src,
        dst_ref=dst,
        send_sem=send_sem,
        recv_sem=recv_sem,
        device_id=device,
        device_id_type=MESH,
    )


def await_recv(dst, sem, device):
    remote(dst, dst, sem, sem, device).wait_recv()


def await_send(src, sem, device):
    remote(src, src, sem, sem, device).wait_send()


class Chain:
    def __init__(self, S, z, s, own, land, cross, fin, sems, lag=4):
        self.S, self.s, self.lag, self.sems = S, s, lag, sems
        self.own, self.land, self.cross, self.fin = own, land, cross, fin
        low = 1 - (2 * z) // S
        self.depth = low * z + (1 - low) * (S - 1 - z)
        self.inward = (z + 2 * low - 1, s)
        self.outward = (z + 1 - 2 * low, s)
        self.mid = S // 2 - 1
        self.pieces = own.shape[0]
        self.slots = self.pieces + lag * self.mid + lag * max(self.mid - 1, 0)

    def give_out(self, start, stop):
        @pl.when(self.depth == 0)
        def _():
            def step(p, carry):
                remote(
                    self.own.at[p], self.land.at[p], self.sems.at[0, p], self.sems.at[1, p], self.inward
                ).start()
                return carry

            lax.fori_loop(start, stop, step, 0)

    def slot(self, k):
        p = k - self.lag * (self.depth - 1)

        @pl.when((self.depth > 0) & (p >= 0) & (p < self.pieces))
        def _():
            await_recv(self.land.at[p], self.sems.at[1, p], self.outward)
            both = self.own[p].astype(F32) + self.land[p].astype(F32)
            self.own[p] = both.astype(BF16)

            @pl.when(self.depth < self.mid)
            def _():
                remote(
                    self.own.at[p], self.land.at[p], self.sems.at[0, p], self.sems.at[1, p], self.inward
                ).start()

            @pl.when(self.depth == self.mid)
            def _():
                remote(
                    self.own.at[p], self.cross.at[p], self.sems.at[2, p], self.sems.at[3, p], self.inward
                ).start()

        x = k - self.lag * self.mid

        @pl.when((self.depth == self.mid) & (x >= 0) & (x < self.pieces))
        def _():
            await_recv(self.cross.at[x], self.sems.at[3, x], self.inward)
            both = self.own[x].astype(F32) + self.cross[x].astype(F32)
            self.fin[x] = both.astype(BF16)
            remote(
                self.fin.at[x], self.fin.at[x], self.sems.at[4, x], self.sems.at[5, x], self.outward
            ).start()

        b = k - self.lag * self.mid - self.lag * (self.mid - self.depth)

        @pl.when((self.depth < self.mid) & (self.depth > 0) & (b >= 0) & (b < self.pieces))
        def _():
            await_recv(self.fin.at[b], self.sems.at[5, b], self.inward)
            remote(
                self.fin.at[b], self.fin.at[b], self.sems.at[4, b], self.sems.at[5, b], self.outward
            ).start()

    def run(self, start, stop):
        def step(k, carry):
            self.slot(k)
            return carry

        lax.fori_loop(start, stop, step, 0)

    def settle(self):
        def step(p, carry):
            @pl.when(self.depth == 0)
            def _():
                await_recv(self.fin.at[p], self.sems.at[5, p], self.inward)

            @pl.when(self.depth < self.mid)
            def _():
                await_send(self.own.at[p], self.sems.at[0, p], self.inward)

            @pl.when(self.depth == self.mid)
            def _():
                await_send(self.own.at[p], self.sems.at[2, p], self.inward)

            @pl.when(self.depth > 0)
            def _():
                await_send(self.fin.at[p], self.sems.at[4, p], self.outward)

            return carry

        lax.fori_loop(0, self.pieces, step, 0)


class Gather:
    def __init__(self, C, chip, peer, rows, slot, ss, rs):
        self.C, self.chip, self.peer, self.rows, self.slot = C, chip, peer, rows, slot
        self.ss, self.rs = ss, rs

    def half(self, ref, h):
        return ref.at[pl.ds(h * (self.rows // 2), self.rows // 2)]

    def block(self, j):
        return self.slot(flip(self.chip, j, self.C))

    def send(self, src):
        dst = self.slot(self.chip)
        if self.C == 4:
            for j, first in ((1, 0), (2, 1)):
                for h in (first, 1 - first):
                    remote(
                        self.half(src, h), self.half(dst, h), self.ss.at[j, h], self.rs.at[j, h], self.peer(j)
                    ).start()
        else:
            for j in range(self.C - 1, 0, -1):
                remote(src, dst, self.ss.at[j, 0], self.rs.at[j, 0], self.peer(j)).start()

    def relay(self):
        if self.C == 4:
            for j, h, to in ((1, 0, 2), (2, 1, 1)):
                part = self.half(self.block(j), h)
                await_recv(part, self.rs.at[j, h], self.peer(j))
                remote(part, part, self.ss.at[3, h], self.rs.at[3, h], self.peer(to)).start()

    def arrived(self, j):
        if self.C == 4:
            for want, h in ((1, 1), (2, 0), (3, 0), (3, 1)):

                @pl.when(j == want)
                def _(want=want, h=h):
                    await_recv(self.half(self.block(want), h), self.rs.at[want, h], self.peer(want))
        else:

            @pl.when(j > 0)
            def _():
                await_recv(self.block(j), self.rs.at[j, 0], self.peer(j))

    def settle(self):
        own = self.slot(self.chip)
        if self.C == 4:
            for j in range(1, 4):
                for h in range(2):
                    await_send(self.half(own, h), self.ss.at[j, h], self.peer(j))
        else:
            for j in range(1, self.C):
                await_send(own, self.ss.at[j, 0], self.peer(j))


class Scatter:
    def __init__(self, C, peer, rows, stage, recv, ss, rs):
        self.C, self.peer, self.rows = C, peer, rows
        self.stage, self.recv, self.ss, self.rs = stage, recv, ss, rs

    def give(self, j, h, to):
        part = pl.ds(h * (self.rows // 2), self.rows // 2)
        remote(
            self.stage.at[j, part], self.recv.at[j, part], self.ss.at[j, h], self.rs.at[j, h], self.peer(to)
        ).start()

    def take(self, j, h, source):
        part = pl.ds(h * (self.rows // 2), self.rows // 2)
        await_recv(self.recv.at[j, part], self.rs.at[j, h], self.peer(source))
        return part

    def send(self, make):
        if self.C != 4:

            def step(k, carry):
                j = self.C - 1 - k
                self.stage[j] = make(j).astype(BF16)
                remote(
                    self.stage.at[j], self.recv.at[j], self.ss.at[j, 0], self.rs.at[j, 0], self.peer(j)
                ).start()
                return carry

            lax.fori_loop(0, self.C - 1, step, 0)
            return make(0)
        self.stage[3] = make(3).astype(BF16)
        self.give(3, 0, 2)
        self.give(3, 1, 1)
        self.stage[1] = make(1).astype(BF16)
        self.give(1, 1, 1)
        self.stage[2] = make(2).astype(BF16)
        self.give(2, 0, 2)
        own = make(0)
        for h, source, j in ((0, 2, 1), (1, 1, 2)):
            part = self.take(3, h, source)
            both = self.stage[j, part].astype(F32) + self.recv[3, part].astype(F32)
            self.stage[j, part] = both.astype(BF16)
            self.give(j, h, j)
        return own

    def collect(self, total):
        if self.C != 4:
            for j in range(1, self.C):
                await_recv(self.recv.at[j], self.rs.at[j, 0], self.peer(j))
                total = total + self.recv[j].astype(F32)
            return total
        for j in (1, 2):
            self.take(j, 2 - j, j)
            self.take(j, j - 1, j)
            total = total + self.recv[j].astype(F32)
        return total

    def settle(self):
        for j in range(1, self.C):
            if self.C == 4:
                for h in range(2):
                    part = pl.ds(h * (self.rows // 2), self.rows // 2)
                    await_send(self.stage.at[j, part], self.ss.at[j, h], self.peer(j))
            else:
                await_send(self.stage.at[j], self.ss.at[j, 0], self.peer(j))


def rows_dot(a, b):
    return lax.dot_general(a, b, (((1,), (0,)), ((), ())), preferred_element_type=F32)


def rows_dot_t(a, b):
    return lax.dot_general(a, b, (((1,), (1,)), ((), ())), preferred_element_type=F32)


def cols_dot(a, b):
    return lax.dot_general(a, b, (((0,), (0,)), ((), ())), preferred_element_type=F32)


def entry_kernel(
    dims,
    pos_hbm,
    inp_hbm,
    table_ref,
    wqkv_ref,
    wup_ref,
    wdn_ref,
    wout_ref,
    seg_hbm,
    bup_in_hbm,
    row0_ref,
    row1_ref,
    row2_ref,
    row3_ref,
    row4_ref,
    row5_ref,
    row6_ref,
    row7_ref,
    q_ref,
    kv_ref,
    hid_half_ref,
    hidden_ref,
    wq_ref,
    wup2_ref,
    wdn_o_ref,
    wout_o_ref,
    par_all_ref,
    bup2_ref,
    pos_glob_ref,
    lohi_ref,
    pos_ref,
    inp_ref,
    seg_ref,
    bup_in_ref,
    rows_ref,
    table_v,
    pstage,
    precv,
    cstage,
    crecv,
    qst,
    kvst,
    wup_own,
    par_ref,
    bup_ref,
    pos_ss,
    pos_rs,
    par_ss,
    par_rs,
    posz_ss,
    posz_rs,
    wq_ss,
    wq_rs,
    wqf_ss,
    wqf_rs,
    wup_ss,
    wup_rs,
    wupf_ss,
    wupf_rs,
    misc_ss,
    misc_rs,
    rsp_ss,
    rsp_rs,
    rsc_ss,
    rsc_rs,
    ag_ss,
    ag_rs,
    qx_ss,
    qx_rs,
    zx_ss,
    zx_rs,
    loc,
):
    S, n, C, L, D, hc, R, F2 = dims
    z = lax.axis_index("seq")
    s = lax.axis_index("shard")
    core = lax.rem(s, 2)
    chip = s // 2
    other = 1 - core
    partner = 2 * chip + other
    h2 = 2 * hc
    Dn = D // n

    rows = (row0_ref, row1_ref, row2_ref, row3_ref, row4_ref, row5_ref, row6_ref, row7_ref)
    smalls = [
        pltpu.make_async_copy(pos_hbm, pos_ref, loc.at[6]),
        pltpu.make_async_copy(seg_hbm, seg_ref, loc.at[7]),
        pltpu.make_async_copy(bup_in_hbm, bup_in_ref, loc.at[8]),
    ] + [
        pltpu.make_async_copy(row, rows_ref.at[i], loc.at[9 + i]) for i, row in enumerate(rows)
    ]
    for small in smalls:
        small.start()
    inp_copy = pltpu.make_async_copy(inp_hbm, inp_ref, loc.at[17])
    inp_copy.start()
    table_copy = pltpu.make_async_copy(table_ref, table_v, loc.at[0])
    table_copy.start()
    own_wq = []
    for part in range(3):
        own_wq.append(
            pltpu.make_async_copy(
                wqkv_ref.at[:, pl.ds(pl.multiple_of(part * D + chip * h2, 128), h2)],
                wq_ref.at[s, :, part * h2 : (part + 1) * h2],
                loc.at[1 + part],
            )
        )
        own_wq[-1].start()
    own_wup_in = pltpu.make_async_copy(
        wup_ref.at[:, pl.ds(pl.multiple_of(chip * F2, 128), F2)], wup_own, loc.at[4]
    )
    own_wup_in.start()

    for small in smalls:
        small.wait()
    for i in range(8):
        par_ref[i : i + 1] = rows_ref[i].astype(F32)
    bup_ref[...] = bup_in_ref[...].astype(F32)
    F1 = F2 // 2
    bup_mine = pl.ds(pl.multiple_of(core * F1, 128), F1)
    bup_theirs = pl.ds(pl.multiple_of(other * F1, 128), F1)
    bup2_ref[:, bup_mine] = bup_ref[...]

    barrier = pltpu.get_barrier_semaphore()
    for d in range(1, n):
        pl.semaphore_signal(barrier, inc=1, device_id=(z, flip(s, d, n)), device_id_type=MESH)
    for d in range(1, S):
        pl.semaphore_signal(barrier, inc=1, device_id=(lax.rem(z + d, S), s), device_id_type=MESH)

    for d in (1, S - 1):
        pl.semaphore_signal(
            barrier, inc=1, device_id=(lax.rem(z + d, S), partner), device_id_type=MESH
        )
    pl.semaphore_wait(barrier, n - 1 + S - 1 + 2)

    pos_glob_ref[z, s] = pos_ref[...]
    par_all_ref[s] = par_ref[...]
    for d in range(1, n):
        peer = (z, flip(s, d, n))
        remote(pos_ref, pos_glob_ref.at[z, s], pos_ss.at[d], pos_rs.at[d], peer).start()
        remote(par_ref, par_all_ref.at[s], par_ss.at[d], par_rs.at[d], peer).start()

    for own in own_wq:
        own.wait()

    def wq_src(peer_chip, part):
        return wqkv_ref.at[:, pl.ds(pl.multiple_of(part * D + peer_chip * h2, 128), h2)]

    for j in range(C - 1, 0, -1):
        pc = flip(chip, j, C)
        for part in range(3):
            remote(
                wq_src(pc, part),
                wq_ref.at[s, :, part * h2 : (part + 1) * h2],
                wq_ss.at[j, part],
                wq_rs.at[j, part],
                (z, 2 * pc + core),
            ).start()
    remote(wq_ref.at[s], wq_ref.at[s], wqf_ss.at[0], wqf_rs.at[0], (z, partner)).start()

    for d in range(1, n):
        src = flip(s, d, n)
        await_recv(pos_glob_ref.at[z, src], pos_rs.at[d], (z, src))
    for d in range(1, S):
        remote(
            pos_glob_ref.at[z],
            pos_glob_ref.at[z],
            posz_ss.at[d],
            posz_rs.at[d],
            (lax.rem(z + d, S), s),
        ).start()

    table_copy.wait()
    inp_copy.wait()
    lane_ids = lax.broadcasted_iota(jnp.int32, (L, R), 1) + s * R

    def picked(block):
        ids = jnp.broadcast_to(pos_glob_ref[z, block], (L, L)).T
        ids = jnp.concatenate([ids] * (R // L), axis=1)
        hot = jnp.where(ids == lane_ids, 1.0, 0.0).astype(BF16)
        return rows_dot(hot, table_v[...])

    def send_partner(j):
        pstage[j] = picked(2 * flip(chip, j, C) + other).astype(BF16)
        remote(pstage.at[j], precv.at[j], rsp_ss.at[j], rsp_rs.at[j], (z, partner)).start()

    def combined(j):
        mine = picked(2 * flip(chip, j, C) + core)
        await_recv(precv.at[j], rsp_rs.at[j], (z, partner))
        return mine + precv[j].astype(F32)

    def peer(j):
        return (z, 2 * flip(chip, j, C) + core)

    def partner_step(k, carry):
        send_partner(C - 1 - k)
        return carry

    lax.fori_loop(0, C, partner_step, 0)
    rows_sum = Scatter(C, peer, L, cstage, crecv, rsc_ss, rsc_rs)
    hidden = rows_sum.send(combined) + inp_ref[...].astype(F32)

    for j in range(1, C):
        src = 2 * flip(chip, j, C) + core
        for part in range(3):
            await_recv(
                wq_ref.at[src, :, part * h2 : (part + 1) * h2], wq_rs.at[j, part], (z, src)
            )
        remote(wq_ref.at[src], wq_ref.at[src], wqf_ss.at[j], wqf_rs.at[j], (z, partner)).start()

    hidden = rows_sum.collect(hidden)
    hidden_ref[...] = hidden
    hid_half_ref[chip] = hidden.astype(BF16)
    gather = Gather(C, chip, peer, L, lambda c: hid_half_ref.at[c], ag_ss, ag_rs)
    gather.send(hid_half_ref.at[chip])

    own_wup_in.wait()
    own_wup_out = pltpu.make_async_copy(wup_own, wup2_ref.at[s], loc.at[5])
    own_wup_out.start()
    for j in range(C - 1, 0, -1):
        pc = flip(chip, j, C)
        remote(
            wup_ref.at[:, pl.ds(pl.multiple_of(pc * F2, 128), F2)],
            wup2_ref.at[s],
            wup_ss.at[j],
            wup_rs.at[j],
            (z, 2 * pc + core),
        ).start()
    remote(wup_own, wup2_ref.at[s], wupf_ss.at[0], wupf_rs.at[0], (z, partner)).start()
    remote(wdn_ref, wdn_o_ref, misc_ss.at[0], misc_rs.at[0], (z, partner)).start()
    remote(wout_ref, wout_o_ref, misc_ss.at[1], misc_rs.at[1], (z, partner)).start()
    remote(bup_ref, bup2_ref.at[:, bup_mine], misc_ss.at[2], misc_rs.at[2], (z, partner)).start()

    for j in range(C):
        src = 2 * flip(chip, j, C) + other
        await_recv(wq_ref.at[src], wqf_rs.at[j], (z, partner))
    for d in range(1, n):
        src = flip(s, d, n)
        await_recv(par_all_ref.at[src], par_rs.at[d], (z, src))
    bias = jnp.concatenate([par_all_ref[2 * chip], par_all_ref[2 * chip + 1]], axis=1)
    bias_q, bias_v = bias[6:7], bias[7:8]
    first_core = core == 0

    def project(j, carry):
        c = flip(chip, j, C)

        gather.arrived(j)
        res = rows_dot(hid_half_ref[c], wq_ref[...].reshape(D, 3 * h2))
        query = (res[:, :h2] + bias_q).astype(BF16) * score_scale
        key = res[:, h2 : 2 * h2].astype(BF16)
        value = (res[:, 2 * h2 :] + bias_v).astype(BF16)
        q_ref[c, core] = jnp.where(first_core, query[:, :hc], query[:, hc:])
        kv_ref[1, c, core, :, :hc] = jnp.where(first_core, key[:, :hc], key[:, hc:])
        kv_ref[1, c, core, :, hc:] = jnp.where(first_core, value[:, :hc], value[:, hc:])
        qst[j] = jnp.where(first_core, query[:, hc:], query[:, :hc])
        kvst[j, :, :hc] = jnp.where(first_core, key[:, hc:], key[:, :hc])
        kvst[j, :, hc:] = jnp.where(first_core, value[:, hc:], value[:, :hc])
        own_kv = kv_ref.at[1, c, core]

        @pl.when(z < S - 1)
        def _():
            remote(
                own_kv, kv_ref.at[0, c, core], zx_ss.at[j, 0], zx_rs.at[j, 0], (z + 1, s)
            ).start()
            remote(
                kvst.at[j], kv_ref.at[0, c, core], zx_ss.at[j, 1], zx_rs.at[j, 1], (z + 1, partner)
            ).start()

        @pl.when(z > 0)
        def _():
            remote(
                own_kv, kv_ref.at[2, c, core], zx_ss.at[j, 2], zx_rs.at[j, 2], (z - 1, s)
            ).start()
            remote(
                kvst.at[j], kv_ref.at[2, c, core], zx_ss.at[j, 3], zx_rs.at[j, 3], (z - 1, partner)
            ).start()

        remote(qst.at[j], q_ref.at[c, core], qx_ss.at[j, 0], qx_rs.at[j, 0], (z, partner)).start()
        remote(
            kvst.at[j], kv_ref.at[1, c, core], qx_ss.at[j, 1], qx_rs.at[j, 1], (z, partner)
        ).start()
        return carry

    own_segs = jnp.concatenate([seg_ref[z * n + i] for i in range(n)], axis=1)

    def count(g, carry):
        low, high = carry
        keys = jnp.broadcast_to(seg_ref[g], (L, L)).T
        lows, highs = [], []
        for i in range(n):
            mine = own_segs[:, i * L : (i + 1) * L]
            lows.append(jnp.sum(jnp.where(keys < mine, 1.0, 0.0), axis=0, keepdims=True))
            highs.append(jnp.sum(jnp.where(keys <= mine, 1.0, 0.0), axis=0, keepdims=True))
        return low + jnp.concatenate(lows, axis=1), high + jnp.concatenate(highs, axis=1)

    none = jnp.zeros((1, n * L), F32)
    low, high = lax.fori_loop(0, S * n, count, (none, none))
    origin = ((z - 1) * n * L).astype(F32)
    lohi_ref[0:1] = low - origin
    lohi_ref[1:2] = high - origin

    gather.relay()
    lax.fori_loop(0, C, project, 0)

    for j in range(1, C):
        src = 2 * flip(chip, j, C) + core
        await_recv(wup2_ref.at[src], wup_rs.at[j], (z, src))
        remote(
            wup2_ref.at[src], wup2_ref.at[src], wupf_ss.at[j], wupf_rs.at[j], (z, partner)
        ).start()

    def settle(j, carry):
        c = flip(chip, j, C)
        await_recv(q_ref.at[c, other], qx_rs.at[j, 0], (z, partner))
        await_recv(kv_ref.at[1, c, other], qx_rs.at[j, 1], (z, partner))
        await_send(qst.at[j], qx_ss.at[j, 0], (z, partner))
        await_send(kvst.at[j], qx_ss.at[j, 1], (z, partner))

        @pl.when(z > 0)
        def _():
            await_recv(kv_ref.at[0, c, core], zx_rs.at[j, 0], (z - 1, s))
            await_recv(kv_ref.at[0, c, other], zx_rs.at[j, 1], (z - 1, partner))
            await_send(kvst.at[j], zx_ss.at[j, 2], (z - 1, s))
            await_send(kvst.at[j], zx_ss.at[j, 3], (z - 1, partner))

        @pl.when(z < S - 1)
        def _():
            await_recv(kv_ref.at[2, c, core], zx_rs.at[j, 2], (z + 1, s))
            await_recv(kv_ref.at[2, c, other], zx_rs.at[j, 3], (z + 1, partner))
            await_send(kvst.at[j], zx_ss.at[j, 0], (z + 1, s))
            await_send(kvst.at[j], zx_ss.at[j, 1], (z + 1, partner))

        await_send(pstage.at[j], rsp_ss.at[j], (z, partner))
        await_send(wq_ref.at[s], wqf_ss.at[j], (z, partner))
        await_recv(wup2_ref.at[2 * c + other], wupf_rs.at[j], (z, partner))
        await_send(wup2_ref.at[s], wupf_ss.at[j], (z, partner))
        return carry

    lax.fori_loop(0, C, settle, 0)
    gather.settle()
    rows_sum.settle()
    for j in range(1, C):
        await_send(wup_own, wup_ss.at[j], peer(j))
        for part in range(3):
            await_send(
                wq_ref.at[s, :, part * h2 : (part + 1) * h2], wq_ss.at[j, part], peer(j)
            )
    for d in range(1, n):
        peer = (z, flip(s, d, n))
        await_send(pos_ref, pos_ss.at[d], peer)
        await_send(par_ref, par_ss.at[d], peer)
    for d in range(1, S):
        src = lax.rem(z + S - d, S)
        await_recv(pos_glob_ref.at[src], posz_rs.at[d], (src, s))
        await_send(pos_glob_ref.at[z], posz_ss.at[d], (lax.rem(z + d, S), s))
    for i, (mine, got) in enumerate(
        ((wdn_ref, wdn_o_ref), (wout_ref, wout_o_ref), (bup_ref, bup2_ref.at[:, bup_theirs]))
    ):
        await_recv(got, misc_rs.at[i], (z, partner))
        await_send(mine, misc_ss.at[i], (z, partner))
    own_wup_out.wait()


def entry_call(S, n, pos, inp, table, wqkv, wup, wdn, wout, seg, bup, rows):
    C = n // 2
    L, D = inp.shape
    hc = D // n
    R = table.shape[0]
    F = wup.shape[1]
    F1, F2 = F // n, 2 * F // n
    dims = (S, n, C, L, D, hc, R, F2)
    dma = pltpu.SemaphoreType.DMA
    vm = pl.BlockSpec(memory_space=pltpu.VMEM)
    anyw = pl.BlockSpec(memory_space=pl.ANY)
    hbm = pl.BlockSpec(memory_space=pltpu.HBM)
    sds = jax.ShapeDtypeStruct
    return pl.pallas_call(
        functools.partial(entry_kernel, dims),
        out_shape=(
            sds((C, 2, L, hc), BF16),
            sds((3, C, 2, L, 2 * hc), BF16),
            sds((C, L, D), BF16),
            sds((L, D), F32),
            sds((n, D // n, 6 * hc), BF16),
            sds((n, D // n, F2), BF16),
            sds((F1, D), BF16),
            sds((D // n, D), BF16),
            sds((n, 8, hc), F32),
            sds((1, F2), F32),
            sds((S, n, 1, L), jnp.int32),
            sds((2, n * L), F32),
        ),
        in_specs=[hbm] * 17,
        out_specs=(vm, vm, vm, vm, vm, anyw, anyw, anyw, vm, vm, vm, vm),
        scratch_shapes=[
            pltpu.VMEM((1, L), jnp.int32),
            pltpu.VMEM((L, D), BF16),
            pltpu.VMEM((S * n, 1, L), jnp.int32),
            pltpu.VMEM((1, F1), BF16),
            pltpu.VMEM((8, 1, hc), BF16),
            pltpu.VMEM((R, D), BF16),
            pltpu.VMEM((C, L, D), BF16),
            pltpu.VMEM((C, L, D), BF16),
            pltpu.VMEM((C, L, D), BF16),
            pltpu.VMEM((C, L, D), BF16),
            pltpu.VMEM((C, L, hc), BF16),
            pltpu.VMEM((C, L, 2 * hc), BF16),
            pltpu.VMEM((D // n, F2), BF16),
            pltpu.VMEM((8, hc), F32),
            pltpu.VMEM((1, F1), F32),
            dma((n,)),
            dma((n,)),
            dma((n,)),
            dma((n,)),
            dma((S,)),
            dma((S,)),
            dma((C, 3)),
            dma((C, 3)),
            dma((C,)),
            dma((C,)),
            dma((C,)),
            dma((C,)),
            dma((C,)),
            dma((C,)),
            dma((3,)),
            dma((3,)),
            dma((C,)),
            dma((C,)),
            dma((C, 2)),
            dma((C, 2)),
            dma((C, 2)),
            dma((C, 2)),
            dma((C, 2)),
            dma((C, 2)),
            dma((C, 4)),
            dma((C, 4)),
            dma((18,)),
        ],
        compiler_params=pltpu.CompilerParams(
            collective_id=0, has_side_effects=True, vmem_limit_bytes=ENTRY_VMEM * MIB
        ),
        name="entry_stage",
    )(*[
        pltpu.with_memory_space_constraint(v, pltpu.HBM)
        for v in (pos, inp, table, wqkv, wup, wdn, wout, seg, bup, *rows)
    ])


def key_blocks(lohi_ref, rows, bk):
    first = jnp.min(lohi_ref[0:1, rows]).astype(jnp.int32)
    last = jnp.max(lohi_ref[1:2, rows]).astype(jnp.int32)
    return first // bk, (last + bk - 1) // bk


def attend_kernel(dims, q_ref, kv_ref, lohi_ref, att_ref, lse_ref, vt_ref):
    P_, hc, hh, bq, bk = dims
    lanes = lax.broadcasted_iota(jnp.int32, (bq, hc), 1) // HEAD_DIM
    nq = P_ // bq

    def flip_value(kb, carry):
        at = pl.multiple_of(kb * bk, bk)
        vt_ref[kb] = kv_ref[pl.ds(at, bk), hc:].T
        return carry

    first, last = key_blocks(lohi_ref, pl.ds(0, P_), bk)
    lax.fori_loop(first, last, flip_value, 0)

    def one_query_block(qi, carry):
        rows = pl.ds(pl.multiple_of(qi * bq, bq), bq)
        query = q_ref[rows, :]
        heads_q = [jnp.where(lanes == h, query, jnp.zeros_like(query)) for h in range(hh)]
        low = lohi_ref[0:1, rows].astype(jnp.int32)
        high = lohi_ref[1:2, rows].astype(jnp.int32)
        first, last = key_blocks(lohi_ref, rows, bk)

        def one_key_block(kb, state):
            at = pl.multiple_of(kb * bk, bk)
            keys = kv_ref[pl.ds(at, bk), :hc]
            ids = lax.broadcasted_iota(jnp.int32, (bk, bq), 0) + kb * bk
            keep = (ids >= low) & (ids < high)
            fresh = []
            for h in range(hh):
                top, total, acc = state[h]
                scores = jnp.where(keep, rows_dot_t(keys, heads_q[h]), neg_large)
                new_top = jnp.maximum(top, jnp.max(scores, axis=0, keepdims=True))
                weights = jnp.exp(scores - new_top)
                shrink = jnp.exp(top - new_top)
                total = total * shrink + jnp.sum(weights, axis=0, keepdims=True)
                values = vt_ref[kb, h * HEAD_DIM : (h + 1) * HEAD_DIM, :]
                acc = acc * shrink + rows_dot(values, weights.astype(BF16))
                fresh.append((new_top, total, acc))
            return tuple(fresh)

        start = tuple(
            (
                jnp.full((1, bq), neg_large, F32),
                jnp.zeros((1, bq), F32),
                jnp.zeros((HEAD_DIM, bq), F32),
            )
            for _ in range(hh)
        )
        state = lax.fori_loop(first, last, one_key_block, start)
        mixed = jnp.concatenate([acc / total for _, total, acc in state], axis=0)
        att_ref[rows, :] = mixed.T.astype(BF16)
        for h in range(hh):
            lse_ref[h : h + 1, rows] = state[h][0] + jnp.log(state[h][1])
        return carry

    lax.fori_loop(0, nq, one_query_block, 0)


def attend_call(q, kv, lohi, bq, bk):
    P_, hc = q.shape
    hh = hc // HEAD_DIM
    vm = pl.BlockSpec(memory_space=pltpu.VMEM)
    return pl.pallas_call(
        functools.partial(attend_kernel, (P_, hc, hh, bq, bk)),
        out_shape=(
            jax.ShapeDtypeStruct((P_, hc), BF16),
            jax.ShapeDtypeStruct((hh, P_), F32),
        ),
        in_specs=[vm, vm, vm],
        out_specs=(vm, vm),
        scratch_shapes=[pltpu.VMEM((3 * P_ // bk, hc, bk), BF16)],
        compiler_params=pltpu.CompilerParams(vmem_limit_bytes=ATTEND_VMEM * MIB),
        name="attend_stage",
    )(q, kv, lohi)


def attend_back_kernel(
    dims, q_ref, kv_ref, lohi_ref, att_ref, datt_ref, lse_ref, dq_ref, dkv_ref, kt_ref, acc_ref
):
    P_, hc, hh, bq, bk = dims
    lanes = lax.broadcasted_iota(jnp.int32, (bq, hc), 1) // HEAD_DIM
    nq = P_ // bq
    acc_ref[...] = jnp.zeros_like(acc_ref)

    def flip_key(kb, carry):
        at = pl.multiple_of(kb * bk, bk)
        kt_ref[kb] = kv_ref[pl.ds(at, bk), :hc].T
        return carry

    first, last = key_blocks(lohi_ref, pl.ds(0, P_), bk)
    lax.fori_loop(first, last, flip_key, 0)

    def one_query_block(qi, carry):
        rows = pl.ds(pl.multiple_of(qi * bq, bq), bq)
        query, grad = q_ref[rows, :], datt_ref[rows, :]
        zero = jnp.zeros_like(query)
        heads_q = [jnp.where(lanes == h, query, zero) for h in range(hh)]
        heads_g = [jnp.where(lanes == h, grad, zero) for h in range(hh)]
        stack_q = jnp.concatenate(heads_q, axis=0)
        stack_g = jnp.concatenate(heads_g, axis=0)
        product = (grad.astype(F32) * att_ref[rows, :].astype(F32)).T
        delta = [
            jnp.sum(product[h * HEAD_DIM : (h + 1) * HEAD_DIM], axis=0, keepdims=True)
            for h in range(hh)
        ]
        logs = [lse_ref[h : h + 1, rows] for h in range(hh)]
        low = lohi_ref[0:1, rows].astype(jnp.int32)
        high = lohi_ref[1:2, rows].astype(jnp.int32)
        first, last = key_blocks(lohi_ref, rows, bk)

        def one_key_block(kb, state):
            at = pl.multiple_of(kb * bk, bk)
            keys = kv_ref[pl.ds(at, bk), :hc]
            values = kv_ref[pl.ds(at, bk), hc:]
            ids = lax.broadcasted_iota(jnp.int32, (bk, bq), 0) + kb * bk
            keep = (ids >= low) & (ids < high)
            fresh, all_p, all_s = [], [], []
            for h in range(hh):
                scores = rows_dot_t(keys, heads_q[h])
                probs = jnp.where(keep, jnp.exp(scores - logs[h]), 0.0)
                grad_probs = rows_dot_t(values, heads_g[h])
                grad_scores = (probs * (grad_probs - delta[h])).astype(BF16)
                all_p.append(probs.astype(BF16))
                all_s.append(grad_scores)
                key_cols = kt_ref[kb, h * HEAD_DIM : (h + 1) * HEAD_DIM, :]
                fresh.append(state[h] + rows_dot(key_cols, grad_scores))
            acc_ref[pl.ds(at, bk), :hc] += rows_dot(jnp.concatenate(all_s, axis=1), stack_q)
            acc_ref[pl.ds(at, bk), hc:] += rows_dot(jnp.concatenate(all_p, axis=1), stack_g)
            return tuple(fresh)

        start = tuple(jnp.zeros((HEAD_DIM, bq), F32) for _ in range(hh))
        state = lax.fori_loop(first, last, one_key_block, start)
        dq_ref[rows, :] = (jnp.concatenate(state, axis=0).T * score_scale).astype(BF16)
        return carry

    lax.fori_loop(0, nq, one_query_block, 0)
    dkv_ref[...] = acc_ref[...].astype(BF16)


def attend_back_call(q, kv, lohi, att, datt, lse, bq, bk):
    P_, hc = q.shape
    hh = hc // HEAD_DIM
    vm = pl.BlockSpec(memory_space=pltpu.VMEM)
    return pl.pallas_call(
        functools.partial(attend_back_kernel, (P_, hc, hh, bq, bk)),
        out_shape=(
            jax.ShapeDtypeStruct((P_, hc), BF16),
            jax.ShapeDtypeStruct((3 * P_, 2 * hc), BF16),
        ),
        in_specs=[vm, vm, vm, vm, vm, vm],
        out_specs=(vm, vm),
        scratch_shapes=[
            pltpu.VMEM((3 * P_ // bk, hc, bk), BF16),
            pltpu.VMEM((3 * P_, 2 * hc), F32),
        ],
        compiler_params=pltpu.CompilerParams(vmem_limit_bytes=BACK_VMEM * MIB),
        name="attend_back_stage",
    )(q, kv, lohi, att, datt, lse)


def layer_stats(summed):
    center = summed - jnp.mean(summed, axis=1, keepdims=True)
    inverse = lax.rsqrt(jnp.mean(center * center, axis=1, keepdims=True) + epsilon)
    return center * inverse, inverse


def layer_back(grad, normed, inverse):
    first = jnp.mean(grad, axis=1, keepdims=True)
    second = jnp.mean(grad * normed, axis=1, keepdims=True)
    return inverse * (grad - first - normed * second)


def col_sum(x):
    return jnp.sum(x, axis=0, keepdims=True)


def middle_kernel(
    dims,
    att_ref,
    hidden_ref,
    cot_ref,
    par_ref,
    wout_ref,
    wout_o_ref,
    wup_ref,
    wdn_ref,
    wdn_o_ref,
    bup_ref,
    result_ref,
    dfirst_ref,
    datt_ref,
    gdn_ref,
    gup_ref,
    gout_ref,
    stats_ref,
    gbup_ref,
    gdn_done_ref,
    wout_v,
    wup_v,
    wdn_v,
    attp,
    fa,
    da,
    dfa,
    act,
    slope,
    dup,
    stage,
    recv,
    normed_v,
    first_v,
    dnorm_v,
    gdn_v,
    gdn_r,
    gdn_h,
    gdn_l,
    gdn_x,
    gdn_f,
    gup_v,
    gup_r,
    gout_v,
    gout_r,
    gb_v,
    gb_r,
    dattst,
    ap_ss,
    ap_rs,
    sc_ss,
    sc_rs,
    ag_ss,
    ag_rs,
    gx_ss,
    gx_rs,
    dx_ss,
    dx_rs,
    zsem,
    loc,
):
    S, n, C, L, D, hc, F1 = dims
    Dn, F2, Ph = D // n, 2 * F1, C * L
    z = lax.axis_index("seq")
    s = lax.axis_index("shard")
    core = lax.rem(s, 2)
    chip = s // 2
    other = 1 - core
    partner = (z, 2 * chip + other)

    loads = [
        pltpu.make_async_copy(wout_ref, wout_v.at[core], loc.at[0]),
        pltpu.make_async_copy(wout_o_ref, wout_v.at[other], loc.at[1]),
        pltpu.make_async_copy(wup_ref, wup_v, loc.at[2]),
        pltpu.make_async_copy(wdn_ref, wdn_v.at[core], loc.at[3]),
        pltpu.make_async_copy(wdn_o_ref, wdn_v.at[other], loc.at[4]),
    ]
    for load in loads:
        load.start()

    def peer(j):
        return (z, 2 * flip(chip, j, C) + core)

    barrier = pltpu.get_barrier_semaphore()
    pl.semaphore_signal(barrier, inc=1, device_id=partner, device_id_type=MESH)
    for j in range(1, C):
        pl.semaphore_signal(barrier, inc=1, device_id=peer(j), device_id_type=MESH)
    for d in (1, S - 1):
        pl.semaphore_signal(barrier, inc=1, device_id=(lax.rem(z + d, S), s), device_id_type=MESH)
    pl.semaphore_wait(barrier, C + 2)

    def put_stat(row, value):
        for i in range(n):
            stats_ref[i, row : row + 1] = value[:, i * hc : (i + 1) * hc]

    def give(i, src, dst):
        remote(src, dst, gx_ss.at[i], gx_rs.at[i], partner).start()

    def taken(i, src, dst):
        await_recv(dst, gx_rs.at[i], partner)

    def gather_of(r, buf):
        return Gather(C, chip, peer, L, lambda c: buf.at[c], ag_ss.at[r], ag_rs.at[r])

    gathers = [gather_of(0, fa), gather_of(1, da), gather_of(2, dfa)]
    out_sum = Scatter(C, peer, L, stage.at[0], recv.at[0], sc_ss.at[0], sc_rs.at[0])

    def hand(r, j, part):
        stage[r, j] = part.astype(BF16)
        remote(
            stage.at[r, j], recv.at[r, j], sc_ss.at[r, j, 0], sc_rs.at[r, j, 0], peer(j)
        ).start()

    def collected(r, total):
        for j in range(1, C):
            await_recv(recv.at[r, j], sc_rs.at[r, j, 0], peer(j))
            total = total + recv[r, j].astype(F32)
        return total

    par = jnp.concatenate([par_ref[i] for i in range(n)], axis=1)
    b_out, gain1, shift1 = par[0:1], par[1:2], par[2:3]
    b_down, gain2, shift2 = par[3:4], par[4:5], par[5:6]

    remote(att_ref.at[:, other], attp, ap_ss.at[0], ap_rs.at[0], partner).start()
    loads[0].wait()
    loads[1].wait()
    await_recv(attp, ap_rs.at[0], partner)

    def out_part(j):
        c = flip(chip, j, C)
        return rows_dot(att_ref[c, core], wout_v[core]) + rows_dot(attp[c], wout_v[other])

    first_sum = out_sum.collect(out_sum.send(out_part) + hidden_ref[...] + b_out)
    normed_one, inverse_one = layer_stats(first_sum)
    normed_v[...] = normed_one
    first_norm = normed_one * gain1 + shift1
    first_v[...] = first_norm
    fa[chip] = first_norm.astype(BF16)
    gathers[0].send(fa.at[chip])

    loads[2].wait()
    loads[3].wait()
    loads[4].wait()
    first_core = core == 0
    bias_up = bup_ref[...]

    def up_part(j):
        c = flip(chip, j, C)
        pre = rows_dot(fa[c], wup_v[...].reshape(D, F2)) + bias_up
        half = 0.5 * (1.0 + lax.erf(pre * root_half))
        act[c] = (pre * half).astype(BF16)
        slope[c] = half + pre * jnp.exp(-0.5 * pre * pre) * inv_root_two_pi
        return rows_dot(act[c], wdn_v[...].reshape(F2, D))

    own = up_part(0)
    gathers[0].relay()

    def up_step(j, carry):
        gathers[0].arrived(j)
        hand(1, j, up_part(j))
        return carry

    lax.fori_loop(1, C, up_step, 0)
    second_sum = collected(1, own + first_v[...] + b_down)
    normed_two, inverse_two = layer_stats(second_sum)
    result_ref[...] = (normed_two * gain2 + shift2).astype(BF16)
    grad_rows = cot_ref[...].astype(F32)
    put_stat(0, col_sum(grad_rows * normed_two))
    put_stat(1, col_sum(grad_rows))
    d_second = layer_back(grad_rows * gain2, normed_two, inverse_two)
    put_stat(2, col_sum(d_second))
    dnorm_v[...] = d_second
    da[chip] = d_second.astype(BF16)
    gathers[1].send(da.at[chip])

    def down_back(j):
        c = flip(chip, j, C)
        d_up = rows_dot_t(da[c], wdn_v[...].reshape(F2, D)) * slope[c]
        gb_v[...] += col_sum(d_up)
        dup[c] = d_up.astype(BF16)
        return rows_dot_t(dup[c], wup_v[...].reshape(D, F2))

    gb_v[...] = jnp.zeros_like(gb_v)
    own = down_back(0)
    gathers[1].relay()

    def back_step(j, carry):
        gathers[1].arrived(j)
        hand(2, j, down_back(j))
        return carry

    lax.fori_loop(1, C, back_step, 0)
    dnorm_v[...] = dnorm_v[...] + own

    tile = 256
    da_all = da[...].reshape(Ph, D)

    per_half = F1 // tile
    per_tile = gdn_v.shape[1] // per_half

    def down_grad(i, carry):
        t = lax.rem(i + other * per_half, 2 * per_half)
        cols = pl.ds(pl.multiple_of(t * tile, tile), tile)
        res = cols_dot(act[:, :, cols].reshape(Ph, tile), da_all).astype(BF16)
        gdn_v[t // per_half, pl.ds(lax.rem(t, per_half) * per_tile, per_tile)] = res.reshape(
            per_tile, tile // per_tile, D
        )
        return carry

    lax.fori_loop(0, per_half, down_grad, 0)
    give(0, gdn_v.at[other], gdn_r)
    lax.fori_loop(per_half, 2 * per_half, down_grad, 0)

    def up_grad(c, carry):
        cols = pl.ds(pl.multiple_of(c * 2 * Dn, 128), 2 * Dn)
        res = cols_dot(fa[:, :, cols].reshape(Ph, 2 * Dn), dup[...].reshape(Ph, F2)).astype(BF16)
        gup_v[c, 0] = res[:Dn]
        gup_v[c, 1] = res[Dn:]
        return carry

    early = gdn_h.shape[0]
    taken(0, None, gdn_r)
    gdn_h[...] = (gdn_v[core, :early].astype(F32) + gdn_r[:early].astype(F32)).astype(BF16)
    gdn_ref[...] = (gdn_v[core, early:].astype(F32) + gdn_r[early:].astype(F32)).astype(BF16)
    chain = Chain(S, z, s, gdn_h, gdn_l, gdn_x, gdn_f, zsem, 2)
    chain.give_out(0, early)

    lax.fori_loop(0, C, up_grad, 0)
    give(1, gup_v.at[:, other], gup_r)
    gb_r[0] = jnp.where(first_core, gb_v[:, F1:], gb_v[:, :F1])
    give(2, gb_r.at[0], gb_r.at[1])
    chain.run(0, 2)
    d_first_norm = collected(2, dnorm_v[...])
    normed_one = normed_v[...]
    put_stat(3, col_sum(d_first_norm * normed_one))
    put_stat(4, col_sum(d_first_norm))
    d_first = layer_back(d_first_norm * gain1, normed_one, inverse_one)
    put_stat(5, col_sum(d_first))
    stats_ref[:, 6:8] = jnp.zeros((n, 2, hc), F32)
    dfirst_ref[...] = d_first
    dfa[chip] = d_first.astype(BF16)
    gathers[2].send(dfa.at[chip])

    def att_back(j, carry):
        chain.run(2 * j + 2, 2 * j + 4)

        @pl.when(j == 1)
        def _():
            gathers[2].relay()

        gathers[2].arrived(j)
        c = flip(chip, j, C)
        datt_ref[c, core] = rows_dot_t(dfa[c], wout_v[core]).astype(BF16)
        dattst[j] = rows_dot_t(dfa[c], wout_v[other]).astype(BF16)
        remote(dattst.at[j], datt_ref.at[c, core], dx_ss.at[j], dx_rs.at[j], partner).start()
        return carry

    lax.fori_loop(0, C, att_back, 0)
    dfa_all = dfa[...].reshape(Ph, D)
    gout_v[0] = cols_dot(attp[...].reshape(Ph, hc), dfa_all).astype(BF16)
    give(3, gout_v.at[0], gout_r)
    gout_v[1] = cols_dot(att_ref[:, core].reshape(Ph, hc), dfa_all).astype(BF16)

    chain.run(2 * C + 2, chain.slots)
    taken(1, None, gup_r)
    gup_ref[...] = (gup_v[:, core].astype(F32) + gup_r[...].astype(F32)).astype(BF16)
    taken(2, None, gb_r.at[1])
    gbup_ref[...] = jnp.where(first_core, gb_v[:, :F1], gb_v[:, F1:]) + gb_r[1]
    taken(3, None, gout_r)
    gout_ref[...] = (gout_v[1].astype(F32) + gout_r[...].astype(F32)).astype(BF16)

    chain.settle()
    out_sum.settle()
    for gather in gathers:
        gather.settle()
    gdn_done_ref[...] = gdn_f[...]
    await_send(attp, ap_ss.at[0], partner)
    await_send(gdn_r, gx_ss.at[0], partner)
    await_send(gup_r, gx_ss.at[1], partner)
    await_send(gb_r.at[0], gx_ss.at[2], partner)
    await_send(gout_r, gx_ss.at[3], partner)

    def settle(j, carry):
        c = flip(chip, j, C)
        await_recv(datt_ref.at[c, other], dx_rs.at[j], partner)
        await_send(dattst.at[j], dx_ss.at[j], partner)

        @pl.when(j > 0)
        def _():
            for r in range(1, 3):
                await_send(stage.at[r, j], sc_ss.at[r, j, 0], peer(j))

        return carry

    lax.fori_loop(0, C, settle, 0)


def middle_call(S, n, att, hidden, cot, par, wout, wout_o, wup2, wdn, wdn_o, bup):
    C = n // 2
    L, D = hidden.shape
    hc = D // n
    F1 = wdn.shape[0]
    F2 = 2 * F1
    dims = (S, n, C, L, D, hc, F1)
    dma = pltpu.SemaphoreType.DMA
    vm = pl.BlockSpec(memory_space=pltpu.VMEM)
    anyw = pl.BlockSpec(memory_space=pl.ANY)
    sds = jax.ShapeDtypeStruct
    Dn = D // n
    pc, early = 16, EARLY_PIECES
    return pl.pallas_call(
        functools.partial(middle_kernel, dims),
        out_shape=(
            sds((L, D), BF16),
            sds((L, D), F32),
            sds((C, 2, L, hc), BF16),
            sds((pc - early, F1 // pc, D), BF16),
            sds((C, Dn, F2), BF16),
            sds((hc, D), BF16),
            sds((n, 8, hc), F32),
            sds((1, F1), F32),
            sds((early, F1 // pc, D), BF16),
        ),
        in_specs=[vm, vm, vm, vm, anyw, anyw, anyw, anyw, anyw, vm],
        out_specs=(vm,) * 9,
        scratch_shapes=[
            pltpu.VMEM((2, hc, D), BF16),
            pltpu.VMEM((n, Dn, F2), BF16),
            pltpu.VMEM((2, F1, D), BF16),
            pltpu.VMEM((C, L, hc), BF16),
            pltpu.VMEM((C, L, D), BF16),
            pltpu.VMEM((C, L, D), BF16),
            pltpu.VMEM((C, L, D), BF16),
            pltpu.VMEM((C, L, F2), BF16),
            pltpu.VMEM((C, L, F2), F32),
            pltpu.VMEM((C, L, F2), BF16),
            pltpu.VMEM((3, C, L, D), BF16),
            pltpu.VMEM((3, C, L, D), BF16),
            pltpu.VMEM((L, D), F32),
            pltpu.VMEM((L, D), F32),
            pltpu.VMEM((L, D), F32),
            pltpu.VMEM((2, pc, F1 // pc, D), BF16),
            pltpu.VMEM((pc, F1 // pc, D), BF16),
            pltpu.VMEM((early, F1 // pc, D), BF16),
            pltpu.VMEM((early, F1 // pc, D), BF16),
            pltpu.VMEM((early, F1 // pc, D), BF16),
            pltpu.VMEM((early, F1 // pc, D), BF16),
            pltpu.VMEM((C, 2, Dn, F2), BF16),
            pltpu.VMEM((C, Dn, F2), BF16),
            pltpu.VMEM((2, hc, D), BF16),
            pltpu.VMEM((hc, D), BF16),
            pltpu.VMEM((1, F2), F32),
            pltpu.VMEM((2, 1, F1), F32),
            pltpu.VMEM((C, L, hc), BF16),
            dma((1,)),
            dma((1,)),
            dma((3, C, 2)),
            dma((3, C, 2)),
            dma((3, C, 2)),
            dma((3, C, 2)),
            dma((4,)),
            dma((4,)),
            dma((C,)),
            dma((C,)),
            dma((6, early)),
            dma((5,)),
        ],
        compiler_params=pltpu.CompilerParams(
            collective_id=1, has_side_effects=True, vmem_limit_bytes=MIDDLE_VMEM * MIB
        ),
        name="middle_stage",
    )(att, hidden, cot, par, wout, wout_o, wup2, wdn, wdn_o, bup)


def exit_kernel(
    dims,
    dq_ref,
    dkv_ref,
    hid_ref,
    wq_ref,
    dfirst_ref,
    stats_ref,
    gbup_ref,
    pos_ref,
    gupc_ref,
    goutc_ref,
    gdnc_ref,
    ginp_ref,
    dh_ref,
    gq_f,
    up_f,
    out_f,
    dn_f,
    gtable_ref,
    small_ref,
    gbo_ref,
    zr,
    own3,
    got3,
    x6,
    stage,
    recv,
    dhb,
    gq_v,
    gq_r,
    gq_s,
    gq_o,
    gq_l,
    gq_x,
    up_o,
    up_l,
    up_x,
    out_o,
    out_l,
    out_x,
    dn_o,
    dn_l,
    dn_x,
    plane,
    prod,
    st_r,
    st_v,
    zst,
    zgb,
    zk_ss,
    zk_rs,
    x_ss,
    x_rs,
    sc_ss,
    sc_rs,
    st_ss,
    st_rs,
    zs_ss,
    zs_rs,
    gq_ss,
    gq_rs,
    gx_ss,
    gx_rs,
    ua_ss,
    ua_rs,
    qc,
    uc,
    oc,
    dc,
    zl_ss,
    zl_rs,
    ag_ss,
    ag_rs,
    pf_ss,
    pf_rs,
    loc,
):
    S, n, C, L, D, hc, F1, R, rt = dims
    Dn, Ph = D // n, C * L
    z = lax.axis_index("seq")
    s = lax.axis_index("shard")
    core = lax.rem(s, 2)
    chip = s // 2
    other = 1 - core
    twin = 2 * chip + other
    partner = (z, twin)
    first_core = core == 0

    def peer(j):
        return (z, 2 * flip(chip, j, C) + core)

    barrier = pltpu.get_barrier_semaphore()
    for d in range(1, n):
        pl.semaphore_signal(barrier, inc=1, device_id=(z, flip(s, d, n)), device_id_type=MESH)
    for d in range(1, S):
        pl.semaphore_signal(barrier, inc=1, device_id=(lax.rem(z + d, S), s), device_id_type=MESH)
    pl.semaphore_wait(barrier, n - 1 + S - 1)

    for j in range(C - 1, -1, -1):
        c = flip(chip, j, C)

        @pl.when(z > 0)
        def _():
            remote(
                dkv_ref.at[0, c], zr.at[1, c], zk_ss.at[j, 0], zk_rs.at[j, 1], (z - 1, s)
            ).start()

        @pl.when(z < S - 1)
        def _():
            remote(
                dkv_ref.at[2, c], zr.at[0, c], zk_ss.at[j, 1], zk_rs.at[j, 0], (z + 1, s)
            ).start()

    quarter = Dn // 4
    mine = pl.ds(4 * chip, 4)

    def block_of(j):
        return pl.ds(4 * flip(chip, j, C), 4)

    for j in range(C - 1, 0, -1):
        remote(
            gupc_ref.at[flip(chip, j, C)], up_o.at[mine], ua_ss.at[j], ua_rs.at[j], peer(j)
        ).start()
    up_o[mine] = gupc_ref[chip]
    out_o[...] = goutc_ref[...].reshape(4, quarter, D)
    dn_o[...] = gdnc_ref[...]
    wide = Chain(S, z, s, up_o, up_l, up_x, up_f, uc)
    square = Chain(S, z, s, out_o, out_l, out_x, out_f, oc)
    late = Chain(S, z, s, dn_o, dn_l, dn_x, dn_f, dc)
    inner = Chain(S, z, s, gq_o, gq_l, gq_x, gq_f, qc)
    late.give_out(0, late.pieces)
    square.give_out(0, square.pieces)
    starts = [0, late.pieces, late.pieces + square.pieces]
    starts.append(starts[2] + wide.pieces)
    last_step = starts[3] + inner.slots

    def chain_step(m, carry=0):
        for chain, begin in zip((late, square, wide, inner), starts):
            chain.slot(m - begin)
        return carry

    def chain_steps(begin, end):
        lax.fori_loop(begin, end, chain_step, 0)

    st_r[s] = stats_ref[s]
    for d in range(1, n):
        to = flip(s, d, n)
        remote(stats_ref.at[to], st_r.at[s], st_ss.at[d], st_rs.at[d], (z, to)).start()

    def fold(k, carry):
        j = C - 1 - k
        c = flip(chip, j, C)
        whole = dkv_ref[1, c].astype(F32)

        @pl.when(z > 0)
        def _():
            await_recv(zr.at[0, c], zk_rs.at[j, 0], (z - 1, s))

        @pl.when(z < S - 1)
        def _():
            await_recv(zr.at[1, c], zk_rs.at[j, 1], (z + 1, s))

        whole = whole + jnp.where(z > 0, zr[0, c].astype(F32), 0.0)
        whole = whole + jnp.where(z < S - 1, zr[1, c].astype(F32), 0.0)
        whole = whole.astype(BF16)
        own3[c, :, :, :hc] = dq_ref[c]
        own3[c, :, :, hc:] = whole
        remote(own3.at[c, other], got3.at[c], x_ss.at[j], x_rs.at[j], partner).start()
        sums = jnp.sum(own3[c].astype(F32), axis=(0, 1), keepdims=False)
        st_v[0:1] += sums[None, :hc]
        st_v[1:2] += sums[None, 2 * hc :]
        return carry

    st_v[...] = jnp.zeros_like(st_v)
    lax.fori_loop(0, C, fold, 0)

    def partial(j):
        c = flip(chip, j, C)
        await_recv(got3.at[c], x_rs.at[j], partner)
        mine, theirs = own3[c, core], got3[c]
        low = jnp.where(first_core, mine, theirs)
        high = jnp.where(first_core, theirs, mine)
        pieces = []
        for part in range(3):
            pieces += [low[:, part * hc : (part + 1) * hc], high[:, part * hc : (part + 1) * hc]]
        x6[c] = jnp.concatenate(pieces, axis=1)
        return rows_dot_t(x6[c], wq_ref[...].reshape(D, 6 * hc))

    tokens_sum = Scatter(C, peer, L, stage, recv, sc_ss, sc_rs)
    total = tokens_sum.send(partial) + dfirst_ref[...]
    chain_steps(0, 2)

    def qkv_grad(c, carry):
        chain_step(2 + c)
        cols = pl.ds(pl.multiple_of(c * 2 * Dn, 128), 2 * Dn)
        res = cols_dot(hid_ref[:, :, cols].reshape(Ph, 2 * Dn), x6[...].reshape(Ph, 6 * hc))
        gq_v[c] = res.astype(BF16).reshape(2, 4, quarter, 6 * hc)
        return carry

    lax.fori_loop(0, C, qkv_grad, 0)
    remote(gq_v.at[:, other], gq_r, gq_ss.at[0], gq_rs.at[0], partner).start()

    sums = st_r[s]
    for d in range(1, n):
        src = flip(s, d, n)
        await_recv(st_r.at[src], st_rs.at[d], (z, src))
    sums = st_r[0]
    for i in range(1, n):
        sums = sums + st_r[i]
    zst[z] = sums
    zst[z, 6:8] = st_v[...]
    zgb[z] = gbup_ref[...]
    for d in range(1, S):
        to = (lax.rem(z + d, S), s)
        remote(zst.at[z], zst.at[z], zs_ss.at[d, 0], zs_rs.at[d, 0], to).start()
        remote(zgb.at[z], zgb.at[z], zs_ss.at[d, 1], zs_rs.at[d, 1], to).start()

    for j in range(1, C):
        await_recv(up_o.at[block_of(j)], ua_rs.at[j], peer(j))
    wide.give_out(0, 2)
    chain_steps(C + 2, C + 4)
    await_recv(gq_r, gq_rs.at[0], partner)
    gq_s[...] = (gq_v[:, core].astype(F32) + gq_r[...].astype(F32)).astype(BF16)
    for j in range(C - 1, 0, -1):
        remote(
            gq_s.at[flip(chip, j, C)], gq_o.at[mine], gx_ss.at[j], gx_rs.at[j], peer(j)
        ).start()
    gq_o[mine] = gq_s[chip]

    total = tokens_sum.collect(total)
    ginp = total.astype(BF16)
    ginp_ref[...] = ginp
    dhb[...] = ginp
    keep = pltpu.make_async_copy(dhb, dh_ref.at[z, s], loc.at[0])
    keep.start()

    def gather_of(at):
        return Gather(
            C, chip, peer, L, lambda c: dh_ref.at[at, 2 * c + core], ag_ss.at[at], ag_rs.at[at]
        )

    def broadcast(src, at):
        gather_of(at).send(src)
        remote(src, dh_ref.at[at, s], pf_ss.at[at, 0], pf_rs.at[at, 0], partner).start()

    def pass_on(d):
        @pl.when(z - d >= 0)
        def _():
            gather_of(z - d).relay()

        if d:

            @pl.when(z + d <= S - 1)
            def _():
                gather_of(z + d).relay()

    @pl.when(z < S - 1)
    def _():
        remote(dhb, dh_ref.at[z, s], zl_ss.at[z, 0], zl_rs.at[z, 0], (z + 1, s)).start()

    @pl.when(z > 0)
    def _():
        remote(dhb, dh_ref.at[z, s], zl_ss.at[z, 1], zl_rs.at[z, 1], (z - 1, s)).start()

    broadcast(dhb, z)
    wide.give_out(2, wide.pieces)
    chain_steps(C + 4, C + 7)
    def next_planes(d):
        @pl.when(z - d >= 0)
        def _():
            at = z - d
            await_recv(dh_ref.at[at, s], zl_rs.at[at, 0], (z - 1, s))

            @pl.when(z < S - 1)
            def _():
                remote(
                    dh_ref.at[at, s], dh_ref.at[at, s], zl_ss.at[at, 0], zl_rs.at[at, 0], (z + 1, s)
                ).start()

            broadcast(dh_ref.at[at, s], at)

        @pl.when(z + d <= S - 1)
        def _():
            at = z + d
            await_recv(dh_ref.at[at, s], zl_rs.at[at, 1], (z + 1, s))

            @pl.when(z > 0)
            def _():
                remote(
                    dh_ref.at[at, s], dh_ref.at[at, s], zl_ss.at[at, 1], zl_rs.at[at, 1], (z - 1, s)
                ).start()

            broadcast(dh_ref.at[at, s], at)

    def relay(at):
        for j in range(1, C):
            src = 2 * flip(chip, j, C) + core
            gather_of(at).arrived(j)
            remote(
                dh_ref.at[at, src], dh_ref.at[at, src], pf_ss.at[at, j], pf_rs.at[at, j], partner
            ).start()

    def plane_sum(t, step):
        at = flip(z, t, S)
        chain_step(step)
        relay(at)
        chain_step(step + 1)

        for j in range(C):
            src = 2 * flip(chip, j, C) + other
            await_recv(dh_ref.at[at, src], pf_rs.at[at, j], partner)

        if t == 0:
            keep.wait()

        load = pltpu.make_async_copy(dh_ref.at[at], plane, loc.at[1])
        load.start()
        load.wait()

        def rows_tile(r, carry):
            chain_step(step + 2 + r)
            start = pl.multiple_of(r * rt, rt)
            ids = lax.broadcasted_iota(jnp.int32, (rt, L), 0) + (start + s * R)
            hot = jnp.concatenate(
                [jnp.where(ids == pos_ref[at, i], 1.0, 0.0).astype(BF16) for i in range(n)], axis=1
            )
            prod[at, pl.ds(start, rt), :] = rows_dot(hot, plane[...].reshape(n * L, D))
            return carry

        lax.fori_loop(0, R // rt, rows_tile, 0)

    next_planes(1)
    pass_on(0)
    chain_steps(C + 7, C + 11)
    step = C + 11
    for t in range(S):
        if t + 2 < S:
            next_planes(t + 2)
        if t + 1 < S:
            pass_on(t + 1)
        if t == 0:
            for j in range(1, C):
                await_recv(gq_o.at[block_of(j)], gx_rs.at[j], peer(j))
            inner.give_out(0, inner.pieces)
        chain_steps(step, step + 2)
        plane_sum(t, step + 2)
        step += 4 + R // rt

    def add_tile(r, carry):
        at = pl.ds(pl.multiple_of(r * rt, rt), rt)
        rows = prod[0, at]
        for i in range(1, S):
            rows = rows + prod[i, at]
        gtable_ref[at] = rows.astype(BF16)
        return carry

    lax.fori_loop(0, R // rt, add_tile, 0)

    chain_steps(step, last_step)
    for d in range(1, S):
        src = lax.rem(z + S - d, S)
        await_recv(zst.at[src], zs_rs.at[d, 0], (src, s))
        await_recv(zgb.at[src], zs_rs.at[d, 1], (src, s))
    small, big = zst[0], zgb[0]
    for i in range(1, S):
        small = small + zst[i]
        big = big + zgb[i]
    small_ref[...] = small
    gbo_ref[...] = big

    def settle_plane(at, carry):
        for j in range(C):
            await_send(dhb, pf_ss.at[at, j], partner)
        gather_of(at).settle()
        return carry

    lax.fori_loop(0, S, settle_plane, 0)
    for at in range(S):

        @pl.when((z >= at) & (z < S - 1))
        def _():
            await_send(dhb, zl_ss.at[at, 0], (z + 1, s))

        @pl.when((z <= at) & (z > 0))
        def _():
            await_send(dhb, zl_ss.at[at, 1], (z - 1, s))

    for j in range(C):

        @pl.when(z > 0)
        def _():
            await_send(zr.at[0, 0], zk_ss.at[j, 0], (z - 1, s))

        @pl.when(z < S - 1)
        def _():
            await_send(zr.at[0, 0], zk_ss.at[j, 1], (z + 1, s))

        await_send(got3.at[0], x_ss.at[j], partner)
    for d in range(1, n):
        await_send(st_r.at[s], st_ss.at[d], (z, flip(s, d, n)))
    for d in range(1, S):
        to = (lax.rem(z + d, S), s)
        await_send(zst.at[z], zs_ss.at[d, 0], to)
        await_send(zgb.at[z], zs_ss.at[d, 1], to)
    for j in range(1, C):
        await_send(gq_s.at[chip], gx_ss.at[j], peer(j))
        await_send(gupc_ref.at[chip], ua_ss.at[j], peer(j))
    tokens_sum.settle()
    wide.settle()
    square.settle()
    late.settle()
    inner.settle()
    await_send(gq_r, gq_ss.at[0], partner)


def exit_call(S, n, R, dq, dkv, hid_half, wq, dfirst, stats, gbup, pos, gupc, goutc, gdnc):
    C = n // 2
    L, D = dfirst.shape
    hc = D // n
    F1 = gbup.shape[1]
    Dn = D // n
    F2 = gupc.shape[3]
    dims = (S, n, C, L, D, hc, F1, R, 256)
    dma = pltpu.SemaphoreType.DMA
    vm = pl.BlockSpec(memory_space=pltpu.VMEM)
    anyw = pl.BlockSpec(memory_space=pl.ANY)
    sds = jax.ShapeDtypeStruct
    return pl.pallas_call(
        functools.partial(exit_kernel, dims),
        out_shape=(
            sds((L, D), BF16),
            sds((S, n, L, D), BF16),
            sds((4 * C, Dn // 4, 6 * hc), BF16),
            sds((4 * C, Dn // 4, F2), BF16),
            sds((4, Dn // 4, D), BF16),
            sds(gdnc.shape, BF16),
            sds((R, D), BF16),
            sds((8, hc), F32),
            sds((1, F1), F32),
        ),
        in_specs=[vm] * 11,
        out_specs=(vm, anyw) + (vm,) * 7,
        scratch_shapes=[
            pltpu.VMEM((2, C, 2, L, 2 * hc), BF16),
            pltpu.VMEM((C, 2, L, 3 * hc), BF16),
            pltpu.VMEM((C, L, 3 * hc), BF16),
            pltpu.VMEM((C, L, 6 * hc), BF16),
            pltpu.VMEM((C, L, D), BF16),
            pltpu.VMEM((C, L, D), BF16),
            pltpu.VMEM((L, D), BF16),
            pltpu.VMEM((C, 2, 4, Dn // 4, 6 * hc), BF16),
            pltpu.VMEM((C, 4, Dn // 4, 6 * hc), BF16),
            pltpu.VMEM((C, 4, Dn // 4, 6 * hc), BF16),
            pltpu.VMEM((4 * C, Dn // 4, 6 * hc), BF16),
            pltpu.VMEM((4 * C, Dn // 4, 6 * hc), BF16),
            pltpu.VMEM((4 * C, Dn // 4, 6 * hc), BF16),
            pltpu.VMEM((4 * C, Dn // 4, F2), BF16),
            pltpu.VMEM((4 * C, Dn // 4, F2), BF16),
            pltpu.VMEM((4 * C, Dn // 4, F2), BF16),
            pltpu.VMEM((4, Dn // 4, D), BF16),
            pltpu.VMEM((4, Dn // 4, D), BF16),
            pltpu.VMEM((4, Dn // 4, D), BF16),
            pltpu.VMEM(gdnc.shape, BF16),
            pltpu.VMEM(gdnc.shape, BF16),
            pltpu.VMEM(gdnc.shape, BF16),
            pltpu.VMEM((n, L, D), BF16),
            pltpu.VMEM((S, R, D), F32),
            pltpu.VMEM((n, 8, hc), F32),
            pltpu.VMEM((2, hc), F32),
            pltpu.VMEM((S, 8, hc), F32),
            pltpu.VMEM((S, 1, F1), F32),
            dma((C, 2)),
            dma((C, 2)),
            dma((C,)),
            dma((C,)),
            dma((C, 2)),
            dma((C, 2)),
            dma((n,)),
            dma((n,)),
            dma((S, 2)),
            dma((S, 2)),
            dma((1,)),
            dma((1,)),
            dma((C,)),
            dma((C,)),
            dma((C,)),
            dma((C,)),
            dma((6, 4 * C)),
            dma((6, 4 * C)),
            dma((6, 4)),
            dma((6, gdnc.shape[0])),
            dma((S, 2)),
            dma((S, 2)),
            dma((S, C, 2)),
            dma((S, C, 2)),
            dma((S, C)),
            dma((S, C)),
            dma((2,)),
        ],
        compiler_params=pltpu.CompilerParams(
            collective_id=2, has_side_effects=True, vmem_limit_bytes=EXIT_VMEM * MIB
        ),
        name="exit_stage",
    )(dq, dkv, hid_half, wq, dfirst, stats, gbup, pos, gupc, goutc, gdnc)


def finish_kernel(
    dims,
    table_ref,
    gq_ref,
    up_ref,
    out_ref,
    early_ref,
    late_ref,
    res_ref,
    inp_ref,
    small_ref,
    gb_ref,
    table_o,
    gq_o,
    up_o,
    out_o,
    dn_o,
    res_o,
    inp_o,
    gb_o,
    *small_o,
):
    C, D, hc = dims
    i = pl.program_id(0)
    h2 = 2 * hc
    F2 = up_ref.shape[3]
    table_o[...] = table_ref[...].astype(F32)
    for c in range(C):
        up_o[:, c * F2 : (c + 1) * F2] = up_ref[c, 0].astype(F32)
        for part in range(3):
            gq_o[:, part * D + c * h2 : part * D + (c + 1) * h2] = gq_ref[
                c, 0, :, part * h2 : (part + 1) * h2
            ].astype(F32)
    out_o[...] = out_ref[0].astype(F32)
    piece = early_ref.shape[0] * early_ref.shape[1]
    dn_o[...] = jnp.where(i < 4, early_ref[...], late_ref[...]).reshape(piece, D).astype(F32)
    res_o[...] = res_ref[...]
    inp_o[...] = inp_ref[...]
    gb_o[...] = gb_ref[...]
    for r, o in enumerate(small_o):
        o[...] = small_ref[r : r + 1]


def finish_call(n, table, gq, up, out, early, late, res, inp, small, gb):
    C = n // 2
    R, D = table.shape
    L = res.shape[0]
    Dn = D // n
    hc = Dn
    q, F2 = up.shape[1:]
    h = q // 2
    piece = early.shape[1]
    F1 = gb.shape[1]
    sds = jax.ShapeDtypeStruct
    steps = 8
    two = lambda rows, cols: pl.BlockSpec((rows, cols), lambda i: (i, 0))
    quad = lambda cols: pl.BlockSpec((C, 1, h, cols), lambda i: (0, i // 2, i % 2, 0))
    fixed = lambda rows, cols: pl.BlockSpec((rows, cols), lambda i: (0, 0))
    return pl.pallas_call(
        functools.partial(finish_kernel, (C, D, hc)),
        grid=(steps,),
        out_shape=(
            sds((R, D), F32),
            sds((Dn, 3 * D), F32),
            sds((Dn, C * F2), F32),
            sds((Dn, D), F32),
            sds((F1, D), F32),
            sds((L, D), BF16),
            sds((L, D), BF16),
            sds((1, F1), F32),
        )
        + (sds((1, hc), F32),) * 8,
        in_specs=[
            two(R // steps, D),
            quad(6 * hc),
            quad(F2),
            pl.BlockSpec((1, h, D), lambda i: (i // 2, i % 2, 0)),
            pl.BlockSpec((2, piece, D), lambda i: (jnp.minimum(i, 3), 0, 0)),
            pl.BlockSpec((2, piece, D), lambda i: (jnp.maximum(i - 4, 0), 0, 0)),
            two(L // steps, D),
            two(L // steps, D),
            fixed(8, hc),
            fixed(1, F1),
        ],
        out_specs=(
            two(R // steps, D),
            two(h, 3 * D),
            two(h, C * F2),
            two(h, D),
            two(2 * piece, D),
            two(L // steps, D),
            two(L // steps, D),
            fixed(1, F1),
        )
        + (fixed(1, hc),) * 8,
        compiler_params=pltpu.CompilerParams(vmem_limit_bytes=ATTEND_VMEM * MIB),
        name="finish_stage",
    )(
        table,
        gq.reshape(C, 4, q, 6 * hc),
        up.reshape(C, 4, q, F2),
        out,
        early,
        late,
        res,
        inp,
        small,
        gb,
    )


QUERY_BLOCK = 512
KEY_BLOCK = 512
BACK_KEY_BLOCK = 256
EARLY_PIECES = 8


def local(
    inputs,
    positions,
    segments,
    pos_table,
    w_qkv,
    b_query,
    b_value,
    w_out,
    b_out,
    ln1_gain,
    ln1_bias,
    w_up,
    b_up,
    w_down,
    b_down,
    ln2_gain,
    ln2_bias,
    cotangent,
):
    S, n = lax.axis_size("seq"), lax.axis_size("shard")
    L, D = inputs.shape
    P_, hc, C = L * n, D // n, n // 2
    R = pos_table.shape[0]
    row = lambda v: v.reshape(1, -1)
    rows = [row(v) for v in (b_out, ln1_gain, ln1_bias, b_down, ln2_gain, ln2_bias, b_query, b_value)]
    q, kv, hid_half, hidden, wq, wup2, wdn_o, wout_o, par_all, bup2, pos_glob, lohi = entry_call(
        S,
        n,
        row(positions),
        inputs,
        pos_table,
        w_qkv,
        w_up,
        w_down,
        w_out,
        segments.reshape(S * n, 1, L),
        row(b_up),
        rows,
    )
    q = q.reshape(P_, hc)
    kv = kv.reshape(3 * P_, 2 * hc)
    att, lse = attend_call(q, kv, lohi, QUERY_BLOCK, KEY_BLOCK)
    result, dfirst, datt, gdn_late, gup, gout, stats, gbup, gdn_early = middle_call(
        S,
        n,
        att.reshape(C, 2, L, hc),
        hidden,
        cotangent,
        par_all,
        w_out,
        wout_o,
        wup2,
        w_down,
        wdn_o,
        bup2,
    )
    dq, dkv = attend_back_call(
        q, kv, lohi, att, datt.reshape(P_, hc), lse, QUERY_BLOCK, BACK_KEY_BLOCK
    )
    ginp, dh, gqkv, gup, gout, gdn_late, gtable, small, gbo = exit_call(
        S,
        n,
        R,
        dq.reshape(C, 2, L, hc),
        dkv.reshape(3, C, 2, L, 2 * hc),
        hid_half,
        wq,
        dfirst,
        stats,
        gbup,
        pos_glob,
        gup.reshape(C, 4, D // n // 4, gup.shape[2]),
        gout,
        gdn_late,
    )
    gtable, gqkv, gup, gout, gdn, result, ginp, gbo, *small = finish_call(
        n, gtable, gqkv, gup, gout, gdn_early, gdn_late, result, ginp, small, gbo
    )
    small = [v[0] for v in small]
    return (
        result,
        ginp,
        gtable,
        gqkv,
        small[6],
        small[7],
        gout,
        small[5],
        small[3],
        small[4],
        gup,
        gbo[0],
        gdn,
        small[2],
        small[0],
        small[1],
    )


def solution(mesh):
    in_specs = (
        P(("seq", "shard"), None),
        P(("seq", "shard")),
        P(),
        P("shard", None),
        P("shard", None),
        P("shard"),
        P("shard"),
        P("shard", None),
        P("shard"),
        P("shard"),
        P("shard"),
        P("shard", None),
        P("shard"),
        P("shard", None),
        P("shard"),
        P("shard"),
        P("shard"),
        P(("seq", "shard"), None),
    )
    out_specs = (
        P(("seq", "shard"), None),
        P(("seq", "shard"), None),
        P("shard", None),
        P("shard", None),
        P("shard"),
        P("shard"),
        P("shard", None),
        P("shard"),
        P("shard"),
        P("shard"),
        P("shard", None),
        P("shard"),
        P("shard", None),
        P("shard"),
        P("shard"),
        P("shard"),
    )
    return jax.shard_map(local, mesh=mesh, in_specs=in_specs, out_specs=out_specs, check_vma=False)
```
